32 devices in a mesh: dp: 2 (over core), seq: 4 (over z), tensor: 4 (over y, x).
Axes of the slice: x: 2, y: 2, z: 4, core: 2. Of those that a mesh axis runs over, the one named last changes fastest.
Arguments:
- tokens: bfloat16 [4, 4096, 1024], P('dp', ('seq', 'tensor')), may hold values from -6 to 6
- w_query: bfloat16 [1024, 1024], replicated, may hold values from -0.1875 to 0.1875
- w_key: bfloat16 [1024, 1024], replicated, may hold values from -0.1875 to 0.1875
- w_value: bfloat16 [1024, 1024], replicated, may hold values from -0.1875 to 0.1875
- w_ugate: bfloat16 [1024, 1024], replicated, may hold values from -0.1875 to 0.1875
- w_output: bfloat16 [1024, 1024], replicated, may hold values from -0.1875 to 0.1875
- w_left: bfloat16 [1024, 2816], P(None, 'tensor'), may hold values from -0.1875 to 0.1875
- w_right: bfloat16 [1024, 2816], P(None, 'tensor'), may hold values from -0.1875 to 0.1875
- w_down: bfloat16 [2816, 1024], P('tensor'), may hold values from -0.109375 to 0.109375
- decay_rate: float32 [8], replicated, may hold values from 0.00012207031 to 0.05
- cotangent: bfloat16 [4, 4096, 1024], P('dp', ('seq', 'tensor')), may hold values from -6 to 6
Outputs:
- mixed_out: bfloat16 [4, 4096, 1024], P('dp', ('seq', 'tensor'))
- grad_tokens: float32 [4, 4096, 1024], P('dp', ('seq', 'tensor'))
- grad_query: float32 [1024, 1024], replicated
- grad_key: float32 [1024, 1024], replicated
- grad_value: float32 [1024, 1024], replicated
- grad_ugate: float32 [1024, 1024], replicated
- grad_output: float32 [1024, 1024], replicated
- grad_left: float32 [1024, 2816], P(None, 'tensor')
- grad_right: float32 [1024, 2816], P(None, 'tensor')
- grad_down: float32 [2816, 1024], P('tensor')
The draws below stay inside these ranges and needn't reach their ends.
All inputs are finite; a program needn't handle non-finite values.
Results may differ from the reference program's by a relative error of at most 0.017.
Values may be sent and summed in bfloat16 or wider, within the bound.
A program may use at most 320 MiB of HBM per device.

```python
import math
import jax
import jax.numpy as jnp
from jax import lax

D = 1024
HEADS = 8
HEAD = 128
FF = 2816
GROUP = 256
ITEMS = 4
LENGTH = 4096


def steps_of(key, extent, cuts, low, high):
    factor_of = 1.0
    for axis_at, shards_of in cuts:
        steps = jax.random.uniform(jax.random.fold_in(jax.random.fold_in(key, 6), axis_at), (shards_of,), jnp.float32, low / len(cuts), high / len(cuts))
        factor_of = factor_of * jnp.repeat(jnp.exp(steps), extent[axis_at] // shards_of).reshape((-1,) + (1,) * (len(extent) - 1 - axis_at))
    return factor_of


def noise(rng, extent, scale, reach, shards=(), kind=jnp.bfloat16):
    values = jax.random.normal(rng, extent, jnp.float32) * scale
    if len(shards) > 0:
        values = steps_of(rng, extent, shards, -0.22, 0.18) * values
    return jnp.clip(values, min=-reach, max=reach).astype(kind)


def setup_inputs(seed: int = 0) -> dict:
    key_of = jax.random.split(jax.random.key(seed), 12)
    return {
        "tokens": noise(key_of[0], (ITEMS, LENGTH, D), 1.0, 6.0, ((0, 2), (1, 16))),
        "w_query": noise(key_of[1], (D, D), D ** -0.5, 0.1875),
        "w_key": noise(key_of[2], (D, D), D ** -0.5, 0.1875),
        "w_value": noise(key_of[3], (D, D), D ** -0.5, 0.1875),
        "w_ugate": noise(key_of[4], (D, D), D ** -0.5, 0.1875),
        "w_output": noise(key_of[5], (D, D), D ** -0.5, 0.1875),
        "w_left": noise(key_of[6], (D, FF), D ** -0.5, 0.1875, ((1, 4),)),
        "w_right": noise(key_of[7], (D, FF), D ** -0.5, 0.1875, ((1, 4),)),
        "w_down": noise(key_of[8], (FF, D), FF ** -0.5, 0.109375, ((0, 4),)),
        "decay_rate": jnp.clip(jnp.exp(jax.random.uniform(key_of[9], (HEADS,), jnp.float32, math.log(0.00012207031), math.log(0.05))), 0.00012207031, 0.05),
        "cotangent": noise(key_of[10], (ITEMS, LENGTH, D), 1.0, 6.0, ((0, 2), (1, 16))),
    }


EPS = 1e-06
precise = lax.Precision.HIGHEST

@jax.custom_vjp
def low(v):
    return lax.optimization_barrier(v.astype(jnp.bfloat16)).astype(jnp.float32)

@jax.custom_vjp
def low_back(v):
    return v

def low_keep(v):
    return (low(v), None)

def low_pass(kept, grad):
    return (grad,)

def back_keep(v):
    return (v, None)

def back_low(kept, grad):
    return (low(grad),)
low.defvjp(low_keep, low_pass)
low_back.defvjp(back_keep, back_low)

def matmul(first, second):
    return jnp.dot(first, second, precision=precise)

def rms_norm(values):
    return values * lax.rsqrt(lax.optimization_barrier(jnp.mean(values * values, axis=-1, keepdims=True)) + EPS)

def rotate(values, cosine, sine_part):
    half_dim = values.shape[-1] // 2
    first_half = values[..., :half_dim]
    second_half = values[..., half_dim:]
    return jnp.concatenate([first_half * cosine - second_half * sine_part, second_half * cosine + first_half * sine_part], axis=-1)

def block_layer(tokens_in, w_query, w_key, w_value, w_ugate, w_output, w_left, w_right, w_down, decay_rate):
    length_all = tokens_in.shape[0]
    groups = length_all // GROUP
    normed = low(rms_norm(tokens_in))
    query_pre = low_back(matmul(normed, w_query))
    key_pre = low_back(matmul(normed, w_key))
    value_pre = low_back(matmul(normed, w_value))
    ugate = low_back(matmul(normed, w_ugate))
    places = jnp.arange(length_all, dtype=jnp.float32)
    frequency = 10000.0 ** (-jnp.arange(HEAD // 2, dtype=jnp.float32) / (HEAD // 2))
    angles = places[:, None] * frequency[None, :]
    cosine = jnp.cos(angles).reshape(groups, 1, GROUP, HEAD // 2)
    sine_part = jnp.sin(angles).reshape(groups, 1, GROUP, HEAD // 2)

    def split_heads(values):
        return values.reshape(groups, GROUP, HEADS, HEAD).transpose(0, 2, 1, 3)
    query_rot = rotate(split_heads(jax.nn.silu(query_pre)), cosine, sine_part)
    key_rot = rotate(split_heads(jax.nn.silu(key_pre)), cosine, sine_part)
    query_low = low(query_rot)
    key_low = low(key_rot)
    value_low = low(split_heads(value_pre))
    step_pos = jnp.arange(GROUP, dtype=jnp.float32)
    lag_steps = step_pos[:, None] - step_pos[None, :]
    decay_mask = jnp.where(lag_steps >= 0, jnp.exp(-decay_rate[:, None, None] * jnp.maximum(lag_steps, 0.0)), 0.0)
    query_weight = jnp.exp(-decay_rate[:, None] * (step_pos + 1.0))
    key_weight = jnp.exp(-decay_rate[:, None] * (GROUP - 1.0 - step_pos))
    carry_decay = jnp.exp(-decay_rate * GROUP)[:, None, None]
    query_dec = low(query_rot * query_weight[:, :, None])
    key_dec = low(key_rot * key_weight[:, :, None])

    def group_step(state_in, pieces):
        query_piece, key_piece, value_piece, qdec_piece, kdec_piece = pieces
        scores = low_back(jnp.einsum('hie,hje->hij', query_piece, key_piece, precision=precise))
        weights_low = low(scores * decay_mask)
        inner_part = jnp.einsum('hij,hje->hie', weights_low, value_piece, precision=precise)
        outer_part = jnp.einsum('hie,hef->hif', qdec_piece, low(state_in), precision=precise)
        local_state = low_back(jnp.einsum('hje,hjf->hef', kdec_piece, value_piece, precision=precise))
        return (carry_decay * state_in + local_state, inner_part + outer_part)
    initial = jnp.zeros((HEADS, HEAD, HEAD), jnp.float32)
    final_state, attended = lax.scan(jax.checkpoint(group_step), initial, (query_low, key_low, value_low, query_dec, key_dec))
    attended = low_back(attended)
    merged = attended.transpose(0, 2, 1, 3).reshape(length_all, HEADS * HEAD)
    gated = low(rms_norm(merged) * ugate)
    branch = low_back(matmul(gated, w_output))
    residual = tokens_in + branch
    normed_two = low(rms_norm(residual))
    left_half = low_back(matmul(normed_two, w_left))
    right_half = low_back(matmul(normed_two, w_right))
    product = low(left_half * right_half)
    return residual + low_back(matmul(product, w_down))

def reference(tokens, w_query, w_key, w_value, w_ugate, w_output, w_left, w_right, w_down, decay_rate, cotangent):
    weights = tuple((matrix.astype(jnp.float32) for matrix in (w_query, w_key, w_value, w_ugate, w_output, w_left, w_right, w_down)))
    tokens_all = tokens.astype(jnp.float32)
    cot_all = cotangent.astype(jnp.float32)

    def item_step(totals, pieces):
        token_item, cot_item = pieces

        def forward(token_in, *matrices):
            return block_layer(token_in, *matrices, decay_rate)
        result, pullback = jax.vjp(forward, token_item, *weights)
        gradients = pullback(cot_item)
        updated = tuple((running + gradient for running, gradient in zip(totals, gradients[1:])))
        return (updated, (result, gradients[0]))
    initial = tuple((jnp.zeros_like(matrix) for matrix in weights))
    totals, outputs = lax.scan(item_step, initial, (tokens_all, cot_all))
    results, grad_in = outputs
    return (results.astype(jnp.bfloat16), grad_in, totals[0], totals[1], totals[2], totals[3], totals[4], totals[5], totals[6], totals[7])
```

```python
import jax
import jax.numpy as jnp
from jax import lax
from jax.sharding import PartitionSpec as P

EPS = 1e-06
F32 = jnp.float32
BF16 = jnp.bfloat16


def swap(value, axis, bit):
    count = lax.axis_size(axis)
    return jax.tree.map(
        lambda v: lax.ppermute(v, axis, [(i, i ^ bit) for i in range(count)]), value
    )


def shift(value, axis, step):
    count = lax.axis_size(axis)
    pairs = [(i, i + step) for i in range(count) if 0 <= i + step < count]
    return lax.ppermute(value, axis, pairs)


def take_half(value, which, axis=0):
    half = value.shape[axis] // 2
    return lax.dynamic_slice_in_dim(value, which * half, half, axis)


def join_half(mine, other, which, axis=0):
    return jnp.where(
        which == 0,
        jnp.concatenate([mine, other], axis=axis),
        jnp.concatenate([other, mine], axis=axis),
    )


def carried_state(local, decay_rate, block_len, backward):
    heads = local.shape[1]
    width = lax.axis_size("tensor")
    share = heads // width
    depth = lax.axis_size("seq")
    mine = lax.axis_index("tensor")

    def power(count, rate):
        return jnp.exp(-rate * block_len * count)

    pieces = []
    for b in range(width):
        part = lax.dynamic_slice_in_dim(local, (mine ^ b) * share, share, 1)
        pieces.append(part if b == 0 else swap(part.astype(BF16), "tensor", b).astype(F32))
    rate = lax.dynamic_slice_in_dim(decay_rate, mine * share, share, 0)

    def scaled(coef, part):
        return coef[None, :, None, None] * part

    total = 0.0
    for b in range(width):
        place = mine ^ b
        left = place if backward else width - 1 - place
        total = total + scaled(power(left.astype(F32), rate), pieces[b])
    total_low = total.astype(BF16)
    entering = 0.0
    for j in range(1, depth):
        step = -j if backward else j
        moved = shift(total_low, "seq", step).astype(F32)
        entering = entering + scaled(power(float(width * (j - 1)), rate), moved)
    outs = []
    for d in range(width):
        target = mine ^ d
        inner = (width - 1 - target) if backward else target
        value = scaled(power(inner.astype(F32), rate), entering)
        for b in range(width):
            if b == d:
                continue
            source = mine ^ b
            gap = (source - target - 1) if backward else (target - source - 1)
            coef = jnp.where(gap >= 0, power(jnp.maximum(gap, 0).astype(F32), rate), 0.0)
            value = value + scaled(coef, pieces[b])
        low_value = value.astype(BF16)
        outs.append(low_value if d == 0 else swap(low_value, "tensor", d))
    bit = 1
    while bit < width:
        flip = (mine & bit) != 0
        outs = [jnp.where(flip, outs[u ^ bit], outs[u]) for u in range(width)]
        bit *= 2
    return jnp.concatenate(outs, axis=1)


def reduce_line(value, axis):
    count = lax.axis_size(axis)
    mine = lax.axis_index(axis)
    bits = []
    bit = 1
    while bit < count:
        bits.append(bit)
        bit *= 2
    for bit in bits:
        which = (mine & bit) // bit
        sent = swap(take_half(value, 1 - which).astype(BF16), axis, bit)
        value = take_half(value, which) + sent.astype(F32)
    value = value.astype(BF16)
    for bit in reversed(bits):
        which = (mine & bit) // bit
        value = join_half(value, swap(value, axis, bit), which)
    return value


def norm_rows(values):
    inv_scale = lax.rsqrt(jnp.mean(values * values, axis=-1, keepdims=True) + EPS)
    return (values * inv_scale, inv_scale)


def norm_back(gradient, normed, inv_scale):
    return inv_scale * (gradient - normed * jnp.mean(gradient * normed, axis=-1, keepdims=True))


def rotate(values, cosine, sine_part):
    half_dim = values.shape[-1] // 2
    first_half = values[..., :half_dim]
    second_half = values[..., half_dim:]
    return jnp.concatenate(
        [
            first_half * cosine - second_half * sine_part,
            second_half * cosine + first_half * sine_part,
        ],
        axis=-1,
    )


def rotate_back(values, cosine, sine_part):
    return rotate(values, cosine, -sine_part)


def split_heads(values, head_count):
    seq_count, group_len, model_width = values.shape
    return values.reshape(seq_count, group_len, head_count, model_width // head_count).transpose(
        0, 2, 1, 3
    )


def join_heads(values):
    seq_count, head_count, group_len, head_dim = values.shape
    return values.transpose(0, 2, 1, 3).reshape(seq_count, group_len, head_count * head_dim)


def dot(spec, first, second):
    return jnp.einsum(spec, first, second, preferred_element_type=F32)


def project(inputs, matrix):
    return dot("scd,de->sce", inputs, matrix)


def project_back(gradient, matrix):
    return dot("sce,de->scd", gradient, matrix)


def weight_grad(inputs, gradient):
    return dot("scd,sce->de", inputs, gradient)


def silu_slope(values):
    sigmoid_v = jax.nn.sigmoid(values)
    return sigmoid_v * (1.0 + values * (1.0 - sigmoid_v))


def on_device(
    tokens,
    w_query,
    w_key,
    w_value,
    w_ugate,
    w_output,
    w_left,
    w_right,
    w_down,
    decay_rate,
    cotangent,
):
    seq_count, group_len, model_width = tokens.shape
    head_count = decay_rate.shape[0]
    head_dim = model_width // head_count
    half_dim = head_dim // 2
    row_count = seq_count * group_len
    core = lax.axis_index("dp")

    shard = (w_left, w_right, w_down)
    fetched = swap(tuple(take_half(w, core) for w in shard), "tensor", 2)
    swapped = swap(fetched, "dp", 1)
    other = tuple(join_half(f, s, core) for f, s in zip(fetched, swapped))
    grad_res = cotangent.astype(F32)
    grad_own = cotangent.reshape(row_count, model_width)
    grad_nb = swap(grad_own, "tensor", 1)

    position_block = lax.axis_index(("seq", "tensor"))
    places = (position_block * group_len + jnp.arange(group_len)).astype(F32)
    frequency = 10000.0 ** (-jnp.arange(half_dim, dtype=F32) / half_dim)
    angles = places[:, None] * frequency[None, :]
    cosine = jnp.cos(angles)
    sine_part = jnp.sin(angles)
    step_pos = jnp.arange(group_len, dtype=F32)
    lag_steps = step_pos[:, None] - step_pos[None, :]
    decay_mask = jnp.where(
        lag_steps >= 0, jnp.exp(-decay_rate[:, None, None] * jnp.maximum(lag_steps, 0.0)), 0.0
    )
    query_weight = jnp.exp(-decay_rate[:, None] * (step_pos + 1.0))[:, :, None]
    key_weight = jnp.exp(-decay_rate[:, None] * (group_len - 1.0 - step_pos))[:, :, None]

    inputs = tokens.astype(F32)
    normed_one, scale_one = norm_rows(inputs)
    normed_low = normed_one.astype(BF16)
    key_pre = project(normed_low, w_key)
    value_pre = project(normed_low, w_value)
    key_rot = rotate(split_heads(jax.nn.silu(key_pre), head_count), cosine, sine_part)
    key_low = key_rot.astype(BF16)
    value_low = split_heads(value_pre, head_count).astype(BF16)
    key_dec = (key_rot * key_weight).astype(BF16)
    local_state = dot("shje,shjf->shef", key_dec, value_low)
    state_low = carried_state(local_state, decay_rate, group_len, False)

    query_pre = project(normed_low, w_query)
    ugate = project(normed_low, w_ugate)
    query_rot = rotate(split_heads(jax.nn.silu(query_pre), head_count), cosine, sine_part)
    query_low = query_rot.astype(BF16)
    query_dec = (query_rot * query_weight).astype(BF16)
    scores = dot("shie,shje->shij", query_low, key_low)
    weights_low = (scores * decay_mask).astype(BF16)
    inner_part = dot("shij,shje->shie", weights_low, value_low)
    outer_part = dot("shie,shef->shif", query_dec, state_low)
    merged = join_heads(inner_part + outer_part)
    normed_att, scale_att = norm_rows(merged)
    gated_low = (normed_att * ugate).astype(BF16)
    residual = inputs + project(gated_low, w_output)
    normed_two, scale_two = norm_rows(residual)
    rows_own = normed_two.astype(BF16).reshape(row_count, model_width)
    rows_nb = swap(rows_own, "tensor", 1)

    def hidden_part(rows, grads):
        mixed = 0.0
        back = 0.0
        kept = []
        for left, right, down in (shard, other):
            e1 = jnp.dot(rows, left, preferred_element_type=F32)
            e2 = jnp.dot(rows, right, preferred_element_type=F32)
            product = (e1 * e2).astype(BF16)
            dm = dot("rd,fd->rf", grads, down)
            de1 = (dm * e2).astype(BF16)
            de2 = (dm * e1).astype(BF16)
            mixed = mixed + jnp.dot(product, down, preferred_element_type=F32)
            back = back + dot("rf,df->rd", de1, left) + dot("rf,df->rd", de2, right)
            kept.append((de1, de2, product))
        return mixed, back, kept

    mixed_nb, back_nb, kept_nb = hidden_part(rows_nb, grad_nb)
    back_in = swap(back_nb.astype(BF16), "tensor", 1)
    mixed_in = swap(mixed_nb.astype(BF16), "tensor", 1)
    mixed_own, back_own, kept_own = hidden_part(rows_own, grad_own)

    shape = (seq_count, group_len, model_width)
    mixed_out = (residual + (mixed_own + mixed_in.astype(F32)).reshape(shape)).astype(BF16)

    rows_all = jnp.concatenate([rows_own, rows_nb], axis=0)
    grads_all = jnp.concatenate([grad_own, grad_nb], axis=0)
    halves = []
    for at in range(2):
        de1, de2, product = (
            jnp.concatenate([first, second], axis=0)
            for first, second in zip(kept_own[at], kept_nb[at])
        )
        full = (
            dot("rd,rf->df", rows_all, de1),
            dot("rd,rf->df", rows_all, de2),
            dot("rf,rd->fd", product, grads_all),
        )
        sent = swap(tuple(take_half(g, 1 - core).astype(BF16) for g in full), "dp", 1)
        halves.append(tuple(take_half(g, core) + s.astype(F32) for g, s in zip(full, sent)))
    from_y = swap(tuple(g.astype(BF16) for g in halves[1]), "tensor", 2)
    hidden_grads = []
    for mine, theirs in zip(halves[0], from_y):
        part = reduce_line(mine + theirs.astype(F32), "seq")
        hidden_grads.append(join_half(part, swap(part, "dp", 1), core).astype(F32))

    grad_normed_two = (back_own + back_in.astype(F32)).reshape(shape)
    grad_mid = grad_res + norm_back(grad_normed_two, normed_two, scale_two)
    grad_branch = grad_mid.astype(BF16)
    grad_gated = project_back(grad_branch, w_output)
    grad_output = weight_grad(gated_low, grad_branch)
    grad_ugate_pre = (grad_gated * normed_att).astype(BF16)
    grad_merged = norm_back(grad_gated * ugate, normed_att, scale_att)
    grad_att = split_heads(grad_merged, head_count).astype(BF16)
    grad_state_in = dot("shie,shif->shef", query_dec, grad_att)
    grad_local_low = carried_state(grad_state_in, decay_rate, group_len, True)

    grad_weights = dot("shie,shje->shij", grad_att, value_low)
    grad_value_heads = dot("shij,shie->shje", weights_low, grad_att)
    grad_scores = (grad_weights * decay_mask).astype(BF16)
    grad_query_rot = dot("shij,shje->shie", grad_scores, key_low)
    grad_key_rot = dot("shij,shie->shje", grad_scores, query_low)
    grad_query_dec = dot("shif,shef->shie", grad_att, state_low)
    grad_query_rot = grad_query_rot + grad_query_dec * query_weight
    grad_query_pre = (
        join_heads(rotate_back(grad_query_rot, cosine, sine_part)) * silu_slope(query_pre)
    ).astype(BF16)
    grad_query = weight_grad(normed_low, grad_query_pre)
    grad_ugate = weight_grad(normed_low, grad_ugate_pre)

    grad_key_dec = dot("shef,shjf->shje", grad_local_low, value_low)
    grad_value_heads = grad_value_heads + dot("shje,shef->shjf", key_dec, grad_local_low)
    grad_key_rot = grad_key_rot + grad_key_dec * key_weight
    grad_key_pre = (
        join_heads(rotate_back(grad_key_rot, cosine, sine_part)) * silu_slope(key_pre)
    ).astype(BF16)
    grad_value_pre = join_heads(grad_value_heads).astype(BF16)
    grad_normed_one = (
        project_back(grad_query_pre, w_query)
        + project_back(grad_key_pre, w_key)
        + project_back(grad_value_pre, w_value)
        + project_back(grad_ugate_pre, w_ugate)
    )
    grad_tokens = grad_mid + norm_back(grad_normed_one, normed_one, scale_one)
    grad_key = weight_grad(normed_low, grad_key_pre)
    grad_value = weight_grad(normed_low, grad_value_pre)

    everyone = ("dp", "seq", "tensor")
    grad_output, grad_ugate = lax.psum(
        (grad_output.astype(BF16), grad_ugate.astype(BF16)), everyone
    )
    grad_query = lax.psum(grad_query.astype(BF16), everyone)
    grad_key, grad_value = lax.psum((grad_key.astype(BF16), grad_value.astype(BF16)), everyone)
    attention_grads = tuple(
        g.astype(F32) for g in (grad_query, grad_key, grad_value, grad_ugate, grad_output)
    )
    return (mixed_out, grad_tokens) + attention_grads + tuple(hidden_grads)


def solution(mesh):
    rows = P("dp", ("seq", "tensor"), None)
    columns = P(None, "tensor")
    return jax.shard_map(
        on_device,
        mesh=mesh,
        in_specs=(rows, P(), P(), P(), P(), P(), columns, columns, P("tensor", None), P(), rows),
        out_specs=(rows, rows, P(), P(), P(), P(), P(), columns, columns, P("tensor", None)),
        check_vma=False,
    )
```

```python
import jax
import jax.numpy as jnp
from jax import lax
from jax.experimental import pallas as pl
from jax.experimental.pallas import tpu as pltpu
from jax.sharding import PartitionSpec as P

EPS = 1e-06
F32 = jnp.float32
BF16 = jnp.bfloat16


def swap(value, axis, bit):
    count = lax.axis_size(axis)
    return jax.tree.map(
        lambda v: lax.ppermute(v, axis, [(i, i ^ bit) for i in range(count)]), value
    )


def shift(value, axis, step):
    count = lax.axis_size(axis)
    pairs = [(i, i + step) for i in range(count) if 0 <= i + step < count]
    return lax.ppermute(value, axis, pairs)


def take_half(value, which, axis=0):
    half = value.shape[axis] // 2
    return lax.dynamic_slice_in_dim(value, which * half, half, axis)


def join_half(mine, other, which, axis=0):
    return jnp.where(
        which == 0,
        jnp.concatenate([mine, other], axis=axis),
        jnp.concatenate([other, mine], axis=axis),
    )


def carried_state(local, decay_rate, block_len, backward):
    heads = local.shape[1]
    width = lax.axis_size("tensor")
    share = heads // width
    depth = lax.axis_size("seq")
    mine = lax.axis_index("tensor")

    def power(count, rate):
        return jnp.exp(-rate * block_len * count)

    pieces = []
    for b in range(width):
        part = lax.dynamic_slice_in_dim(local, (mine ^ b) * share, share, 1)
        pieces.append(part if b == 0 else swap(part.astype(BF16), "tensor", b).astype(F32))
    rate = lax.dynamic_slice_in_dim(decay_rate, mine * share, share, 0)

    def scaled(coef, part):
        return coef[None, :, None, None] * part

    total = 0.0
    for b in range(width):
        place = mine ^ b
        left = place if backward else width - 1 - place
        total = total + scaled(power(left.astype(F32), rate), pieces[b])
    total_low = total.astype(BF16)
    entering = 0.0
    for j in range(1, depth):
        step = -j if backward else j
        moved = shift(total_low, "seq", step).astype(F32)
        entering = entering + scaled(power(float(width * (j - 1)), rate), moved)
    outs = []
    for d in range(width):
        target = mine ^ d
        inner = (width - 1 - target) if backward else target
        value = scaled(power(inner.astype(F32), rate), entering)
        for b in range(width):
            if b == d:
                continue
            source = mine ^ b
            gap = (source - target - 1) if backward else (target - source - 1)
            coef = jnp.where(gap >= 0, power(jnp.maximum(gap, 0).astype(F32), rate), 0.0)
            value = value + scaled(coef, pieces[b])
        low_value = value.astype(BF16)
        outs.append(low_value if d == 0 else swap(low_value, "tensor", d))
    bit = 1
    while bit < width:
        flip = (mine & bit) != 0
        outs = [jnp.where(flip, outs[u ^ bit], outs[u]) for u in range(width)]
        bit *= 2
    return jnp.concatenate(outs, axis=1)


CHUNK = 256
LAG = 2


def added(first, second):
    return (first.astype(F32) + second.astype(F32)).astype(BF16)


def reduce_kernel(
    depth,
    grads,
    pair_in,
    down_in,
    out,
    pair_out,
    down_out,
    own,
    core_in,
    first_in,
    second_in,
    line_in,
    line_mid,
    pair_line,
    pair_mid,
    down_line,
    down_mid,
    sems,
    pair_sems,
    down_sems,
    load_sem,
):
    core = lax.axis_index("dp")
    slot = lax.axis_index("tensor")
    place = lax.axis_index("seq")
    rows = own.shape[0]
    chunks = rows // CHUNK
    half, quarter, eighth = CHUNK // 2, CHUNK // 4, CHUNK // 8
    low_side = place < depth // 2
    outermost = (place == 0) | (place == depth - 1)
    middle = (place == depth // 2 - 1) | (place == depth // 2)
    inward = jnp.where(low_side, place + 1, place - 1)
    outward = jnp.where(low_side, place - 1, place + 1)

    barrier = pltpu.get_barrier_semaphore()

    def greet(peer):
        pl.semaphore_signal(
            barrier, inc=1, device_id=peer, device_id_type=pl.DeviceIdType.MESH
        )

    greet({"dp": 1 - core})
    greet({"tensor": slot ^ 1})
    greet({"tensor": slot ^ 2})

    @pl.when(place > 0)
    def _():
        greet({"seq": place - 1})

    @pl.when(place < depth - 1)
    def _():
        greet({"seq": place + 1})

    pl.semaphore_wait(barrier, jnp.where(outermost, 4, 5))

    def remote(source, target, sem, at, peer):
        return pltpu.make_async_remote_copy(
            src_ref=source,
            dst_ref=target,
            send_sem=sem.at[0, at],
            recv_sem=sem.at[1, at],
            device_id=peer,
            device_id_type=pl.DeviceIdType.MESH,
        )

    def span(start, size):
        return pl.ds(pl.multiple_of(start, size), size)

    def bits(q):
        first = jnp.where(q % 2 == 0, 1, 2)
        second = 3 - first
        return first, second, (slot & first) // first, (slot & second) // second

    def base(q):
        return pl.multiple_of(q * CHUNK, CHUNK)

    def to_core(q):
        return remote(
            own.at[span(base(q) + (1 - core) * half, half)],
            core_in.at[q],
            sems.at[0],
            q,
            {"dp": 1 - core},
        )

    def to_first(q):
        first, _, f, _ = bits(q)
        return remote(
            core_in.at[q, span((1 - f) * quarter, quarter)],
            first_in.at[q],
            sems.at[1],
            q,
            {"tensor": slot ^ first},
        )

    def to_second(q):
        _, second, _, g = bits(q)
        return remote(
            first_in.at[q, span((1 - g) * eighth, eighth)],
            second_in.at[q],
            sems.at[2],
            q,
            {"tensor": slot ^ second},
        )

    def block(q):
        _, _, f, g = bits(q)
        return base(q) + core * half + f * quarter + g * eighth

    def back_second(q):
        _, second, _, _ = bits(q)
        at = span(block(q), eighth)
        return remote(out.at[at], out.at[at], sems.at[3], q, {"tensor": slot ^ second})

    def back_first(q):
        first, _, f, _ = bits(q)
        at = span(base(q) + core * half + f * quarter, quarter)
        return remote(out.at[at], out.at[at], sems.at[4], q, {"tensor": slot ^ first})

    def back_core(q):
        at = span(base(q) + core * half, half)
        return remote(out.at[at], out.at[at], sems.at[5], q, {"dp": 1 - core})

    class Line:
        def __init__(self, mine, came, met, total, sem, offset):
            self.mine, self.came, self.met, self.total = mine, came, met, total
            self.sem, self.offset = sem, offset

        def inwards(self, q, source):
            return remote(
                source, self.came(q), self.sem.at[self.offset], q, {"seq": inward}
            )

        def across(self, q):
            return remote(
                self.came(q),
                self.met(q),
                self.sem.at[self.offset + 1],
                q,
                {"seq": depth - 1 - place},
            )

        def outwards(self, q):
            return remote(
                self.total(q), self.total(q), self.sem.at[self.offset + 2], q, {"seq": outward}
            )

        def step_in(self, q):
            @pl.when(outermost)
            def _():
                self.inwards(q, self.mine(q)).start()

        def step_middle(self, q):
            @pl.when(jnp.logical_not(outermost))
            def _():
                self.inwards(q, self.mine(q)).wait_recv()
                came = self.came(q)
                came[...] = added(self.mine(q)[...], came[...])

                @pl.when(middle)
                def _():
                    self.across(q).start()

                @pl.when(jnp.logical_not(middle))
                def _():
                    self.inwards(q, came).start()

        def step_out(self, q):
            @pl.when(middle)
            def _():
                self.across(q).wait_recv()
                self.total(q)[...] = added(self.came(q)[...], self.met(q)[...])

            @pl.when(jnp.logical_not(outermost))
            def _():
                @pl.when(jnp.logical_not(middle))
                def _():
                    self.outwards(q).wait_recv()

                self.outwards(q).start()

        def step_last(self, q):
            @pl.when(outermost)
            def _():
                self.outwards(q).wait_recv()

        def settle(self, q):
            @pl.when(outermost)
            def _():
                self.inwards(q, self.mine(q)).wait_send()

            @pl.when(jnp.logical_not(outermost))
            def _():
                @pl.when(middle)
                def _():
                    self.across(q).wait_send()

                @pl.when(jnp.logical_not(middle))
                def _():
                    self.inwards(q, self.came(q)).wait_send()

                self.outwards(q).wait_send()

    def second_mine(q):
        return second_in.at[q]

    line = Line(
        second_mine,
        lambda q: line_in.at[q],
        lambda q: line_mid.at[q],
        lambda q: out.at[span(block(q), eighth)],
        sems,
        6,
    )
    pair_chunks = pair_line.shape[0]
    pair_rows = pair_line.shape[1]
    per_side = pair_chunks // 2
    pair = Line(
        lambda q: pair_in.at[span(q * pair_rows, pair_rows)],
        lambda q: pair_line.at[q],
        lambda q: pair_mid.at[q],
        lambda q: pair_out.at[q // per_side, core, span((q % per_side) * pair_rows, pair_rows)],
        pair_sems,
        0,
    )
    down_chunks = down_line.shape[0]
    down_rows = down_line.shape[1]
    down_half = down_line.shape[2]
    down = Line(
        lambda q: down_in.at[span(q * down_rows, down_rows)],
        lambda q: down_line.at[q],
        lambda q: down_mid.at[q],
        lambda q: down_out.at[span(q * down_rows, down_rows), span(core * down_half, down_half)],
        down_sems,
        0,
    )

    def pair_core(q):
        return remote(pair.total(q), pair.total(q), pair_sems.at[3], q, {"dp": 1 - core})

    def down_core(q):
        return remote(down.total(q), down.total(q), down_sems.at[3], q, {"dp": 1 - core})

    size = rows // len(grads)
    loads = [
        pltpu.make_async_copy(g, own.at[pl.ds(i * size, size)], load_sem.at[i])
        for i, g in enumerate(grads)
    ]
    for load in loads:
        load.start()
    per_load = size // CHUNK
    for i, load in enumerate(loads):
        load.wait()

        @pl.loop(i * per_load, (i + 1) * per_load)
        def _(q):
            to_core(q).start()

    def stage_a(q):
        to_core(q).wait_recv()
        came = core_in.at[q]
        came[...] = added(own[span(base(q) + core * half, half)], came[...])

    def stage_b(q):
        _, _, f, _ = bits(q)
        to_first(q).wait_recv()
        came = first_in.at[q]
        came[...] = added(core_in[q, span(f * quarter, quarter)], came[...])

    def stage_c(q):
        _, _, _, g = bits(q)
        to_second(q).wait_recv()
        came = second_in.at[q]
        came[...] = added(first_in[q, span(g * eighth, eighth)], came[...])

    pairs = chunks // 2

    def during(step, lag, count, action):
        i = step - lag

        @pl.when((i >= 0) & (i < count))
        def _():
            action(i)

    def both(action):
        def run(i):
            action(2 * i)
            action(2 * i + 1)

        return run

    def start(copy):
        return lambda q: copy(q).start()

    def arrived(copy, following):
        def run(q):
            copy(q).wait_recv()
            following(q).start()

        return run

    def last_then_second(q):
        line.step_last(q)
        back_second(q).start()

    steps = max(pairs + 7 * LAG, pair_chunks + down_chunks + 4 * LAG) + 1

    @pl.loop(0, steps)
    def _(step):
        during(step, 7 * LAG, pairs, both(arrived(back_first, back_core)))
        during(step, 6 * LAG, pairs, both(arrived(back_second, back_first)))
        during(step, 5 * LAG, pairs, both(last_then_second))
        during(step, 4 * LAG, pairs, both(line.step_out))
        during(step, 3 * LAG, pairs, both(line.step_middle))
        during(step, 2 * LAG, pairs, both(stage_c))
        during(step, LAG, pairs, both(stage_b))
        during(step, 0, pairs, both(stage_a))
        during(step, 2 * LAG, pairs, both(line.step_in))
        during(step, LAG, pairs, both(start(to_second)))
        during(step, 0, pairs, both(start(to_first)))
        for stream, count, late, send in (
            (pair, pair_chunks, 0, pair_core),
            (down, down_chunks, pair_chunks, down_core),
        ):
            def finish(q, stream=stream, send=send):
                stream.step_last(q)
                send(q).start()

            during(step, late + 3 * LAG, count, finish)
            during(step, late + 2 * LAG, count, stream.step_out)
            during(step, late + LAG, count, stream.step_middle)
            during(step, late, count, stream.step_in)

    @pl.loop(0, chunks)
    def _(q):
        back_core(q).wait_recv()
        for copy in (to_core, to_first, to_second, back_second, back_first, back_core):
            copy(q).wait_send()
        line.settle(q)

    for stream, count, send in ((pair, pair_chunks, pair_core), (down, down_chunks, down_core)):

        @pl.loop(0, count)
        def _(q, stream=stream, send=send):
            send(q).wait()
            stream.settle(q)


def reduce_grads(grads, pair_half, down_half, depth):
    size, width = grads[0].shape
    rows = size * len(grads)
    chunks = rows // CHUNK
    hidden = pair_half.shape[1]
    pair_chunks, down_chunks = 8, 4
    pair_rows = pair_half.shape[0] // pair_chunks
    down_rows = down_half.shape[0] // down_chunks
    down_cols = down_half.shape[1]
    vmem = pl.BlockSpec(memory_space=pltpu.VMEM)

    def body(*refs):
        reduce_kernel(depth, refs[: len(grads)], *refs[len(grads) :])

    return pl.pallas_call(
        body,
        out_shape=(
            jax.ShapeDtypeStruct((rows, width), BF16),
            jax.ShapeDtypeStruct((2, 2, pair_half.shape[0] // 2, hidden), BF16),
            jax.ShapeDtypeStruct((down_half.shape[0], 2 * down_cols), BF16),
        ),
        in_specs=[pl.BlockSpec(memory_space=pl.ANY)] * len(grads) + [vmem, vmem],
        out_specs=(vmem, vmem, vmem),
        scratch_shapes=[
            pltpu.VMEM((rows, width), BF16),
            pltpu.VMEM((chunks, CHUNK // 2, width), BF16),
            pltpu.VMEM((chunks, CHUNK // 4, width), BF16),
            pltpu.VMEM((chunks, CHUNK // 8, width), BF16),
            pltpu.VMEM((chunks, CHUNK // 8, width), BF16),
            pltpu.VMEM((chunks, CHUNK // 8, width), BF16),
            pltpu.VMEM((pair_chunks, pair_rows, hidden), BF16),
            pltpu.VMEM((pair_chunks, pair_rows, hidden), BF16),
            pltpu.VMEM((down_chunks, down_rows, down_cols), BF16),
            pltpu.VMEM((down_chunks, down_rows, down_cols), BF16),
            pltpu.SemaphoreType.DMA((9, 2, chunks)),
            pltpu.SemaphoreType.DMA((4, 2, pair_chunks)),
            pltpu.SemaphoreType.DMA((4, 2, down_chunks)),
            pltpu.SemaphoreType.DMA((len(grads),)),
        ],
        compiler_params=pltpu.CompilerParams(
            collective_id=1, has_side_effects=True, vmem_limit_bytes=60 * 1024 * 1024
        ),
        name="reduce_grads",
    )(*grads, pair_half, down_half)


def norm_rows(values):
    inv_scale = lax.rsqrt(jnp.mean(values * values, axis=-1, keepdims=True) + EPS)
    return (values * inv_scale, inv_scale)


def norm_back(gradient, normed, inv_scale):
    return inv_scale * (gradient - normed * jnp.mean(gradient * normed, axis=-1, keepdims=True))


def rotate(values, cosine, sine_part):
    half_dim = values.shape[-1] // 2
    first_half = values[..., :half_dim]
    second_half = values[..., half_dim:]
    return jnp.concatenate(
        [
            first_half * cosine - second_half * sine_part,
            second_half * cosine + first_half * sine_part,
        ],
        axis=-1,
    )


def rotate_back(values, cosine, sine_part):
    return rotate(values, cosine, -sine_part)


def split_heads(values, head_count):
    seq_count, group_len, model_width = values.shape
    return values.reshape(seq_count, group_len, head_count, model_width // head_count).transpose(
        0, 2, 1, 3
    )


def join_heads(values):
    seq_count, head_count, group_len, head_dim = values.shape
    return values.transpose(0, 2, 1, 3).reshape(seq_count, group_len, head_count * head_dim)


def dot(spec, first, second):
    return jnp.einsum(spec, first, second, preferred_element_type=F32)


def project(inputs, matrix):
    return dot("scd,de->sce", inputs, matrix)


def project_back(gradient, matrix):
    return dot("sce,de->scd", gradient, matrix)


def weight_grad(inputs, gradient):
    return dot("scd,sce->de", inputs, gradient)


def silu_slope(values):
    sigmoid_v = jax.nn.sigmoid(values)
    return sigmoid_v * (1.0 + values * (1.0 - sigmoid_v))


def on_device(
    tokens,
    w_query,
    w_key,
    w_value,
    w_ugate,
    w_output,
    w_left,
    w_right,
    w_down,
    decay_rate,
    cotangent,
):
    seq_count, group_len, model_width = tokens.shape
    head_count = decay_rate.shape[0]
    head_dim = model_width // head_count
    half_dim = head_dim // 2
    row_count = seq_count * group_len
    core = lax.axis_index("dp")

    shard = (w_left, w_right, w_down)
    fetched = swap(tuple(take_half(w, core) for w in shard), "tensor", 2)
    swapped = swap(fetched, "dp", 1)
    other = tuple(join_half(f, s, core) for f, s in zip(fetched, swapped))
    grad_res = cotangent.astype(F32)
    grad_own = cotangent.reshape(row_count, model_width)
    grad_nb = swap(grad_own, "tensor", 1)

    position_block = lax.axis_index(("seq", "tensor"))
    places = (position_block * group_len + jnp.arange(group_len)).astype(F32)
    frequency = 10000.0 ** (-jnp.arange(half_dim, dtype=F32) / half_dim)
    angles = places[:, None] * frequency[None, :]
    cosine = jnp.cos(angles)
    sine_part = jnp.sin(angles)
    step_pos = jnp.arange(group_len, dtype=F32)
    lag_steps = step_pos[:, None] - step_pos[None, :]
    decay_mask = jnp.where(
        lag_steps >= 0, jnp.exp(-decay_rate[:, None, None] * jnp.maximum(lag_steps, 0.0)), 0.0
    )
    query_weight = jnp.exp(-decay_rate[:, None] * (step_pos + 1.0))[:, :, None]
    key_weight = jnp.exp(-decay_rate[:, None] * (group_len - 1.0 - step_pos))[:, :, None]

    inputs = tokens.astype(F32)
    normed_one, scale_one = norm_rows(inputs)
    normed_low = normed_one.astype(BF16)
    key_pre = project(normed_low, w_key)
    value_pre = project(normed_low, w_value)
    key_rot = rotate(split_heads(jax.nn.silu(key_pre), head_count), cosine, sine_part)
    key_low = key_rot.astype(BF16)
    value_low = split_heads(value_pre, head_count).astype(BF16)
    key_dec = (key_rot * key_weight).astype(BF16)
    local_state = dot("shje,shjf->shef", key_dec, value_low)
    state_low = carried_state(local_state, decay_rate, group_len, False)

    query_pre = project(normed_low, w_query)
    ugate = project(normed_low, w_ugate)
    query_rot = rotate(split_heads(jax.nn.silu(query_pre), head_count), cosine, sine_part)
    query_low = query_rot.astype(BF16)
    query_dec = (query_rot * query_weight).astype(BF16)
    scores = dot("shie,shje->shij", query_low, key_low)
    weights_low = (scores * decay_mask).astype(BF16)
    inner_part = dot("shij,shje->shie", weights_low, value_low)
    outer_part = dot("shie,shef->shif", query_dec, state_low)
    merged = join_heads(inner_part + outer_part)
    normed_att, scale_att = norm_rows(merged)
    gated_low = (normed_att * ugate).astype(BF16)
    residual = inputs + project(gated_low, w_output)
    normed_two, scale_two = norm_rows(residual)
    rows_own = normed_two.astype(BF16).reshape(row_count, model_width)
    rows_nb = swap(rows_own, "tensor", 1)

    def hidden_part(rows, grads):
        mixed = 0.0
        back = 0.0
        kept = []
        for left, right, down in (shard, other):
            e1 = jnp.dot(rows, left, preferred_element_type=F32)
            e2 = jnp.dot(rows, right, preferred_element_type=F32)
            product = (e1 * e2).astype(BF16)
            dm = dot("rd,fd->rf", grads, down)
            de1 = (dm * e2).astype(BF16)
            de2 = (dm * e1).astype(BF16)
            mixed = mixed + jnp.dot(product, down, preferred_element_type=F32)
            back = back + dot("rf,df->rd", de1, left) + dot("rf,df->rd", de2, right)
            kept.append((de1, de2, product))
        return mixed, back, kept

    mixed_nb, back_nb, kept_nb = hidden_part(rows_nb, grad_nb)
    back_in = swap(back_nb.astype(BF16), "tensor", 1)
    mixed_in = swap(mixed_nb.astype(BF16), "tensor", 1)
    mixed_own, back_own, kept_own = hidden_part(rows_own, grad_own)

    shape = (seq_count, group_len, model_width)
    mixed_out = (residual + (mixed_own + mixed_in.astype(F32)).reshape(shape)).astype(BF16)

    rows_all = jnp.concatenate([rows_own, rows_nb], axis=0)
    grads_all = jnp.concatenate([grad_own, grad_nb], axis=0)
    halves = []
    for at in range(2):
        de1, de2, product = (
            jnp.concatenate([first, second], axis=0)
            for first, second in zip(kept_own[at], kept_nb[at])
        )
        full = (
            (dot("rd,rf->df", rows_all, de1), 0),
            (dot("rd,rf->df", rows_all, de2), 0),
            (dot("rf,rd->fd", product, grads_all), 1),
        )
        sent = swap(
            tuple(take_half(g, 1 - core, axis).astype(BF16) for g, axis in full), "dp", 1
        )
        halves.append(
            tuple(take_half(g, core, axis) + s.astype(F32) for (g, axis), s in zip(full, sent))
        )
    from_y = swap(tuple(g.astype(BF16) for g in halves[1]), "tensor", 2)
    left_half, right_half, down_half = (
        added(mine, theirs) for mine, theirs in zip(halves[0], from_y)
    )

    grad_normed_two = (back_own + back_in.astype(F32)).reshape(shape)
    grad_mid = grad_res + norm_back(grad_normed_two, normed_two, scale_two)
    grad_branch = grad_mid.astype(BF16)
    grad_gated = project_back(grad_branch, w_output)
    grad_output = weight_grad(gated_low, grad_branch)
    grad_ugate_pre = (grad_gated * normed_att).astype(BF16)
    grad_merged = norm_back(grad_gated * ugate, normed_att, scale_att)
    grad_att = split_heads(grad_merged, head_count).astype(BF16)
    grad_state_in = dot("shie,shif->shef", query_dec, grad_att)
    grad_local_low = carried_state(grad_state_in, decay_rate, group_len, True)

    grad_weights = dot("shie,shje->shij", grad_att, value_low)
    grad_value_heads = dot("shij,shie->shje", weights_low, grad_att)
    grad_scores = (grad_weights * decay_mask).astype(BF16)
    grad_query_rot = dot("shij,shje->shie", grad_scores, key_low)
    grad_key_rot = dot("shij,shie->shje", grad_scores, query_low)
    grad_query_dec = dot("shif,shef->shie", grad_att, state_low)
    grad_query_rot = grad_query_rot + grad_query_dec * query_weight
    grad_query_pre = (
        join_heads(rotate_back(grad_query_rot, cosine, sine_part)) * silu_slope(query_pre)
    ).astype(BF16)
    grad_query = weight_grad(normed_low, grad_query_pre)
    grad_ugate = weight_grad(normed_low, grad_ugate_pre)

    grad_key_dec = dot("shef,shjf->shje", grad_local_low, value_low)
    grad_value_heads = grad_value_heads + dot("shje,shef->shjf", key_dec, grad_local_low)
    grad_key_rot = grad_key_rot + grad_key_dec * key_weight
    grad_key_pre = (
        join_heads(rotate_back(grad_key_rot, cosine, sine_part)) * silu_slope(key_pre)
    ).astype(BF16)
    grad_value_pre = join_heads(grad_value_heads).astype(BF16)
    grad_normed_one = (
        project_back(grad_query_pre, w_query)
        + project_back(grad_key_pre, w_key)
        + project_back(grad_value_pre, w_value)
        + project_back(grad_ugate_pre, w_ugate)
    )
    grad_tokens = grad_mid + norm_back(grad_normed_one, normed_one, scale_one)
    grad_key = weight_grad(normed_low, grad_key_pre)
    grad_value = weight_grad(normed_low, grad_value_pre)

    partial = (grad_query, grad_key, grad_value, grad_ugate, grad_output)
    sums, pair_sums, down_sums = reduce_grads(
        tuple(g.astype(BF16) for g in partial),
        jnp.concatenate([left_half, right_half], axis=0),
        down_half,
        lax.axis_size("seq"),
    )
    attention_grads = tuple(
        sums[i * model_width : (i + 1) * model_width].astype(F32) for i in range(len(partial))
    )
    pair_sums = pair_sums.reshape(2, model_width, -1).astype(F32)
    hidden_grads = (pair_sums[0], pair_sums[1], down_sums.astype(F32))
    return (mixed_out, grad_tokens) + attention_grads + hidden_grads


def solution(mesh):
    rows = P("dp", ("seq", "tensor"), None)
    columns = P(None, "tensor")
    return jax.shard_map(
        on_device,
        mesh=mesh,
        in_specs=(rows, P(), P(), P(), P(), P(), columns, columns, P("tensor", None), P(), rows),
        out_specs=(rows, rows, P(), P(), P(), P(), P(), columns, columns, P("tensor", None)),
        check_vma=False,
    )
```

```python
import jax
import jax.numpy as jnp
from jax import lax
from jax.experimental import pallas as pl
from jax.experimental.pallas import tpu as pltpu
from jax.sharding import PartitionSpec as P


EPS = 1e-06
F32 = jnp.float32
BF16 = jnp.bfloat16


def swap(value, axis, bit):
    count = lax.axis_size(axis)
    return jax.tree.map(
        lambda v: lax.ppermute(v, axis, [(i, i ^ bit) for i in range(count)]), value
    )


def shift(value, axis, step):
    count = lax.axis_size(axis)
    pairs = [(i, i + step) for i in range(count) if 0 <= i + step < count]
    return lax.ppermute(value, axis, pairs)


def take_half(value, which, axis=0):
    half = value.shape[axis] // 2
    return lax.dynamic_slice_in_dim(value, which * half, half, axis)


def carried_state(local, decay_rate, block_len, backward):
    heads = local.shape[1]
    width = lax.axis_size("tensor")
    share = heads // width
    depth = lax.axis_size("seq")
    mine = lax.axis_index("tensor")

    def power(count, rate):
        return jnp.exp(-rate * block_len * count)

    pieces = []
    for b in range(width):
        part = lax.dynamic_slice_in_dim(local, (mine ^ b) * share, share, 1)
        pieces.append(part if b == 0 else swap(part.astype(BF16), "tensor", b).astype(F32))
    rate = lax.dynamic_slice_in_dim(decay_rate, mine * share, share, 0)

    def scaled(coef, part):
        return coef[None, :, None, None] * part

    total = 0.0
    for b in range(width):
        place = mine ^ b
        left = place if backward else width - 1 - place
        total = total + scaled(power(left.astype(F32), rate), pieces[b])
    total_low = total.astype(BF16)
    entering = 0.0
    for j in range(1, depth):
        step = -j if backward else j
        moved = shift(total_low, "seq", step).astype(F32)
        entering = entering + scaled(power(float(width * (j - 1)), rate), moved)
    outs = []
    for d in range(width):
        target = mine ^ d
        inner = (width - 1 - target) if backward else target
        value = scaled(power(inner.astype(F32), rate), entering)
        for b in range(width):
            if b == d:
                continue
            source = mine ^ b
            gap = (source - target - 1) if backward else (target - source - 1)
            coef = jnp.where(gap >= 0, power(jnp.maximum(gap, 0).astype(F32), rate), 0.0)
            value = value + scaled(coef, pieces[b])
        low_value = value.astype(BF16)
        outs.append(low_value if d == 0 else swap(low_value, "tensor", d))
    bit = 1
    while bit < width:
        flip = (mine & bit) != 0
        outs = [jnp.where(flip, outs[u ^ bit], outs[u]) for u in range(width)]
        bit *= 2
    return jnp.concatenate(outs, axis=1)


CHUNK = 256
LAG = 2


def added(first, second):
    return (first.astype(F32) + second.astype(F32)).astype(BF16)


def reduce_kernel(
    depth,
    grads,
    pair_in,
    out,
    pair_out,
    own,
    core_in,
    first_in,
    second_in,
    line_in,
    line_mid,
    pair_line,
    pair_mid,
    sems,
    pair_sems,
    load_sem,
):
    core = lax.axis_index("dp")
    slot = lax.axis_index("tensor")
    place = lax.axis_index("seq")
    rows = own.shape[0]
    chunks = rows // CHUNK
    half, quarter, eighth = CHUNK // 2, CHUNK // 4, CHUNK // 8
    low_side = place < depth // 2
    outermost = (place == 0) | (place == depth - 1)
    middle = (place == depth // 2 - 1) | (place == depth // 2)
    inward = jnp.where(low_side, place + 1, place - 1)
    outward = jnp.where(low_side, place - 1, place + 1)

    barrier = pltpu.get_barrier_semaphore()

    def greet(peer):
        pl.semaphore_signal(
            barrier, inc=1, device_id=peer, device_id_type=pl.DeviceIdType.MESH
        )

    greet({"dp": 1 - core})
    greet({"tensor": slot ^ 1})
    greet({"tensor": slot ^ 2})

    @pl.when(place > 0)
    def _():
        greet({"seq": place - 1})

    @pl.when(place < depth - 1)
    def _():
        greet({"seq": place + 1})

    pl.semaphore_wait(barrier, jnp.where(outermost, 4, 5))

    def remote(source, target, sem, at, peer):
        return pltpu.make_async_remote_copy(
            src_ref=source,
            dst_ref=target,
            send_sem=sem.at[0, at],
            recv_sem=sem.at[1, at],
            device_id=peer,
            device_id_type=pl.DeviceIdType.MESH,
        )

    def span(start, size):
        return pl.ds(pl.multiple_of(start, size), size)

    def bits(q):
        first = jnp.where(q % 2 == 0, 1, 2)
        second = 3 - first
        return first, second, (slot & first) // first, (slot & second) // second

    def base(q):
        return pl.multiple_of(q * CHUNK, CHUNK)

    def to_core(q):
        return remote(
            own.at[span(base(q) + (1 - core) * half, half)],
            core_in.at[q],
            sems.at[0],
            q,
            {"dp": 1 - core},
        )

    def to_first(q):
        first, _, f, _ = bits(q)
        return remote(
            core_in.at[q, span((1 - f) * quarter, quarter)],
            first_in.at[q],
            sems.at[1],
            q,
            {"tensor": slot ^ first},
        )

    def to_second(q):
        _, second, _, g = bits(q)
        return remote(
            first_in.at[q, span((1 - g) * eighth, eighth)],
            second_in.at[q],
            sems.at[2],
            q,
            {"tensor": slot ^ second},
        )

    def block(q):
        _, _, f, g = bits(q)
        return base(q) + core * half + f * quarter + g * eighth

    def back_second(q):
        _, second, _, _ = bits(q)
        at = span(block(q), eighth)
        return remote(out.at[at], out.at[at], sems.at[3], q, {"tensor": slot ^ second})

    def back_first(q):
        first, _, f, _ = bits(q)
        at = span(base(q) + core * half + f * quarter, quarter)
        return remote(out.at[at], out.at[at], sems.at[4], q, {"tensor": slot ^ first})

    def back_core(q):
        at = span(base(q) + core * half, half)
        return remote(out.at[at], out.at[at], sems.at[5], q, {"dp": 1 - core})

    class Line:
        def __init__(self, mine, came, met, total, sem, offset):
            self.mine, self.came, self.met, self.total = mine, came, met, total
            self.sem, self.offset = sem, offset

        def inwards(self, q, source):
            return remote(
                source, self.came(q), self.sem.at[self.offset], q, {"seq": inward}
            )

        def across(self, q):
            return remote(
                self.came(q),
                self.met(q),
                self.sem.at[self.offset + 1],
                q,
                {"seq": depth - 1 - place},
            )

        def outwards(self, q):
            return remote(
                self.total(q), self.total(q), self.sem.at[self.offset + 2], q, {"seq": outward}
            )

        def step_in(self, q):
            @pl.when(outermost)
            def _():
                self.inwards(q, self.mine(q)).start()

        def step_middle(self, q):
            @pl.when(jnp.logical_not(outermost))
            def _():
                self.inwards(q, self.mine(q)).wait_recv()
                came = self.came(q)
                came[...] = added(self.mine(q)[...], came[...])

                @pl.when(middle)
                def _():
                    self.across(q).start()

                @pl.when(jnp.logical_not(middle))
                def _():
                    self.inwards(q, came).start()

        def step_out(self, q):
            @pl.when(middle)
            def _():
                self.across(q).wait_recv()
                self.total(q)[...] = added(self.came(q)[...], self.met(q)[...])

            @pl.when(jnp.logical_not(outermost))
            def _():
                @pl.when(jnp.logical_not(middle))
                def _():
                    self.outwards(q).wait_recv()

                self.outwards(q).start()

        def step_last(self, q):
            @pl.when(outermost)
            def _():
                self.outwards(q).wait_recv()

        def settle(self, q):
            @pl.when(outermost)
            def _():
                self.inwards(q, self.mine(q)).wait_send()

            @pl.when(jnp.logical_not(outermost))
            def _():
                @pl.when(middle)
                def _():
                    self.across(q).wait_send()

                @pl.when(jnp.logical_not(middle))
                def _():
                    self.inwards(q, self.came(q)).wait_send()

                self.outwards(q).wait_send()

    def second_mine(q):
        return second_in.at[q]

    line = Line(
        second_mine,
        lambda q: line_in.at[q],
        lambda q: line_mid.at[q],
        lambda q: out.at[span(block(q), eighth)],
        sems,
        6,
    )
    pair_chunks, pair_rows, pair_cols = pair_line.shape
    pair = Line(
        lambda q: pair_in.at[span(q * pair_rows, pair_rows)],
        lambda q: pair_line.at[q],
        lambda q: pair_mid.at[q],
        lambda q: pair_out.at[span(q * pair_rows, pair_rows), span(core * pair_cols, pair_cols)],
        pair_sems,
        0,
    )

    def pair_core(q):
        return remote(pair.total(q), pair.total(q), pair_sems.at[3], q, {"dp": 1 - core})

    size = rows // len(grads)
    loads = [
        pltpu.make_async_copy(g, own.at[pl.ds(i * size, size)], load_sem.at[i])
        for i, g in enumerate(grads)
    ]
    for load in loads:
        load.start()
    per_load = size // CHUNK
    for i, load in enumerate(loads):
        load.wait()

        @pl.loop(i * per_load, (i + 1) * per_load)
        def _(q):
            to_core(q).start()

    def stage_a(q):
        to_core(q).wait_recv()
        came = core_in.at[q]
        came[...] = added(own[span(base(q) + core * half, half)], came[...])

    def stage_b(q):
        _, _, f, _ = bits(q)
        to_first(q).wait_recv()
        came = first_in.at[q]
        came[...] = added(core_in[q, span(f * quarter, quarter)], came[...])

    def stage_c(q):
        _, _, _, g = bits(q)
        to_second(q).wait_recv()
        came = second_in.at[q]
        came[...] = added(first_in[q, span(g * eighth, eighth)], came[...])

    pairs = chunks // 2

    def during(step, lag, count, action):
        i = step - lag

        @pl.when((i >= 0) & (i < count))
        def _():
            action(i)

    def both(action):
        def run(i):
            action(2 * i)
            action(2 * i + 1)

        return run

    def start(copy):
        return lambda q: copy(q).start()

    def arrived(copy, following):
        def run(q):
            copy(q).wait_recv()
            following(q).start()

        return run

    def last_then_second(q):
        line.step_last(q)
        back_second(q).start()

    def finish_pair(q):
        pair.step_last(q)
        pair_core(q).start()

    steps = max(pairs + 7 * LAG, pair_chunks + 3 * LAG) + 1

    @pl.loop(0, steps)
    def _(step):
        during(step, 7 * LAG, pairs, both(arrived(back_first, back_core)))
        during(step, 6 * LAG, pairs, both(arrived(back_second, back_first)))
        during(step, 5 * LAG, pairs, both(last_then_second))
        during(step, 4 * LAG, pairs, both(line.step_out))
        during(step, 3 * LAG, pairs, both(line.step_middle))
        during(step, 2 * LAG, pairs, both(stage_c))
        during(step, LAG, pairs, both(stage_b))
        during(step, 0, pairs, both(stage_a))
        during(step, 2 * LAG, pairs, both(line.step_in))
        during(step, LAG, pairs, both(start(to_second)))
        during(step, 0, pairs, both(start(to_first)))
        during(step, 3 * LAG, pair_chunks, finish_pair)
        during(step, 2 * LAG, pair_chunks, pair.step_out)
        during(step, LAG, pair_chunks, pair.step_middle)
        during(step, 0, pair_chunks, pair.step_in)

    @pl.loop(0, chunks)
    def _(q):
        back_core(q).wait_recv()
        for copy in (to_core, to_first, to_second, back_second, back_first, back_core):
            copy(q).wait_send()
        line.settle(q)

    @pl.loop(0, pair_chunks)
    def _(q):
        pair_core(q).wait()
        pair.settle(q)


def reduce_grads(grads, pair_half, depth):
    size, width = grads[0].shape
    rows = size * len(grads)
    chunks = rows // CHUNK
    pair_chunks = 12
    pair_rows, pair_cols = pair_half.shape[0] // pair_chunks, pair_half.shape[1]
    vmem = pl.BlockSpec(memory_space=pltpu.VMEM)

    def body(*refs):
        reduce_kernel(depth, refs[: len(grads)], *refs[len(grads) :])

    return pl.pallas_call(
        body,
        out_shape=(
            jax.ShapeDtypeStruct((rows, width), BF16),
            jax.ShapeDtypeStruct((pair_half.shape[0], 2 * pair_cols), BF16),
        ),
        in_specs=[pl.BlockSpec(memory_space=pl.ANY)] * len(grads) + [vmem],
        out_specs=(vmem, vmem),
        scratch_shapes=[
            pltpu.VMEM((rows, width), BF16),
            pltpu.VMEM((chunks, CHUNK // 2, width), BF16),
            pltpu.VMEM((chunks, CHUNK // 4, width), BF16),
            pltpu.VMEM((chunks, CHUNK // 8, width), BF16),
            pltpu.VMEM((chunks, CHUNK // 8, width), BF16),
            pltpu.VMEM((chunks, CHUNK // 8, width), BF16),
            pltpu.VMEM((pair_chunks, pair_rows, pair_cols), BF16),
            pltpu.VMEM((pair_chunks, pair_rows, pair_cols), BF16),
            pltpu.SemaphoreType.DMA((9, 2, chunks)),
            pltpu.SemaphoreType.DMA((4, 2, pair_chunks)),
            pltpu.SemaphoreType.DMA((len(grads),)),
        ],
        compiler_params=pltpu.CompilerParams(
            collective_id=1, has_side_effects=True, vmem_limit_bytes=60 * 1024 * 1024
        ),
        name="reduce_grads",
    )(*grads, pair_half)


ROWS = 256


def times(x, w):
    return jnp.dot(x, w, preferred_element_type=F32)


def times_back(x, w):
    return lax.dot_general(x, w, (((1,), (1,)), ((), ())), preferred_element_type=F32)


def times_rows(x, y):
    return lax.dot_general(x, y, (((0,), (0,)), ((), ())), preferred_element_type=F32)


def hidden_kernel(rows, grads, left, right, down, fetched, swapped, *rest):
    mixed, back, own_kept, other_kept, acc_mixed, acc_back = rest[-6:]
    core = lax.axis_index("dp")
    _, half = fetched.shape[1:]
    here = pl.ds(pl.multiple_of(core * half, half), half)
    there = pl.ds(pl.multiple_of((1 - core) * half, half), half)

    def gates(kept, e1, e2, dm):
        kept[2] = (e1 * e2).astype(BF16)
        kept[0] = (dm * e2).astype(BF16)
        kept[1] = (dm * e1).astype(BF16)
        return kept[2], kept[0], kept[1]

    x, dy = rows[...], grads[...]
    mid, de1, de2 = gates(
        own_kept, times_back(x, left[...]), times_back(x, right[...]), times_back(dy, down[...])
    )
    acc_mixed[...] = times(mid, down[...])
    acc_back[...] = times(de1, left[...]) + times(de2, right[...])
    x_a, x_b = rows[:, here], rows[:, there]
    mid, de1, de2 = gates(
        other_kept,
        times_back(x_a, fetched[0]) + times_back(x_b, swapped[0]),
        times_back(x_a, fetched[1]) + times_back(x_b, swapped[1]),
        times_back(grads[:, here], fetched[2]) + times_back(grads[:, there], swapped[2]),
    )
    for at, part in ((here, fetched), (there, swapped)):
        mixed[:, at] = (acc_mixed[:, at] + times(mid, part[2])).astype(mixed.dtype)
        back[:, at] = (acc_back[:, at] + times(de1, part[0]) + times(de2, part[1])).astype(
            back.dtype
        )


def hidden_part(rows, grads, weights, kept, out_type):
    count, width = rows.shape
    hidden = weights[0].shape[0]
    first = 0 if kept is None else count // ROWS

    def whole(array):
        return pl.BlockSpec(array.shape, lambda i: (0,) * array.ndim)

    row_spec = pl.BlockSpec((ROWS, width), lambda i: (i, 0))
    kept_spec = pl.BlockSpec((3, ROWS, hidden), lambda i: (0, i + first, 0))
    extra = [] if kept is None else list(kept)
    held = 2 + len(weights)

    def body(*refs):
        hidden_kernel(*refs[:held], *refs[held + len(extra) :])

    outs = pl.pallas_call(
        body,
        grid=(count // ROWS,),
        out_shape=(jax.ShapeDtypeStruct((count, width), out_type),) * 2
        + (jax.ShapeDtypeStruct((3, 2 * count, hidden), BF16),) * 2,
        in_specs=[row_spec, row_spec]
        + [whole(w) for w in weights]
        + [pl.BlockSpec(memory_space=pl.ANY)] * len(extra),
        out_specs=(row_spec, row_spec, kept_spec, kept_spec),
        scratch_shapes=[pltpu.VMEM((ROWS, width), F32), pltpu.VMEM((ROWS, width), F32)],
        input_output_aliases={held + i: 2 + i for i in range(len(extra))},
        compiler_params=pltpu.CompilerParams(vmem_limit_bytes=56 * 1024 * 1024),
        cost_estimate=pl.CostEstimate(
            flops=24 * count * width * hidden,
            bytes_accessed=12 * width * hidden + 12 * count * hidden + 12 * count * width,
            transcendentals=0,
        ),
        name="hidden_part",
    )(rows, grads, *weights, *extra)
    return outs[0], outs[1], outs[2:]


def hidden_grads_kernel(kept, rows_own, rows_nb, grads_own, grads_nb, mine, theirs):
    core = lax.axis_index("dp")
    half = mine.shape[2]
    count = rows_own.shape[0]
    for out, which in ((mine, core), (theirs, 1 - core)):
        at = pl.ds(pl.multiple_of(which * half, half), half)

        @pl.when(pl.program_id(0) < 2)
        def _(out=out, at=at):
            out[0] = (
                times_rows(kept[0, :count], rows_own[:, at])
                + times_rows(kept[0, count:], rows_nb[:, at])
            ).astype(BF16)

        @pl.when(pl.program_id(0) == 2)
        def _(out=out, at=at):
            out[0] = (
                times_rows(kept[0, :count], grads_own[:, at])
                + times_rows(kept[0, count:], grads_nb[:, at])
            ).astype(BF16)


def hidden_grads(kept, rows_own, rows_nb, grads_own, grads_nb):
    count, width = rows_own.shape
    hidden = kept.shape[2]
    whole = pl.BlockSpec((count, width), lambda i: (0, 0))
    out_spec = pl.BlockSpec((1, hidden, width // 2), lambda i: (i, 0, 0))
    return pl.pallas_call(
        hidden_grads_kernel,
        grid=(3,),
        out_shape=(jax.ShapeDtypeStruct((3, hidden, width // 2), BF16),) * 2,
        in_specs=[pl.BlockSpec((1, 2 * count, hidden), lambda i: (i, 0, 0))] + [whole] * 4,
        out_specs=(out_spec, out_spec),
        compiler_params=pltpu.CompilerParams(vmem_limit_bytes=40 * 1024 * 1024),
        cost_estimate=pl.CostEstimate(
            flops=12 * count * width * hidden,
            bytes_accessed=12 * count * hidden + 8 * count * width + 6 * width * hidden,
            transcendentals=0,
        ),
        name="hidden_grads",
    )(kept, rows_own, rows_nb, grads_own, grads_nb)


def norm_rows(values):
    inv_scale = lax.rsqrt(jnp.mean(values * values, axis=-1, keepdims=True) + EPS)
    return (values * inv_scale, inv_scale)


def norm_back(gradient, normed, inv_scale):
    return inv_scale * (gradient - normed * jnp.mean(gradient * normed, axis=-1, keepdims=True))


def rotate(values, cosine, sine_part):
    half_dim = values.shape[-1] // 2
    first_half = values[..., :half_dim]
    second_half = values[..., half_dim:]
    return jnp.concatenate(
        [
            first_half * cosine - second_half * sine_part,
            second_half * cosine + first_half * sine_part,
        ],
        axis=-1,
    )


def rotate_back(values, cosine, sine_part):
    return rotate(values, cosine, -sine_part)


def split_heads(values, head_count):
    seq_count, group_len, model_width = values.shape
    return values.reshape(seq_count, group_len, head_count, model_width // head_count).transpose(
        0, 2, 1, 3
    )


def join_heads(values):
    seq_count, head_count, group_len, head_dim = values.shape
    return values.transpose(0, 2, 1, 3).reshape(seq_count, group_len, head_count * head_dim)


def dot(spec, first, second):
    return jnp.einsum(spec, first, second, preferred_element_type=F32)


def project(inputs, matrix):
    return dot("scd,de->sce", inputs, matrix)


def project_back(gradient, matrix):
    return dot("sce,de->scd", gradient, matrix)


def weight_grad(inputs, gradient):
    return dot("scd,sce->de", inputs, gradient)


def silu_slope(values):
    sigmoid_v = jax.nn.sigmoid(values)
    return sigmoid_v * (1.0 + values * (1.0 - sigmoid_v))


def on_device(
    tokens,
    w_query,
    w_key,
    w_value,
    w_ugate,
    w_output,
    w_left,
    w_right,
    w_down,
    decay_rate,
    cotangent,
):
    seq_count, group_len, model_width = tokens.shape
    head_count = decay_rate.shape[0]
    head_dim = model_width // head_count
    half_dim = head_dim // 2
    row_count = seq_count * group_len
    core = lax.axis_index("dp")

    shard = (w_left.T, w_right.T, w_down)
    fetched = swap(jnp.stack([take_half(w, core, 1) for w in shard]), "tensor", 2)
    weights = shard + (fetched, swap(fetched, "dp", 1))
    grad_res = cotangent.astype(F32)
    grad_own = cotangent.reshape(row_count, model_width)
    grad_nb = swap(grad_own, "tensor", 1)

    position_block = lax.axis_index(("seq", "tensor"))
    places = (position_block * group_len + jnp.arange(group_len)).astype(F32)
    frequency = 10000.0 ** (-jnp.arange(half_dim, dtype=F32) / half_dim)
    angles = places[:, None] * frequency[None, :]
    cosine = jnp.cos(angles)
    sine_part = jnp.sin(angles)
    step_pos = jnp.arange(group_len, dtype=F32)
    lag_steps = step_pos[:, None] - step_pos[None, :]
    decay_mask = jnp.where(
        lag_steps >= 0, jnp.exp(-decay_rate[:, None, None] * jnp.maximum(lag_steps, 0.0)), 0.0
    )
    query_weight = jnp.exp(-decay_rate[:, None] * (step_pos + 1.0))[:, :, None]
    key_weight = jnp.exp(-decay_rate[:, None] * (group_len - 1.0 - step_pos))[:, :, None]

    inputs = tokens.astype(F32)
    normed_one, scale_one = norm_rows(inputs)
    normed_low = normed_one.astype(BF16)
    key_pre = project(normed_low, w_key)
    value_pre = project(normed_low, w_value)
    key_rot = rotate(split_heads(jax.nn.silu(key_pre), head_count), cosine, sine_part)
    key_low = key_rot.astype(BF16)
    value_low = split_heads(value_pre, head_count).astype(BF16)
    key_dec = (key_rot * key_weight).astype(BF16)
    local_state = dot("shje,shjf->shef", key_dec, value_low)
    state_low = carried_state(local_state, decay_rate, group_len, False)

    query_pre = project(normed_low, w_query)
    ugate = project(normed_low, w_ugate)
    query_rot = rotate(split_heads(jax.nn.silu(query_pre), head_count), cosine, sine_part)
    query_low = query_rot.astype(BF16)
    query_dec = (query_rot * query_weight).astype(BF16)
    scores = dot("shie,shje->shij", query_low, key_low)
    weights_low = (scores * decay_mask).astype(BF16)
    inner_part = dot("shij,shje->shie", weights_low, value_low)
    outer_part = dot("shie,shef->shif", query_dec, state_low)
    merged = join_heads(inner_part + outer_part)
    normed_att, scale_att = norm_rows(merged)
    gated_low = (normed_att * ugate).astype(BF16)
    residual = inputs + project(gated_low, w_output)
    normed_two, scale_two = norm_rows(residual)
    rows_own = normed_two.astype(BF16).reshape(row_count, model_width)
    rows_nb = swap(rows_own, "tensor", 1)

    mixed_own, back_own, kept = hidden_part(rows_own, grad_own, weights, None, F32)
    mixed_nb, back_nb, kept = hidden_part(rows_nb, grad_nb, weights, kept, BF16)
    back_in = swap(back_nb, "tensor", 1)
    mixed_in = swap(mixed_nb, "tensor", 1)

    shape = (seq_count, group_len, model_width)

    mine, theirs = hidden_grads(kept[1], rows_own, rows_nb, grad_own, grad_nb)
    moved = swap(theirs, "dp", 1)
    from_y = swap(added(mine, moved), "tensor", 2)
    mine, theirs = hidden_grads(kept[0], rows_own, rows_nb, grad_own, grad_nb)
    moved = swap(theirs, "dp", 1)
    shard_half = (mine.astype(F32) + moved.astype(F32) + from_y.astype(F32)).astype(BF16)

    grad_normed_two = (back_own + back_in.astype(F32)).reshape(shape)
    grad_mid = grad_res + norm_back(grad_normed_two, normed_two, scale_two)
    grad_branch = grad_mid.astype(BF16)
    grad_gated = project_back(grad_branch, w_output)
    grad_output = weight_grad(gated_low, grad_branch)
    grad_ugate_pre = (grad_gated * normed_att).astype(BF16)
    grad_merged = norm_back(grad_gated * ugate, normed_att, scale_att)
    grad_att = split_heads(grad_merged, head_count).astype(BF16)
    grad_state_in = dot("shie,shif->shef", query_dec, grad_att)
    grad_local_low = carried_state(grad_state_in, decay_rate, group_len, True)

    grad_weights = dot("shie,shje->shij", grad_att, value_low)
    grad_value_heads = dot("shij,shie->shje", weights_low, grad_att)
    grad_scores = (grad_weights * decay_mask).astype(BF16)
    grad_query_rot = dot("shij,shje->shie", grad_scores, key_low)
    grad_key_rot = dot("shij,shie->shje", grad_scores, query_low)
    grad_query_dec = dot("shif,shef->shie", grad_att, state_low)
    grad_query_rot = grad_query_rot + grad_query_dec * query_weight
    grad_query_pre = (
        join_heads(rotate_back(grad_query_rot, cosine, sine_part)) * silu_slope(query_pre)
    ).astype(BF16)
    grad_query = weight_grad(normed_low, grad_query_pre)
    grad_ugate = weight_grad(normed_low, grad_ugate_pre)

    grad_key_dec = dot("shef,shjf->shje", grad_local_low, value_low)
    grad_value_heads = grad_value_heads + dot("shje,shef->shjf", key_dec, grad_local_low)
    grad_key_rot = grad_key_rot + grad_key_dec * key_weight
    grad_key_pre = (
        join_heads(rotate_back(grad_key_rot, cosine, sine_part)) * silu_slope(key_pre)
    ).astype(BF16)
    grad_value_pre = join_heads(grad_value_heads).astype(BF16)
    grad_normed_one = (
        project_back(grad_query_pre, w_query)
        + project_back(grad_key_pre, w_key)
        + project_back(grad_value_pre, w_value)
        + project_back(grad_ugate_pre, w_ugate)
    )
    grad_tokens = grad_mid + norm_back(grad_normed_one, normed_one, scale_one)
    grad_key = weight_grad(normed_low, grad_key_pre)
    grad_value = weight_grad(normed_low, grad_value_pre)

    partial = (grad_query, grad_key, grad_value, grad_ugate, grad_output)
    hidden = w_down.shape[0]
    sums, hidden_sums = reduce_grads(
        tuple(g.astype(BF16) for g in partial),
        shard_half.reshape(3 * hidden, model_width // 2),
        lax.axis_size("seq"),
    )
    sums, mixed_in, mixed_own, residual = lax.optimization_barrier(
        (sums, mixed_in, mixed_own, residual)
    )
    mixed_out = (residual + (mixed_own + mixed_in.astype(F32)).reshape(shape)).astype(BF16)
    attention_grads = tuple(
        sums[i * model_width : (i + 1) * model_width].astype(F32) for i in range(len(partial))
    )
    left_sum, right_sum, down_sum = (
        hidden_sums[i * hidden : (i + 1) * hidden].astype(F32) for i in range(3)
    )
    return (mixed_out, grad_tokens) + attention_grads + (left_sum.T, right_sum.T, down_sum)


def solution(mesh):
    rows = P("dp", ("seq", "tensor"), None)
    columns = P(None, "tensor")
    return jax.shard_map(
        on_device,
        mesh=mesh,
        in_specs=(rows, P(), P(), P(), P(), P(), columns, columns, P("tensor", None), P(), rows),
        out_specs=(rows, rows, P(), P(), P(), P(), P(), columns, columns, P("tensor", None)),
        check_vma=False,
    )
```

```python
import functools

import jax
import jax.numpy as jnp
from jax import lax
from jax.experimental import pallas as pl
from jax.experimental.pallas import tpu as pltpu
from jax.sharding import PartitionSpec as P


EPS = 1e-06
F32 = jnp.float32
BF16 = jnp.bfloat16


def swap(value, axis, bit):
    count = lax.axis_size(axis)
    return jax.tree.map(
        lambda v: lax.ppermute(v, axis, [(i, i ^ bit) for i in range(count)]), value
    )


CHUNK = 256
LAG = 2


def added(first, second):
    return (first.astype(F32) + second.astype(F32)).astype(BF16)


def reduce_kernel(
    depth,
    grads,
    pair_in,
    out,
    pair_out,
    own,
    core_in,
    first_in,
    second_in,
    line_in,
    line_mid,
    pair_line,
    pair_mid,
    sems,
    pair_sems,
    load_sem,
):
    core = lax.axis_index("dp")
    slot = lax.axis_index("tensor")
    place = lax.axis_index("seq")
    rows = own.shape[0]
    chunks = rows // CHUNK
    half, quarter, eighth = CHUNK // 2, CHUNK // 4, CHUNK // 8
    low_side = place < depth // 2
    outermost = (place == 0) | (place == depth - 1)
    middle = (place == depth // 2 - 1) | (place == depth // 2)
    inward = jnp.where(low_side, place + 1, place - 1)
    outward = jnp.where(low_side, place - 1, place + 1)

    barrier = pltpu.get_barrier_semaphore()

    def greet(peer):
        pl.semaphore_signal(
            barrier, inc=1, device_id=peer, device_id_type=pl.DeviceIdType.MESH
        )

    greet({"dp": 1 - core})
    greet({"tensor": slot ^ 1})
    greet({"tensor": slot ^ 2})

    @pl.when(place > 0)
    def _():
        greet({"seq": place - 1})

    @pl.when(place < depth - 1)
    def _():
        greet({"seq": place + 1})

    pl.semaphore_wait(barrier, jnp.where(outermost, 4, 5))

    def remote(source, target, sem, at, peer):
        return pltpu.make_async_remote_copy(
            src_ref=source,
            dst_ref=target,
            send_sem=sem.at[0, at],
            recv_sem=sem.at[1, at],
            device_id=peer,
            device_id_type=pl.DeviceIdType.MESH,
        )

    def span(start, size):
        return pl.ds(pl.multiple_of(start, size), size)

    def bits(q):
        first = jnp.where(q % 2 == 0, 1, 2)
        second = 3 - first
        return first, second, (slot & first) // first, (slot & second) // second

    def base(q):
        return pl.multiple_of(q * CHUNK, CHUNK)

    def to_core(q):
        return remote(
            own.at[span(base(q) + (1 - core) * half, half)],
            core_in.at[q],
            sems.at[0],
            q,
            {"dp": 1 - core},
        )

    def to_first(q):
        first, _, f, _ = bits(q)
        return remote(
            core_in.at[q, span((1 - f) * quarter, quarter)],
            first_in.at[q],
            sems.at[1],
            q,
            {"tensor": slot ^ first},
        )

    def to_second(q):
        _, second, _, g = bits(q)
        return remote(
            first_in.at[q, span((1 - g) * eighth, eighth)],
            second_in.at[q],
            sems.at[2],
            q,
            {"tensor": slot ^ second},
        )

    def block(q):
        _, _, f, g = bits(q)
        return base(q) + core * half + f * quarter + g * eighth

    def back_second(q):
        _, second, _, _ = bits(q)
        at = span(block(q), eighth)
        return remote(out.at[at], out.at[at], sems.at[3], q, {"tensor": slot ^ second})

    def back_first(q):
        first, _, f, _ = bits(q)
        at = span(base(q) + core * half + f * quarter, quarter)
        return remote(out.at[at], out.at[at], sems.at[4], q, {"tensor": slot ^ first})

    def back_core(q):
        at = span(base(q) + core * half, half)
        return remote(out.at[at], out.at[at], sems.at[5], q, {"dp": 1 - core})

    class Line:
        def __init__(self, mine, came, met, total, sem, offset):
            self.mine, self.came, self.met, self.total = mine, came, met, total
            self.sem, self.offset = sem, offset

        def inwards(self, q, source):
            return remote(
                source, self.came(q), self.sem.at[self.offset], q, {"seq": inward}
            )

        def across(self, q):
            return remote(
                self.came(q),
                self.met(q),
                self.sem.at[self.offset + 1],
                q,
                {"seq": depth - 1 - place},
            )

        def outwards(self, q):
            return remote(
                self.total(q), self.total(q), self.sem.at[self.offset + 2], q, {"seq": outward}
            )

        def step_in(self, q):
            @pl.when(outermost)
            def _():
                self.inwards(q, self.mine(q)).start()

        def step_middle(self, q):
            @pl.when(jnp.logical_not(outermost))
            def _():
                self.inwards(q, self.mine(q)).wait_recv()
                came = self.came(q)
                came[...] = added(self.mine(q)[...], came[...])

                @pl.when(middle)
                def _():
                    self.across(q).start()

                @pl.when(jnp.logical_not(middle))
                def _():
                    self.inwards(q, came).start()

        def step_out(self, q):
            @pl.when(middle)
            def _():
                self.across(q).wait_recv()
                self.total(q)[...] = added(self.came(q)[...], self.met(q)[...])

            @pl.when(jnp.logical_not(outermost))
            def _():
                @pl.when(jnp.logical_not(middle))
                def _():
                    self.outwards(q).wait_recv()

                self.outwards(q).start()

        def step_last(self, q):
            @pl.when(outermost)
            def _():
                self.outwards(q).wait_recv()

        def settle(self, q):
            @pl.when(outermost)
            def _():
                self.inwards(q, self.mine(q)).wait_send()

            @pl.when(jnp.logical_not(outermost))
            def _():
                @pl.when(middle)
                def _():
                    self.across(q).wait_send()

                @pl.when(jnp.logical_not(middle))
                def _():
                    self.inwards(q, self.came(q)).wait_send()

                self.outwards(q).wait_send()

    def second_mine(q):
        return second_in.at[q]

    line = Line(
        second_mine,
        lambda q: line_in.at[q],
        lambda q: line_mid.at[q],
        lambda q: out.at[span(block(q), eighth)],
        sems,
        6,
    )
    pair_chunks, pair_rows, pair_cols = pair_line.shape
    pair = Line(
        lambda q: pair_in.at[span(q * pair_rows, pair_rows)],
        lambda q: pair_line.at[q],
        lambda q: pair_mid.at[q],
        lambda q: pair_out.at[span(q * pair_rows, pair_rows), span(core * pair_cols, pair_cols)],
        pair_sems,
        0,
    )

    def pair_core(q):
        return remote(pair.total(q), pair.total(q), pair_sems.at[3], q, {"dp": 1 - core})

    size = rows // len(grads)
    loads = [
        pltpu.make_async_copy(g, own.at[pl.ds(i * size, size)], load_sem.at[i])
        for i, g in enumerate(grads)
    ]
    for load in loads:
        load.start()
    per_load = size // CHUNK
    for i, load in enumerate(loads):
        load.wait()

        @pl.loop(i * per_load, (i + 1) * per_load)
        def _(q):
            to_core(q).start()

    def stage_a(q):
        to_core(q).wait_recv()
        came = core_in.at[q]
        came[...] = added(own[span(base(q) + core * half, half)], came[...])

    def stage_b(q):
        _, _, f, _ = bits(q)
        to_first(q).wait_recv()
        came = first_in.at[q]
        came[...] = added(core_in[q, span(f * quarter, quarter)], came[...])

    def stage_c(q):
        _, _, _, g = bits(q)
        to_second(q).wait_recv()
        came = second_in.at[q]
        came[...] = added(first_in[q, span(g * eighth, eighth)], came[...])

    pairs = chunks // 2

    def during(step, lag, count, action):
        i = step - lag

        @pl.when((i >= 0) & (i < count))
        def _():
            action(i)

    def both(action):
        def run(i):
            action(2 * i)
            action(2 * i + 1)

        return run

    def start(copy):
        return lambda q: copy(q).start()

    def arrived(copy, following):
        def run(q):
            copy(q).wait_recv()
            following(q).start()

        return run

    def last_then_second(q):
        line.step_last(q)
        back_second(q).start()

    def finish_pair(q):
        pair.step_last(q)
        pair_core(q).start()

    steps = max(pairs + 7 * LAG, pair_chunks + 3 * LAG) + 1

    @pl.loop(0, steps)
    def _(step):
        during(step, 7 * LAG, pairs, both(arrived(back_first, back_core)))
        during(step, 6 * LAG, pairs, both(arrived(back_second, back_first)))
        during(step, 5 * LAG, pairs, both(last_then_second))
        during(step, 4 * LAG, pairs, both(line.step_out))
        during(step, 3 * LAG, pairs, both(line.step_middle))
        during(step, 2 * LAG, pairs, both(stage_c))
        during(step, LAG, pairs, both(stage_b))
        during(step, 0, pairs, both(stage_a))
        during(step, 2 * LAG, pairs, both(line.step_in))
        during(step, LAG, pairs, both(start(to_second)))
        during(step, 0, pairs, both(start(to_first)))
        during(step, 3 * LAG, pair_chunks, finish_pair)
        during(step, 2 * LAG, pair_chunks, pair.step_out)
        during(step, LAG, pair_chunks, pair.step_middle)
        during(step, 0, pair_chunks, pair.step_in)

    @pl.loop(0, chunks)
    def _(q):
        back_core(q).wait_recv()
        for copy in (to_core, to_first, to_second, back_second, back_first, back_core):
            copy(q).wait_send()
        line.settle(q)

    @pl.loop(0, pair_chunks)
    def _(q):
        pair_core(q).wait()
        pair.settle(q)


def reduce_grads(grads, pair_half, depth):
    size, width = grads[0].shape
    rows = size * len(grads)
    chunks = rows // CHUNK
    pair_chunks = 12
    pair_rows, pair_cols = pair_half.shape[0] // pair_chunks, pair_half.shape[1]
    vmem = pl.BlockSpec(memory_space=pltpu.VMEM)

    def body(*refs):
        reduce_kernel(depth, refs[: len(grads)], *refs[len(grads) :])

    return pl.pallas_call(
        body,
        out_shape=(
            jax.ShapeDtypeStruct((rows, width), BF16),
            jax.ShapeDtypeStruct((pair_half.shape[0], 2 * pair_cols), BF16),
        ),
        in_specs=[pl.BlockSpec(memory_space=pl.ANY)] * len(grads) + [vmem],
        out_specs=(vmem, vmem),
        scratch_shapes=[
            pltpu.VMEM((rows, width), BF16),
            pltpu.VMEM((chunks, CHUNK // 2, width), BF16),
            pltpu.VMEM((chunks, CHUNK // 4, width), BF16),
            pltpu.VMEM((chunks, CHUNK // 8, width), BF16),
            pltpu.VMEM((chunks, CHUNK // 8, width), BF16),
            pltpu.VMEM((chunks, CHUNK // 8, width), BF16),
            pltpu.VMEM((pair_chunks, pair_rows, pair_cols), BF16),
            pltpu.VMEM((pair_chunks, pair_rows, pair_cols), BF16),
            pltpu.SemaphoreType.DMA((9, 2, chunks)),
            pltpu.SemaphoreType.DMA((4, 2, pair_chunks)),
            pltpu.SemaphoreType.DMA((len(grads),)),
        ],
        compiler_params=pltpu.CompilerParams(
            collective_id=1, has_side_effects=True, vmem_limit_bytes=60 * 1024 * 1024
        ),
        name="reduce_grads",
    )(*grads, pair_half)


ROWS = 256


def times(x, w):
    return jnp.dot(x, w, preferred_element_type=F32)


def times_back(x, w):
    return lax.dot_general(x, w, (((1,), (1,)), ((), ())), preferred_element_type=F32)


def times_rows(x, y):
    return lax.dot_general(x, y, (((0,), (0,)), ((), ())), preferred_element_type=F32)


def hidden_kernel(rows, grads, left, right, down, other, *rest):
    mixed, back, own_kept, other_kept, acc_mixed, acc_back = rest[-6:]

    def unit(kept, w_left, w_right, w_down):
        e1, e2 = times_back(rows[...], w_left), times_back(rows[...], w_right)
        dm = times_back(grads[...], w_down)
        kept[2] = (e1 * e2).astype(BF16)
        kept[0] = (dm * e2).astype(BF16)
        kept[1] = (dm * e1).astype(BF16)
        return times(kept[2], w_down), times(kept[0], w_left) + times(kept[1], w_right)

    acc_mixed[...], acc_back[...] = unit(own_kept, left[...], right[...], down[...])
    more_mixed, more_back = unit(other_kept, other[0], other[1], other[2])
    mixed[...] = (acc_mixed[...] + more_mixed).astype(mixed.dtype)
    back[...] = (acc_back[...] + more_back).astype(back.dtype)


def hidden_part(rows, grads, weights, kept, out_type):
    count, width = rows.shape
    hidden = weights[0].shape[0]
    first = 0 if kept is None else count // ROWS

    def whole(array):
        return pl.BlockSpec(array.shape, lambda i: (0,) * array.ndim)

    row_spec = pl.BlockSpec((ROWS, width), lambda i: (i, 0))
    kept_spec = pl.BlockSpec((3, ROWS, hidden), lambda i: (0, i + first, 0))
    extra = [] if kept is None else list(kept)
    held = 2 + len(weights)

    def body(*refs):
        hidden_kernel(*refs[:held], *refs[held + len(extra) :])

    outs = pl.pallas_call(
        body,
        grid=(count // ROWS,),
        out_shape=(jax.ShapeDtypeStruct((count, width), out_type),) * 2
        + (jax.ShapeDtypeStruct((3, 2 * count, hidden), BF16),) * 2,
        in_specs=[row_spec, row_spec]
        + [whole(w) for w in weights]
        + [pl.BlockSpec(memory_space=pl.ANY)] * len(extra),
        out_specs=(row_spec, row_spec, kept_spec, kept_spec),
        scratch_shapes=[pltpu.VMEM((ROWS, width), F32), pltpu.VMEM((ROWS, width), F32)],
        input_output_aliases={held + i: 2 + i for i in range(len(extra))},
        compiler_params=pltpu.CompilerParams(vmem_limit_bytes=56 * 1024 * 1024),
        cost_estimate=pl.CostEstimate(
            flops=24 * count * width * hidden,
            bytes_accessed=12 * width * hidden + 12 * count * hidden + 12 * count * width,
            transcendentals=0,
        ),
        name="hidden_part",
    )(rows, grads, *weights, *extra)
    return outs[0], outs[1], outs[2:]


def hidden_grads_kernel(kept, rows_own, rows_nb, grads_own, grads_nb, mine, theirs):
    core = lax.axis_index("dp")
    half = mine.shape[2]
    count = rows_own.shape[0]
    for out, which in ((mine, core), (theirs, 1 - core)):
        at = pl.ds(pl.multiple_of(which * half, half), half)

        @pl.when(pl.program_id(0) < 2)
        def _(out=out, at=at):
            out[0] = (
                times_rows(kept[0, :count], rows_own[:, at])
                + times_rows(kept[0, count:], rows_nb[:, at])
            ).astype(BF16)

        @pl.when(pl.program_id(0) == 2)
        def _(out=out, at=at):
            out[0] = (
                times_rows(kept[0, :count], grads_own[:, at])
                + times_rows(kept[0, count:], grads_nb[:, at])
            ).astype(BF16)


def hidden_grads(kept, rows_own, rows_nb, grads_own, grads_nb):
    count, width = rows_own.shape
    hidden = kept.shape[2]
    whole = pl.BlockSpec((count, width), lambda i: (0, 0))
    out_spec = pl.BlockSpec((1, hidden, width // 2), lambda i: (i, 0, 0))
    return pl.pallas_call(
        hidden_grads_kernel,
        grid=(3,),
        out_shape=(jax.ShapeDtypeStruct((3, hidden, width // 2), BF16),) * 2,
        in_specs=[pl.BlockSpec((1, 2 * count, hidden), lambda i: (i, 0, 0))] + [whole] * 4,
        out_specs=(out_spec, out_spec),
        compiler_params=pltpu.CompilerParams(vmem_limit_bytes=40 * 1024 * 1024),
        cost_estimate=pl.CostEstimate(
            flops=12 * count * width * hidden,
            bytes_accessed=12 * count * hidden + 8 * count * width + 6 * width * hidden,
            transcendentals=0,
        ),
        name="hidden_grads",
    )(kept, rows_own, rows_nb, grads_own, grads_nb)


MESH = pl.DeviceIdType.MESH


class States:
    def __init__(self, depth, width, backward, powers, local, came, total, far, outs, states, sems):
        self.depth, self.width, self.backward, self.powers = depth, width, backward, powers
        self.local, self.came, self.total, self.far = local, came, total, far
        self.outs, self.states, self.sems = outs, states, sems
        self.slot = lax.axis_index("tensor")
        self.place = lax.axis_index("seq")
        self.share = local.shape[0] // width

    def greet(self, more=()):
        barrier = pltpu.get_barrier_semaphore()
        for peer in more:
            pl.semaphore_signal(barrier, inc=1, device_id=peer, device_id_type=MESH)
        for b in range(1, self.width):
            pl.semaphore_signal(
                barrier, inc=1, device_id={"tensor": self.slot ^ b}, device_id_type=MESH
            )
        for j in range(1, self.depth):
            peer = lax.rem(self.place + j, self.depth)
            pl.semaphore_signal(barrier, inc=1, device_id={"seq": peer}, device_id_type=MESH)
        pl.semaphore_wait(barrier, self.width + self.depth - 2 + len(more))

    def copy(self, source, target, at, peer):
        return pltpu.make_async_remote_copy(
            src_ref=source,
            dst_ref=target,
            send_sem=self.sems.at[0, at],
            recv_sem=self.sems.at[1, at],
            device_id=peer,
            device_id_type=MESH,
        )

    def group(self, slot):
        return pl.ds(slot * self.share, self.share)

    def to_peer(self, b):
        peer = self.slot ^ b
        return self.copy(
            self.local.at[self.group(peer)], self.came.at[b - 1], b - 1, {"tensor": peer}
        )

    def to_far(self, j):
        peer = self.place - j if self.backward else self.place + j
        return self.copy(self.total, self.far.at[j - 1], self.width + j - 2, {"seq": peer})

    def has_far(self, j):
        return self.place >= j if self.backward else self.place + j < self.depth

    def from_far(self, j):
        return self.place + j < self.depth if self.backward else self.place >= j

    def to_owner(self, d):
        at = self.width + self.depth - 2 + d - 1
        return self.copy(
            self.outs.at[d - 1],
            self.states.at[self.group(self.slot)],
            at,
            {"tensor": self.slot ^ d},
        )

    def power(self, count, head):
        return self.powers[count, head]

    def piece(self, b, k, s):
        if b == 0:
            return self.local[self.slot * self.share + k, s].astype(F32)
        return self.came[b - 1, k, s].astype(F32)

    def gather(self):
        for b in range(1, self.width):
            self.to_peer(b).wait_recv()
        for k in range(self.share):
            head = self.slot * self.share + k
            for s in range(self.local.shape[1]):
                value = 0.0
                for b in range(self.width):
                    spot = self.slot ^ b
                    left = spot if self.backward else self.width - 1 - spot
                    value = value + self.power(left, head) * self.piece(b, k, s)
                self.total[k, s] = value.astype(BF16)
        for j in range(1, self.depth):

            @pl.when(self.has_far(j))
            def _(j=j):
                self.to_far(j).start()

    def send_back(self, entering):
        for j in range(1, self.depth):

            @pl.when(self.from_far(j))
            def _(j=j):
                self.to_far(j).wait_recv()

            @pl.when(jnp.logical_not(self.from_far(j)))
            def _(j=j):
                self.far[j - 1] = jnp.zeros(self.far.shape[1:], BF16)

        for k in range(self.share):
            head = self.slot * self.share + k
            for s in range(self.local.shape[1]):
                value = 0.0
                for j in range(1, self.depth):
                    value = value + self.power(self.width * (j - 1), head) * self.far[
                        j - 1, k, s
                    ].astype(F32)
                entering[k, s] = value
        for d in list(range(1, self.width)) + [0]:
            target = self.slot ^ d
            inner = self.width - 1 - target if self.backward else target
            for k in range(self.share):
                head = self.slot * self.share + k
                for s in range(self.local.shape[1]):
                    value = self.power(inner, head) * entering[k, s]
                    for b in range(self.width):
                        if b == d:
                            continue
                        source = self.slot ^ b
                        gap = source - target - 1 if self.backward else target - source - 1
                        coef = jnp.where(gap >= 0, self.power(jnp.maximum(gap, 0), head), 0.0)
                        value = value + coef * self.piece(b, k, s)
                    if d == 0:
                        self.states[head, s] = value.astype(BF16)
                    else:
                        self.outs[d - 1, k, s] = value.astype(BF16)
        for d in range(1, self.width):
            self.to_owner(d).start()

    def arrive(self):
        for d in range(1, self.width):
            at = self.width + self.depth - 2 + d - 1
            self.copy(
                self.outs.at[d - 1],
                self.states.at[self.group(self.slot ^ d)],
                at,
                {"tensor": self.slot ^ d},
            ).wait_recv()

    def settle(self):
        for b in range(1, self.width):
            self.to_peer(b).wait_send()
            self.to_owner(b).wait_send()
        for j in range(1, self.depth):

            @pl.when(self.has_far(j))
            def _(j=j):
                self.to_far(j).wait_send()


def state_scratch(heads, seqs, head_dim, width, depth):
    share = heads // width
    low = functools.partial(pltpu.VMEM, dtype=BF16)
    return [
        low((heads, seqs, head_dim, head_dim)),
        low((width - 1, share, seqs, head_dim, head_dim)),
        low((share, seqs, head_dim, head_dim)),
        low((depth - 1, share, seqs, head_dim, head_dim)),
        low((width - 1, share, seqs, head_dim, head_dim)),
        pltpu.VMEM((share, seqs, head_dim, head_dim), F32),
        pltpu.SemaphoreType.DMA((2, 2 * (width - 1) + depth - 1)),
    ]


def turn(values, cosine, sine_part):
    return values * cosine + pltpu.roll(values, values.shape[-1] // 2, 1) * sine_part


def square_mean(values):
    return jnp.mean(values * values, axis=-1, keepdims=True)


def decays(rates, head, length, dim):
    rate = rates[head]
    place = lax.broadcasted_iota(jnp.int32, (length, dim), 0).astype(F32)
    query = jnp.exp(-rate[:, :dim] * (place + 1.0))
    key = jnp.exp(-rate[:, :dim] * (length - 1.0 - place))
    return query, key


def lag_decay(rates, head, length):
    lag = (
        lax.broadcasted_iota(jnp.int32, (length, length), 0)
        - lax.broadcasted_iota(jnp.int32, (length, length), 1)
    ).astype(F32)
    return jnp.where(lag >= 0, jnp.exp(-rates[head] * jnp.maximum(lag, 0.0)), 0.0)


def attend_kernel(
    depth,
    width,
    seqs,
    x,
    w_key,
    w_value,
    late_query,
    late_gate,
    late_output,
    left,
    right,
    down,
    grads,
    rates,
    powers,
    cosine,
    sine_part,
    residual,
    normed_two,
    attended,
    query_pre,
    key_pre,
    gate,
    normed_one,
    query_low,
    key_low,
    value_low,
    query_dec,
    key_dec,
    scores_low,
    gated,
    states,
    other,
    grads_nb,
    w_query,
    w_gate,
    w_output,
    local,
    came,
    total,
    far,
    outs,
    entering,
    sems,
    load_sem,
    bulk_sems,
):
    rows, model = x.shape
    length = rows // seqs
    dim = cosine.shape[1]
    tile = model // width
    loads = [
        pltpu.make_async_copy(a, b, load_sem.at[i])
        for i, (a, b) in enumerate(
            ((late_query, w_query), (late_gate, w_gate), (late_output, w_output))
        )
    ]
    for load in loads:
        load.start()
    exchange = States(
        depth, width, False, powers, local, came, total, far, outs, states, sems
    )
    core = lax.axis_index("dp")
    parity = lax.rem(exchange.place, 2)
    shard = (left, right, down)
    part_rows, part_cols = left.shape[0] // 2, model // 2
    columns_here = pl.ds(pl.multiple_of(core * part_cols, part_cols), part_cols)

    def rows_of(which):
        return pl.ds(pl.multiple_of(which * part_rows, part_rows), part_rows)

    def send(source, target, at, peer):
        return pltpu.make_async_remote_copy(
            src_ref=source,
            dst_ref=target,
            send_sem=bulk_sems.at[0, at],
            recv_sem=bulk_sems.at[1, at],
            device_id=peer,
            device_id_type=MESH,
        )

    def fetch(m):
        at = (rows_of(parity), columns_here)
        return send(
            shard[m].at[at], other.at[(m,) + at], m, {"tensor": exchange.slot ^ 2}
        )

    def relay(m):
        at = other.at[m, rows_of(parity), columns_here]
        return send(at, at, 3 + m, {"seq": exchange.place + 1 - 2 * parity})

    def share(m, which):
        spot = parity if which == 0 else 1 - parity
        at = other.at[m, rows_of(spot), columns_here]
        return send(at, at, 6 + 2 * m + which, {"dp": 1 - core})

    def cross(s):
        at = pl.ds(s * length, length)
        return send(grads.at[at], grads_nb.at[at], 12 + s, {"tensor": exchange.slot ^ 1})

    def pass_on(m):
        fetch(m).wait_recv()
        relay(m).start()
        share(m, 0).start()

    def pass_last(m):
        relay(m).wait_recv()
        share(m, 1).start()

    exchange.greet((({"dp": 1 - core}),))
    fetch(0).start()
    cross(0).start()
    fetch(1).start()
    for s in range(seqs):
        at = pl.ds(s * length, length)
        value = x[at].astype(F32)
        normed_one[at] = (value * lax.rsqrt(square_mean(value) + EPS)).astype(BF16)

    per_tile = tile // dim

    @pl.loop(1, width + 1)
    def _(step):
        b = lax.rem(step, width)
        spot = exchange.slot ^ b
        columns = pl.ds(pl.multiple_of(spot * tile, tile), tile)
        key_pre[:, columns] = times(normed_one[...], w_key[:, columns])
        value_low[:, columns] = times(normed_one[...], w_value[:, columns]).astype(BF16)
        for k in range(per_tile):
            head = spot * per_tile + k
            own = pl.ds(pl.multiple_of(spot * tile + k * dim, dim), dim)
            _, key_weight = decays(rates, head, length, dim)
            for s in range(seqs):
                at = pl.ds(s * length, length)
                turned = turn(jax.nn.silu(key_pre[at, own]), cosine[...], sine_part[...])
                key_low[at, own] = turned.astype(BF16)
                dec = (turned * key_weight).astype(BF16)
                key_dec[at, own] = dec
                local[head, s] = times_rows(dec, value_low[at, own]).astype(BF16)

        for b_static in range(1, width):

            @pl.when(b == b_static)
            def _(b_static=b_static):
                exchange.to_peer(b_static).start()

    for s in range(1, seqs):
        cross(s).start()
    fetch(2).start()
    pass_on(0)
    loads[0].wait()
    loads[1].wait()

    def inner(spot):
        columns = pl.ds(pl.multiple_of(spot * tile, tile), tile)
        query_pre[:, columns] = times(normed_one[...], w_query[:, columns])
        gate[:, columns] = times(normed_one[...], w_gate[:, columns])
        for k in range(per_tile):
            head = spot * per_tile + k
            own = pl.ds(pl.multiple_of(spot * tile + k * dim, dim), dim)
            query_weight, _ = decays(rates, head, length, dim)
            mask = lag_decay(rates, head, length)
            for s in range(seqs):
                at = pl.ds(s * length, length)
                turned = turn(jax.nn.silu(query_pre[at, own]), cosine[...], sine_part[...])
                low_query = turned.astype(BF16)
                query_low[at, own] = low_query
                query_dec[at, own] = (turned * query_weight).astype(BF16)
                low_scores = (times_back(low_query, key_low[at, own]) * mask).astype(BF16)
                scores_low[head, s] = low_scores
                attended[at, own] = times(low_scores, value_low[at, own])

    half = width // 2

    @pl.loop(0, half)
    def _(spot):
        inner(spot)

    exchange.gather()
    pass_on(1)

    @pl.loop(half, width)
    def _(spot):
        inner(spot)

    exchange.send_back(entering)
    pass_last(0)
    pass_on(2)
    loads[2].wait()
    exchange.arrive()
    pass_last(1)

    @pl.loop(0, width * per_tile)
    def _(head):
        own = pl.ds(pl.multiple_of(head * dim, dim), dim)
        for s in range(seqs):
            at = pl.ds(s * length, length)
            attended[at, own] += times(query_dec[at, own], states[head, s])

    for s in range(seqs):
        at = pl.ds(s * length, length)
        value = attended[at]
        gated[at] = (value * lax.rsqrt(square_mean(value) + EPS) * gate[at]).astype(BF16)

    @pl.loop(0, width)
    def _(spot):
        columns = pl.ds(pl.multiple_of(spot * tile, tile), tile)
        residual[:, columns] = x[:, columns].astype(F32) + times(
            gated[...], w_output[:, columns]
        )

    for s in range(seqs):
        at = pl.ds(s * length, length)
        value = residual[at]
        normed_two[at] = (value * lax.rsqrt(square_mean(value) + EPS)).astype(BF16)
    pass_last(2)
    exchange.settle()
    for m in range(3):
        fetch(m).wait_send()
        relay(m).wait_send()
        share(m, 0).wait()
        share(m, 1).wait()
    for s in range(seqs):
        cross(s).wait()


def attend(x, weights, shard, grads, rates, powers, cosine, sine_part, seqs, depth, width):
    rows, model = x.shape
    heads = rates.shape[0]
    dim = model // heads
    length = rows // seqs
    vmem = pl.BlockSpec(memory_space=pltpu.VMEM)
    anywhere = pl.BlockSpec(memory_space=pl.ANY)
    wide = jax.ShapeDtypeStruct((rows, model), F32)
    low = jax.ShapeDtypeStruct((rows, model), BF16)
    w_query, w_key, w_value, w_gate, w_output = weights
    return pl.pallas_call(
        functools.partial(attend_kernel, depth, width, seqs),
        out_shape=(wide, low, wide, wide, wide, wide)
        + (low,) * 6
        + (
            jax.ShapeDtypeStruct((heads, seqs, length, length), BF16),
            low,
            jax.ShapeDtypeStruct((heads, seqs, dim, dim), BF16),
            jax.ShapeDtypeStruct((3,) + shard[0].shape, BF16),
            low,
        ),
        in_specs=[vmem] * 3 + [anywhere] * 7 + [vmem] * 4,
        out_specs=(vmem,) * 15 + (anywhere,) * 2,
        scratch_shapes=[pltpu.VMEM((model, model), BF16)] * 3
        + state_scratch(heads, seqs, dim, width, depth)
        + [pltpu.SemaphoreType.DMA((3,)), pltpu.SemaphoreType.DMA((2, 12 + seqs))],
        compiler_params=pltpu.CompilerParams(
            collective_id=2, has_side_effects=True, vmem_limit_bytes=56 * 1024 * 1024
        ),
        name="attend",
    )(
        x,
        w_key,
        w_value,
        w_query,
        w_gate,
        w_output,
        *shard,
        grads,
        rates,
        powers,
        cosine,
        sine_part,
    )


def retreat_kernel(
    depth,
    width,
    seqs,
    residual,
    back_own,
    back_in,
    grads,
    w_output,
    attended,
    gate,
    rates,
    powers,
    cosine,
    sine_part,
    mixed_nb,
    half_nb,
    *rest,
):
    late = rest[:14]
    (
        grad_mid_low,
        gate_low,
        query_out,
        key_out,
        value_out,
        grad_tokens,
        mixed_in,
        from_y,
    ) = rest[14:22]
    held = rest[22:36]
    (
        query_low,
        key_low,
        value_low,
        query_dec,
        scores_low,
        states_in,
        query_pre,
        w_query,
        w_gate,
        key_dec,
        key_pre,
        w_key,
        w_value,
        x,
    ) = held
    (
        states,
        grad_mid,
        work,
        grad_att,
        value_part,
        key_part,
        local,
        came,
        total,
        far,
        outs,
        entering,
        sems,
        load_sem,
        bulk_sems,
    ) = rest[36:]
    rows, model = residual.shape
    length = rows // seqs
    dim = cosine.shape[1]
    tile = model // width
    per_tile = tile // dim
    loads = [
        pltpu.make_async_copy(a, b, load_sem.at[i]) for i, (a, b) in enumerate(zip(late, held))
    ]
    for load in loads:
        load.start()
    exchange = States(
        depth, width, True, powers, local, came, total, far, outs, states, sems
    )

    def send(source, target, at, peer):
        return pltpu.make_async_remote_copy(
            src_ref=source,
            dst_ref=target,
            send_sem=bulk_sems.at[0, at],
            recv_sem=bulk_sems.at[1, at],
            device_id=peer,
            device_id_type=MESH,
        )

    def cross(s):
        at = pl.ds(s * length, length)
        return send(mixed_nb.at[at], mixed_in.at[at], s, {"tensor": exchange.slot ^ 1})

    def hand(m):
        return send(half_nb.at[m], from_y.at[m], seqs + m, {"tensor": exchange.slot ^ 2})

    exchange.greet()
    cross(0).start()
    hand(0).start()

    def spans():
        return [pl.ds(s * length, length) for s in range(seqs)]

    for at in spans():
        value = residual[at]
        scale = lax.rsqrt(square_mean(value) + EPS)
        normed = value * scale
        grad = back_own[at] + back_in[at].astype(F32)
        grad = grads[at].astype(F32) + scale * (
            grad - normed * jnp.mean(grad * normed, axis=-1, keepdims=True)
        )
        grad_mid[at] = grad
        grad_mid_low[at] = grad.astype(BF16)

    def columns_of(spot):
        return pl.ds(pl.multiple_of(spot * tile, tile), tile)

    @pl.loop(0, width)
    def _(spot):
        work[:, columns_of(spot)] = times_back(grad_mid_low[...], w_output[columns_of(spot)])

    for at in spans():
        value = attended[at]
        scale = lax.rsqrt(square_mean(value) + EPS)
        normed = value * scale
        grad = work[at]
        gate_low[at] = (grad * normed).astype(BF16)
        grad = grad * gate[at]
        grad_att[at] = (
            scale * (grad - normed * jnp.mean(grad * normed, axis=-1, keepdims=True))
        ).astype(BF16)

    for load in loads[:7]:
        load.wait()

    @pl.loop(1, width + 1)
    def _(step):
        b = lax.rem(step, width)
        spot = exchange.slot ^ b
        for k in range(per_tile):
            own = pl.ds(pl.multiple_of(spot * tile + k * dim, dim), dim)
            for s, at in enumerate(spans()):
                local[spot * per_tile + k, s] = times_rows(
                    query_dec[at, own], grad_att[at, own]
                ).astype(BF16)

        for b_static in range(1, width):

            @pl.when(b == b_static)
            def _(b_static=b_static):
                exchange.to_peer(b_static).start()

    for s in range(1, seqs):
        cross(s).start()
    hand(1).start()

    def slope(values):
        sigmoid_v = jax.nn.sigmoid(values)
        return sigmoid_v * (1.0 + values * (1.0 - sigmoid_v))

    def inner(spot):
        for k in range(per_tile):
            head = spot * per_tile + k
            own = pl.ds(pl.multiple_of(spot * tile + k * dim, dim), dim)
            query_weight, _ = decays(rates, head, length, dim)
            mask = lag_decay(rates, head, length)
            for s, at in enumerate(spans()):
                grad = grad_att[at, own]
                value_part[at, own] = times_rows(scores_low[head, s], grad)
                score = (times_back(grad, value_low[at, own]) * mask).astype(BF16)
                key_part[at, own] = times_rows(score, query_low[at, own])
                turned = times(score, key_low[at, own]) + query_weight * times_back(
                    grad, states_in[head, s]
                )
                query_out[at, own] = (
                    turn(turned, cosine[...], -sine_part[...]) * slope(query_pre[at, own])
                ).astype(BF16)

    half = width // 2

    @pl.loop(0, half)
    def _(spot):
        inner(spot)

    exchange.gather()

    @pl.loop(half, width)
    def _(spot):
        inner(spot)

    exchange.send_back(entering)
    hand(2).start()
    for load in loads[7:]:
        load.wait()

    @pl.loop(0, width)
    def _(spot):
        at = columns_of(spot)
        work[:, at] = times_back(query_out[...], w_query[at]) + times_back(
            gate_low[...], w_gate[at]
        )

    exchange.arrive()

    @pl.loop(0, width * per_tile)
    def _(head):
        own = pl.ds(pl.multiple_of(head * dim, dim), dim)
        _, key_weight = decays(rates, head, length, dim)
        for s, at in enumerate(spans()):
            state = states[head, s]
            value_out[at, own] = (
                value_part[at, own] + times(key_dec[at, own], state)
            ).astype(BF16)
            turned = key_part[at, own] + key_weight * times_back(value_low[at, own], state)
            key_out[at, own] = (
                turn(turned, cosine[...], -sine_part[...]) * slope(key_pre[at, own])
            ).astype(BF16)

    @pl.loop(0, width)
    def _(spot):
        at = columns_of(spot)
        work[:, at] += times_back(key_out[...], w_key[at]) + times_back(
            value_out[...], w_value[at]
        )

    for at in spans():
        value = x[at].astype(F32)
        scale = lax.rsqrt(square_mean(value) + EPS)
        normed = value * scale
        grad = work[at]
        grad_tokens[at] = grad_mid[at] + scale * (
            grad - normed * jnp.mean(grad * normed, axis=-1, keepdims=True)
        )
    exchange.settle()
    for s in range(seqs):
        cross(s).wait()
    for m in range(3):
        hand(m).wait()


def retreat(early, tables, bulk, late, seqs, depth, width):
    rows, model = early[0].shape
    heads = tables[0].shape[0]
    dim = model // heads
    vmem = pl.BlockSpec(memory_space=pltpu.VMEM)
    anywhere = pl.BlockSpec(memory_space=pl.ANY)
    wide = jax.ShapeDtypeStruct((rows, model), F32)
    low = jax.ShapeDtypeStruct((rows, model), BF16)
    return pl.pallas_call(
        functools.partial(retreat_kernel, depth, width, seqs),
        out_shape=(low,) * 5 + (wide, low, jax.ShapeDtypeStruct(bulk[1].shape, BF16)),
        in_specs=[vmem] * (len(early) + len(tables)) + [anywhere] * (len(bulk) + len(late)),
        out_specs=(vmem,) * 6 + (anywhere,) * 2,
        scratch_shapes=[pltpu.VMEM(v.shape, v.dtype) for v in late]
        + [
            pltpu.VMEM((heads, seqs, dim, dim), BF16),
            pltpu.VMEM((rows, model), F32),
            pltpu.VMEM((rows, model), F32),
            pltpu.VMEM((rows, model), BF16),
            pltpu.VMEM((rows, model), F32),
            pltpu.VMEM((rows, model), F32),
        ]
        + state_scratch(heads, seqs, dim, width, depth)
        + [pltpu.SemaphoreType.DMA((len(late),)), pltpu.SemaphoreType.DMA((2, seqs + 3))],
        compiler_params=pltpu.CompilerParams(
            collective_id=3, has_side_effects=True, vmem_limit_bytes=60 * 1024 * 1024
        ),
        name="retreat",
    )(*early, *tables, *bulk, *late)


def on_device(
    tokens,
    w_query,
    w_key,
    w_value,
    w_ugate,
    w_output,
    w_left,
    w_right,
    w_down,
    decay_rate,
    cotangent,
):
    seq_count, group_len, model_width = tokens.shape
    head_count = decay_rate.shape[0]
    head_dim = model_width // head_count
    half_dim = head_dim // 2
    row_count = seq_count * group_len

    shard = (w_left.T, w_right.T, w_down)
    grad_own = cotangent.reshape(row_count, model_width)

    position_block = lax.axis_index(("seq", "tensor"))
    places = (position_block * group_len + jnp.arange(group_len)).astype(F32)
    frequency = 10000.0 ** (-jnp.arange(half_dim, dtype=F32) / half_dim)
    angles = places[:, None] * frequency[None, :]
    cosine, sine_part = jnp.cos(angles), jnp.sin(angles)
    cosine = jnp.concatenate([cosine, cosine], axis=1)
    sine_part = jnp.concatenate([-sine_part, sine_part], axis=1)
    rows_in = tokens.reshape(row_count, model_width)
    depth = lax.axis_size("seq")
    width = lax.axis_size("tensor")
    rates = jnp.broadcast_to(decay_rate[:, None, None], (head_count, 1, group_len))
    blocks = jnp.arange(depth * width, dtype=F32)[:, None, None, None]
    powers = jnp.broadcast_to(
        jnp.exp(-decay_rate[None, :, None, None] * group_len * blocks),
        (depth * width, head_count, 1, head_dim),
    )
    (
        residual,
        rows_own,
        merged,
        query_pre,
        key_pre,
        ugate,
        normed_low,
        query_low,
        key_low,
        value_low,
        query_dec,
        key_dec,
        weights_low,
        gated_low,
        state_low,
        other,
        grad_nb,
    ) = attend(
        rows_in,
        (w_query, w_key, w_value, w_ugate, w_output),
        shard,
        grad_own,
        rates,
        powers,
        cosine,
        sine_part,
        seq_count,
        depth,
        width,
    )
    rows_nb = swap(rows_own, "tensor", 1)

    mixed_own, back_own, kept = hidden_part(rows_own, grad_own, shard + (other,), None, F32)
    mixed_nb, back_nb, kept = hidden_part(rows_nb, grad_nb, shard + (other,), kept, BF16)
    back_in = swap(back_nb, "tensor", 1)
    mine, theirs = hidden_grads(kept[1], rows_own, rows_nb, grad_own, grad_nb)
    moved = swap(theirs, "dp", 1)
    half_nb = added(mine, moved)
    mine, theirs = hidden_grads(kept[0], rows_own, rows_nb, grad_own, grad_nb)
    moved = swap(theirs, "dp", 1)

    (
        grad_branch,
        grad_ugate_pre,
        grad_query_pre,
        grad_key_pre,
        grad_value_pre,
        grad_tokens,
        mixed_in,
        from_y,
    ) = retreat(
        (residual, back_own, back_in, grad_own, w_output, merged, ugate),
        (rates, powers, cosine, sine_part),
        (mixed_nb, half_nb),
        (
            query_low,
            key_low,
            value_low,
            query_dec,
            weights_low,
            state_low,
            query_pre,
            w_query,
            w_ugate,
            key_dec,
            key_pre,
            w_key,
            w_value,
            rows_in,
        ),
        seq_count,
        depth,
        width,
    )

    def weight_grad(rows, gradient):
        return jnp.einsum("rd,re->de", rows, gradient, preferred_element_type=F32)

    partial = (
        weight_grad(normed_low, grad_query_pre),
        weight_grad(normed_low, grad_key_pre),
        weight_grad(normed_low, grad_value_pre),
        weight_grad(normed_low, grad_ugate_pre),
        weight_grad(gated_low, grad_branch),
    )
    shard_half = (mine.astype(F32) + moved.astype(F32) + from_y.astype(F32)).astype(BF16)
    hidden = w_down.shape[0]
    sums, hidden_sums = reduce_grads(
        tuple(g.astype(BF16) for g in partial),
        shard_half.reshape(3 * hidden, model_width // 2),
        lax.axis_size("seq"),
    )
    mixed_out = (residual + mixed_own + mixed_in.astype(F32)).astype(BF16)
    attention_grads = tuple(
        sums[i * model_width : (i + 1) * model_width].astype(F32) for i in range(len(partial))
    )
    left_sum, right_sum, down_sum = (
        hidden_sums[i * hidden : (i + 1) * hidden].astype(F32) for i in range(3)
    )
    return (
        (mixed_out.reshape(tokens.shape), grad_tokens.reshape(tokens.shape))
        + attention_grads
        + (left_sum.T, right_sum.T, down_sum)
    )


def solution(mesh):
    rows = P("dp", ("seq", "tensor"), None)
    columns = P(None, "tensor")
    return jax.shard_map(
        on_device,
        mesh=mesh,
        in_specs=(rows, P(), P(), P(), P(), P(), columns, columns, P("tensor", None), P(), rows),
        out_specs=(rows, rows, P(), P(), P(), P(), P(), columns, columns, P("tensor", None)),
        check_vma=False,
    )
```

```python
import functools

import jax
import jax.numpy as jnp
from jax import lax
from jax.experimental import pallas as pl
from jax.experimental.pallas import tpu as pltpu
from jax.sharding import PartitionSpec as P


EPS = 1e-06
F32 = jnp.float32
BF16 = jnp.bfloat16


CHUNK = 256
LAG = 1


def added(first, second):
    return (first.astype(F32) + second.astype(F32)).astype(BF16)


def reduce_kernel(
    depth,
    grads,
    pair_own,
    pair_first,
    pair_rest,
    out,
    pair_out,
    pair_in,
    own,
    core_in,
    first_in,
    second_in,
    line_in,
    line_mid,
    pair_line,
    pair_mid,
    sems,
    pair_sems,
    load_sem,
):
    core = lax.axis_index("dp")
    slot = lax.axis_index("tensor")
    place = lax.axis_index("seq")
    rows = own.shape[0]
    chunks = rows // CHUNK
    half, quarter, eighth = CHUNK // 2, CHUNK // 4, CHUNK // 8
    low_side = place < depth // 2
    outermost = (place == 0) | (place == depth - 1)
    middle = (place == depth // 2 - 1) | (place == depth // 2)
    inward = jnp.where(low_side, place + 1, place - 1)
    outward = jnp.where(low_side, place - 1, place + 1)

    barrier = pltpu.get_barrier_semaphore()

    def greet(peer):
        pl.semaphore_signal(
            barrier, inc=1, device_id=peer, device_id_type=pl.DeviceIdType.MESH
        )

    greet({"dp": 1 - core})
    greet({"tensor": slot ^ 1})
    greet({"tensor": slot ^ 2})

    @pl.when(place > 0)
    def _():
        greet({"seq": place - 1})

    @pl.when(place < depth - 1)
    def _():
        greet({"seq": place + 1})

    pl.semaphore_wait(barrier, jnp.where(outermost, 4, 5))

    def remote(source, target, sem, at, peer):
        return pltpu.make_async_remote_copy(
            src_ref=source,
            dst_ref=target,
            send_sem=sem.at[0, at],
            recv_sem=sem.at[1, at],
            device_id=peer,
            device_id_type=pl.DeviceIdType.MESH,
        )

    def span(start, size):
        return pl.ds(pl.multiple_of(start, size), size)

    def bits(q):
        first = jnp.where(q % 2 == 0, 1, 2)
        second = 3 - first
        return first, second, (slot & first) // first, (slot & second) // second

    def base(q):
        return pl.multiple_of(q * CHUNK, CHUNK)

    def to_core(q):
        return remote(
            own.at[span(base(q) + (1 - core) * half, half)],
            core_in.at[q],
            sems.at[0],
            q,
            {"dp": 1 - core},
        )

    def to_first(q):
        first, _, f, _ = bits(q)
        return remote(
            core_in.at[q, span((1 - f) * quarter, quarter)],
            first_in.at[q],
            sems.at[1],
            q,
            {"tensor": slot ^ first},
        )

    def to_second(q):
        _, second, _, g = bits(q)
        return remote(
            first_in.at[q, span((1 - g) * eighth, eighth)],
            second_in.at[q],
            sems.at[2],
            q,
            {"tensor": slot ^ second},
        )

    def block(q):
        _, _, f, g = bits(q)
        return base(q) + core * half + f * quarter + g * eighth

    def back_second(q):
        _, second, _, _ = bits(q)
        at = span(block(q), eighth)
        return remote(out.at[at], out.at[at], sems.at[3], q, {"tensor": slot ^ second})

    def back_first(q):
        first, _, f, _ = bits(q)
        at = span(base(q) + core * half + f * quarter, quarter)
        return remote(out.at[at], out.at[at], sems.at[4], q, {"tensor": slot ^ first})

    def back_core(q):
        at = span(base(q) + core * half, half)
        return remote(out.at[at], out.at[at], sems.at[5], q, {"dp": 1 - core})

    class Line:
        def __init__(self, mine, came, met, total, sem, offset):
            self.mine, self.came, self.met, self.total = mine, came, met, total
            self.sem, self.offset = sem, offset

        def inwards(self, q, source):
            return remote(
                source, self.came(q), self.sem.at[self.offset], q, {"seq": inward}
            )

        def across(self, q):
            return remote(
                self.came(q),
                self.met(q),
                self.sem.at[self.offset + 1],
                q,
                {"seq": depth - 1 - place},
            )

        def outwards(self, q):
            return remote(
                self.total(q), self.total(q), self.sem.at[self.offset + 2], q, {"seq": outward}
            )

        def step_in(self, q):
            @pl.when(outermost)
            def _():
                self.inwards(q, self.mine(q)).start()

        def step_middle(self, q):
            @pl.when(jnp.logical_not(outermost))
            def _():
                self.inwards(q, self.mine(q)).wait_recv()
                came = self.came(q)
                came[...] = added(self.mine(q)[...], came[...])

                @pl.when(middle)
                def _():
                    self.across(q).start()

                @pl.when(jnp.logical_not(middle))
                def _():
                    self.inwards(q, came).start()

        def step_out(self, q):
            @pl.when(middle)
            def _():
                self.across(q).wait_recv()
                self.total(q)[...] = added(self.came(q)[...], self.met(q)[...])

            @pl.when(jnp.logical_not(outermost))
            def _():
                @pl.when(jnp.logical_not(middle))
                def _():
                    self.outwards(q).wait_recv()

                self.outwards(q).start()

        def step_last(self, q):
            @pl.when(outermost)
            def _():
                self.outwards(q).wait_recv()

        def settle(self, q):
            @pl.when(outermost)
            def _():
                self.inwards(q, self.mine(q)).wait_send()

            @pl.when(jnp.logical_not(outermost))
            def _():
                @pl.when(middle)
                def _():
                    self.across(q).wait_send()

                @pl.when(jnp.logical_not(middle))
                def _():
                    self.inwards(q, self.came(q)).wait_send()

                self.outwards(q).wait_send()

    def second_mine(q):
        return second_in.at[q]

    line = Line(
        second_mine,
        lambda q: line_in.at[q],
        lambda q: line_mid.at[q],
        lambda q: out.at[span(block(q), eighth)],
        sems,
        6,
    )
    pair_chunks, pair_rows, pair_cols = pair_line.shape
    pair = Line(
        lambda q: pair_in.at[span(q * pair_rows, pair_rows)],
        lambda q: pair_line.at[q],
        lambda q: pair_mid.at[q],
        lambda q: pair_out.at[span(q * pair_rows, pair_rows), span(core * pair_cols, pair_cols)],
        pair_sems,
        0,
    )

    def pair_core(q):
        return remote(pair.total(q), pair.total(q), pair_sems.at[3], q, {"dp": 1 - core})

    size = rows // len(grads)
    loads = [
        pltpu.make_async_copy(g, own.at[pl.ds(i * size, size)], load_sem.at[i])
        for i, g in enumerate(grads)
    ]
    for load in loads:
        load.start()
    per_load = size // CHUNK
    for i, load in enumerate(loads):
        load.wait()

        @pl.loop(i * per_load, (i + 1) * per_load)
        def _(q):
            to_core(q).start()

    hidden = pair_first.shape[0]
    for m in range(3):
        theirs = pair_first[...] if m == 0 else pair_rest[m - 1]
        pair_in[pl.ds(m * hidden, hidden)] = added(pair_own[m], theirs)

    def stage_a(q):
        to_core(q).wait_recv()
        came = core_in.at[q]
        came[...] = added(own[span(base(q) + core * half, half)], came[...])

    def stage_b(q):
        _, _, f, _ = bits(q)
        to_first(q).wait_recv()
        came = first_in.at[q]
        came[...] = added(core_in[q, span(f * quarter, quarter)], came[...])

    def stage_c(q):
        _, _, _, g = bits(q)
        to_second(q).wait_recv()
        came = second_in.at[q]
        came[...] = added(first_in[q, span(g * eighth, eighth)], came[...])

    pairs = chunks // 2

    def during(step, lag, count, action):
        i = step - lag

        @pl.when((i >= 0) & (i < count))
        def _():
            action(i)

    def both(action):
        def run(i):
            action(2 * i)
            action(2 * i + 1)

        return run

    def start(copy):
        return lambda q: copy(q).start()

    def arrived(copy, following):
        def run(q):
            copy(q).wait_recv()
            following(q).start()

        return run

    def last_then_second(q):
        line.step_last(q)
        back_second(q).start()

    def finish_pair(q):
        pair.step_last(q)
        pair_core(q).start()

    steps = max(pairs + 7 * LAG, pair_chunks + 3 * LAG) + 1

    @pl.loop(0, steps)
    def _(step):
        during(step, 7 * LAG, pairs, both(arrived(back_first, back_core)))
        during(step, 6 * LAG, pairs, both(arrived(back_second, back_first)))
        during(step, 5 * LAG, pairs, both(last_then_second))
        during(step, 4 * LAG, pairs, both(line.step_out))
        during(step, 3 * LAG, pairs, both(line.step_middle))
        during(step, 2 * LAG, pairs, both(stage_c))
        during(step, LAG, pairs, both(stage_b))
        during(step, 0, pairs, both(stage_a))
        during(step, 2 * LAG, pairs, both(line.step_in))
        during(step, LAG, pairs, both(start(to_second)))
        during(step, 0, pairs, both(start(to_first)))
        during(step, 3 * LAG, pair_chunks, finish_pair)
        during(step, 2 * LAG, pair_chunks, pair.step_out)
        during(step, LAG, pair_chunks, pair.step_middle)
        during(step, 0, pair_chunks, pair.step_in)

    @pl.loop(0, chunks)
    def _(q):
        back_core(q).wait_recv()
        for copy in (to_core, to_first, to_second, back_second, back_first, back_core):
            copy(q).wait_send()
        line.settle(q)

    @pl.loop(0, pair_chunks)
    def _(q):
        pair_core(q).wait()
        pair.settle(q)


def reduce_grads(grads, half_own, first_y, rest_y, depth):
    size, width = grads[0].shape
    rows = size * len(grads)
    chunks = rows // CHUNK
    pair_chunks = 12
    total_rows, pair_cols = 3 * half_own.shape[1], half_own.shape[2]
    pair_rows = total_rows // pair_chunks
    vmem = pl.BlockSpec(memory_space=pltpu.VMEM)

    def body(*refs):
        reduce_kernel(depth, refs[: len(grads)], *refs[len(grads) :])

    return pl.pallas_call(
        body,
        out_shape=(
            jax.ShapeDtypeStruct((rows, width), BF16),
            jax.ShapeDtypeStruct((total_rows, 2 * pair_cols), BF16),
        ),
        in_specs=[pl.BlockSpec(memory_space=pl.ANY)] * len(grads) + [vmem] * 3,
        out_specs=(vmem, vmem),
        scratch_shapes=[
            pltpu.VMEM((total_rows, pair_cols), BF16),
            pltpu.VMEM((rows, width), BF16),
            pltpu.VMEM((chunks, CHUNK // 2, width), BF16),
            pltpu.VMEM((chunks, CHUNK // 4, width), BF16),
            pltpu.VMEM((chunks, CHUNK // 8, width), BF16),
            pltpu.VMEM((chunks, CHUNK // 8, width), BF16),
            pltpu.VMEM((chunks, CHUNK // 8, width), BF16),
            pltpu.VMEM((pair_chunks, pair_rows, pair_cols), BF16),
            pltpu.VMEM((pair_chunks, pair_rows, pair_cols), BF16),
            pltpu.SemaphoreType.DMA((9, 2, chunks)),
            pltpu.SemaphoreType.DMA((4, 2, pair_chunks)),
            pltpu.SemaphoreType.DMA((len(grads),)),
        ],
        compiler_params=pltpu.CompilerParams(
            collective_id=1, has_side_effects=True, vmem_limit_bytes=50 * 1024 * 1024
        ),
        name="reduce_grads",
    )(*grads, half_own, first_y, rest_y)


ROWS = 256


def times(x, w):
    return jnp.dot(x, w, preferred_element_type=F32)


def times_back(x, w):
    return lax.dot_general(x, w, (((1,), (1,)), ((), ())), preferred_element_type=F32)


def times_rows(x, y):
    return lax.dot_general(x, y, (((0,), (0,)), ((), ())), preferred_element_type=F32)


def hidden_kernel(
    rows_own,
    grads_own,
    grads_nb,
    late_left,
    late_right,
    late_down,
    late_other,
    mixed,
    back,
    half_own,
    half_nb,
    back_in,
    from_y,
    both,
    own,
    other,
    kept,
    theirs,
    moved,
    acc_mixed,
    acc_back,
    load_sem,
    sems,
):
    core = lax.axis_index("dp")
    slot = lax.axis_index("tensor")
    count, width = rows_own.shape
    half = width // 2
    blocks = count // ROWS
    pairs = (
        (late_left, own.at[0]),
        (late_right, own.at[1]),
        (late_down, own.at[2]),
        (late_other, other),
        (rows_own, both.at[0, :count]),
        (grads_own, both.at[1, :count]),
        (grads_nb, both.at[1, count:]),
    )
    loads = [pltpu.make_async_copy(a, b, load_sem.at[i]) for i, (a, b) in enumerate(pairs)]
    for i in (4, 5, 0, 1, 2, 3, 6):
        loads[i].start()

    def send(source, target, at, peer):
        return pltpu.make_async_remote_copy(
            src_ref=source,
            dst_ref=target,
            send_sem=sems.at[0, at],
            recv_sem=sems.at[1, at],
            device_id=peer,
            device_id_type=MESH,
        )

    def span(i):
        return pl.ds(pl.multiple_of(i * ROWS, ROWS), ROWS)

    def out_rows(i):
        return send(
            rows_own.at[span(i)], both.at[0, span(blocks + i)], i, {"tensor": slot ^ 1}
        )

    def return_rows(i):
        return send(
            back.at[span(blocks + i)], back_in.at[span(i)], blocks + i, {"tensor": slot ^ 1}
        )

    def to_core(which, m):
        return send(
            theirs.at[which, m], moved.at[which, m], 2 * blocks + 3 * which + m, {"dp": 1 - core}
        )

    hand = send(half_nb.at[0], from_y, 2 * blocks + 6, {"tensor": slot ^ 2})
    barrier = pltpu.get_barrier_semaphore()
    for peer in ({"tensor": slot ^ 1}, {"tensor": slot ^ 2}, {"dp": 1 - core}):
        pl.semaphore_signal(barrier, inc=1, device_id=peer, device_id_type=MESH)
    pl.semaphore_wait(barrier, 3)
    for i in range(blocks):
        out_rows(i).start()
    for load in loads:
        load.wait()

    def unit(i, which, weights):
        rows, grads = both[0, span(i)], both[1, span(i)]
        e1, e2 = times_back(rows, weights[0]), times_back(rows, weights[1])
        dm = times_back(grads, weights[2])
        mid = (e1 * e2).astype(BF16)
        de1 = (dm * e2).astype(BF16)
        de2 = (dm * e1).astype(BF16)
        kept[which, 2, span(i)] = mid
        kept[which, 0, span(i)] = de1
        kept[which, 1, span(i)] = de2
        return times(mid, weights[2]), times(de1, weights[0]) + times(de2, weights[1])

    @pl.loop(0, 2 * blocks)
    def _(i):
        @pl.when(i >= blocks)
        def _():
            out_rows(i - blocks).wait_recv()

        acc_mixed[...], acc_back[...] = unit(i, 0, own)
        more_mixed, more_back = unit(i, 1, other)
        mixed[span(i)] = (acc_mixed[...] + more_mixed).astype(BF16)
        back[span(i)] = (acc_back[...] + more_back).astype(BF16)

        @pl.when(i >= blocks)
        def _():
            return_rows(i - blocks).start()

    here = pl.ds(pl.multiple_of(core * half, half), half)
    there = pl.ds(pl.multiple_of((1 - core) * half, half), half)
    for which, out in ((1, half_nb), (0, half_own)):

        @pl.loop(0, 3)
        def _(m, which=which, out=out):
            theirs[which, m] = times_rows(kept[which, m], both[m // 2, :, there]).astype(BF16)
            to_core(which, m).start()
            out[m] = times_rows(kept[which, m], both[m // 2, :, here]).astype(BF16)

        for m in range(3):
            to_core(which, m).wait_recv()
            out[m] = added(out[m], moved[which, m])
        if which == 1:
            hand.start()
    for i in range(blocks):
        out_rows(i).wait_send()
        return_rows(i).wait()
    for which in range(2):
        for m in range(3):
            to_core(which, m).wait_send()
    hand.wait()


def hidden_part(rows_own, grads_own, grads_nb, shard, other):
    count, width = rows_own.shape
    hidden = shard[0].shape[0]
    vmem = pl.BlockSpec(memory_space=pltpu.VMEM)
    anywhere = pl.BlockSpec(memory_space=pl.ANY)
    half = jax.ShapeDtypeStruct((3, hidden, width // 2), BF16)
    two = jax.ShapeDtypeStruct((2 * count, width), BF16)
    return pl.pallas_call(
        hidden_kernel,
        out_shape=(
            two,
            two,
            half,
            half,
            jax.ShapeDtypeStruct((count, width), BF16),
            jax.ShapeDtypeStruct((hidden, width // 2), BF16),
        ),
        in_specs=[anywhere] * 7,
        out_specs=(vmem,) * 4 + (anywhere,) * 2,
        scratch_shapes=[
            pltpu.VMEM((2, 2 * count, width), BF16),
            pltpu.VMEM((3, hidden, width), BF16),
            pltpu.VMEM((3, hidden, width), BF16),
            pltpu.VMEM((2, 3, 2 * count, hidden), BF16),
            pltpu.VMEM((2, 3, hidden, width // 2), BF16),
            pltpu.VMEM((2, 3, hidden, width // 2), BF16),
            pltpu.VMEM((ROWS, width), F32),
            pltpu.VMEM((ROWS, width), F32),
            pltpu.SemaphoreType.DMA((7,)),
            pltpu.SemaphoreType.DMA((2, 2 * (count // ROWS) + 7)),
        ],
        compiler_params=pltpu.CompilerParams(
            collective_id=4, has_side_effects=True, vmem_limit_bytes=54 * 1024 * 1024
        ),
        name="hidden_part",
    )(rows_own, grads_own, grads_nb, *shard, other)


MESH = pl.DeviceIdType.MESH


class States:
    def __init__(self, depth, width, backward, powers, local, came, total, far, outs, states, sems):
        self.depth, self.width, self.backward, self.powers = depth, width, backward, powers
        self.local, self.came, self.total, self.far = local, came, total, far
        self.outs, self.states, self.sems = outs, states, sems
        self.slot = lax.axis_index("tensor")
        self.place = lax.axis_index("seq")
        self.share = local.shape[0] // width

    def greet(self, more=()):
        barrier = pltpu.get_barrier_semaphore()
        for peer in more:
            pl.semaphore_signal(barrier, inc=1, device_id=peer, device_id_type=MESH)
        for b in range(1, self.width):
            pl.semaphore_signal(
                barrier, inc=1, device_id={"tensor": self.slot ^ b}, device_id_type=MESH
            )
        for j in range(1, self.depth):
            peer = lax.rem(self.place + j, self.depth)
            pl.semaphore_signal(barrier, inc=1, device_id={"seq": peer}, device_id_type=MESH)
        pl.semaphore_wait(barrier, self.width + self.depth - 2 + len(more))

    def copy(self, source, target, at, peer):
        return pltpu.make_async_remote_copy(
            src_ref=source,
            dst_ref=target,
            send_sem=self.sems.at[0, at],
            recv_sem=self.sems.at[1, at],
            device_id=peer,
            device_id_type=MESH,
        )

    def group(self, slot):
        return pl.ds(slot * self.share, self.share)

    def to_peer(self, b):
        peer = self.slot ^ b
        return self.copy(
            self.local.at[self.group(peer)], self.came.at[b - 1], b - 1, {"tensor": peer}
        )

    def to_far(self, j):
        peer = self.place - j if self.backward else self.place + j
        return self.copy(self.total, self.far.at[j - 1], self.width + j - 2, {"seq": peer})

    def has_far(self, j):
        return self.place >= j if self.backward else self.place + j < self.depth

    def from_far(self, j):
        return self.place + j < self.depth if self.backward else self.place >= j

    def to_owner(self, d):
        at = self.width + self.depth - 2 + d - 1
        return self.copy(
            self.outs.at[d - 1],
            self.states.at[self.group(self.slot)],
            at,
            {"tensor": self.slot ^ d},
        )

    def power(self, count, head):
        return self.powers[count, head]

    def piece(self, b, k, s):
        if b == 0:
            return self.local[self.slot * self.share + k, s].astype(F32)
        return self.came[b - 1, k, s].astype(F32)

    def gather(self):
        for b in range(1, self.width):
            self.to_peer(b).wait_recv()
        for k in range(self.share):
            head = self.slot * self.share + k
            for s in range(self.local.shape[1]):
                value = 0.0
                for b in range(self.width):
                    spot = self.slot ^ b
                    left = spot if self.backward else self.width - 1 - spot
                    value = value + self.power(left, head) * self.piece(b, k, s)
                self.total[k, s] = value.astype(BF16)
        for j in range(1, self.depth):

            @pl.when(self.has_far(j))
            def _(j=j):
                self.to_far(j).start()

    def send_back(self, entering):
        for j in range(1, self.depth):

            @pl.when(self.from_far(j))
            def _(j=j):
                self.to_far(j).wait_recv()

            @pl.when(jnp.logical_not(self.from_far(j)))
            def _(j=j):
                self.far[j - 1] = jnp.zeros(self.far.shape[1:], BF16)

        for k in range(self.share):
            head = self.slot * self.share + k
            for s in range(self.local.shape[1]):
                value = 0.0
                for j in range(1, self.depth):
                    value = value + self.power(self.width * (j - 1), head) * self.far[
                        j - 1, k, s
                    ].astype(F32)
                entering[k, s] = value
        for d in list(range(1, self.width)) + [0]:
            target = self.slot ^ d
            inner = self.width - 1 - target if self.backward else target
            for k in range(self.share):
                head = self.slot * self.share + k
                for s in range(self.local.shape[1]):
                    value = self.power(inner, head) * entering[k, s]
                    for b in range(self.width):
                        if b == d:
                            continue
                        source = self.slot ^ b
                        gap = source - target - 1 if self.backward else target - source - 1
                        coef = jnp.where(gap >= 0, self.power(jnp.maximum(gap, 0), head), 0.0)
                        value = value + coef * self.piece(b, k, s)
                    if d == 0:
                        self.states[head, s] = value.astype(BF16)
                    else:
                        self.outs[d - 1, k, s] = value.astype(BF16)
        for d in range(1, self.width):
            self.to_owner(d).start()

    def arrive(self):
        for d in range(1, self.width):
            at = self.width + self.depth - 2 + d - 1
            self.copy(
                self.outs.at[d - 1],
                self.states.at[self.group(self.slot ^ d)],
                at,
                {"tensor": self.slot ^ d},
            ).wait_recv()

    def settle(self):
        for b in range(1, self.width):
            self.to_peer(b).wait_send()
            self.to_owner(b).wait_send()
        for j in range(1, self.depth):

            @pl.when(self.has_far(j))
            def _(j=j):
                self.to_far(j).wait_send()


def state_scratch(heads, seqs, head_dim, width, depth):
    share = heads // width
    low = functools.partial(pltpu.VMEM, dtype=BF16)
    return [
        low((heads, seqs, head_dim, head_dim)),
        low((width - 1, share, seqs, head_dim, head_dim)),
        low((share, seqs, head_dim, head_dim)),
        low((depth - 1, share, seqs, head_dim, head_dim)),
        low((width - 1, share, seqs, head_dim, head_dim)),
        pltpu.VMEM((share, seqs, head_dim, head_dim), F32),
        pltpu.SemaphoreType.DMA((2, 2 * (width - 1) + depth - 1)),
    ]


def turn(values, cosine, sine_part):
    return values * cosine + pltpu.roll(values, values.shape[-1] // 2, 1) * sine_part


def square_mean(values):
    return jnp.mean(values * values, axis=-1, keepdims=True)


def decays(rates, head, length, dim):
    rate = rates[head]
    place = lax.broadcasted_iota(jnp.int32, (length, dim), 0).astype(F32)
    query = jnp.exp(-rate[:, :dim] * (place + 1.0))
    key = jnp.exp(-rate[:, :dim] * (length - 1.0 - place))
    return query, key


def lag_decay(rates, head, length):
    lag = (
        lax.broadcasted_iota(jnp.int32, (length, length), 0)
        - lax.broadcasted_iota(jnp.int32, (length, length), 1)
    ).astype(F32)
    return jnp.where(lag >= 0, jnp.exp(-rates[head] * jnp.maximum(lag, 0.0)), 0.0)


def attend_kernel(
    depth,
    width,
    seqs,
    x,
    w_key,
    w_value,
    late_query,
    late_gate,
    late_output,
    left,
    right,
    down,
    grads,
    rates,
    powers,
    cosine,
    sine_part,
    residual,
    normed_two,
    attended,
    query_pre,
    key_pre,
    gate,
    normed_one,
    query_low,
    key_low,
    value_low,
    query_dec,
    key_dec,
    scores_low,
    gated,
    states,
    other,
    grads_nb,
    w_query,
    w_gate,
    w_output,
    local,
    came,
    total,
    far,
    outs,
    entering,
    sems,
    load_sem,
    bulk_sems,
):
    rows, model = x.shape
    length = rows // seqs
    dim = cosine.shape[1]
    tile = model // width
    loads = [
        pltpu.make_async_copy(a, b, load_sem.at[i])
        for i, (a, b) in enumerate(
            ((late_query, w_query), (late_gate, w_gate), (late_output, w_output))
        )
    ]
    for load in loads:
        load.start()
    exchange = States(
        depth, width, False, powers, local, came, total, far, outs, states, sems
    )
    core = lax.axis_index("dp")
    parity = lax.rem(exchange.place, 2)
    shard = (left, right, down)
    part_rows, part_cols = left.shape[0] // 2, model // 2
    columns_here = pl.ds(pl.multiple_of(core * part_cols, part_cols), part_cols)

    def rows_of(which):
        return pl.ds(pl.multiple_of(which * part_rows, part_rows), part_rows)

    def send(source, target, at, peer):
        return pltpu.make_async_remote_copy(
            src_ref=source,
            dst_ref=target,
            send_sem=bulk_sems.at[0, at],
            recv_sem=bulk_sems.at[1, at],
            device_id=peer,
            device_id_type=MESH,
        )

    def fetch(m):
        at = (rows_of(parity), columns_here)
        return send(
            shard[m].at[at], other.at[(m,) + at], m, {"tensor": exchange.slot ^ 2}
        )

    def relay(m):
        at = other.at[m, rows_of(parity), columns_here]
        return send(at, at, 3 + m, {"seq": exchange.place + 1 - 2 * parity})

    def share(m, which):
        spot = parity if which == 0 else 1 - parity
        at = other.at[m, rows_of(spot), columns_here]
        return send(at, at, 6 + 2 * m + which, {"dp": 1 - core})

    def cross(s):
        at = pl.ds(s * length, length)
        return send(grads.at[at], grads_nb.at[at], 12 + s, {"tensor": exchange.slot ^ 1})

    def pass_on(m):
        fetch(m).wait_recv()
        relay(m).start()
        share(m, 0).start()

    def pass_last(m):
        relay(m).wait_recv()
        share(m, 1).start()

    exchange.greet((({"dp": 1 - core}),))
    fetch(0).start()
    cross(0).start()
    fetch(1).start()
    for s in range(seqs):
        at = pl.ds(s * length, length)
        value = x[at].astype(F32)
        normed_one[at] = (value * lax.rsqrt(square_mean(value) + EPS)).astype(BF16)

    per_tile = tile // dim

    @pl.loop(1, width + 1)
    def _(step):
        b = lax.rem(step, width)
        spot = exchange.slot ^ b
        columns = pl.ds(pl.multiple_of(spot * tile, tile), tile)
        key_pre[:, columns] = times(normed_one[...], w_key[:, columns])
        value_low[:, columns] = times(normed_one[...], w_value[:, columns]).astype(BF16)
        for k in range(per_tile):
            head = spot * per_tile + k
            own = pl.ds(pl.multiple_of(spot * tile + k * dim, dim), dim)
            _, key_weight = decays(rates, head, length, dim)
            for s in range(seqs):
                at = pl.ds(s * length, length)
                turned = turn(jax.nn.silu(key_pre[at, own]), cosine[...], sine_part[...])
                key_low[at, own] = turned.astype(BF16)
                dec = (turned * key_weight).astype(BF16)
                key_dec[at, own] = dec
                local[head, s] = times_rows(dec, value_low[at, own]).astype(BF16)

        for b_static in range(1, width):

            @pl.when(b == b_static)
            def _(b_static=b_static):
                exchange.to_peer(b_static).start()

    for s in range(1, seqs):
        cross(s).start()
    fetch(2).start()
    pass_on(0)
    loads[0].wait()
    loads[1].wait()

    def inner(spot):
        columns = pl.ds(pl.multiple_of(spot * tile, tile), tile)
        query_pre[:, columns] = times(normed_one[...], w_query[:, columns])
        gate[:, columns] = times(normed_one[...], w_gate[:, columns])
        for k in range(per_tile):
            head = spot * per_tile + k
            own = pl.ds(pl.multiple_of(spot * tile + k * dim, dim), dim)
            query_weight, _ = decays(rates, head, length, dim)
            mask = lag_decay(rates, head, length)
            for s in range(seqs):
                at = pl.ds(s * length, length)
                turned = turn(jax.nn.silu(query_pre[at, own]), cosine[...], sine_part[...])
                low_query = turned.astype(BF16)
                query_low[at, own] = low_query
                query_dec[at, own] = (turned * query_weight).astype(BF16)
                low_scores = (times_back(low_query, key_low[at, own]) * mask).astype(BF16)
                scores_low[head, s] = low_scores
                attended[at, own] = times(low_scores, value_low[at, own])

    half = width // 2

    @pl.loop(0, half)
    def _(spot):
        inner(spot)

    exchange.gather()
    pass_on(1)

    @pl.loop(half, width)
    def _(spot):
        inner(spot)

    exchange.send_back(entering)
    pass_last(0)
    pass_on(2)
    loads[2].wait()
    exchange.arrive()
    pass_last(1)

    @pl.loop(0, width * per_tile)
    def _(head):
        own = pl.ds(pl.multiple_of(head * dim, dim), dim)
        for s in range(seqs):
            at = pl.ds(s * length, length)
            attended[at, own] += times(query_dec[at, own], states[head, s])

    for s in range(seqs):
        at = pl.ds(s * length, length)
        value = attended[at]
        gated[at] = (value * lax.rsqrt(square_mean(value) + EPS) * gate[at]).astype(BF16)

    @pl.loop(0, width)
    def _(spot):
        columns = pl.ds(pl.multiple_of(spot * tile, tile), tile)
        residual[:, columns] = x[:, columns].astype(F32) + times(
            gated[...], w_output[:, columns]
        )

    for s in range(seqs):
        at = pl.ds(s * length, length)
        value = residual[at]
        normed_two[at] = (value * lax.rsqrt(square_mean(value) + EPS)).astype(BF16)
    pass_last(2)
    exchange.settle()
    for m in range(3):
        fetch(m).wait_send()
        relay(m).wait_send()
        share(m, 0).wait()
        share(m, 1).wait()
    for s in range(seqs):
        cross(s).wait()


def attend(x, weights, shard, grads, rates, powers, cosine, sine_part, seqs, depth, width):
    rows, model = x.shape
    heads = rates.shape[0]
    dim = model // heads
    length = rows // seqs
    vmem = pl.BlockSpec(memory_space=pltpu.VMEM)
    anywhere = pl.BlockSpec(memory_space=pl.ANY)
    wide = jax.ShapeDtypeStruct((rows, model), F32)
    low = jax.ShapeDtypeStruct((rows, model), BF16)
    w_query, w_key, w_value, w_gate, w_output = weights
    return pl.pallas_call(
        functools.partial(attend_kernel, depth, width, seqs),
        out_shape=(wide, low, wide, wide, wide, wide)
        + (low,) * 6
        + (
            jax.ShapeDtypeStruct((heads, seqs, length, length), BF16),
            low,
            jax.ShapeDtypeStruct((heads, seqs, dim, dim), BF16),
            jax.ShapeDtypeStruct((3,) + shard[0].shape, BF16),
            low,
        ),
        in_specs=[vmem] * 3 + [anywhere] * 7 + [vmem] * 4,
        out_specs=(vmem,) * 15 + (anywhere,) * 2,
        scratch_shapes=[pltpu.VMEM((model, model), BF16)] * 3
        + state_scratch(heads, seqs, dim, width, depth)
        + [pltpu.SemaphoreType.DMA((3,)), pltpu.SemaphoreType.DMA((2, 12 + seqs))],
        compiler_params=pltpu.CompilerParams(
            collective_id=2, has_side_effects=True, vmem_limit_bytes=56 * 1024 * 1024
        ),
        name="attend",
    )(
        x,
        w_key,
        w_value,
        w_query,
        w_gate,
        w_output,
        *shard,
        grads,
        rates,
        powers,
        cosine,
        sine_part,
    )


def retreat_kernel(
    depth,
    width,
    seqs,
    residual,
    back_own,
    back_in,
    grads,
    w_output,
    attended,
    gate,
    rates,
    powers,
    cosine,
    sine_part,
    mixed_nb,
    half_nb,
    *rest,
):
    late = rest[:14]
    (
        grad_mid_low,
        gate_low,
        query_out,
        key_out,
        value_out,
        grad_tokens,
        mixed_in,
        from_y,
    ) = rest[14:22]
    held = rest[22:36]
    (
        query_low,
        key_low,
        value_low,
        query_dec,
        scores_low,
        states_in,
        query_pre,
        w_query,
        w_gate,
        key_dec,
        key_pre,
        w_key,
        w_value,
        x,
    ) = held
    (
        states,
        grad_mid,
        work,
        grad_att,
        value_part,
        key_part,
        local,
        came,
        total,
        far,
        outs,
        entering,
        sems,
        load_sem,
        bulk_sems,
    ) = rest[36:]
    rows, model = residual.shape
    length = rows // seqs
    dim = cosine.shape[1]
    tile = model // width
    per_tile = tile // dim
    loads = [
        pltpu.make_async_copy(a, b, load_sem.at[i]) for i, (a, b) in enumerate(zip(late, held))
    ]
    for load in loads:
        load.start()
    exchange = States(
        depth, width, True, powers, local, came, total, far, outs, states, sems
    )

    def send(source, target, at, peer):
        return pltpu.make_async_remote_copy(
            src_ref=source,
            dst_ref=target,
            send_sem=bulk_sems.at[0, at],
            recv_sem=bulk_sems.at[1, at],
            device_id=peer,
            device_id_type=MESH,
        )

    def cross(s):
        at = pl.ds(s * length, length)
        source = mixed_nb.at[pl.ds(rows + s * length, length)]
        return send(source, mixed_in.at[at], s, {"tensor": exchange.slot ^ 1})

    def hand(m):
        return send(
            half_nb.at[m + 1], from_y.at[m], seqs + m, {"tensor": exchange.slot ^ 2}
        )

    exchange.greet()
    cross(0).start()
    hand(0).start()

    def spans():
        return [pl.ds(s * length, length) for s in range(seqs)]

    for at in spans():
        value = residual[at]
        scale = lax.rsqrt(square_mean(value) + EPS)
        normed = value * scale
        grad = back_own[at].astype(F32) + back_in[at].astype(F32)
        grad = grads[at].astype(F32) + scale * (
            grad - normed * jnp.mean(grad * normed, axis=-1, keepdims=True)
        )
        grad_mid[at] = grad
        grad_mid_low[at] = grad.astype(BF16)

    def columns_of(spot):
        return pl.ds(pl.multiple_of(spot * tile, tile), tile)

    @pl.loop(0, width)
    def _(spot):
        work[:, columns_of(spot)] = times_back(grad_mid_low[...], w_output[columns_of(spot)])

    for at in spans():
        value = attended[at]
        scale = lax.rsqrt(square_mean(value) + EPS)
        normed = value * scale
        grad = work[at]
        gate_low[at] = (grad * normed).astype(BF16)
        grad = grad * gate[at]
        grad_att[at] = (
            scale * (grad - normed * jnp.mean(grad * normed, axis=-1, keepdims=True))
        ).astype(BF16)

    for load in loads[:7]:
        load.wait()

    @pl.loop(1, width + 1)
    def _(step):
        b = lax.rem(step, width)
        spot = exchange.slot ^ b
        for k in range(per_tile):
            own = pl.ds(pl.multiple_of(spot * tile + k * dim, dim), dim)
            for s, at in enumerate(spans()):
                local[spot * per_tile + k, s] = times_rows(
                    query_dec[at, own], grad_att[at, own]
                ).astype(BF16)

        for b_static in range(1, width):

            @pl.when(b == b_static)
            def _(b_static=b_static):
                exchange.to_peer(b_static).start()

    for s in range(1, seqs):
        cross(s).start()
    hand(1).start()

    def slope(values):
        sigmoid_v = jax.nn.sigmoid(values)
        return sigmoid_v * (1.0 + values * (1.0 - sigmoid_v))

    def inner(spot):
        for k in range(per_tile):
            head = spot * per_tile + k
            own = pl.ds(pl.multiple_of(spot * tile + k * dim, dim), dim)
            query_weight, _ = decays(rates, head, length, dim)
            mask = lag_decay(rates, head, length)
            for s, at in enumerate(spans()):
                grad = grad_att[at, own]
                value_part[at, own] = times_rows(scores_low[head, s], grad)
                score = (times_back(grad, value_low[at, own]) * mask).astype(BF16)
                key_part[at, own] = times_rows(score, query_low[at, own])
                turned = times(score, key_low[at, own]) + query_weight * times_back(
                    grad, states_in[head, s]
                )
                query_out[at, own] = (
                    turn(turned, cosine[...], -sine_part[...]) * slope(query_pre[at, own])
                ).astype(BF16)

    half = width // 2

    @pl.loop(0, half)
    def _(spot):
        inner(spot)

    exchange.gather()

    @pl.loop(half, width)
    def _(spot):
        inner(spot)

    exchange.send_back(entering)
    for load in loads[7:]:
        load.wait()

    @pl.loop(0, width)
    def _(spot):
        at = columns_of(spot)
        work[:, at] = times_back(query_out[...], w_query[at]) + times_back(
            gate_low[...], w_gate[at]
        )

    exchange.arrive()

    @pl.loop(0, width * per_tile)
    def _(head):
        own = pl.ds(pl.multiple_of(head * dim, dim), dim)
        _, key_weight = decays(rates, head, length, dim)
        for s, at in enumerate(spans()):
            state = states[head, s]
            value_out[at, own] = (
                value_part[at, own] + times(key_dec[at, own], state)
            ).astype(BF16)
            turned = key_part[at, own] + key_weight * times_back(value_low[at, own], state)
            key_out[at, own] = (
                turn(turned, cosine[...], -sine_part[...]) * slope(key_pre[at, own])
            ).astype(BF16)

    @pl.loop(0, width)
    def _(spot):
        at = columns_of(spot)
        work[:, at] += times_back(key_out[...], w_key[at]) + times_back(
            value_out[...], w_value[at]
        )

    for at in spans():
        value = x[at].astype(F32)
        scale = lax.rsqrt(square_mean(value) + EPS)
        normed = value * scale
        grad = work[at]
        grad_tokens[at] = grad_mid[at] + scale * (
            grad - normed * jnp.mean(grad * normed, axis=-1, keepdims=True)
        )
    exchange.settle()
    for s in range(seqs):
        cross(s).wait()
    for m in range(2):
        hand(m).wait()


def retreat(early, tables, bulk, late, seqs, depth, width):
    rows, model = early[0].shape
    heads = tables[0].shape[0]
    dim = model // heads
    vmem = pl.BlockSpec(memory_space=pltpu.VMEM)
    anywhere = pl.BlockSpec(memory_space=pl.ANY)
    wide = jax.ShapeDtypeStruct((rows, model), F32)
    low = jax.ShapeDtypeStruct((rows, model), BF16)
    return pl.pallas_call(
        functools.partial(retreat_kernel, depth, width, seqs),
        out_shape=(low,) * 5 + (wide, low, jax.ShapeDtypeStruct((2,) + bulk[1].shape[1:], BF16)),
        in_specs=[vmem] * (len(early) + len(tables)) + [anywhere] * (len(bulk) + len(late)),
        out_specs=(vmem,) * 6 + (anywhere,) * 2,
        scratch_shapes=[pltpu.VMEM(v.shape, v.dtype) for v in late]
        + [
            pltpu.VMEM((heads, seqs, dim, dim), BF16),
            pltpu.VMEM((rows, model), F32),
            pltpu.VMEM((rows, model), F32),
            pltpu.VMEM((rows, model), BF16),
            pltpu.VMEM((rows, model), F32),
            pltpu.VMEM((rows, model), F32),
        ]
        + state_scratch(heads, seqs, dim, width, depth)
        + [pltpu.SemaphoreType.DMA((len(late),)), pltpu.SemaphoreType.DMA((2, seqs + 2))],
        compiler_params=pltpu.CompilerParams(
            collective_id=3, has_side_effects=True, vmem_limit_bytes=60 * 1024 * 1024
        ),
        name="retreat",
    )(*early, *tables, *bulk, *late)


def on_device(
    tokens,
    w_query,
    w_key,
    w_value,
    w_ugate,
    w_output,
    w_left,
    w_right,
    w_down,
    decay_rate,
    cotangent,
):
    seq_count, group_len, model_width = tokens.shape
    head_count = decay_rate.shape[0]
    head_dim = model_width // head_count
    half_dim = head_dim // 2
    row_count = seq_count * group_len
    core = lax.axis_index("dp")

    shard = (w_left.T, w_right.T, w_down)
    grad_own = cotangent.reshape(row_count, model_width)

    position_block = lax.axis_index(("seq", "tensor"))
    places = (position_block * group_len + jnp.arange(group_len)).astype(F32)
    frequency = 10000.0 ** (-jnp.arange(half_dim, dtype=F32) / half_dim)
    angles = places[:, None] * frequency[None, :]
    cosine, sine_part = jnp.cos(angles), jnp.sin(angles)
    cosine = jnp.concatenate([cosine, cosine], axis=1)
    sine_part = jnp.concatenate([-sine_part, sine_part], axis=1)
    rows_in = tokens.reshape(row_count, model_width)
    depth = lax.axis_size("seq")
    width = lax.axis_size("tensor")
    rates = jnp.broadcast_to(decay_rate[:, None, None], (head_count, 1, group_len))
    blocks = jnp.arange(depth * width, dtype=F32)[:, None, None, None]
    powers = jnp.broadcast_to(
        jnp.exp(-decay_rate[None, :, None, None] * group_len * blocks),
        (depth * width, head_count, 1, head_dim),
    )
    (
        residual,
        rows_own,
        merged,
        query_pre,
        key_pre,
        ugate,
        normed_low,
        query_low,
        key_low,
        value_low,
        query_dec,
        key_dec,
        weights_low,
        gated_low,
        state_low,
        other,
        grad_nb,
    ) = attend(
        rows_in,
        (w_query, w_key, w_value, w_ugate, w_output),
        shard,
        grad_own,
        rates,
        powers,
        cosine,
        sine_part,
        seq_count,
        depth,
        width,
    )
    mixed, back, half_own, half_nb, back_in, first_y = hidden_part(
        rows_own, grad_own, grad_nb, shard, other
    )
    (
        grad_branch,
        grad_ugate_pre,
        grad_query_pre,
        grad_key_pre,
        grad_value_pre,
        grad_tokens,
        mixed_in,
        from_y,
    ) = retreat(
        (residual, back, back_in, grad_own, w_output, merged, ugate),
        (rates, powers, cosine, sine_part),
        (mixed, half_nb),
        (
            query_low,
            key_low,
            value_low,
            query_dec,
            weights_low,
            state_low,
            query_pre,
            w_query,
            w_ugate,
            key_dec,
            key_pre,
            w_key,
            w_value,
            rows_in,
        ),
        seq_count,
        depth,
        width,
    )

    def weight_grad(rows, gradient):
        return jnp.einsum("rd,re->de", rows, gradient, preferred_element_type=F32)

    partial = (
        weight_grad(normed_low, grad_query_pre),
        weight_grad(normed_low, grad_key_pre),
        weight_grad(normed_low, grad_value_pre),
        weight_grad(normed_low, grad_ugate_pre),
        weight_grad(gated_low, grad_branch),
    )
    hidden = w_down.shape[0]
    sums, hidden_sums = reduce_grads(
        tuple(g.astype(BF16) for g in partial), half_own, first_y, from_y, depth
    )
    mixed_out = (
        residual + mixed[:row_count].astype(F32) + mixed_in.astype(F32)
    ).astype(BF16)
    attention_grads = tuple(
        sums[i * model_width : (i + 1) * model_width].astype(F32) for i in range(len(partial))
    )
    left_sum, right_sum, down_sum = (
        hidden_sums[i * hidden : (i + 1) * hidden].astype(F32) for i in range(3)
    )
    return (
        (mixed_out.reshape(tokens.shape), grad_tokens.reshape(tokens.shape))
        + attention_grads
        + (left_sum.T, right_sum.T, down_sum)
    )


def solution(mesh):
    rows = P("dp", ("seq", "tensor"), None)
    columns = P(None, "tensor")
    return jax.shard_map(
        on_device,
        mesh=mesh,
        in_specs=(rows, P(), P(), P(), P(), P(), columns, columns, P("tensor", None), P(), rows),
        out_specs=(rows, rows, P(), P(), P(), P(), P(), columns, columns, P("tensor", None)),
        check_vma=False,
    )
```

```python
import functools

import jax
import jax.numpy as jnp
from jax import lax
from jax.experimental import pallas as pl
from jax.experimental.pallas import tpu as pltpu
from jax.sharding import PartitionSpec as P


EPS = 1e-06
F32 = jnp.float32
BF16 = jnp.bfloat16


CHUNK = 256
LAG = 1


def added(first, second):
    return (first.astype(F32) + second.astype(F32)).astype(BF16)


RING = 8


def reduce_kernel(
    depth,
    factors,
    pair_own,
    pair_first,
    pair_rest,
    out,
    pair_out,
    pair_in,
    left_side,
    right_side,
    own,
    core_in,
    first_in,
    second_in,
    line_in,
    line_mid,
    pair_line,
    pair_mid,
    sems,
    pair_sems,
    load_sem,
):
    core = lax.axis_index("dp")
    slot = lax.axis_index("tensor")
    place = lax.axis_index("seq")
    rows = out.shape[0]
    chunks = rows // CHUNK
    half, quarter, eighth = CHUNK // 2, CHUNK // 4, CHUNK // 8
    low_side = place < depth // 2
    outermost = (place == 0) | (place == depth - 1)
    middle = (place == depth // 2 - 1) | (place == depth // 2)
    inward = jnp.where(low_side, place + 1, place - 1)
    outward = jnp.where(low_side, place - 1, place + 1)

    barrier = pltpu.get_barrier_semaphore()

    def greet(peer):
        pl.semaphore_signal(
            barrier, inc=1, device_id=peer, device_id_type=pl.DeviceIdType.MESH
        )

    greet({"dp": 1 - core})
    greet({"tensor": slot ^ 1})
    greet({"tensor": slot ^ 2})

    @pl.when(place > 0)
    def _():
        greet({"seq": place - 1})

    @pl.when(place < depth - 1)
    def _():
        greet({"seq": place + 1})

    pl.semaphore_wait(barrier, jnp.where(outermost, 4, 5))

    def remote(source, target, sem, at, peer):
        return pltpu.make_async_remote_copy(
            src_ref=source,
            dst_ref=target,
            send_sem=sem.at[0, at],
            recv_sem=sem.at[1, at],
            device_id=peer,
            device_id_type=pl.DeviceIdType.MESH,
        )

    def span(start, size):
        return pl.ds(pl.multiple_of(start, size), size)

    def bits(q):
        first = jnp.where(q % 2 == 0, 1, 2)
        second = 3 - first
        return first, second, (slot & first) // first, (slot & second) // second

    def base(q):
        return pl.multiple_of(q * CHUNK, CHUNK)

    def to_core(q):
        return remote(
            own.at[q % RING, span((1 - core) * half, half)],
            core_in.at[q],
            sems.at[0],
            q,
            {"dp": 1 - core},
        )

    def to_first(q):
        first, _, f, _ = bits(q)
        return remote(
            core_in.at[q, span((1 - f) * quarter, quarter)],
            first_in.at[q],
            sems.at[1],
            q,
            {"tensor": slot ^ first},
        )

    def to_second(q):
        _, second, _, g = bits(q)
        return remote(
            first_in.at[q, span((1 - g) * eighth, eighth)],
            second_in.at[q],
            sems.at[2],
            q,
            {"tensor": slot ^ second},
        )

    def block(q):
        _, _, f, g = bits(q)
        return base(q) + core * half + f * quarter + g * eighth

    def back_second(q):
        _, second, _, _ = bits(q)
        at = span(block(q), eighth)
        return remote(out.at[at], out.at[at], sems.at[3], q, {"tensor": slot ^ second})

    def back_first(q):
        first, _, f, _ = bits(q)
        at = span(base(q) + core * half + f * quarter, quarter)
        return remote(out.at[at], out.at[at], sems.at[4], q, {"tensor": slot ^ first})

    def back_core(q):
        at = span(base(q) + core * half, half)
        return remote(out.at[at], out.at[at], sems.at[5], q, {"dp": 1 - core})

    class Line:
        def __init__(self, mine, came, met, total, sem, offset):
            self.mine, self.came, self.met, self.total = mine, came, met, total
            self.sem, self.offset = sem, offset

        def inwards(self, q, source):
            return remote(
                source, self.came(q), self.sem.at[self.offset], q, {"seq": inward}
            )

        def across(self, q):
            return remote(
                self.came(q),
                self.met(q),
                self.sem.at[self.offset + 1],
                q,
                {"seq": depth - 1 - place},
            )

        def outwards(self, q):
            return remote(
                self.total(q), self.total(q), self.sem.at[self.offset + 2], q, {"seq": outward}
            )

        def step_in(self, q):
            @pl.when(outermost)
            def _():
                self.inwards(q, self.mine(q)).start()

        def step_middle(self, q):
            @pl.when(jnp.logical_not(outermost))
            def _():
                self.inwards(q, self.mine(q)).wait_recv()
                came = self.came(q)
                came[...] = added(self.mine(q)[...], came[...])

                @pl.when(middle)
                def _():
                    self.across(q).start()

                @pl.when(jnp.logical_not(middle))
                def _():
                    self.inwards(q, came).start()

        def step_out(self, q):
            @pl.when(middle)
            def _():
                self.across(q).wait_recv()
                self.total(q)[...] = added(self.came(q)[...], self.met(q)[...])

            @pl.when(jnp.logical_not(outermost))
            def _():
                @pl.when(jnp.logical_not(middle))
                def _():
                    self.outwards(q).wait_recv()

                self.outwards(q).start()

        def step_last(self, q):
            @pl.when(outermost)
            def _():
                self.outwards(q).wait_recv()

        def settle(self, q):
            @pl.when(outermost)
            def _():
                self.inwards(q, self.mine(q)).wait_send()

            @pl.when(jnp.logical_not(outermost))
            def _():
                @pl.when(middle)
                def _():
                    self.across(q).wait_send()

                @pl.when(jnp.logical_not(middle))
                def _():
                    self.inwards(q, self.came(q)).wait_send()

                self.outwards(q).wait_send()

    def second_mine(q):
        return second_in.at[q]

    line = Line(
        second_mine,
        lambda q: line_in.at[q],
        lambda q: line_mid.at[q],
        lambda q: out.at[span(block(q), eighth)],
        sems,
        6,
    )
    pair_chunks, pair_rows, pair_cols = pair_line.shape
    pair = Line(
        lambda q: pair_in.at[span(q * pair_rows, pair_rows)],
        lambda q: pair_line.at[q],
        lambda q: pair_mid.at[q],
        lambda q: pair_out.at[span(q * pair_rows, pair_rows), span(core * pair_cols, pair_cols)],
        pair_sems,
        0,
    )

    def pair_core(q):
        return remote(pair.total(q), pair.total(q), pair_sems.at[3], q, {"dp": 1 - core})

    rights = len(factors) - 2
    loads = [
        pltpu.make_async_copy(g, t, load_sem.at[i])
        for i, (g, t) in enumerate(
            zip(
                factors,
                [left_side.at[0], left_side.at[1]] + [right_side.at[i] for i in range(rights)],
            )
        )
    ]
    for load in loads:
        load.start()
    for load in loads:
        load.wait()
    per_matrix = chunks // rights

    def make(q):
        @pl.when(q >= RING)
        def _():
            to_core(q - RING).wait_send()

        m = q // per_matrix
        columns = pl.ds(pl.multiple_of((q % per_matrix) * CHUNK, CHUNK), CHUNK)
        own[q % RING] = times_rows(
            left_side[m // (rights - 1), :, columns], right_side[m]
        ).astype(BF16)

    hidden = pair_first.shape[0]
    for m in range(3):
        theirs = pair_first[...] if m == 0 else pair_rest[m - 1]
        pair_in[pl.ds(m * hidden, hidden)] = added(pair_own[m], theirs)

    def stage_a(q):
        to_core(q).wait_recv()
        came = core_in.at[q]
        came[...] = added(own[q % RING, span(core * half, half)], came[...])

    def stage_b(q):
        _, _, f, _ = bits(q)
        to_first(q).wait_recv()
        came = first_in.at[q]
        came[...] = added(core_in[q, span(f * quarter, quarter)], came[...])

    def stage_c(q):
        _, _, _, g = bits(q)
        to_second(q).wait_recv()
        came = second_in.at[q]
        came[...] = added(first_in[q, span(g * eighth, eighth)], came[...])

    pairs = chunks // 2

    def during(step, lag, count, action):
        i = step - lag

        @pl.when((i >= 0) & (i < count))
        def _():
            action(i)

    def both(action):
        def run(i):
            action(2 * i)
            action(2 * i + 1)

        return run

    def start(copy):
        return lambda q: copy(q).start()

    def arrived(copy, following):
        def run(q):
            copy(q).wait_recv()
            following(q).start()

        return run

    def last_then_second(q):
        line.step_last(q)
        back_second(q).start()

    def finish_pair(q):
        pair.step_last(q)
        pair_core(q).start()

    steps = max(pairs + 8 * LAG, pair_chunks + 3 * LAG) + 1

    @pl.loop(0, steps)
    def _(step):
        during(step, 8 * LAG, pairs, both(arrived(back_first, back_core)))
        during(step, 7 * LAG, pairs, both(arrived(back_second, back_first)))
        during(step, 6 * LAG, pairs, both(last_then_second))
        during(step, 5 * LAG, pairs, both(line.step_out))
        during(step, 4 * LAG, pairs, both(line.step_middle))
        during(step, 3 * LAG, pairs, both(stage_c))
        during(step, 2 * LAG, pairs, both(stage_b))
        during(step, LAG, pairs, both(stage_a))
        during(step, 3 * LAG, pairs, both(line.step_in))
        during(step, 2 * LAG, pairs, both(start(to_second)))
        during(step, LAG, pairs, both(start(to_first)))
        during(step, 0, pairs, both(make))
        during(step, 0, pairs, both(start(to_core)))
        during(step, 3 * LAG, pair_chunks, finish_pair)
        during(step, 2 * LAG, pair_chunks, pair.step_out)
        during(step, LAG, pair_chunks, pair.step_middle)
        during(step, 0, pair_chunks, pair.step_in)

    @pl.loop(0, chunks)
    def _(q):
        back_core(q).wait_recv()
        for copy in (to_first, to_second, back_second, back_first, back_core):
            copy(q).wait_send()

        @pl.when(q >= chunks - RING)
        def _():
            to_core(q).wait_send()

        line.settle(q)

    @pl.loop(0, pair_chunks)
    def _(q):
        pair_core(q).wait()
        pair.settle(q)


def reduce_grads(factors, half_own, first_y, rest_y, depth):
    count, width = factors[0].shape
    rights = len(factors) - 2
    rows = width * rights
    chunks = rows // CHUNK
    pair_chunks = 12
    total_rows, pair_cols = 3 * half_own.shape[1], half_own.shape[2]
    pair_rows = total_rows // pair_chunks
    vmem = pl.BlockSpec(memory_space=pltpu.VMEM)

    def body(*refs):
        reduce_kernel(depth, refs[: len(factors)], *refs[len(factors) :])

    return pl.pallas_call(
        body,
        out_shape=(
            jax.ShapeDtypeStruct((rows, width), BF16),
            jax.ShapeDtypeStruct((total_rows, 2 * pair_cols), BF16),
        ),
        in_specs=[pl.BlockSpec(memory_space=pl.ANY)] * len(factors) + [vmem] * 3,
        out_specs=(vmem, vmem),
        scratch_shapes=[
            pltpu.VMEM((total_rows, pair_cols), BF16),
            pltpu.VMEM((2, count, width), BF16),
            pltpu.VMEM((rights, count, width), BF16),
            pltpu.VMEM((RING, CHUNK, width), BF16),
            pltpu.VMEM((chunks, CHUNK // 2, width), BF16),
            pltpu.VMEM((chunks, CHUNK // 4, width), BF16),
            pltpu.VMEM((chunks, CHUNK // 8, width), BF16),
            pltpu.VMEM((chunks, CHUNK // 8, width), BF16),
            pltpu.VMEM((chunks, CHUNK // 8, width), BF16),
            pltpu.VMEM((pair_chunks, pair_rows, pair_cols), BF16),
            pltpu.VMEM((pair_chunks, pair_rows, pair_cols), BF16),
            pltpu.SemaphoreType.DMA((9, 2, chunks)),
            pltpu.SemaphoreType.DMA((4, 2, pair_chunks)),
            pltpu.SemaphoreType.DMA((len(factors),)),
        ],
        compiler_params=pltpu.CompilerParams(
            collective_id=1, has_side_effects=True, vmem_limit_bytes=50 * 1024 * 1024
        ),
        name="reduce_grads",
    )(*factors, half_own, first_y, rest_y)


ROWS = 256


def times(x, w):
    return jnp.dot(x, w, preferred_element_type=F32)


def times_back(x, w):
    return lax.dot_general(x, w, (((1,), (1,)), ((), ())), preferred_element_type=F32)


def times_rows(x, y):
    return lax.dot_general(x, y, (((0,), (0,)), ((), ())), preferred_element_type=F32)


def hidden_kernel(
    rows_own,
    grads_own,
    grads_nb,
    late_left,
    late_right,
    late_down,
    late_other,
    mixed,
    back,
    half_own,
    half_nb,
    back_in,
    from_y,
    both,
    own,
    other,
    kept,
    theirs,
    moved,
    acc_mixed,
    acc_back,
    load_sem,
    sems,
):
    core = lax.axis_index("dp")
    slot = lax.axis_index("tensor")
    count, width = rows_own.shape
    half = width // 2
    blocks = count // ROWS
    pairs = (
        (late_left, own.at[0]),
        (late_right, own.at[1]),
        (late_down, own.at[2]),
        (late_other, other),
        (rows_own, both.at[0, :count]),
        (grads_own, both.at[1, :count]),
        (grads_nb, both.at[1, count:]),
    )
    loads = [pltpu.make_async_copy(a, b, load_sem.at[i]) for i, (a, b) in enumerate(pairs)]
    for i in (4, 5, 0, 1, 2, 3, 6):
        loads[i].start()

    def send(source, target, at, peer):
        return pltpu.make_async_remote_copy(
            src_ref=source,
            dst_ref=target,
            send_sem=sems.at[0, at],
            recv_sem=sems.at[1, at],
            device_id=peer,
            device_id_type=MESH,
        )

    def span(i):
        return pl.ds(pl.multiple_of(i * ROWS, ROWS), ROWS)

    def out_rows(i):
        return send(
            rows_own.at[span(i)], both.at[0, span(blocks + i)], i, {"tensor": slot ^ 1}
        )

    def return_rows(i):
        return send(
            back.at[span(blocks + i)], back_in.at[span(i)], blocks + i, {"tensor": slot ^ 1}
        )

    def to_core(which, m):
        return send(
            theirs.at[which, m], moved.at[which, m], 2 * blocks + 3 * which + m, {"dp": 1 - core}
        )

    hand = send(half_nb.at[0], from_y, 2 * blocks + 6, {"tensor": slot ^ 2})
    barrier = pltpu.get_barrier_semaphore()
    for peer in ({"tensor": slot ^ 1}, {"tensor": slot ^ 2}, {"dp": 1 - core}):
        pl.semaphore_signal(barrier, inc=1, device_id=peer, device_id_type=MESH)
    pl.semaphore_wait(barrier, 3)
    for i in range(blocks):
        out_rows(i).start()
    for load in loads:
        load.wait()

    def unit(i, which, weights):
        rows, grads = both[0, span(i)], both[1, span(i)]
        e1, e2 = times_back(rows, weights[0]), times_back(rows, weights[1])
        dm = times_back(grads, weights[2])
        mid = (e1 * e2).astype(BF16)
        de1 = (dm * e2).astype(BF16)
        de2 = (dm * e1).astype(BF16)
        kept[which, 2, span(i)] = mid
        kept[which, 0, span(i)] = de1
        kept[which, 1, span(i)] = de2
        return times(mid, weights[2]), times(de1, weights[0]) + times(de2, weights[1])

    @pl.loop(0, 2 * blocks)
    def _(i):
        @pl.when(i >= blocks)
        def _():
            out_rows(i - blocks).wait_recv()

        acc_mixed[...], acc_back[...] = unit(i, 0, own)
        more_mixed, more_back = unit(i, 1, other)
        mixed[span(i)] = (acc_mixed[...] + more_mixed).astype(BF16)
        back[span(i)] = (acc_back[...] + more_back).astype(BF16)

        @pl.when(i >= blocks)
        def _():
            return_rows(i - blocks).start()

    here = pl.ds(pl.multiple_of(core * half, half), half)
    there = pl.ds(pl.multiple_of((1 - core) * half, half), half)
    for which, out in ((1, half_nb), (0, half_own)):

        @pl.loop(0, 3)
        def _(m, which=which, out=out):
            theirs[which, m] = times_rows(kept[which, m], both[m // 2, :, there]).astype(BF16)
            to_core(which, m).start()
            out[m] = times_rows(kept[which, m], both[m // 2, :, here]).astype(BF16)

        for m in range(3):
            to_core(which, m).wait_recv()
            out[m] = added(out[m], moved[which, m])
        if which == 1:
            hand.start()
    for i in range(blocks):
        out_rows(i).wait_send()
        return_rows(i).wait()
    for which in range(2):
        for m in range(3):
            to_core(which, m).wait_send()
    hand.wait()


def hidden_part(rows_own, grads_own, grads_nb, shard, other):
    count, width = rows_own.shape
    hidden = shard[0].shape[0]
    vmem = pl.BlockSpec(memory_space=pltpu.VMEM)
    anywhere = pl.BlockSpec(memory_space=pl.ANY)
    half = jax.ShapeDtypeStruct((3, hidden, width // 2), BF16)
    two = jax.ShapeDtypeStruct((2 * count, width), BF16)
    return pl.pallas_call(
        hidden_kernel,
        out_shape=(
            two,
            two,
            half,
            half,
            jax.ShapeDtypeStruct((count, width), BF16),
            jax.ShapeDtypeStruct((hidden, width // 2), BF16),
        ),
        in_specs=[anywhere] * 7,
        out_specs=(vmem,) * 4 + (anywhere,) * 2,
        scratch_shapes=[
            pltpu.VMEM((2, 2 * count, width), BF16),
            pltpu.VMEM((3, hidden, width), BF16),
            pltpu.VMEM((3, hidden, width), BF16),
            pltpu.VMEM((2, 3, 2 * count, hidden), BF16),
            pltpu.VMEM((2, 3, hidden, width // 2), BF16),
            pltpu.VMEM((2, 3, hidden, width // 2), BF16),
            pltpu.VMEM((ROWS, width), F32),
            pltpu.VMEM((ROWS, width), F32),
            pltpu.SemaphoreType.DMA((7,)),
            pltpu.SemaphoreType.DMA((2, 2 * (count // ROWS) + 7)),
        ],
        compiler_params=pltpu.CompilerParams(
            collective_id=4, has_side_effects=True, vmem_limit_bytes=54 * 1024 * 1024
        ),
        name="hidden_part",
    )(rows_own, grads_own, grads_nb, *shard, other)


MESH = pl.DeviceIdType.MESH


class States:
    def __init__(self, depth, width, backward, powers, local, came, total, far, outs, states, sems):
        self.depth, self.width, self.backward, self.powers = depth, width, backward, powers
        self.local, self.came, self.total, self.far = local, came, total, far
        self.outs, self.states, self.sems = outs, states, sems
        self.slot = lax.axis_index("tensor")
        self.place = lax.axis_index("seq")
        self.share = local.shape[0] // width

    def greet(self, more=()):
        barrier = pltpu.get_barrier_semaphore()
        for peer in more:
            pl.semaphore_signal(barrier, inc=1, device_id=peer, device_id_type=MESH)
        for b in range(1, self.width):
            pl.semaphore_signal(
                barrier, inc=1, device_id={"tensor": self.slot ^ b}, device_id_type=MESH
            )
        for j in range(1, self.depth):
            peer = lax.rem(self.place + j, self.depth)
            pl.semaphore_signal(barrier, inc=1, device_id={"seq": peer}, device_id_type=MESH)
        pl.semaphore_wait(barrier, self.width + self.depth - 2 + len(more))

    def copy(self, source, target, at, peer):
        return pltpu.make_async_remote_copy(
            src_ref=source,
            dst_ref=target,
            send_sem=self.sems.at[0, at],
            recv_sem=self.sems.at[1, at],
            device_id=peer,
            device_id_type=MESH,
        )

    def group(self, slot):
        return pl.ds(slot * self.share, self.share)

    def to_peer(self, b):
        peer = self.slot ^ b
        return self.copy(
            self.local.at[self.group(peer)], self.came.at[b - 1], b - 1, {"tensor": peer}
        )

    def to_far(self, j):
        peer = self.place - j if self.backward else self.place + j
        return self.copy(self.total, self.far.at[j - 1], self.width + j - 2, {"seq": peer})

    def has_far(self, j):
        return self.place >= j if self.backward else self.place + j < self.depth

    def from_far(self, j):
        return self.place + j < self.depth if self.backward else self.place >= j

    def to_owner(self, d):
        at = self.width + self.depth - 2 + d - 1
        return self.copy(
            self.outs.at[d - 1],
            self.states.at[self.group(self.slot)],
            at,
            {"tensor": self.slot ^ d},
        )

    def power(self, count, head):
        return self.powers[count, head]

    def piece(self, b, k, s):
        if b == 0:
            return self.local[self.slot * self.share + k, s].astype(F32)
        return self.came[b - 1, k, s].astype(F32)

    def gather(self):
        for b in range(1, self.width):
            self.to_peer(b).wait_recv()
        for k in range(self.share):
            head = self.slot * self.share + k
            for s in range(self.local.shape[1]):
                value = 0.0
                for b in range(self.width):
                    spot = self.slot ^ b
                    left = spot if self.backward else self.width - 1 - spot
                    value = value + self.power(left, head) * self.piece(b, k, s)
                self.total[k, s] = value.astype(BF16)
        for j in range(1, self.depth):

            @pl.when(self.has_far(j))
            def _(j=j):
                self.to_far(j).start()

    def send_back(self, entering):
        for j in range(1, self.depth):

            @pl.when(self.from_far(j))
            def _(j=j):
                self.to_far(j).wait_recv()

            @pl.when(jnp.logical_not(self.from_far(j)))
            def _(j=j):
                self.far[j - 1] = jnp.zeros(self.far.shape[1:], BF16)

        for k in range(self.share):
            head = self.slot * self.share + k
            for s in range(self.local.shape[1]):
                value = 0.0
                for j in range(1, self.depth):
                    value = value + self.power(self.width * (j - 1), head) * self.far[
                        j - 1, k, s
                    ].astype(F32)
                entering[k, s] = value
        for d in list(range(1, self.width)) + [0]:
            target = self.slot ^ d
            inner = self.width - 1 - target if self.backward else target
            for k in range(self.share):
                head = self.slot * self.share + k
                for s in range(self.local.shape[1]):
                    value = self.power(inner, head) * entering[k, s]
                    for b in range(self.width):
                        if b == d:
                            continue
                        source = self.slot ^ b
                        gap = source - target - 1 if self.backward else target - source - 1
                        coef = jnp.where(gap >= 0, self.power(jnp.maximum(gap, 0), head), 0.0)
                        value = value + coef * self.piece(b, k, s)
                    if d == 0:
                        self.states[head, s] = value.astype(BF16)
                    else:
                        self.outs[d - 1, k, s] = value.astype(BF16)
        for d in range(1, self.width):
            self.to_owner(d).start()

    def arrive(self):
        for d in range(1, self.width):
            at = self.width + self.depth - 2 + d - 1
            self.copy(
                self.outs.at[d - 1],
                self.states.at[self.group(self.slot ^ d)],
                at,
                {"tensor": self.slot ^ d},
            ).wait_recv()

    def settle(self):
        for b in range(1, self.width):
            self.to_peer(b).wait_send()
            self.to_owner(b).wait_send()
        for j in range(1, self.depth):

            @pl.when(self.has_far(j))
            def _(j=j):
                self.to_far(j).wait_send()


def state_scratch(heads, seqs, head_dim, width, depth):
    share = heads // width
    low = functools.partial(pltpu.VMEM, dtype=BF16)
    return [
        low((heads, seqs, head_dim, head_dim)),
        low((width - 1, share, seqs, head_dim, head_dim)),
        low((share, seqs, head_dim, head_dim)),
        low((depth - 1, share, seqs, head_dim, head_dim)),
        low((width - 1, share, seqs, head_dim, head_dim)),
        pltpu.VMEM((share, seqs, head_dim, head_dim), F32),
        pltpu.SemaphoreType.DMA((2, 2 * (width - 1) + depth - 1)),
    ]


def turn(values, cosine, sine_part):
    return values * cosine + pltpu.roll(values, values.shape[-1] // 2, 1) * sine_part


def square_mean(values):
    return jnp.mean(values * values, axis=-1, keepdims=True)


def decays(rates, head, length, dim):
    rate = rates[head]
    place = lax.broadcasted_iota(jnp.int32, (length, dim), 0).astype(F32)
    query = jnp.exp(-rate[:, :dim] * (place + 1.0))
    key = jnp.exp(-rate[:, :dim] * (length - 1.0 - place))
    return query, key


def lag_decay(rates, head, length):
    lag = (
        lax.broadcasted_iota(jnp.int32, (length, length), 0)
        - lax.broadcasted_iota(jnp.int32, (length, length), 1)
    ).astype(F32)
    return jnp.where(lag >= 0, jnp.exp(-rates[head] * jnp.maximum(lag, 0.0)), 0.0)


def attend_kernel(
    depth,
    width,
    seqs,
    x,
    w_key,
    w_value,
    late_query,
    late_gate,
    late_output,
    left,
    right,
    down,
    grads,
    rates,
    powers,
    cosine,
    sine_part,
    residual,
    normed_two,
    attended,
    query_pre,
    key_pre,
    gate,
    normed_one,
    query_low,
    key_low,
    value_low,
    query_dec,
    key_dec,
    scores_low,
    gated,
    states,
    other,
    grads_nb,
    w_query,
    w_gate,
    w_output,
    local,
    came,
    total,
    far,
    outs,
    entering,
    sems,
    load_sem,
    bulk_sems,
):
    rows, model = x.shape
    length = rows // seqs
    dim = cosine.shape[1]
    tile = model // width
    loads = [
        pltpu.make_async_copy(a, b, load_sem.at[i])
        for i, (a, b) in enumerate(
            ((late_query, w_query), (late_gate, w_gate), (late_output, w_output))
        )
    ]
    for load in loads:
        load.start()
    exchange = States(
        depth, width, False, powers, local, came, total, far, outs, states, sems
    )
    core = lax.axis_index("dp")
    parity = lax.rem(exchange.place, 2)
    shard = (left, right, down)
    part_rows, part_cols = left.shape[0] // 2, model // 2
    columns_here = pl.ds(pl.multiple_of(core * part_cols, part_cols), part_cols)

    def rows_of(which):
        return pl.ds(pl.multiple_of(which * part_rows, part_rows), part_rows)

    def send(source, target, at, peer):
        return pltpu.make_async_remote_copy(
            src_ref=source,
            dst_ref=target,
            send_sem=bulk_sems.at[0, at],
            recv_sem=bulk_sems.at[1, at],
            device_id=peer,
            device_id_type=MESH,
        )

    def fetch(m):
        at = (rows_of(parity), columns_here)
        return send(
            shard[m].at[at], other.at[(m,) + at], m, {"tensor": exchange.slot ^ 2}
        )

    def relay(m):
        at = other.at[m, rows_of(parity), columns_here]
        return send(at, at, 3 + m, {"seq": exchange.place + 1 - 2 * parity})

    def share(m, which):
        spot = parity if which == 0 else 1 - parity
        at = other.at[m, rows_of(spot), columns_here]
        return send(at, at, 6 + 2 * m + which, {"dp": 1 - core})

    def cross(s):
        at = pl.ds(s * length, length)
        return send(grads.at[at], grads_nb.at[at], 12 + s, {"tensor": exchange.slot ^ 1})

    def pass_on(m):
        fetch(m).wait_recv()
        relay(m).start()
        share(m, 0).start()

    def pass_last(m):
        relay(m).wait_recv()
        share(m, 1).start()

    exchange.greet((({"dp": 1 - core}),))
    fetch(0).start()
    cross(0).start()
    fetch(1).start()
    for s in range(seqs):
        at = pl.ds(s * length, length)
        value = x[at].astype(F32)
        normed_one[at] = (value * lax.rsqrt(square_mean(value) + EPS)).astype(BF16)

    per_tile = tile // dim

    @pl.loop(1, width + 1)
    def _(step):
        b = lax.rem(step, width)
        spot = exchange.slot ^ b
        columns = pl.ds(pl.multiple_of(spot * tile, tile), tile)
        key_pre[:, columns] = times(normed_one[...], w_key[:, columns])
        value_low[:, columns] = times(normed_one[...], w_value[:, columns]).astype(BF16)
        for k in range(per_tile):
            head = spot * per_tile + k
            own = pl.ds(pl.multiple_of(spot * tile + k * dim, dim), dim)
            _, key_weight = decays(rates, head, length, dim)
            for s in range(seqs):
                at = pl.ds(s * length, length)
                turned = turn(jax.nn.silu(key_pre[at, own]), cosine[...], sine_part[...])
                key_low[at, own] = turned.astype(BF16)
                dec = (turned * key_weight).astype(BF16)
                key_dec[at, own] = dec
                local[head, s] = times_rows(dec, value_low[at, own]).astype(BF16)

        for b_static in range(1, width):

            @pl.when(b == b_static)
            def _(b_static=b_static):
                exchange.to_peer(b_static).start()

    for s in range(1, seqs):
        cross(s).start()
    fetch(2).start()
    pass_on(0)
    loads[0].wait()
    loads[1].wait()

    def inner(spot):
        columns = pl.ds(pl.multiple_of(spot * tile, tile), tile)
        query_pre[:, columns] = times(normed_one[...], w_query[:, columns])
        gate[:, columns] = times(normed_one[...], w_gate[:, columns])
        for k in range(per_tile):
            head = spot * per_tile + k
            own = pl.ds(pl.multiple_of(spot * tile + k * dim, dim), dim)
            query_weight, _ = decays(rates, head, length, dim)
            mask = lag_decay(rates, head, length)
            for s in range(seqs):
                at = pl.ds(s * length, length)
                turned = turn(jax.nn.silu(query_pre[at, own]), cosine[...], sine_part[...])
                low_query = turned.astype(BF16)
                query_low[at, own] = low_query
                query_dec[at, own] = (turned * query_weight).astype(BF16)
                low_scores = (times_back(low_query, key_low[at, own]) * mask).astype(BF16)
                scores_low[head, s] = low_scores
                attended[at, own] = times(low_scores, value_low[at, own])

    half = width // 2

    @pl.loop(0, half)
    def _(spot):
        inner(spot)

    exchange.gather()
    pass_on(1)

    @pl.loop(half, width)
    def _(spot):
        inner(spot)

    exchange.send_back(entering)
    pass_last(0)
    pass_on(2)
    loads[2].wait()
    exchange.arrive()
    pass_last(1)

    @pl.loop(0, width * per_tile)
    def _(head):
        own = pl.ds(pl.multiple_of(head * dim, dim), dim)
        for s in range(seqs):
            at = pl.ds(s * length, length)
            attended[at, own] += times(query_dec[at, own], states[head, s])

    for s in range(seqs):
        at = pl.ds(s * length, length)
        value = attended[at]
        gated[at] = (value * lax.rsqrt(square_mean(value) + EPS) * gate[at]).astype(BF16)

    @pl.loop(0, width)
    def _(spot):
        columns = pl.ds(pl.multiple_of(spot * tile, tile), tile)
        residual[:, columns] = x[:, columns].astype(F32) + times(
            gated[...], w_output[:, columns]
        )

    for s in range(seqs):
        at = pl.ds(s * length, length)
        value = residual[at]
        normed_two[at] = (value * lax.rsqrt(square_mean(value) + EPS)).astype(BF16)
    pass_last(2)
    exchange.settle()
    for m in range(3):
        fetch(m).wait_send()
        relay(m).wait_send()
        share(m, 0).wait()
        share(m, 1).wait()
    for s in range(seqs):
        cross(s).wait()


def attend(x, weights, shard, grads, rates, powers, cosine, sine_part, seqs, depth, width):
    rows, model = x.shape
    heads = rates.shape[0]
    dim = model // heads
    length = rows // seqs
    vmem = pl.BlockSpec(memory_space=pltpu.VMEM)
    anywhere = pl.BlockSpec(memory_space=pl.ANY)
    wide = jax.ShapeDtypeStruct((rows, model), F32)
    low = jax.ShapeDtypeStruct((rows, model), BF16)
    w_query, w_key, w_value, w_gate, w_output = weights
    return pl.pallas_call(
        functools.partial(attend_kernel, depth, width, seqs),
        out_shape=(wide, low, wide, wide, wide, wide)
        + (low,) * 6
        + (
            jax.ShapeDtypeStruct((heads, seqs, length, length), BF16),
            low,
            jax.ShapeDtypeStruct((heads, seqs, dim, dim), BF16),
            jax.ShapeDtypeStruct((3,) + shard[0].shape, BF16),
            low,
        ),
        in_specs=[vmem] * 3 + [anywhere] * 7 + [vmem] * 4,
        out_specs=(vmem,) * 15 + (anywhere,) * 2,
        scratch_shapes=[pltpu.VMEM((model, model), BF16)] * 3
        + state_scratch(heads, seqs, dim, width, depth)
        + [pltpu.SemaphoreType.DMA((3,)), pltpu.SemaphoreType.DMA((2, 12 + seqs))],
        compiler_params=pltpu.CompilerParams(
            collective_id=2, has_side_effects=True, vmem_limit_bytes=56 * 1024 * 1024
        ),
        name="attend",
    )(
        x,
        w_key,
        w_value,
        w_query,
        w_gate,
        w_output,
        *shard,
        grads,
        rates,
        powers,
        cosine,
        sine_part,
    )


def retreat_kernel(
    depth,
    width,
    seqs,
    residual,
    back_own,
    back_in,
    grads,
    w_output,
    attended,
    gate,
    rates,
    powers,
    cosine,
    sine_part,
    mixed_nb,
    half_nb,
    *rest,
):
    late = rest[:14]
    (
        grad_mid_low,
        gate_low,
        query_out,
        key_out,
        value_out,
        grad_tokens,
        mixed_in,
        from_y,
    ) = rest[14:22]
    held = rest[22:36]
    (
        query_low,
        key_low,
        value_low,
        query_dec,
        scores_low,
        states_in,
        query_pre,
        w_query,
        w_gate,
        key_dec,
        key_pre,
        w_key,
        w_value,
        x,
    ) = held
    (
        states,
        grad_mid,
        work,
        grad_att,
        value_part,
        key_part,
        local,
        came,
        total,
        far,
        outs,
        entering,
        sems,
        load_sem,
        bulk_sems,
    ) = rest[36:]
    rows, model = residual.shape
    length = rows // seqs
    dim = cosine.shape[1]
    tile = model // width
    per_tile = tile // dim
    loads = [
        pltpu.make_async_copy(a, b, load_sem.at[i]) for i, (a, b) in enumerate(zip(late, held))
    ]
    for load in loads:
        load.start()
    exchange = States(
        depth, width, True, powers, local, came, total, far, outs, states, sems
    )

    def send(source, target, at, peer):
        return pltpu.make_async_remote_copy(
            src_ref=source,
            dst_ref=target,
            send_sem=bulk_sems.at[0, at],
            recv_sem=bulk_sems.at[1, at],
            device_id=peer,
            device_id_type=MESH,
        )

    def cross(s):
        at = pl.ds(s * length, length)
        source = mixed_nb.at[pl.ds(rows + s * length, length)]
        return send(source, mixed_in.at[at], s, {"tensor": exchange.slot ^ 1})

    def hand(m):
        return send(
            half_nb.at[m + 1], from_y.at[m], seqs + m, {"tensor": exchange.slot ^ 2}
        )

    exchange.greet()
    cross(0).start()
    hand(0).start()

    def spans():
        return [pl.ds(s * length, length) for s in range(seqs)]

    for at in spans():
        value = residual[at]
        scale = lax.rsqrt(square_mean(value) + EPS)
        normed = value * scale
        grad = back_own[at].astype(F32) + back_in[at].astype(F32)
        grad = grads[at].astype(F32) + scale * (
            grad - normed * jnp.mean(grad * normed, axis=-1, keepdims=True)
        )
        grad_mid[at] = grad
        grad_mid_low[at] = grad.astype(BF16)

    def columns_of(spot):
        return pl.ds(pl.multiple_of(spot * tile, tile), tile)

    @pl.loop(0, width)
    def _(spot):
        work[:, columns_of(spot)] = times_back(grad_mid_low[...], w_output[columns_of(spot)])

    for at in spans():
        value = attended[at]
        scale = lax.rsqrt(square_mean(value) + EPS)
        normed = value * scale
        grad = work[at]
        gate_low[at] = (grad * normed).astype(BF16)
        grad = grad * gate[at]
        grad_att[at] = (
            scale * (grad - normed * jnp.mean(grad * normed, axis=-1, keepdims=True))
        ).astype(BF16)

    for load in loads[:7]:
        load.wait()

    @pl.loop(1, width + 1)
    def _(step):
        b = lax.rem(step, width)
        spot = exchange.slot ^ b
        for k in range(per_tile):
            own = pl.ds(pl.multiple_of(spot * tile + k * dim, dim), dim)
            for s, at in enumerate(spans()):
                local[spot * per_tile + k, s] = times_rows(
                    query_dec[at, own], grad_att[at, own]
                ).astype(BF16)

        for b_static in range(1, width):

            @pl.when(b == b_static)
            def _(b_static=b_static):
                exchange.to_peer(b_static).start()

    for s in range(1, seqs):
        cross(s).start()
    hand(1).start()

    def slope(values):
        sigmoid_v = jax.nn.sigmoid(values)
        return sigmoid_v * (1.0 + values * (1.0 - sigmoid_v))

    def inner(spot):
        for k in range(per_tile):
            head = spot * per_tile + k
            own = pl.ds(pl.multiple_of(spot * tile + k * dim, dim), dim)
            query_weight, _ = decays(rates, head, length, dim)
            mask = lag_decay(rates, head, length)
            for s, at in enumerate(spans()):
                grad = grad_att[at, own]
                value_part[at, own] = times_rows(scores_low[head, s], grad)
                score = (times_back(grad, value_low[at, own]) * mask).astype(BF16)
                key_part[at, own] = times_rows(score, query_low[at, own])
                turned = times(score, key_low[at, own]) + query_weight * times_back(
                    grad, states_in[head, s]
                )
                query_out[at, own] = (
                    turn(turned, cosine[...], -sine_part[...]) * slope(query_pre[at, own])
                ).astype(BF16)

    half = width // 2

    @pl.loop(0, half)
    def _(spot):
        inner(spot)

    exchange.gather()

    @pl.loop(half, width)
    def _(spot):
        inner(spot)

    exchange.send_back(entering)
    for load in loads[7:]:
        load.wait()

    @pl.loop(0, width)
    def _(spot):
        at = columns_of(spot)
        work[:, at] = times_back(query_out[...], w_query[at]) + times_back(
            gate_low[...], w_gate[at]
        )

    exchange.arrive()

    @pl.loop(0, width * per_tile)
    def _(head):
        own = pl.ds(pl.multiple_of(head * dim, dim), dim)
        _, key_weight = decays(rates, head, length, dim)
        for s, at in enumerate(spans()):
            state = states[head, s]
            value_out[at, own] = (
                value_part[at, own] + times(key_dec[at, own], state)
            ).astype(BF16)
            turned = key_part[at, own] + key_weight * times_back(value_low[at, own], state)
            key_out[at, own] = (
                turn(turned, cosine[...], -sine_part[...]) * slope(key_pre[at, own])
            ).astype(BF16)

    @pl.loop(0, width)
    def _(spot):
        at = columns_of(spot)
        work[:, at] += times_back(key_out[...], w_key[at]) + times_back(
            value_out[...], w_value[at]
        )

    for at in spans():
        value = x[at].astype(F32)
        scale = lax.rsqrt(square_mean(value) + EPS)
        normed = value * scale
        grad = work[at]
        grad_tokens[at] = grad_mid[at] + scale * (
            grad - normed * jnp.mean(grad * normed, axis=-1, keepdims=True)
        )
    exchange.settle()
    for s in range(seqs):
        cross(s).wait()
    for m in range(2):
        hand(m).wait()


def retreat(early, tables, bulk, late, seqs, depth, width):
    rows, model = early[0].shape
    heads = tables[0].shape[0]
    dim = model // heads
    vmem = pl.BlockSpec(memory_space=pltpu.VMEM)
    anywhere = pl.BlockSpec(memory_space=pl.ANY)
    wide = jax.ShapeDtypeStruct((rows, model), F32)
    low = jax.ShapeDtypeStruct((rows, model), BF16)
    return pl.pallas_call(
        functools.partial(retreat_kernel, depth, width, seqs),
        out_shape=(low,) * 5 + (wide, low, jax.ShapeDtypeStruct((2,) + bulk[1].shape[1:], BF16)),
        in_specs=[vmem] * (len(early) + len(tables)) + [anywhere] * (len(bulk) + len(late)),
        out_specs=(vmem,) * 6 + (anywhere,) * 2,
        scratch_shapes=[pltpu.VMEM(v.shape, v.dtype) for v in late]
        + [
            pltpu.VMEM((heads, seqs, dim, dim), BF16),
            pltpu.VMEM((rows, model), F32),
            pltpu.VMEM((rows, model), F32),
            pltpu.VMEM((rows, model), BF16),
            pltpu.VMEM((rows, model), F32),
            pltpu.VMEM((rows, model), F32),
        ]
        + state_scratch(heads, seqs, dim, width, depth)
        + [pltpu.SemaphoreType.DMA((len(late),)), pltpu.SemaphoreType.DMA((2, seqs + 2))],
        compiler_params=pltpu.CompilerParams(
            collective_id=3, has_side_effects=True, vmem_limit_bytes=60 * 1024 * 1024
        ),
        name="retreat",
    )(*early, *tables, *bulk, *late)


def on_device(
    tokens,
    w_query,
    w_key,
    w_value,
    w_ugate,
    w_output,
    w_left,
    w_right,
    w_down,
    decay_rate,
    cotangent,
):
    seq_count, group_len, model_width = tokens.shape
    head_count = decay_rate.shape[0]
    head_dim = model_width // head_count
    half_dim = head_dim // 2
    row_count = seq_count * group_len
    core = lax.axis_index("dp")

    shard = (w_left.T, w_right.T, w_down)
    grad_own = cotangent.reshape(row_count, model_width)

    position_block = lax.axis_index(("seq", "tensor"))
    places = (position_block * group_len + jnp.arange(group_len)).astype(F32)
    frequency = 10000.0 ** (-jnp.arange(half_dim, dtype=F32) / half_dim)
    angles = places[:, None] * frequency[None, :]
    cosine, sine_part = jnp.cos(angles), jnp.sin(angles)
    cosine = jnp.concatenate([cosine, cosine], axis=1)
    sine_part = jnp.concatenate([-sine_part, sine_part], axis=1)
    rows_in = tokens.reshape(row_count, model_width)
    depth = lax.axis_size("seq")
    width = lax.axis_size("tensor")
    rates = jnp.broadcast_to(decay_rate[:, None, None], (head_count, 1, group_len))
    blocks = jnp.arange(depth * width, dtype=F32)[:, None, None, None]
    powers = jnp.broadcast_to(
        jnp.exp(-decay_rate[None, :, None, None] * group_len * blocks),
        (depth * width, head_count, 1, head_dim),
    )
    (
        residual,
        rows_own,
        merged,
        query_pre,
        key_pre,
        ugate,
        normed_low,
        query_low,
        key_low,
        value_low,
        query_dec,
        key_dec,
        weights_low,
        gated_low,
        state_low,
        other,
        grad_nb,
    ) = attend(
        rows_in,
        (w_query, w_key, w_value, w_ugate, w_output),
        shard,
        grad_own,
        rates,
        powers,
        cosine,
        sine_part,
        seq_count,
        depth,
        width,
    )
    mixed, back, half_own, half_nb, back_in, first_y = hidden_part(
        rows_own, grad_own, grad_nb, shard, other
    )
    (
        grad_branch,
        grad_ugate_pre,
        grad_query_pre,
        grad_key_pre,
        grad_value_pre,
        grad_tokens,
        mixed_in,
        from_y,
    ) = retreat(
        (residual, back, back_in, grad_own, w_output, merged, ugate),
        (rates, powers, cosine, sine_part),
        (mixed, half_nb),
        (
            query_low,
            key_low,
            value_low,
            query_dec,
            weights_low,
            state_low,
            query_pre,
            w_query,
            w_ugate,
            key_dec,
            key_pre,
            w_key,
            w_value,
            rows_in,
        ),
        seq_count,
        depth,
        width,
    )

    hidden = w_down.shape[0]
    sums, hidden_sums = reduce_grads(
        (
            normed_low,
            gated_low,
            grad_query_pre,
            grad_key_pre,
            grad_value_pre,
            grad_ugate_pre,
            grad_branch,
        ),
        half_own,
        first_y,
        from_y,
        depth,
    )
    mixed_out = (
        residual + mixed[:row_count].astype(F32) + mixed_in.astype(F32)
    ).astype(BF16)
    attention_grads = tuple(
        sums[i * model_width : (i + 1) * model_width].astype(F32) for i in range(5)
    )
    left_sum, right_sum, down_sum = (
        hidden_sums[i * hidden : (i + 1) * hidden].astype(F32) for i in range(3)
    )
    return (
        (mixed_out.reshape(tokens.shape), grad_tokens.reshape(tokens.shape))
        + attention_grads
        + (left_sum.T, right_sum.T, down_sum)
    )


def solution(mesh):
    rows = P("dp", ("seq", "tensor"), None)
    columns = P(None, "tensor")
    return jax.shard_map(
        on_device,
        mesh=mesh,
        in_specs=(rows, P(), P(), P(), P(), P(), columns, columns, P("tensor", None), P(), rows),
        out_specs=(rows, rows, P(), P(), P(), P(), P(), columns, columns, P("tensor", None)),
        check_vma=False,
    )
```

```python
import functools

import jax
import jax.numpy as jnp
from jax import lax
from jax.experimental import pallas as pl
from jax.experimental.pallas import tpu as pltpu
from jax.sharding import PartitionSpec as P


EPS = 1e-06
F32 = jnp.float32
BF16 = jnp.bfloat16


CHUNK = 256
LAG = 1


def added(first, second):
    return (first.astype(F32) + second.astype(F32)).astype(BF16)


RING = 8


def reduce_kernel(
    depth,
    factors,
    pair_own,
    pair_first,
    pair_rest,
    out,
    pair_out,
    pair_in,
    left_side,
    right_side,
    own,
    core_in,
    first_in,
    second_in,
    line_in,
    line_mid,
    pair_line,
    pair_mid,
    sems,
    pair_sems,
    load_sem,
):
    core = lax.axis_index("dp")
    slot = lax.axis_index("tensor")
    place = lax.axis_index("seq")
    rows = out.shape[0]
    chunks = rows // CHUNK
    half, quarter, eighth = CHUNK // 2, CHUNK // 4, CHUNK // 8
    low_side = place < depth // 2
    outermost = (place == 0) | (place == depth - 1)
    middle = (place == depth // 2 - 1) | (place == depth // 2)
    inward = jnp.where(low_side, place + 1, place - 1)
    outward = jnp.where(low_side, place - 1, place + 1)

    barrier = pltpu.get_barrier_semaphore()

    def greet(peer):
        pl.semaphore_signal(
            barrier, inc=1, device_id=peer, device_id_type=pl.DeviceIdType.MESH
        )

    greet({"dp": 1 - core})
    greet({"tensor": slot ^ 1})
    greet({"tensor": slot ^ 2})

    @pl.when(place > 0)
    def _():
        greet({"seq": place - 1})

    @pl.when(place < depth - 1)
    def _():
        greet({"seq": place + 1})

    pl.semaphore_wait(barrier, jnp.where(outermost, 4, 5))

    def remote(source, target, sem, at, peer):
        return pltpu.make_async_remote_copy(
            src_ref=source,
            dst_ref=target,
            send_sem=sem.at[0, at],
            recv_sem=sem.at[1, at],
            device_id=peer,
            device_id_type=pl.DeviceIdType.MESH,
        )

    def span(start, size):
        return pl.ds(pl.multiple_of(start, size), size)

    def bits(q):
        first = jnp.where(q % 2 == 0, 1, 2)
        second = 3 - first
        return first, second, (slot & first) // first, (slot & second) // second

    def base(q):
        return pl.multiple_of(q * CHUNK, CHUNK)

    def to_core(q):
        return remote(
            own.at[q % RING, span((1 - core) * half, half)],
            core_in.at[q],
            sems.at[0],
            q,
            {"dp": 1 - core},
        )

    def to_first(q):
        first, _, f, _ = bits(q)
        return remote(
            core_in.at[q, span((1 - f) * quarter, quarter)],
            first_in.at[q],
            sems.at[1],
            q,
            {"tensor": slot ^ first},
        )

    def to_second(q):
        _, second, _, g = bits(q)
        return remote(
            first_in.at[q, span((1 - g) * eighth, eighth)],
            second_in.at[q],
            sems.at[2],
            q,
            {"tensor": slot ^ second},
        )

    def block(q):
        _, _, f, g = bits(q)
        return base(q) + core * half + f * quarter + g * eighth

    def back_second(q):
        _, second, _, _ = bits(q)
        at = span(block(q), eighth)
        return remote(out.at[at], out.at[at], sems.at[3], q, {"tensor": slot ^ second})

    def back_first(q):
        first, _, f, _ = bits(q)
        at = span(base(q) + core * half + f * quarter, quarter)
        return remote(out.at[at], out.at[at], sems.at[4], q, {"tensor": slot ^ first})

    def back_core(q):
        at = span(base(q) + core * half, half)
        return remote(out.at[at], out.at[at], sems.at[5], q, {"dp": 1 - core})

    class Line:
        def __init__(self, mine, came, met, total, sem, offset):
            self.mine, self.came, self.met, self.total = mine, came, met, total
            self.sem, self.offset = sem, offset

        def inwards(self, q, source):
            return remote(
                source, self.came(q), self.sem.at[self.offset], q, {"seq": inward}
            )

        def across(self, q):
            return remote(
                self.came(q),
                self.met(q),
                self.sem.at[self.offset + 1],
                q,
                {"seq": depth - 1 - place},
            )

        def outwards(self, q):
            return remote(
                self.total(q), self.total(q), self.sem.at[self.offset + 2], q, {"seq": outward}
            )

        def step_in(self, q):
            @pl.when(outermost)
            def _():
                self.inwards(q, self.mine(q)).start()

        def step_middle(self, q):
            @pl.when(jnp.logical_not(outermost))
            def _():
                self.inwards(q, self.mine(q)).wait_recv()
                came = self.came(q)
                came[...] = added(self.mine(q)[...], came[...])

                @pl.when(middle)
                def _():
                    self.across(q).start()

                @pl.when(jnp.logical_not(middle))
                def _():
                    self.inwards(q, came).start()

        def step_out(self, q):
            @pl.when(middle)
            def _():
                self.across(q).wait_recv()
                self.total(q)[...] = added(self.came(q)[...], self.met(q)[...])

            @pl.when(jnp.logical_not(outermost))
            def _():
                @pl.when(jnp.logical_not(middle))
                def _():
                    self.outwards(q).wait_recv()

                self.outwards(q).start()

        def step_last(self, q):
            @pl.when(outermost)
            def _():
                self.outwards(q).wait_recv()

        def settle(self, q):
            @pl.when(outermost)
            def _():
                self.inwards(q, self.mine(q)).wait_send()

            @pl.when(jnp.logical_not(outermost))
            def _():
                @pl.when(middle)
                def _():
                    self.across(q).wait_send()

                @pl.when(jnp.logical_not(middle))
                def _():
                    self.inwards(q, self.came(q)).wait_send()

                self.outwards(q).wait_send()

    def second_mine(q):
        return second_in.at[q]

    line = Line(
        second_mine,
        lambda q: line_in.at[q],
        lambda q: line_mid.at[q],
        lambda q: out.at[span(block(q), eighth)],
        sems,
        6,
    )
    pair_chunks, pair_rows, pair_cols = pair_line.shape
    pair = Line(
        lambda q: pair_in.at[span(q * pair_rows, pair_rows)],
        lambda q: pair_line.at[q],
        lambda q: pair_mid.at[q],
        lambda q: pair_out.at[span(q * pair_rows, pair_rows), span(core * pair_cols, pair_cols)],
        pair_sems,
        0,
    )

    def pair_core(q):
        return remote(pair.total(q), pair.total(q), pair_sems.at[3], q, {"dp": 1 - core})

    rights = len(factors) - 2
    loads = [
        pltpu.make_async_copy(g, t, load_sem.at[i])
        for i, (g, t) in enumerate(
            zip(
                factors,
                [left_side.at[0], left_side.at[1]] + [right_side.at[i] for i in range(rights)],
            )
        )
    ]
    for load in loads:
        load.start()
    for load in loads:
        load.wait()
    per_matrix = chunks // rights

    def make(q):
        @pl.when(q >= RING)
        def _():
            to_core(q - RING).wait_send()

        m = q // per_matrix
        columns = pl.ds(pl.multiple_of((q % per_matrix) * CHUNK, CHUNK), CHUNK)
        own[q % RING] = times_rows(
            left_side[m // (rights - 1), :, columns], right_side[m]
        ).astype(BF16)

    hidden = pair_first.shape[0]
    for m in range(3):
        theirs = pair_first[...] if m == 0 else pair_rest[m - 1]
        pair_in[pl.ds(m * hidden, hidden)] = added(pair_own[m], theirs)

    def stage_a(q):
        to_core(q).wait_recv()
        came = core_in.at[q]
        came[...] = added(own[q % RING, span(core * half, half)], came[...])

    def stage_b(q):
        _, _, f, _ = bits(q)
        to_first(q).wait_recv()
        came = first_in.at[q]
        came[...] = added(core_in[q, span(f * quarter, quarter)], came[...])

    def stage_c(q):
        _, _, _, g = bits(q)
        to_second(q).wait_recv()
        came = second_in.at[q]
        came[...] = added(first_in[q, span(g * eighth, eighth)], came[...])

    pairs = chunks // 2

    def during(step, lag, count, action):
        i = step - lag

        @pl.when((i >= 0) & (i < count))
        def _():
            action(i)

    def both(action):
        def run(i):
            action(2 * i)
            action(2 * i + 1)

        return run

    def start(copy):
        return lambda q: copy(q).start()

    def arrived(copy, following):
        def run(q):
            copy(q).wait_recv()
            following(q).start()

        return run

    def last_then_second(q):
        line.step_last(q)
        back_second(q).start()

    def finish_pair(q):
        pair.step_last(q)
        pair_core(q).start()

    steps = max(pairs + 8 * LAG, pair_chunks + 3 * LAG) + 1

    @pl.loop(0, steps)
    def _(step):
        during(step, 8 * LAG, pairs, both(arrived(back_first, back_core)))
        during(step, 7 * LAG, pairs, both(arrived(back_second, back_first)))
        during(step, 6 * LAG, pairs, both(last_then_second))
        during(step, 5 * LAG, pairs, both(line.step_out))
        during(step, 4 * LAG, pairs, both(line.step_middle))
        during(step, 3 * LAG, pairs, both(stage_c))
        during(step, 2 * LAG, pairs, both(stage_b))
        during(step, LAG, pairs, both(stage_a))
        during(step, 3 * LAG, pairs, both(line.step_in))
        during(step, 2 * LAG, pairs, both(start(to_second)))
        during(step, LAG, pairs, both(start(to_first)))
        during(step, 0, pairs, both(make))
        during(step, 0, pairs, both(start(to_core)))
        during(step, 3 * LAG, pair_chunks, finish_pair)
        during(step, 2 * LAG, pair_chunks, pair.step_out)
        during(step, LAG, pair_chunks, pair.step_middle)
        during(step, 0, pair_chunks, pair.step_in)

    @pl.loop(0, chunks)
    def _(q):
        back_core(q).wait_recv()
        for copy in (to_first, to_second, back_second, back_first, back_core):
            copy(q).wait_send()

        @pl.when(q >= chunks - RING)
        def _():
            to_core(q).wait_send()

        line.settle(q)

    @pl.loop(0, pair_chunks)
    def _(q):
        pair_core(q).wait()
        pair.settle(q)


def reduce_grads(factors, half_own, first_y, rest_y, depth):
    count, width = factors[0].shape
    rights = len(factors) - 2
    rows = width * rights
    chunks = rows // CHUNK
    pair_chunks = 12
    total_rows, pair_cols = 3 * half_own.shape[1], half_own.shape[2]
    pair_rows = total_rows // pair_chunks
    vmem = pl.BlockSpec(memory_space=pltpu.VMEM)

    def body(*refs):
        reduce_kernel(depth, refs[: len(factors)], *refs[len(factors) :])

    return pl.pallas_call(
        body,
        out_shape=(
            jax.ShapeDtypeStruct((rows, width), BF16),
            jax.ShapeDtypeStruct((total_rows, 2 * pair_cols), BF16),
        ),
        in_specs=[pl.BlockSpec(memory_space=pl.ANY)] * len(factors) + [vmem] * 3,
        out_specs=(vmem, vmem),
        scratch_shapes=[
            pltpu.VMEM((total_rows, pair_cols), BF16),
            pltpu.VMEM((2, count, width), BF16),
            pltpu.VMEM((rights, count, width), BF16),
            pltpu.VMEM((RING, CHUNK, width), BF16),
            pltpu.VMEM((chunks, CHUNK // 2, width), BF16),
            pltpu.VMEM((chunks, CHUNK // 4, width), BF16),
            pltpu.VMEM((chunks, CHUNK // 8, width), BF16),
            pltpu.VMEM((chunks, CHUNK // 8, width), BF16),
            pltpu.VMEM((chunks, CHUNK // 8, width), BF16),
            pltpu.VMEM((pair_chunks, pair_rows, pair_cols), BF16),
            pltpu.VMEM((pair_chunks, pair_rows, pair_cols), BF16),
            pltpu.SemaphoreType.DMA((9, 2, chunks)),
            pltpu.SemaphoreType.DMA((4, 2, pair_chunks)),
            pltpu.SemaphoreType.DMA((len(factors),)),
        ],
        compiler_params=pltpu.CompilerParams(
            collective_id=1, has_side_effects=True, vmem_limit_bytes=50 * 1024 * 1024
        ),
        name="reduce_grads",
    )(*factors, half_own, first_y, rest_y)


ROWS = 256


def times(x, w):
    return jnp.dot(x, w, preferred_element_type=F32)


def times_back(x, w):
    return lax.dot_general(x, w, (((1,), (1,)), ((), ())), preferred_element_type=F32)


def times_rows(x, y):
    return lax.dot_general(x, y, (((0,), (0,)), ((), ())), preferred_element_type=F32)


def hidden_kernel(
    rows_own,
    grads_own,
    grads_nb,
    late_left,
    late_right,
    late_down,
    late_other,
    mixed,
    back,
    half_own,
    half_nb,
    back_in,
    from_y,
    both,
    own,
    other,
    kept,
    theirs,
    moved,
    acc_mixed,
    acc_back,
    load_sem,
    sems,
):
    core = lax.axis_index("dp")
    slot = lax.axis_index("tensor")
    count, width = rows_own.shape
    half = width // 2
    blocks = count // ROWS
    pairs = (
        (late_left, own.at[0]),
        (late_right, own.at[1]),
        (late_down, own.at[2]),
        (late_other, other),
        (rows_own, both.at[0, :count]),
        (grads_own, both.at[1, :count]),
        (grads_nb, both.at[1, count:]),
    )
    loads = [pltpu.make_async_copy(a, b, load_sem.at[i]) for i, (a, b) in enumerate(pairs)]
    for i in (4, 5, 0, 1, 2, 3, 6):
        loads[i].start()

    def send(source, target, at, peer):
        return pltpu.make_async_remote_copy(
            src_ref=source,
            dst_ref=target,
            send_sem=sems.at[0, at],
            recv_sem=sems.at[1, at],
            device_id=peer,
            device_id_type=MESH,
        )

    def span(i):
        return pl.ds(pl.multiple_of(i * ROWS, ROWS), ROWS)

    def out_rows(i):
        return send(
            rows_own.at[span(i)], both.at[0, span(blocks + i)], i, {"tensor": slot ^ 1}
        )

    def return_rows(i):
        return send(
            back.at[span(blocks + i)], back_in.at[span(i)], blocks + i, {"tensor": slot ^ 1}
        )

    def to_core(which, m):
        return send(
            theirs.at[which, m], moved.at[which, m], 2 * blocks + 3 * which + m, {"dp": 1 - core}
        )

    hand = send(half_nb.at[0], from_y, 2 * blocks + 6, {"tensor": slot ^ 2})
    barrier = pltpu.get_barrier_semaphore()
    for peer in ({"tensor": slot ^ 1}, {"tensor": slot ^ 2}, {"dp": 1 - core}):
        pl.semaphore_signal(barrier, inc=1, device_id=peer, device_id_type=MESH)
    pl.semaphore_wait(barrier, 3)
    for i in range(blocks):
        out_rows(i).start()
    for i in (4, 5, 0, 1, 2):
        loads[i].wait()

    def unit(i, which, weights):
        rows, grads = both[0, span(i)], both[1, span(i)]
        e1, e2 = times_back(rows, weights[0]), times_back(rows, weights[1])
        dm = times_back(grads, weights[2])
        mid = (e1 * e2).astype(BF16)
        de1 = (dm * e2).astype(BF16)
        de2 = (dm * e1).astype(BF16)
        kept[which, 2, span(i)] = mid
        kept[which, 0, span(i)] = de1
        kept[which, 1, span(i)] = de2
        return times(mid, weights[2]), times(de1, weights[0]) + times(de2, weights[1])

    @pl.loop(0, 2 * blocks)
    def _(i):
        @pl.when(i >= blocks)
        def _():
            out_rows(i - blocks).wait_recv()

        @pl.when(i == blocks)
        def _():
            loads[6].wait()

        acc_mixed[...], acc_back[...] = unit(i, 0, own)

        @pl.when(i == 0)
        def _():
            loads[3].wait()

        more_mixed, more_back = unit(i, 1, other)
        mixed[span(i)] = (acc_mixed[...] + more_mixed).astype(BF16)
        back[span(i)] = (acc_back[...] + more_back).astype(BF16)

        @pl.when(i >= blocks)
        def _():
            return_rows(i - blocks).start()

    here = pl.ds(pl.multiple_of(core * half, half), half)
    there = pl.ds(pl.multiple_of((1 - core) * half, half), half)

    def products(which, out, m):
        theirs[which, m] = times_rows(kept[which, m], both[m // 2, :, there]).astype(BF16)
        to_core(which, m).start()
        out[m] = times_rows(kept[which, m], both[m // 2, :, here]).astype(BF16)

    def combine(which, out, m):
        to_core(which, m).wait_recv()
        out[m] = added(out[m], moved[which, m])

    products(1, half_nb, 0)
    combine(1, half_nb, 0)
    hand.start()

    @pl.loop(1, 3)
    def _(m):
        products(1, half_nb, m)

    @pl.loop(0, 3)
    def _(m):
        products(0, half_own, m)

    for m in range(1, 3):
        combine(1, half_nb, m)
    for m in range(3):
        combine(0, half_own, m)
    for i in range(blocks):
        out_rows(i).wait_send()
        return_rows(i).wait()
    for which in range(2):
        for m in range(3):
            to_core(which, m).wait_send()
    hand.wait()


def hidden_part(rows_own, grads_own, grads_nb, shard, other):
    count, width = rows_own.shape
    hidden = shard[0].shape[0]
    vmem = pl.BlockSpec(memory_space=pltpu.VMEM)
    anywhere = pl.BlockSpec(memory_space=pl.ANY)
    half = jax.ShapeDtypeStruct((3, hidden, width // 2), BF16)
    two = jax.ShapeDtypeStruct((2 * count, width), BF16)
    return pl.pallas_call(
        hidden_kernel,
        out_shape=(
            two,
            two,
            half,
            half,
            jax.ShapeDtypeStruct((count, width), BF16),
            jax.ShapeDtypeStruct((hidden, width // 2), BF16),
        ),
        in_specs=[anywhere] * 7,
        out_specs=(vmem,) * 4 + (anywhere,) * 2,
        scratch_shapes=[
            pltpu.VMEM((2, 2 * count, width), BF16),
            pltpu.VMEM((3, hidden, width), BF16),
            pltpu.VMEM((3, hidden, width), BF16),
            pltpu.VMEM((2, 3, 2 * count, hidden), BF16),
            pltpu.VMEM((2, 3, hidden, width // 2), BF16),
            pltpu.VMEM((2, 3, hidden, width // 2), BF16),
            pltpu.VMEM((ROWS, width), F32),
            pltpu.VMEM((ROWS, width), F32),
            pltpu.SemaphoreType.DMA((7,)),
            pltpu.SemaphoreType.DMA((2, 2 * (count // ROWS) + 7)),
        ],
        compiler_params=pltpu.CompilerParams(
            collective_id=4, has_side_effects=True, vmem_limit_bytes=54 * 1024 * 1024
        ),
        name="hidden_part",
    )(rows_own, grads_own, grads_nb, *shard, other)


MESH = pl.DeviceIdType.MESH


class States:
    def __init__(self, depth, width, backward, powers, local, came, total, far, outs, states, sems):
        self.depth, self.width, self.backward, self.powers = depth, width, backward, powers
        self.local, self.came, self.total, self.far = local, came, total, far
        self.outs, self.states, self.sems = outs, states, sems
        self.slot = lax.axis_index("tensor")
        self.place = lax.axis_index("seq")
        self.share = local.shape[0] // width

    def greet(self, more=()):
        barrier = pltpu.get_barrier_semaphore()
        for peer in more:
            pl.semaphore_signal(barrier, inc=1, device_id=peer, device_id_type=MESH)
        for b in range(1, self.width):
            pl.semaphore_signal(
                barrier, inc=1, device_id={"tensor": self.slot ^ b}, device_id_type=MESH
            )
        for j in range(1, self.depth):
            peer = lax.rem(self.place + j, self.depth)
            pl.semaphore_signal(barrier, inc=1, device_id={"seq": peer}, device_id_type=MESH)
        pl.semaphore_wait(barrier, self.width + self.depth - 2 + len(more))

    def copy(self, source, target, at, peer):
        return pltpu.make_async_remote_copy(
            src_ref=source,
            dst_ref=target,
            send_sem=self.sems.at[0, at],
            recv_sem=self.sems.at[1, at],
            device_id=peer,
            device_id_type=MESH,
        )

    def group(self, slot):
        return pl.ds(slot * self.share, self.share)

    def to_peer(self, b):
        peer = self.slot ^ b
        return self.copy(
            self.local.at[self.group(peer)], self.came.at[b - 1], b - 1, {"tensor": peer}
        )

    def to_far(self, j):
        peer = self.place - j if self.backward else self.place + j
        return self.copy(self.total, self.far.at[j - 1], self.width + j - 2, {"seq": peer})

    def has_far(self, j):
        return self.place >= j if self.backward else self.place + j < self.depth

    def from_far(self, j):
        return self.place + j < self.depth if self.backward else self.place >= j

    def to_owner(self, d):
        at = self.width + self.depth - 2 + d - 1
        return self.copy(
            self.outs.at[d - 1],
            self.states.at[self.group(self.slot)],
            at,
            {"tensor": self.slot ^ d},
        )

    def power(self, count, head):
        return self.powers[count, head]

    def piece(self, b, k, s):
        if b == 0:
            return self.local[self.slot * self.share + k, s].astype(F32)
        return self.came[b - 1, k, s].astype(F32)

    def gather(self):
        for b in range(1, self.width):
            self.to_peer(b).wait_recv()
        for k in range(self.share):
            head = self.slot * self.share + k
            for s in range(self.local.shape[1]):
                value = 0.0
                for b in range(self.width):
                    spot = self.slot ^ b
                    left = spot if self.backward else self.width - 1 - spot
                    value = value + self.power(left, head) * self.piece(b, k, s)
                self.total[k, s] = value.astype(BF16)
        for j in range(1, self.depth):

            @pl.when(self.has_far(j))
            def _(j=j):
                self.to_far(j).start()

    def send_back(self, entering):
        for j in range(1, self.depth):

            @pl.when(self.from_far(j))
            def _(j=j):
                self.to_far(j).wait_recv()

            @pl.when(jnp.logical_not(self.from_far(j)))
            def _(j=j):
                self.far[j - 1] = jnp.zeros(self.far.shape[1:], BF16)

        for k in range(self.share):
            head = self.slot * self.share + k
            for s in range(self.local.shape[1]):
                value = 0.0
                for j in range(1, self.depth):
                    value = value + self.power(self.width * (j - 1), head) * self.far[
                        j - 1, k, s
                    ].astype(F32)
                entering[k, s] = value
        for d in list(range(1, self.width)) + [0]:
            target = self.slot ^ d
            inner = self.width - 1 - target if self.backward else target
            for k in range(self.share):
                head = self.slot * self.share + k
                for s in range(self.local.shape[1]):
                    value = self.power(inner, head) * entering[k, s]
                    for b in range(self.width):
                        if b == d:
                            continue
                        source = self.slot ^ b
                        gap = source - target - 1 if self.backward else target - source - 1
                        coef = jnp.where(gap >= 0, self.power(jnp.maximum(gap, 0), head), 0.0)
                        value = value + coef * self.piece(b, k, s)
                    if d == 0:
                        self.states[head, s] = value.astype(BF16)
                    else:
                        self.outs[d - 1, k, s] = value.astype(BF16)
        for d in range(1, self.width):
            self.to_owner(d).start()

    def arrive(self):
        for d in range(1, self.width):
            at = self.width + self.depth - 2 + d - 1
            self.copy(
                self.outs.at[d - 1],
                self.states.at[self.group(self.slot ^ d)],
                at,
                {"tensor": self.slot ^ d},
            ).wait_recv()

    def settle(self):
        for b in range(1, self.width):
            self.to_peer(b).wait_send()
            self.to_owner(b).wait_send()
        for j in range(1, self.depth):

            @pl.when(self.has_far(j))
            def _(j=j):
                self.to_far(j).wait_send()


def state_scratch(heads, seqs, head_dim, width, depth):
    share = heads // width
    low = functools.partial(pltpu.VMEM, dtype=BF16)
    return [
        low((heads, seqs, head_dim, head_dim)),
        low((width - 1, share, seqs, head_dim, head_dim)),
        low((share, seqs, head_dim, head_dim)),
        low((depth - 1, share, seqs, head_dim, head_dim)),
        low((width - 1, share, seqs, head_dim, head_dim)),
        pltpu.VMEM((share, seqs, head_dim, head_dim), F32),
        pltpu.SemaphoreType.DMA((2, 2 * (width - 1) + depth - 1)),
    ]


def turn(values, cosine, sine_part):
    return values * cosine + pltpu.roll(values, values.shape[-1] // 2, 1) * sine_part


def square_mean(values):
    return jnp.mean(values * values, axis=-1, keepdims=True)


def decays(rates, head, length, dim):
    rate = rates[head]
    place = lax.broadcasted_iota(jnp.int32, (length, dim), 0).astype(F32)
    query = jnp.exp(-rate[:, :dim] * (place + 1.0))
    key = jnp.exp(-rate[:, :dim] * (length - 1.0 - place))
    return query, key


def lag_decay(rates, head, length):
    lag = (
        lax.broadcasted_iota(jnp.int32, (length, length), 0)
        - lax.broadcasted_iota(jnp.int32, (length, length), 1)
    ).astype(F32)
    return jnp.where(lag >= 0, jnp.exp(-rates[head] * jnp.maximum(lag, 0.0)), 0.0)


def attend_kernel(
    depth,
    width,
    seqs,
    x,
    w_key,
    w_value,
    late_query,
    late_gate,
    late_output,
    left,
    right,
    down,
    grads,
    rates,
    powers,
    cosine,
    sine_part,
    residual,
    normed_two,
    attended,
    gated,
    states,
    early_outs,
    other,
    grads_nb,
    early,
    w_query,
    w_gate,
    w_output,
    local,
    came,
    total,
    far,
    outs,
    entering,
    sems,
    load_sem,
    bulk_sems,
    store_sem,
):
    (
        query_pre,
        key_pre,
        gate,
        normed_one,
        query_low,
        key_low,
        value_low,
        query_dec,
        key_dec,
        scores_low,
    ) = early
    stores = [
        pltpu.make_async_copy(a, b, store_sem.at[i])
        for i, (a, b) in enumerate(zip(early, early_outs))
    ]
    rows, model = x.shape
    length = rows // seqs
    dim = cosine.shape[1]
    tile = model // width
    loads = [
        pltpu.make_async_copy(a, b, load_sem.at[i])
        for i, (a, b) in enumerate(
            ((late_query, w_query), (late_gate, w_gate), (late_output, w_output))
        )
    ]
    for load in loads:
        load.start()
    exchange = States(
        depth, width, False, powers, local, came, total, far, outs, states, sems
    )
    core = lax.axis_index("dp")
    parity = lax.rem(exchange.place, 2)
    shard = (left, right, down)
    part_rows, part_cols = left.shape[0] // 2, model // 2
    columns_here = pl.ds(pl.multiple_of(core * part_cols, part_cols), part_cols)

    def rows_of(which):
        return pl.ds(pl.multiple_of(which * part_rows, part_rows), part_rows)

    def send(source, target, at, peer):
        return pltpu.make_async_remote_copy(
            src_ref=source,
            dst_ref=target,
            send_sem=bulk_sems.at[0, at],
            recv_sem=bulk_sems.at[1, at],
            device_id=peer,
            device_id_type=MESH,
        )

    def fetch(m):
        at = (rows_of(parity), columns_here)
        return send(
            shard[m].at[at], other.at[(m,) + at], m, {"tensor": exchange.slot ^ 2}
        )

    def relay(m):
        at = other.at[m, rows_of(parity), columns_here]
        return send(at, at, 3 + m, {"seq": exchange.place + 1 - 2 * parity})

    def share(m, which):
        spot = parity if which == 0 else 1 - parity
        at = other.at[m, rows_of(spot), columns_here]
        return send(at, at, 6 + 2 * m + which, {"dp": 1 - core})

    def cross(s):
        at = pl.ds(s * length, length)
        return send(grads.at[at], grads_nb.at[at], 12 + s, {"tensor": exchange.slot ^ 1})

    def pass_on(m):
        fetch(m).wait_recv()
        relay(m).start()
        share(m, 0).start()

    def pass_last(m):
        relay(m).wait_recv()
        share(m, 1).start()

    exchange.greet((({"dp": 1 - core}),))
    fetch(0).start()
    cross(0).start()
    fetch(1).start()
    for s in range(seqs):
        at = pl.ds(s * length, length)
        value = x[at].astype(F32)
        normed_one[at] = (value * lax.rsqrt(square_mean(value) + EPS)).astype(BF16)

    per_tile = tile // dim

    @pl.loop(1, width + 1)
    def _(step):
        b = lax.rem(step, width)
        spot = exchange.slot ^ b
        columns = pl.ds(pl.multiple_of(spot * tile, tile), tile)
        key_pre[:, columns] = times(normed_one[...], w_key[:, columns])
        value_low[:, columns] = times(normed_one[...], w_value[:, columns]).astype(BF16)
        for k in range(per_tile):
            head = spot * per_tile + k
            own = pl.ds(pl.multiple_of(spot * tile + k * dim, dim), dim)
            _, key_weight = decays(rates, head, length, dim)
            for s in range(seqs):
                at = pl.ds(s * length, length)
                turned = turn(jax.nn.silu(key_pre[at, own]), cosine[...], sine_part[...])
                key_low[at, own] = turned.astype(BF16)
                dec = (turned * key_weight).astype(BF16)
                key_dec[at, own] = dec
                local[head, s] = times_rows(dec, value_low[at, own]).astype(BF16)

        for b_static in range(1, width):

            @pl.when(b == b_static)
            def _(b_static=b_static):
                exchange.to_peer(b_static).start()

    for s in range(1, seqs):
        cross(s).start()
    fetch(2).start()
    pass_on(0)
    loads[0].wait()
    loads[1].wait()

    def inner(spot):
        columns = pl.ds(pl.multiple_of(spot * tile, tile), tile)
        query_pre[:, columns] = times(normed_one[...], w_query[:, columns])
        gate[:, columns] = times(normed_one[...], w_gate[:, columns])
        for k in range(per_tile):
            head = spot * per_tile + k
            own = pl.ds(pl.multiple_of(spot * tile + k * dim, dim), dim)
            query_weight, _ = decays(rates, head, length, dim)
            mask = lag_decay(rates, head, length)
            for s in range(seqs):
                at = pl.ds(s * length, length)
                turned = turn(jax.nn.silu(query_pre[at, own]), cosine[...], sine_part[...])
                low_query = turned.astype(BF16)
                query_low[at, own] = low_query
                query_dec[at, own] = (turned * query_weight).astype(BF16)
                low_scores = (times_back(low_query, key_low[at, own]) * mask).astype(BF16)
                scores_low[head, s] = low_scores
                attended[at, own] = times(low_scores, value_low[at, own])

    half = width // 2

    @pl.loop(0, half)
    def _(spot):
        inner(spot)

    exchange.gather()

    @pl.loop(half, width)
    def _(spot):
        inner(spot)

    exchange.send_back(entering)
    for store in stores:
        store.start()
    pass_on(1)
    pass_on(2)
    pass_last(0)
    loads[2].wait()
    exchange.arrive()
    pass_last(1)

    @pl.loop(0, width * per_tile)
    def _(head):
        own = pl.ds(pl.multiple_of(head * dim, dim), dim)
        for s in range(seqs):
            at = pl.ds(s * length, length)
            attended[at, own] += times(query_dec[at, own], states[head, s])

    for s in range(seqs):
        at = pl.ds(s * length, length)
        value = attended[at]
        gated[at] = (value * lax.rsqrt(square_mean(value) + EPS) * gate[at]).astype(BF16)

    @pl.loop(0, width)
    def _(spot):
        columns = pl.ds(pl.multiple_of(spot * tile, tile), tile)
        residual[:, columns] = x[:, columns].astype(F32) + times(
            gated[...], w_output[:, columns]
        )

    for s in range(seqs):
        at = pl.ds(s * length, length)
        value = residual[at]
        normed_two[at] = (value * lax.rsqrt(square_mean(value) + EPS)).astype(BF16)
    pass_last(2)
    for store in stores:
        store.wait()
    exchange.settle()
    for m in range(3):
        fetch(m).wait_send()
        relay(m).wait_send()
        share(m, 0).wait()
        share(m, 1).wait()
    for s in range(seqs):
        cross(s).wait()


def attend(x, weights, shard, grads, rates, powers, cosine, sine_part, seqs, depth, width):
    rows, model = x.shape
    heads = rates.shape[0]
    dim = model // heads
    length = rows // seqs
    vmem = pl.BlockSpec(memory_space=pltpu.VMEM)
    anywhere = pl.BlockSpec(memory_space=pl.ANY)
    wide = jax.ShapeDtypeStruct((rows, model), F32)
    low = jax.ShapeDtypeStruct((rows, model), BF16)
    w_query, w_key, w_value, w_gate, w_output = weights
    early = (wide,) * 3 + (low,) * 6 + (
        jax.ShapeDtypeStruct((heads, seqs, length, length), BF16),
    )

    def body(*refs):
        at = 14 + 5
        kept = at + len(early)
        scratch = kept + 2
        attend_kernel(
            depth,
            width,
            seqs,
            *refs[:at],
            refs[at:kept],
            *refs[kept:scratch],
            refs[scratch : scratch + len(early)],
            *refs[scratch + len(early) :],
        )

    return pl.pallas_call(
        body,
        out_shape=(
            wide,
            low,
            wide,
            low,
            jax.ShapeDtypeStruct((heads, seqs, dim, dim), BF16),
        )
        + early
        + (jax.ShapeDtypeStruct((3,) + shard[0].shape, BF16), low),
        in_specs=[vmem] * 3 + [anywhere] * 7 + [vmem] * 4,
        out_specs=(vmem,) * 5 + (anywhere,) * (len(early) + 2),
        scratch_shapes=[pltpu.VMEM(v.shape, v.dtype) for v in early]
        + [pltpu.VMEM((model, model), BF16)] * 3
        + state_scratch(heads, seqs, dim, width, depth)
        + [
            pltpu.SemaphoreType.DMA((3,)),
            pltpu.SemaphoreType.DMA((2, 12 + seqs)),
            pltpu.SemaphoreType.DMA((len(early),)),
        ],
        compiler_params=pltpu.CompilerParams(
            collective_id=2, has_side_effects=True, vmem_limit_bytes=56 * 1024 * 1024
        ),
        name="attend",
    )(
        x,
        w_key,
        w_value,
        w_query,
        w_gate,
        w_output,
        *shard,
        grads,
        rates,
        powers,
        cosine,
        sine_part,
    )


def retreat_kernel(
    depth,
    width,
    seqs,
    residual,
    back_own,
    back_in,
    grads,
    rates,
    powers,
    cosine,
    sine_part,
    mixed_nb,
    half_nb,
    *rest,
):
    late = rest[:17]
    (
        grad_mid_low,
        gate_low,
        query_out,
        key_out,
        value_out,
        grad_tokens,
        mixed_in,
        from_y,
    ) = rest[17:25]
    held = rest[25:42]
    (
        w_output,
        attended,
        gate,
        query_low,
        key_low,
        value_low,
        query_dec,
        scores_low,
        states_in,
        query_pre,
        w_query,
        w_gate,
        key_dec,
        key_pre,
        w_key,
        w_value,
        x,
    ) = held
    (
        states,
        grad_mid,
        work,
        grad_att,
        value_part,
        key_part,
        local,
        came,
        total,
        far,
        outs,
        entering,
        sems,
        load_sem,
        bulk_sems,
    ) = rest[42:]
    rows, model = residual.shape
    length = rows // seqs
    dim = cosine.shape[1]
    tile = model // width
    per_tile = tile // dim
    loads = [
        pltpu.make_async_copy(a, b, load_sem.at[i]) for i, (a, b) in enumerate(zip(late, held))
    ]
    for load in loads:
        load.start()
    exchange = States(
        depth, width, True, powers, local, came, total, far, outs, states, sems
    )

    def send(source, target, at, peer):
        return pltpu.make_async_remote_copy(
            src_ref=source,
            dst_ref=target,
            send_sem=bulk_sems.at[0, at],
            recv_sem=bulk_sems.at[1, at],
            device_id=peer,
            device_id_type=MESH,
        )

    crosses, hands = 4, 8
    cross_rows, hand_rows = rows // crosses, 2 * half_nb.shape[1] // hands

    def cross(k):
        at = pl.ds(k * cross_rows, cross_rows)
        source = mixed_nb.at[pl.ds(rows + k * cross_rows, cross_rows)]
        return send(source, mixed_in.at[at], k, {"tensor": exchange.slot ^ 1})

    def hand(k):
        m, at = k // (hands // 2), pl.ds(k % (hands // 2) * hand_rows, hand_rows)
        return send(
            half_nb.at[m + 1, at], from_y.at[m, at], crosses + k, {"tensor": exchange.slot ^ 2}
        )

    def start_bulk(some_crosses, some_hands):
        for k in some_crosses:
            cross(k).start()
        for k in some_hands:
            hand(k).start()

    exchange.greet()
    start_bulk(range(1), range(2))

    def spans():
        return [pl.ds(s * length, length) for s in range(seqs)]

    for at in spans():
        value = residual[at]
        scale = lax.rsqrt(square_mean(value) + EPS)
        normed = value * scale
        grad = back_own[at].astype(F32) + back_in[at].astype(F32)
        grad = grads[at].astype(F32) + scale * (
            grad - normed * jnp.mean(grad * normed, axis=-1, keepdims=True)
        )
        grad_mid[at] = grad
        grad_mid_low[at] = grad.astype(BF16)

    def columns_of(spot):
        return pl.ds(pl.multiple_of(spot * tile, tile), tile)

    for load in loads[:3]:
        load.wait()

    @pl.loop(0, width)
    def _(spot):
        work[:, columns_of(spot)] = times_back(grad_mid_low[...], w_output[columns_of(spot)])

    for at in spans():
        value = attended[at]
        scale = lax.rsqrt(square_mean(value) + EPS)
        normed = value * scale
        grad = work[at]
        gate_low[at] = (grad * normed).astype(BF16)
        grad = grad * gate[at]
        grad_att[at] = (
            scale * (grad - normed * jnp.mean(grad * normed, axis=-1, keepdims=True))
        ).astype(BF16)

    for load in loads[3:10]:
        load.wait()

    @pl.loop(1, width + 1)
    def _(step):
        b = lax.rem(step, width)
        spot = exchange.slot ^ b
        for k in range(per_tile):
            own = pl.ds(pl.multiple_of(spot * tile + k * dim, dim), dim)
            for s, at in enumerate(spans()):
                local[spot * per_tile + k, s] = times_rows(
                    query_dec[at, own], grad_att[at, own]
                ).astype(BF16)

        for b_static in range(1, width):

            @pl.when(b == b_static)
            def _(b_static=b_static):
                exchange.to_peer(b_static).start()

    start_bulk(range(1, 3), range(2, 5))

    def slope(values):
        sigmoid_v = jax.nn.sigmoid(values)
        return sigmoid_v * (1.0 + values * (1.0 - sigmoid_v))

    def inner(spot):
        for k in range(per_tile):
            head = spot * per_tile + k
            own = pl.ds(pl.multiple_of(spot * tile + k * dim, dim), dim)
            query_weight, _ = decays(rates, head, length, dim)
            mask = lag_decay(rates, head, length)
            for s, at in enumerate(spans()):
                grad = grad_att[at, own]
                value_part[at, own] = times_rows(scores_low[head, s], grad)
                score = (times_back(grad, value_low[at, own]) * mask).astype(BF16)
                key_part[at, own] = times_rows(score, query_low[at, own])
                turned = times(score, key_low[at, own]) + query_weight * times_back(
                    grad, states_in[head, s]
                )
                query_out[at, own] = (
                    turn(turned, cosine[...], -sine_part[...]) * slope(query_pre[at, own])
                ).astype(BF16)

    half = width // 2

    @pl.loop(0, half)
    def _(spot):
        inner(spot)

    exchange.gather()

    @pl.loop(half, width)
    def _(spot):
        inner(spot)

    exchange.send_back(entering)
    start_bulk(range(3, crosses), range(5, hands))
    for load in loads[10:]:
        load.wait()

    @pl.loop(0, width)
    def _(spot):
        at = columns_of(spot)
        work[:, at] = times_back(query_out[...], w_query[at]) + times_back(
            gate_low[...], w_gate[at]
        )

    exchange.arrive()

    @pl.loop(0, width * per_tile)
    def _(head):
        own = pl.ds(pl.multiple_of(head * dim, dim), dim)
        _, key_weight = decays(rates, head, length, dim)
        for s, at in enumerate(spans()):
            state = states[head, s]
            value_out[at, own] = (
                value_part[at, own] + times(key_dec[at, own], state)
            ).astype(BF16)
            turned = key_part[at, own] + key_weight * times_back(value_low[at, own], state)
            key_out[at, own] = (
                turn(turned, cosine[...], -sine_part[...]) * slope(key_pre[at, own])
            ).astype(BF16)

    @pl.loop(0, width)
    def _(spot):
        at = columns_of(spot)
        work[:, at] += times_back(key_out[...], w_key[at]) + times_back(
            value_out[...], w_value[at]
        )

    for at in spans():
        value = x[at].astype(F32)
        scale = lax.rsqrt(square_mean(value) + EPS)
        normed = value * scale
        grad = work[at]
        grad_tokens[at] = grad_mid[at] + scale * (
            grad - normed * jnp.mean(grad * normed, axis=-1, keepdims=True)
        )
    exchange.settle()
    for k in range(crosses):
        cross(k).wait()
    for k in range(hands):
        hand(k).wait()


def retreat(early, tables, bulk, late, seqs, depth, width):
    rows, model = early[0].shape
    heads = tables[0].shape[0]
    dim = model // heads
    vmem = pl.BlockSpec(memory_space=pltpu.VMEM)
    anywhere = pl.BlockSpec(memory_space=pl.ANY)
    wide = jax.ShapeDtypeStruct((rows, model), F32)
    low = jax.ShapeDtypeStruct((rows, model), BF16)
    return pl.pallas_call(
        functools.partial(retreat_kernel, depth, width, seqs),
        out_shape=(low,) * 5 + (wide, low, jax.ShapeDtypeStruct((2,) + bulk[1].shape[1:], BF16)),
        in_specs=[vmem] * (len(early) + len(tables)) + [anywhere] * (len(bulk) + len(late)),
        out_specs=(vmem,) * 6 + (anywhere,) * 2,
        scratch_shapes=[pltpu.VMEM(v.shape, v.dtype) for v in late]
        + [
            pltpu.VMEM((heads, seqs, dim, dim), BF16),
            pltpu.VMEM((rows, model), F32),
            pltpu.VMEM((rows, model), F32),
            pltpu.VMEM((rows, model), BF16),
            pltpu.VMEM((rows, model), F32),
            pltpu.VMEM((rows, model), F32),
        ]
        + state_scratch(heads, seqs, dim, width, depth)
        + [pltpu.SemaphoreType.DMA((len(late),)), pltpu.SemaphoreType.DMA((2, 12))],
        compiler_params=pltpu.CompilerParams(
            collective_id=3, has_side_effects=True, vmem_limit_bytes=60 * 1024 * 1024
        ),
        name="retreat",
    )(*early, *tables, *bulk, *late)


def on_device(
    tokens,
    w_query,
    w_key,
    w_value,
    w_ugate,
    w_output,
    w_left,
    w_right,
    w_down,
    decay_rate,
    cotangent,
):
    seq_count, group_len, model_width = tokens.shape
    head_count = decay_rate.shape[0]
    head_dim = model_width // head_count
    half_dim = head_dim // 2
    row_count = seq_count * group_len
    core = lax.axis_index("dp")

    shard = (w_left.T, w_right.T, w_down)
    grad_own = cotangent.reshape(row_count, model_width)

    position_block = lax.axis_index(("seq", "tensor"))
    places = (position_block * group_len + jnp.arange(group_len)).astype(F32)
    frequency = 10000.0 ** (-jnp.arange(half_dim, dtype=F32) / half_dim)
    angles = places[:, None] * frequency[None, :]
    cosine, sine_part = jnp.cos(angles), jnp.sin(angles)
    cosine = jnp.concatenate([cosine, cosine], axis=1)
    sine_part = jnp.concatenate([-sine_part, sine_part], axis=1)
    rows_in = tokens.reshape(row_count, model_width)
    depth = lax.axis_size("seq")
    width = lax.axis_size("tensor")
    rates = jnp.broadcast_to(decay_rate[:, None, None], (head_count, 1, group_len))
    blocks = jnp.arange(depth * width, dtype=F32)[:, None, None, None]
    powers = jnp.broadcast_to(
        jnp.exp(-decay_rate[None, :, None, None] * group_len * blocks),
        (depth * width, head_count, 1, head_dim),
    )
    (
        residual,
        rows_own,
        merged,
        gated_low,
        state_low,
        query_pre,
        key_pre,
        ugate,
        normed_low,
        query_low,
        key_low,
        value_low,
        query_dec,
        key_dec,
        weights_low,
        other,
        grad_nb,
    ) = attend(
        rows_in,
        (w_query, w_key, w_value, w_ugate, w_output),
        shard,
        grad_own,
        rates,
        powers,
        cosine,
        sine_part,
        seq_count,
        depth,
        width,
    )
    mixed, back, half_own, half_nb, back_in, first_y = hidden_part(
        rows_own, grad_own, grad_nb, shard, other
    )
    (
        grad_branch,
        grad_ugate_pre,
        grad_query_pre,
        grad_key_pre,
        grad_value_pre,
        grad_tokens,
        mixed_in,
        from_y,
    ) = retreat(
        (residual, back, back_in, grad_own),
        (rates, powers, cosine, sine_part),
        (mixed, half_nb),
        (
            w_output,
            merged,
            ugate,
            query_low,
            key_low,
            value_low,
            query_dec,
            weights_low,
            state_low,
            query_pre,
            w_query,
            w_ugate,
            key_dec,
            key_pre,
            w_key,
            w_value,
            rows_in,
        ),
        seq_count,
        depth,
        width,
    )

    hidden = w_down.shape[0]
    sums, hidden_sums = reduce_grads(
        (
            normed_low,
            gated_low,
            grad_query_pre,
            grad_key_pre,
            grad_value_pre,
            grad_ugate_pre,
            grad_branch,
        ),
        half_own,
        first_y,
        from_y,
        depth,
    )
    mixed_out = (
        residual + mixed[:row_count].astype(F32) + mixed_in.astype(F32)
    ).astype(BF16)
    attention_grads = tuple(
        sums[i * model_width : (i + 1) * model_width].astype(F32) for i in range(5)
    )
    left_sum, right_sum, down_sum = (
        hidden_sums[i * hidden : (i + 1) * hidden].astype(F32) for i in range(3)
    )
    return (
        (mixed_out.reshape(tokens.shape), grad_tokens.reshape(tokens.shape))
        + attention_grads
        + (left_sum.T, right_sum.T, down_sum)
    )


def solution(mesh):
    rows = P("dp", ("seq", "tensor"), None)
    columns = P(None, "tensor")
    return jax.shard_map(
        on_device,
        mesh=mesh,
        in_specs=(rows, P(), P(), P(), P(), P(), columns, columns, P("tensor", None), P(), rows),
        out_specs=(rows, rows, P(), P(), P(), P(), P(), columns, columns, P("tensor", None)),
        check_vma=False,
    )
```

```python
import functools

import jax
import jax.numpy as jnp
from jax import lax
from jax.experimental import pallas as pl
from jax.experimental.pallas import tpu as pltpu
from jax.sharding import PartitionSpec as P


EPS = 1e-06
F32 = jnp.float32
BF16 = jnp.bfloat16


CHUNK = 256
LAG = 1


def added(first, second):
    return (first.astype(F32) + second.astype(F32)).astype(BF16)


RING = 8


def reduce_kernel(
    depth,
    factors,
    pair_own,
    pair_first,
    pair_rest,
    residual,
    mixed_own,
    mixed_nb,
    out,
    pair_out,
    mixed_out,
    pair_in,
    left_side,
    right_side,
    own,
    core_in,
    first_in,
    second_in,
    line_in,
    line_mid,
    pair_line,
    pair_mid,
    sems,
    pair_sems,
    load_sem,
    keep_sem,
    pair_keep_sem,
    base_part,
    mixed_part,
    pair_more,
    share_sem,
):
    core = lax.axis_index("dp")
    slot = lax.axis_index("tensor")
    place = lax.axis_index("seq")
    rows = out.shape[0]
    chunks = rows // CHUNK
    half, quarter, eighth = CHUNK // 2, CHUNK // 4, CHUNK // 8
    low_side = place < depth // 2
    outermost = (place == 0) | (place == depth - 1)
    middle = (place == depth // 2 - 1) | (place == depth // 2)
    inward = jnp.where(low_side, place + 1, place - 1)
    outward = jnp.where(low_side, place - 1, place + 1)

    barrier = pltpu.get_barrier_semaphore()

    def greet(peer):
        pl.semaphore_signal(
            barrier, inc=1, device_id=peer, device_id_type=pl.DeviceIdType.MESH
        )

    greet({"dp": 1 - core})
    greet({"tensor": slot ^ 1})
    greet({"tensor": slot ^ 2})

    @pl.when(place > 0)
    def _():
        greet({"seq": place - 1})

    @pl.when(place < depth - 1)
    def _():
        greet({"seq": place + 1})

    pl.semaphore_wait(barrier, jnp.where(outermost, 4, 5))

    def remote(source, target, sem, at, peer):
        return pltpu.make_async_remote_copy(
            src_ref=source,
            dst_ref=target,
            send_sem=sem.at[0, at],
            recv_sem=sem.at[1, at],
            device_id=peer,
            device_id_type=pl.DeviceIdType.MESH,
        )

    def span(start, size):
        return pl.ds(pl.multiple_of(start, size), size)

    def bits(q):
        first = jnp.where(q % 2 == 0, 1, 2)
        second = 3 - first
        return first, second, (slot & first) // first, (slot & second) // second

    def base(q):
        return pl.multiple_of(q * CHUNK, CHUNK)

    def to_core(q):
        return remote(
            own.at[q % RING, span((1 - core) * half, half)],
            core_in.at[q],
            sems.at[0],
            q,
            {"dp": 1 - core},
        )

    def to_first(q):
        first, _, f, _ = bits(q)
        return remote(
            core_in.at[q, span((1 - f) * quarter, quarter)],
            first_in.at[q],
            sems.at[1],
            q,
            {"tensor": slot ^ first},
        )

    def to_second(q):
        _, second, _, g = bits(q)
        return remote(
            first_in.at[q, span((1 - g) * eighth, eighth)],
            second_in.at[q],
            sems.at[2],
            q,
            {"tensor": slot ^ second},
        )

    def block(q):
        _, _, f, g = bits(q)
        return base(q) + core * half + f * quarter + g * eighth

    def keep(q):
        return pltpu.make_async_copy(
            line_mid.at[q], out.at[span(block(q), eighth)], keep_sem.at[q]
        )

    def back_second(q):
        _, second, _, _ = bits(q)
        at = span(block(q), eighth)
        return remote(line_mid.at[q], out.at[at], sems.at[3], q, {"tensor": slot ^ second})

    def back_first(q):
        first, _, f, _ = bits(q)
        at = span(base(q) + core * half + f * quarter, quarter)
        return remote(out.at[at], out.at[at], sems.at[4], q, {"tensor": slot ^ first})

    def back_core(q):
        at = span(base(q) + core * half, half)
        return remote(out.at[at], out.at[at], sems.at[5], q, {"dp": 1 - core})

    class Line:
        def __init__(self, mine, came, met, sem, offset):
            self.mine, self.came, self.met = mine, came, met
            self.sem, self.offset = sem, offset

        def inwards(self, q, source):
            return remote(
                source, self.came(q), self.sem.at[self.offset], q, {"seq": inward}
            )

        def across(self, q):
            return remote(
                self.came(q),
                self.met(q),
                self.sem.at[self.offset + 1],
                q,
                {"seq": depth - 1 - place},
            )

        def outwards(self, q):
            return remote(
                self.met(q), self.met(q), self.sem.at[self.offset + 2], q, {"seq": outward}
            )

        def step_in(self, q):
            @pl.when(outermost)
            def _():
                self.inwards(q, self.mine(q)).start()

        def step_middle(self, q):
            @pl.when(jnp.logical_not(outermost))
            def _():
                self.inwards(q, self.mine(q)).wait_recv()
                came = self.came(q)
                came[...] = added(self.mine(q)[...], came[...])

                @pl.when(middle)
                def _():
                    self.across(q).start()

                @pl.when(jnp.logical_not(middle))
                def _():
                    self.inwards(q, came).start()

        def step_out(self, q):
            @pl.when(middle)
            def _():
                self.across(q).wait_recv()
                met = self.met(q)
                met[...] = added(self.came(q)[...], met[...])

            @pl.when(jnp.logical_not(outermost))
            def _():
                @pl.when(jnp.logical_not(middle))
                def _():
                    self.outwards(q).wait_recv()

                self.outwards(q).start()

        def step_last(self, q):
            @pl.when(outermost)
            def _():
                self.outwards(q).wait_recv()

        def settle(self, q):
            @pl.when(outermost)
            def _():
                self.inwards(q, self.mine(q)).wait_send()

            @pl.when(jnp.logical_not(outermost))
            def _():
                @pl.when(middle)
                def _():
                    self.across(q).wait_send()

                @pl.when(jnp.logical_not(middle))
                def _():
                    self.inwards(q, self.came(q)).wait_send()

                self.outwards(q).wait_send()

    def second_mine(q):
        return second_in.at[q]

    line = Line(
        second_mine,
        lambda q: line_in.at[q],
        lambda q: line_mid.at[q],
        sems,
        6,
    )
    pair_chunks, pair_rows, pair_cols = pair_line.shape
    pair = Line(
        lambda q: pair_in.at[span(q * pair_rows, pair_rows)],
        lambda q: pair_line.at[q],
        lambda q: pair_mid.at[q],
        pair_sems,
        0,
    )

    def pair_block(q):
        return pair_out.at[span(q * pair_rows, pair_rows), span(core * pair_cols, pair_cols)]

    def pair_keep(q):
        return pltpu.make_async_copy(pair_mid.at[q], pair_block(q), pair_keep_sem.at[q])

    def pair_core(q):
        return remote(pair_mid.at[q], pair_block(q), pair_sems.at[3], q, {"dp": 1 - core})

    rights = len(factors) - 2
    loads = [
        pltpu.make_async_copy(g, t, load_sem.at[i])
        for i, (g, t) in enumerate(
            zip(
                factors,
                [left_side.at[0], left_side.at[1]] + [right_side.at[i] for i in range(rights)],
            )
        )
    ]
    tokens = residual.shape[0]
    parts = [
        pltpu.make_async_copy(a, b, load_sem.at[len(factors) + i])
        for i, (a, b) in enumerate(
            (
                (residual, base_part),
                (mixed_own.at[:tokens], mixed_part.at[0]),
                (mixed_nb, mixed_part.at[1]),
            )
        )
    ]
    hidden = pair_first.shape[0]
    thirds = [pl.ds(m * hidden, hidden) for m in range(3)]
    shares = [
        pltpu.make_async_copy(pair_own.at[m], pair_in.at[thirds[m]], share_sem.at[0, m])
        for m in range(3)
    ] + [
        pltpu.make_async_copy(
            pair_first if m == 0 else pair_rest.at[m - 1],
            pair_more.at[thirds[m]],
            share_sem.at[1, m],
        )
        for m in range(3)
    ]
    for load in [loads[0], loads[2]] + shares + [loads[1]] + loads[3:] + parts:
        load.start()
    per_matrix = chunks // rights

    def make(q):
        @pl.when(q >= RING)
        def _():
            to_core(q - RING).wait_send()

        m = q // per_matrix
        columns = pl.ds(pl.multiple_of((q % per_matrix) * CHUNK, CHUNK), CHUNK)
        own[q % RING] = times_rows(
            left_side[m // (rights - 1), :, columns], right_side[m]
        ).astype(BF16)

    def stage_a(q):
        to_core(q).wait_recv()
        came = core_in.at[q]
        came[...] = added(own[q % RING, span(core * half, half)], came[...])

    def stage_b(q):
        _, _, f, _ = bits(q)
        to_first(q).wait_recv()
        came = first_in.at[q]
        came[...] = added(core_in[q, span(f * quarter, quarter)], came[...])

    def stage_c(q):
        _, _, _, g = bits(q)
        to_second(q).wait_recv()
        came = second_in.at[q]
        came[...] = added(first_in[q, span(g * eighth, eighth)], came[...])

    pairs = chunks // 2

    def during(step, lag, count, action):
        i = step - lag

        @pl.when((i >= 0) & (i < count))
        def _():
            action(i)

    def both(action):
        def run(i):
            action(2 * i)
            action(2 * i + 1)

        return run

    def start(copy):
        return lambda q: copy(q).start()

    def arrived(copy, following):
        def run(q):
            copy(q).wait_recv()
            following(q).start()

        return run

    def last_then_second(q):
        line.step_last(q)
        keep(q).start()
        back_second(q).start()

    def second_arrived(q):
        back_second(q).wait_recv()
        keep(q).wait()
        back_first(q).start()

    def finish_pair(q):
        pair.step_last(q)
        pair_keep(q).start()
        pair_core(q).start()

    late = 2
    steps = max(pairs + 8 * LAG, pair_chunks + 3 * LAG + late) + 1

    @pl.loop(0, steps)
    def _(step):
        during(step, 8 * LAG, pairs, both(arrived(back_first, back_core)))
        during(step, 7 * LAG, pairs, both(second_arrived))
        during(step, 6 * LAG, pairs, both(last_then_second))
        during(step, 5 * LAG, pairs, both(line.step_out))
        during(step, 4 * LAG, pairs, both(line.step_middle))
        during(step, 3 * LAG, pairs, both(stage_c))
        during(step, 2 * LAG, pairs, both(stage_b))
        during(step, LAG, pairs, both(stage_a))
        during(step, 3 * LAG, pairs, both(line.step_in))
        during(step, 2 * LAG, pairs, both(start(to_second)))
        during(step, LAG, pairs, both(start(to_first)))
        for m in range(rights):

            @pl.when(step == m * per_matrix // 2)
            def _(m=m):
                loads[2 + m].wait()
                if m == 0:
                    loads[0].wait()
                if m == rights - 1:
                    loads[1].wait()

        during(step, 0, pairs, both(make))
        during(step, 0, pairs, both(start(to_core)))

        @pl.when(step == 1)
        def _():
            for share in shares:
                share.wait()
            for at in thirds:
                pair_in[at] = added(pair_in[at], pair_more[at])

        @pl.when(step == 3)
        def _():
            for part in parts:
                part.wait()
            mixed_out[...] = (
                base_part[...] + mixed_part[0].astype(F32) + mixed_part[1].astype(F32)
            ).astype(BF16)

        during(step, 3 * LAG + late, pair_chunks, finish_pair)
        during(step, 2 * LAG + late, pair_chunks, pair.step_out)
        during(step, LAG + late, pair_chunks, pair.step_middle)
        during(step, late, pair_chunks, pair.step_in)

    @pl.loop(0, chunks)
    def _(q):
        back_core(q).wait_recv()
        for copy in (to_first, to_second, back_second, back_first, back_core):
            copy(q).wait_send()

        @pl.when(q >= chunks - RING)
        def _():
            to_core(q).wait_send()

        line.settle(q)

    @pl.loop(0, pair_chunks)
    def _(q):
        pair_core(q).wait()
        pair_keep(q).wait()
        pair.settle(q)


def reduce_grads(factors, half_own, first_y, rest_y, mixed, depth):
    count, width = factors[0].shape
    rights = len(factors) - 2
    rows = width * rights
    chunks = rows // CHUNK
    pair_chunks = 12
    total_rows, pair_cols = 3 * half_own.shape[1], half_own.shape[2]
    pair_rows = total_rows // pair_chunks
    vmem = pl.BlockSpec(memory_space=pltpu.VMEM)
    anywhere = pl.BlockSpec(memory_space=pl.ANY)

    def body(*refs):
        reduce_kernel(depth, refs[: len(factors)], *refs[len(factors) :])

    return pl.pallas_call(
        body,
        out_shape=(
            jax.ShapeDtypeStruct((rows, width), BF16),
            jax.ShapeDtypeStruct((total_rows, 2 * pair_cols), BF16),
            jax.ShapeDtypeStruct((count, width), BF16),
        ),
        in_specs=[anywhere] * (len(factors) + 6),
        out_specs=(anywhere, anywhere, vmem),
        scratch_shapes=[
            pltpu.VMEM((total_rows, pair_cols), BF16),
            pltpu.VMEM((2, count, width), BF16),
            pltpu.VMEM((rights, count, width), BF16),
            pltpu.VMEM((RING, CHUNK, width), BF16),
            pltpu.VMEM((chunks, CHUNK // 2, width), BF16),
            pltpu.VMEM((chunks, CHUNK // 4, width), BF16),
            pltpu.VMEM((chunks, CHUNK // 8, width), BF16),
            pltpu.VMEM((chunks, CHUNK // 8, width), BF16),
            pltpu.VMEM((chunks, CHUNK // 8, width), BF16),
            pltpu.VMEM((pair_chunks, pair_rows, pair_cols), BF16),
            pltpu.VMEM((pair_chunks, pair_rows, pair_cols), BF16),
            pltpu.SemaphoreType.DMA((9, 2, chunks)),
            pltpu.SemaphoreType.DMA((4, 2, pair_chunks)),
            pltpu.SemaphoreType.DMA((len(factors) + 3,)),
            pltpu.SemaphoreType.DMA((chunks,)),
            pltpu.SemaphoreType.DMA((pair_chunks,)),
            pltpu.VMEM((count, width), F32),
            pltpu.VMEM((2, count, width), BF16),
            pltpu.VMEM((total_rows, pair_cols), BF16),
            pltpu.SemaphoreType.DMA((2, 3)),
        ],
        compiler_params=pltpu.CompilerParams(
            collective_id=1, has_side_effects=True, vmem_limit_bytes=60 * 1024 * 1024
        ),
        name="reduce_grads",
    )(*factors, half_own, first_y, rest_y, *mixed)


ROWS = 256


def times(x, w):
    return jnp.dot(x, w, preferred_element_type=F32)


def times_back(x, w):
    return lax.dot_general(x, w, (((1,), (1,)), ((), ())), preferred_element_type=F32)


def times_rows(x, y):
    return lax.dot_general(x, y, (((0,), (0,)), ((), ())), preferred_element_type=F32)


def hidden_kernel(
    rows_own,
    grads_own,
    grads_nb,
    late_left,
    late_right,
    late_down,
    late_other,
    mixed,
    back,
    half_own,
    half_nb,
    back_in,
    from_y,
    both,
    own,
    other,
    kept,
    theirs,
    moved,
    acc_mixed,
    acc_back,
    load_sem,
    sems,
):
    core = lax.axis_index("dp")
    slot = lax.axis_index("tensor")
    count, width = rows_own.shape
    half = width // 2
    blocks = count // ROWS
    pairs = (
        (late_left, own.at[0]),
        (late_right, own.at[1]),
        (late_down, own.at[2]),
        (late_other, other),
        (rows_own, both.at[0, :count]),
        (grads_own, both.at[1, :count]),
        (grads_nb, both.at[1, count:]),
    )
    loads = [pltpu.make_async_copy(a, b, load_sem.at[i]) for i, (a, b) in enumerate(pairs)]
    for i in (4, 5, 0, 1, 2, 3, 6):
        loads[i].start()

    def send(source, target, at, peer):
        return pltpu.make_async_remote_copy(
            src_ref=source,
            dst_ref=target,
            send_sem=sems.at[0, at],
            recv_sem=sems.at[1, at],
            device_id=peer,
            device_id_type=MESH,
        )

    def span(i):
        return pl.ds(pl.multiple_of(i * ROWS, ROWS), ROWS)

    def out_rows(i):
        return send(
            rows_own.at[span(i)], both.at[0, span(blocks + i)], i, {"tensor": slot ^ 1}
        )

    def return_rows(i):
        return send(
            back.at[span(blocks + i)], back_in.at[span(i)], blocks + i, {"tensor": slot ^ 1}
        )

    def to_core(which, m):
        return send(
            theirs.at[which, m], moved.at[which, m], 2 * blocks + 3 * which + m, {"dp": 1 - core}
        )

    hand = send(half_nb.at[0], from_y, 2 * blocks + 6, {"tensor": slot ^ 2})
    barrier = pltpu.get_barrier_semaphore()
    for peer in ({"tensor": slot ^ 1}, {"tensor": slot ^ 2}, {"dp": 1 - core}):
        pl.semaphore_signal(barrier, inc=1, device_id=peer, device_id_type=MESH)
    pl.semaphore_wait(barrier, 3)
    for i in range(blocks):
        out_rows(i).start()
    for i in (4, 5, 0, 1, 2):
        loads[i].wait()

    def unit(i, which, weights):
        rows, grads = both[0, span(i)], both[1, span(i)]
        e1, e2 = times_back(rows, weights[0]), times_back(rows, weights[1])
        dm = times_back(grads, weights[2])
        mid = (e1 * e2).astype(BF16)
        de1 = (dm * e2).astype(BF16)
        de2 = (dm * e1).astype(BF16)
        kept[which, 2, span(i)] = mid
        kept[which, 0, span(i)] = de1
        kept[which, 1, span(i)] = de2
        return times(mid, weights[2]), times(de1, weights[0]) + times(de2, weights[1])

    @pl.loop(0, 2 * blocks)
    def _(i):
        @pl.when(i >= blocks)
        def _():
            out_rows(i - blocks).wait_recv()

        @pl.when(i == blocks)
        def _():
            loads[6].wait()

        acc_mixed[...], acc_back[...] = unit(i, 0, own)

        @pl.when(i == 0)
        def _():
            loads[3].wait()

        more_mixed, more_back = unit(i, 1, other)
        mixed[span(i)] = (acc_mixed[...] + more_mixed).astype(BF16)
        back[span(i)] = (acc_back[...] + more_back).astype(BF16)

        @pl.when(i >= blocks)
        def _():
            return_rows(i - blocks).start()

    here = pl.ds(pl.multiple_of(core * half, half), half)
    there = pl.ds(pl.multiple_of((1 - core) * half, half), half)

    def products(which, out, m):
        theirs[which, m] = times_rows(kept[which, m], both[m // 2, :, there]).astype(BF16)
        to_core(which, m).start()
        out[m] = times_rows(kept[which, m], both[m // 2, :, here]).astype(BF16)

    def combine(which, out, m):
        to_core(which, m).wait_recv()
        out[m] = added(out[m], moved[which, m])

    products(1, half_nb, 0)
    combine(1, half_nb, 0)
    hand.start()

    @pl.loop(1, 3)
    def _(m):
        products(1, half_nb, m)

    @pl.loop(0, 3)
    def _(m):
        products(0, half_own, m)

    for m in range(1, 3):
        combine(1, half_nb, m)
    for m in range(3):
        combine(0, half_own, m)
    for i in range(blocks):
        out_rows(i).wait_send()
        return_rows(i).wait()
    for which in range(2):
        for m in range(3):
            to_core(which, m).wait_send()
    hand.wait()


def hidden_part(rows_own, grads_own, grads_nb, shard, other):
    count, width = rows_own.shape
    hidden = shard[0].shape[0]
    vmem = pl.BlockSpec(memory_space=pltpu.VMEM)
    anywhere = pl.BlockSpec(memory_space=pl.ANY)
    half = jax.ShapeDtypeStruct((3, hidden, width // 2), BF16)
    two = jax.ShapeDtypeStruct((2 * count, width), BF16)
    return pl.pallas_call(
        hidden_kernel,
        out_shape=(
            two,
            two,
            half,
            half,
            jax.ShapeDtypeStruct((count, width), BF16),
            jax.ShapeDtypeStruct((hidden, width // 2), BF16),
        ),
        in_specs=[anywhere] * 7,
        out_specs=(vmem,) * 4 + (anywhere,) * 2,
        scratch_shapes=[
            pltpu.VMEM((2, 2 * count, width), BF16),
            pltpu.VMEM((3, hidden, width), BF16),
            pltpu.VMEM((3, hidden, width), BF16),
            pltpu.VMEM((2, 3, 2 * count, hidden), BF16),
            pltpu.VMEM((2, 3, hidden, width // 2), BF16),
            pltpu.VMEM((2, 3, hidden, width // 2), BF16),
            pltpu.VMEM((ROWS, width), F32),
            pltpu.VMEM((ROWS, width), F32),
            pltpu.SemaphoreType.DMA((7,)),
            pltpu.SemaphoreType.DMA((2, 2 * (count // ROWS) + 7)),
        ],
        compiler_params=pltpu.CompilerParams(
            collective_id=4, has_side_effects=True, vmem_limit_bytes=54 * 1024 * 1024
        ),
        name="hidden_part",
    )(rows_own, grads_own, grads_nb, *shard, other)


MESH = pl.DeviceIdType.MESH


class States:
    def __init__(self, depth, width, backward, powers, local, came, total, far, outs, states, sems):
        self.depth, self.width, self.backward, self.powers = depth, width, backward, powers
        self.local, self.came, self.total, self.far = local, came, total, far
        self.outs, self.states, self.sems = outs, states, sems
        self.slot = lax.axis_index("tensor")
        self.place = lax.axis_index("seq")
        self.share = local.shape[0] // width

    def greet(self, more=()):
        barrier = pltpu.get_barrier_semaphore()
        for peer in more:
            pl.semaphore_signal(barrier, inc=1, device_id=peer, device_id_type=MESH)
        for b in range(1, self.width):
            pl.semaphore_signal(
                barrier, inc=1, device_id={"tensor": self.slot ^ b}, device_id_type=MESH
            )
        for j in range(1, self.depth):
            peer = lax.rem(self.place + j, self.depth)
            pl.semaphore_signal(barrier, inc=1, device_id={"seq": peer}, device_id_type=MESH)
        pl.semaphore_wait(barrier, self.width + self.depth - 2 + len(more))

    def copy(self, source, target, at, peer):
        return pltpu.make_async_remote_copy(
            src_ref=source,
            dst_ref=target,
            send_sem=self.sems.at[0, at],
            recv_sem=self.sems.at[1, at],
            device_id=peer,
            device_id_type=MESH,
        )

    def group(self, slot):
        return pl.ds(slot * self.share, self.share)

    def to_peer(self, b):
        peer = self.slot ^ b
        return self.copy(
            self.local.at[self.group(peer)], self.came.at[b - 1], b - 1, {"tensor": peer}
        )

    def to_far(self, j):
        peer = self.place - j if self.backward else self.place + j
        return self.copy(self.total, self.far.at[j - 1], self.width + j - 2, {"seq": peer})

    def has_far(self, j):
        return self.place >= j if self.backward else self.place + j < self.depth

    def from_far(self, j):
        return self.place + j < self.depth if self.backward else self.place >= j

    def to_owner(self, d):
        at = self.width + self.depth - 2 + d - 1
        return self.copy(
            self.outs.at[d - 1],
            self.states.at[self.group(self.slot)],
            at,
            {"tensor": self.slot ^ d},
        )

    def power(self, count, head):
        return self.powers[count, head]

    def piece(self, b, k, s):
        if b == 0:
            return self.local[self.slot * self.share + k, s].astype(F32)
        return self.came[b - 1, k, s].astype(F32)

    def gather(self):
        for b in range(1, self.width):
            self.to_peer(b).wait_recv()
        for k in range(self.share):
            head = self.slot * self.share + k
            for s in range(self.local.shape[1]):
                value = 0.0
                for b in range(self.width):
                    spot = self.slot ^ b
                    left = spot if self.backward else self.width - 1 - spot
                    value = value + self.power(left, head) * self.piece(b, k, s)
                self.total[k, s] = value.astype(BF16)
        for j in range(1, self.depth):

            @pl.when(self.has_far(j))
            def _(j=j):
                self.to_far(j).start()

    def send_back(self, entering):
        for j in range(1, self.depth):

            @pl.when(self.from_far(j))
            def _(j=j):
                self.to_far(j).wait_recv()

            @pl.when(jnp.logical_not(self.from_far(j)))
            def _(j=j):
                self.far[j - 1] = jnp.zeros(self.far.shape[1:], BF16)

        for k in range(self.share):
            head = self.slot * self.share + k
            for s in range(self.local.shape[1]):
                value = 0.0
                for j in range(1, self.depth):
                    value = value + self.power(self.width * (j - 1), head) * self.far[
                        j - 1, k, s
                    ].astype(F32)
                entering[k, s] = value
        for d in list(range(1, self.width)) + [0]:
            target = self.slot ^ d
            inner = self.width - 1 - target if self.backward else target
            for k in range(self.share):
                head = self.slot * self.share + k
                for s in range(self.local.shape[1]):
                    value = self.power(inner, head) * entering[k, s]
                    for b in range(self.width):
                        if b == d:
                            continue
                        source = self.slot ^ b
                        gap = source - target - 1 if self.backward else target - source - 1
                        coef = jnp.where(gap >= 0, self.power(jnp.maximum(gap, 0), head), 0.0)
                        value = value + coef * self.piece(b, k, s)
                    if d == 0:
                        self.states[head, s] = value.astype(BF16)
                    else:
                        self.outs[d - 1, k, s] = value.astype(BF16)
        for d in range(1, self.width):
            self.to_owner(d).start()

    def arrive(self):
        for d in range(1, self.width):
            at = self.width + self.depth - 2 + d - 1
            self.copy(
                self.outs.at[d - 1],
                self.states.at[self.group(self.slot ^ d)],
                at,
                {"tensor": self.slot ^ d},
            ).wait_recv()

    def settle(self):
        for b in range(1, self.width):
            self.to_peer(b).wait_send()
            self.to_owner(b).wait_send()
        for j in range(1, self.depth):

            @pl.when(self.has_far(j))
            def _(j=j):
                self.to_far(j).wait_send()


def state_scratch(heads, seqs, head_dim, width, depth):
    share = heads // width
    low = functools.partial(pltpu.VMEM, dtype=BF16)
    return [
        low((heads, seqs, head_dim, head_dim)),
        low((width - 1, share, seqs, head_dim, head_dim)),
        low((share, seqs, head_dim, head_dim)),
        low((depth - 1, share, seqs, head_dim, head_dim)),
        low((width - 1, share, seqs, head_dim, head_dim)),
        pltpu.VMEM((share, seqs, head_dim, head_dim), F32),
        pltpu.SemaphoreType.DMA((2, 2 * (width - 1) + depth - 1)),
    ]


def turn(values, cosine, sine_part):
    return values * cosine + pltpu.roll(values, values.shape[-1] // 2, 1) * sine_part


def square_mean(values):
    return jnp.mean(values * values, axis=-1, keepdims=True)


def decays(rates, head, length, dim):
    rate = rates[head]
    place = lax.broadcasted_iota(jnp.int32, (length, dim), 0).astype(F32)
    query = jnp.exp(-rate[:, :dim] * (place + 1.0))
    key = jnp.exp(-rate[:, :dim] * (length - 1.0 - place))
    return query, key


def lag_decay(rates, head, length):
    lag = (
        lax.broadcasted_iota(jnp.int32, (length, length), 0)
        - lax.broadcasted_iota(jnp.int32, (length, length), 1)
    ).astype(F32)
    return jnp.where(lag >= 0, jnp.exp(-rates[head] * jnp.maximum(lag, 0.0)), 0.0)


def attend_kernel(
    depth,
    width,
    seqs,
    first_x,
    first_key,
    first_value,
    late_query,
    late_gate,
    late_output,
    left,
    right,
    down,
    grads,
    rates,
    powers,
    cosine,
    sine_part,
    residual,
    normed_two,
    attended,
    gated,
    states,
    early_outs,
    other,
    grads_nb,
    early,
    x,
    w_key,
    w_value,
    w_query,
    w_gate,
    w_output,
    local,
    came,
    total,
    far,
    outs,
    entering,
    sems,
    load_sem,
    bulk_sems,
    store_sem,
):
    (
        query_pre,
        key_pre,
        gate,
        normed_one,
        query_low,
        key_low,
        value_low,
        query_dec,
        key_dec,
        scores_low,
    ) = early
    stores = [
        pltpu.make_async_copy(a, b, store_sem.at[i])
        for i, (a, b) in enumerate(zip(early, early_outs))
    ]
    rows, model = x.shape
    length = rows // seqs
    dim = cosine.shape[1]
    tile = model // width
    loads = [
        pltpu.make_async_copy(a, b, load_sem.at[i])
        for i, (a, b) in enumerate(
            (
                (late_query, w_query),
                (late_gate, w_gate),
                (late_output, w_output),
                (first_x, x),
                (first_key, w_key),
                (first_value, w_value),
            )
        )
    ]
    loads = loads[3:] + loads[:3]
    for load in loads:
        load.start()
    exchange = States(
        depth, width, False, powers, local, came, total, far, outs, states, sems
    )
    core = lax.axis_index("dp")
    parity = lax.rem(exchange.place, 2)
    shard = (left, right, down)
    part_rows, part_cols = left.shape[0] // 2, model // 2
    columns_here = pl.ds(pl.multiple_of(core * part_cols, part_cols), part_cols)

    def rows_of(which):
        return pl.ds(pl.multiple_of(which * part_rows, part_rows), part_rows)

    def send(source, target, at, peer):
        return pltpu.make_async_remote_copy(
            src_ref=source,
            dst_ref=target,
            send_sem=bulk_sems.at[0, at],
            recv_sem=bulk_sems.at[1, at],
            device_id=peer,
            device_id_type=MESH,
        )

    def fetch(m):
        at = (rows_of(parity), columns_here)
        return send(
            shard[m].at[at], other.at[(m,) + at], m, {"tensor": exchange.slot ^ 2}
        )

    def relay(m):
        at = other.at[m, rows_of(parity), columns_here]
        return send(at, at, 3 + m, {"seq": exchange.place + 1 - 2 * parity})

    def share(m, which):
        spot = parity if which == 0 else 1 - parity
        at = other.at[m, rows_of(spot), columns_here]
        return send(at, at, 6 + 2 * m + which, {"dp": 1 - core})

    def cross(s):
        at = pl.ds(s * length, length)
        return send(grads.at[at], grads_nb.at[at], 12 + s, {"tensor": exchange.slot ^ 1})

    def pass_on(m):
        fetch(m).wait_recv()
        relay(m).start()
        share(m, 0).start()

    def pass_last(m):
        relay(m).wait_recv()
        share(m, 1).start()

    exchange.greet((({"dp": 1 - core}),))
    fetch(0).start()
    cross(0).start()
    fetch(1).start()
    loads[0].wait()
    for s in range(seqs):
        at = pl.ds(s * length, length)
        value = x[at].astype(F32)
        normed_one[at] = (value * lax.rsqrt(square_mean(value) + EPS)).astype(BF16)

    per_tile = tile // dim
    loads[1].wait()
    loads[2].wait()

    @pl.loop(1, width + 1)
    def _(step):
        b = lax.rem(step, width)
        spot = exchange.slot ^ b
        columns = pl.ds(pl.multiple_of(spot * tile, tile), tile)
        key_pre[:, columns] = times(normed_one[...], w_key[:, columns])
        value_low[:, columns] = times(normed_one[...], w_value[:, columns]).astype(BF16)
        for k in range(per_tile):
            head = spot * per_tile + k
            own = pl.ds(pl.multiple_of(spot * tile + k * dim, dim), dim)
            _, key_weight = decays(rates, head, length, dim)
            for s in range(seqs):
                at = pl.ds(s * length, length)
                turned = turn(jax.nn.silu(key_pre[at, own]), cosine[...], sine_part[...])
                key_low[at, own] = turned.astype(BF16)
                dec = (turned * key_weight).astype(BF16)
                key_dec[at, own] = dec
                local[head, s] = times_rows(dec, value_low[at, own]).astype(BF16)

        for b_static in range(1, width):

            @pl.when(b == b_static)
            def _(b_static=b_static):
                exchange.to_peer(b_static).start()

    for s in range(1, seqs):
        cross(s).start()
    fetch(2).start()
    pass_on(0)
    loads[3].wait()
    loads[4].wait()

    def inner(spot):
        columns = pl.ds(pl.multiple_of(spot * tile, tile), tile)
        query_pre[:, columns] = times(normed_one[...], w_query[:, columns])
        gate[:, columns] = times(normed_one[...], w_gate[:, columns])
        for k in range(per_tile):
            head = spot * per_tile + k
            own = pl.ds(pl.multiple_of(spot * tile + k * dim, dim), dim)
            query_weight, _ = decays(rates, head, length, dim)
            mask = lag_decay(rates, head, length)
            for s in range(seqs):
                at = pl.ds(s * length, length)
                turned = turn(jax.nn.silu(query_pre[at, own]), cosine[...], sine_part[...])
                low_query = turned.astype(BF16)
                query_low[at, own] = low_query
                query_dec[at, own] = (turned * query_weight).astype(BF16)
                low_scores = (times_back(low_query, key_low[at, own]) * mask).astype(BF16)
                scores_low[head, s] = low_scores
                attended[at, own] = times(low_scores, value_low[at, own])

    half = width // 2

    @pl.loop(0, half)
    def _(spot):
        inner(spot)

    exchange.gather()

    @pl.loop(half, width)
    def _(spot):
        inner(spot)

    exchange.send_back(entering)
    for store in stores:
        store.start()
    pass_on(1)
    pass_on(2)
    pass_last(0)
    loads[5].wait()
    exchange.arrive()
    pass_last(1)

    @pl.loop(0, width * per_tile)
    def _(head):
        own = pl.ds(pl.multiple_of(head * dim, dim), dim)
        for s in range(seqs):
            at = pl.ds(s * length, length)
            attended[at, own] += times(query_dec[at, own], states[head, s])

    for s in range(seqs):
        at = pl.ds(s * length, length)
        value = attended[at]
        gated[at] = (value * lax.rsqrt(square_mean(value) + EPS) * gate[at]).astype(BF16)

    @pl.loop(0, width)
    def _(spot):
        columns = pl.ds(pl.multiple_of(spot * tile, tile), tile)
        residual[:, columns] = x[:, columns].astype(F32) + times(
            gated[...], w_output[:, columns]
        )

    for s in range(seqs):
        at = pl.ds(s * length, length)
        value = residual[at]
        normed_two[at] = (value * lax.rsqrt(square_mean(value) + EPS)).astype(BF16)
    pass_last(2)
    for store in stores:
        store.wait()
    exchange.settle()
    for m in range(3):
        fetch(m).wait_send()
        relay(m).wait_send()
        share(m, 0).wait()
        share(m, 1).wait()
    for s in range(seqs):
        cross(s).wait()


def attend(x, weights, shard, grads, rates, powers, cosine, sine_part, seqs, depth, width):
    rows, model = x.shape
    heads = rates.shape[0]
    dim = model // heads
    length = rows // seqs
    vmem = pl.BlockSpec(memory_space=pltpu.VMEM)
    anywhere = pl.BlockSpec(memory_space=pl.ANY)
    wide = jax.ShapeDtypeStruct((rows, model), F32)
    low = jax.ShapeDtypeStruct((rows, model), BF16)
    w_query, w_key, w_value, w_gate, w_output = weights
    early = (wide,) * 3 + (low,) * 6 + (
        jax.ShapeDtypeStruct((heads, seqs, length, length), BF16),
    )

    def body(*refs):
        at = 14 + 5
        kept = at + len(early)
        scratch = kept + 2
        attend_kernel(
            depth,
            width,
            seqs,
            *refs[:at],
            refs[at:kept],
            *refs[kept:scratch],
            refs[scratch : scratch + len(early)],
            *refs[scratch + len(early) :],
        )

    return pl.pallas_call(
        body,
        out_shape=(
            wide,
            low,
            wide,
            low,
            jax.ShapeDtypeStruct((heads, seqs, dim, dim), BF16),
        )
        + early
        + (jax.ShapeDtypeStruct((3,) + shard[0].shape, BF16), low),
        in_specs=[anywhere] * 10 + [vmem] * 4,
        out_specs=(vmem,) * 5 + (anywhere,) * (len(early) + 2),
        scratch_shapes=[pltpu.VMEM(v.shape, v.dtype) for v in early]
        + [pltpu.VMEM((rows, model), BF16)]
        + [pltpu.VMEM((model, model), BF16)] * 5
        + state_scratch(heads, seqs, dim, width, depth)
        + [
            pltpu.SemaphoreType.DMA((6,)),
            pltpu.SemaphoreType.DMA((2, 12 + seqs)),
            pltpu.SemaphoreType.DMA((len(early),)),
        ],
        compiler_params=pltpu.CompilerParams(
            collective_id=2, has_side_effects=True, vmem_limit_bytes=56 * 1024 * 1024
        ),
        name="attend",
    )(
        x,
        w_key,
        w_value,
        w_query,
        w_gate,
        w_output,
        *shard,
        grads,
        rates,
        powers,
        cosine,
        sine_part,
    )


def retreat_kernel(
    depth,
    width,
    seqs,
    residual,
    back_own,
    back_in,
    grads,
    rates,
    powers,
    cosine,
    sine_part,
    mixed_nb,
    half_nb,
    *rest,
):
    late = rest[:17]
    (
        grad_mid_low,
        gate_low,
        query_out,
        key_out,
        value_out,
        grad_tokens,
        mixed_in,
        from_y,
    ) = rest[17:25]
    held = rest[25:42]
    (
        w_output,
        attended,
        gate,
        query_low,
        key_low,
        value_low,
        query_dec,
        scores_low,
        states_in,
        query_pre,
        w_query,
        w_gate,
        key_dec,
        key_pre,
        w_key,
        w_value,
        x,
    ) = held
    (
        states,
        grad_mid,
        work,
        grad_att,
        value_part,
        key_part,
        local,
        came,
        total,
        far,
        outs,
        entering,
        sems,
        load_sem,
        bulk_sems,
    ) = rest[42:]
    rows, model = residual.shape
    length = rows // seqs
    dim = cosine.shape[1]
    tile = model // width
    per_tile = tile // dim
    loads = [
        pltpu.make_async_copy(a, b, load_sem.at[i]) for i, (a, b) in enumerate(zip(late, held))
    ]
    for load in loads:
        load.start()
    exchange = States(
        depth, width, True, powers, local, came, total, far, outs, states, sems
    )

    def send(source, target, at, peer):
        return pltpu.make_async_remote_copy(
            src_ref=source,
            dst_ref=target,
            send_sem=bulk_sems.at[0, at],
            recv_sem=bulk_sems.at[1, at],
            device_id=peer,
            device_id_type=MESH,
        )

    crosses, hands = 4, 8
    cross_rows, hand_rows = rows // crosses, 2 * half_nb.shape[1] // hands

    def cross(k):
        at = pl.ds(k * cross_rows, cross_rows)
        source = mixed_nb.at[pl.ds(rows + k * cross_rows, cross_rows)]
        return send(source, mixed_in.at[at], k, {"tensor": exchange.slot ^ 1})

    def hand(k):
        m, at = k // (hands // 2), pl.ds(k % (hands // 2) * hand_rows, hand_rows)
        return send(
            half_nb.at[m + 1, at], from_y.at[m, at], crosses + k, {"tensor": exchange.slot ^ 2}
        )

    def start_bulk(some_crosses, some_hands):
        for k in some_crosses:
            cross(k).start()
        for k in some_hands:
            hand(k).start()

    exchange.greet()
    start_bulk(range(1), range(2))

    def spans():
        return [pl.ds(s * length, length) for s in range(seqs)]

    for at in spans():
        value = residual[at]
        scale = lax.rsqrt(square_mean(value) + EPS)
        normed = value * scale
        grad = back_own[at].astype(F32) + back_in[at].astype(F32)
        grad = grads[at].astype(F32) + scale * (
            grad - normed * jnp.mean(grad * normed, axis=-1, keepdims=True)
        )
        grad_mid[at] = grad
        grad_mid_low[at] = grad.astype(BF16)

    def columns_of(spot):
        return pl.ds(pl.multiple_of(spot * tile, tile), tile)

    for load in loads[:3]:
        load.wait()

    @pl.loop(0, width)
    def _(spot):
        work[:, columns_of(spot)] = times_back(grad_mid_low[...], w_output[columns_of(spot)])

    for at in spans():
        value = attended[at]
        scale = lax.rsqrt(square_mean(value) + EPS)
        normed = value * scale
        grad = work[at]
        gate_low[at] = (grad * normed).astype(BF16)
        grad = grad * gate[at]
        grad_att[at] = (
            scale * (grad - normed * jnp.mean(grad * normed, axis=-1, keepdims=True))
        ).astype(BF16)

    for load in loads[3:10]:
        load.wait()

    @pl.loop(1, width + 1)
    def _(step):
        b = lax.rem(step, width)
        spot = exchange.slot ^ b
        for k in range(per_tile):
            own = pl.ds(pl.multiple_of(spot * tile + k * dim, dim), dim)
            for s, at in enumerate(spans()):
                local[spot * per_tile + k, s] = times_rows(
                    query_dec[at, own], grad_att[at, own]
                ).astype(BF16)

        for b_static in range(1, width):

            @pl.when(b == b_static)
            def _(b_static=b_static):
                exchange.to_peer(b_static).start()

    start_bulk(range(1, 3), range(2, 5))

    def slope(values):
        sigmoid_v = jax.nn.sigmoid(values)
        return sigmoid_v * (1.0 + values * (1.0 - sigmoid_v))

    def inner(spot):
        for k in range(per_tile):
            head = spot * per_tile + k
            own = pl.ds(pl.multiple_of(spot * tile + k * dim, dim), dim)
            query_weight, _ = decays(rates, head, length, dim)
            mask = lag_decay(rates, head, length)
            for s, at in enumerate(spans()):
                grad = grad_att[at, own]
                value_part[at, own] = times_rows(scores_low[head, s], grad)
                score = (times_back(grad, value_low[at, own]) * mask).astype(BF16)
                key_part[at, own] = times_rows(score, query_low[at, own])
                turned = times(score, key_low[at, own]) + query_weight * times_back(
                    grad, states_in[head, s]
                )
                query_out[at, own] = (
                    turn(turned, cosine[...], -sine_part[...]) * slope(query_pre[at, own])
                ).astype(BF16)

    half = width // 2

    @pl.loop(0, half)
    def _(spot):
        inner(spot)

    exchange.gather()

    @pl.loop(half, width)
    def _(spot):
        inner(spot)

    exchange.send_back(entering)
    start_bulk(range(3, crosses), range(5, hands))
    for load in loads[10:]:
        load.wait()

    @pl.loop(0, width)
    def _(spot):
        at = columns_of(spot)
        work[:, at] = times_back(query_out[...], w_query[at]) + times_back(
            gate_low[...], w_gate[at]
        )

    exchange.arrive()

    @pl.loop(0, width * per_tile)
    def _(head):
        own = pl.ds(pl.multiple_of(head * dim, dim), dim)
        _, key_weight = decays(rates, head, length, dim)
        for s, at in enumerate(spans()):
            state = states[head, s]
            value_out[at, own] = (
                value_part[at, own] + times(key_dec[at, own], state)
            ).astype(BF16)
            turned = key_part[at, own] + key_weight * times_back(value_low[at, own], state)
            key_out[at, own] = (
                turn(turned, cosine[...], -sine_part[...]) * slope(key_pre[at, own])
            ).astype(BF16)

    @pl.loop(0, width)
    def _(spot):
        at = columns_of(spot)
        work[:, at] += times_back(key_out[...], w_key[at]) + times_back(
            value_out[...], w_value[at]
        )

    for at in spans():
        value = x[at].astype(F32)
        scale = lax.rsqrt(square_mean(value) + EPS)
        normed = value * scale
        grad = work[at]
        grad_tokens[at] = grad_mid[at] + scale * (
            grad - normed * jnp.mean(grad * normed, axis=-1, keepdims=True)
        )
    exchange.settle()
    for k in range(crosses):
        cross(k).wait()
    for k in range(hands):
        hand(k).wait()


def retreat(early, tables, bulk, late, seqs, depth, width):
    rows, model = early[0].shape
    heads = tables[0].shape[0]
    dim = model // heads
    vmem = pl.BlockSpec(memory_space=pltpu.VMEM)
    anywhere = pl.BlockSpec(memory_space=pl.ANY)
    wide = jax.ShapeDtypeStruct((rows, model), F32)
    low = jax.ShapeDtypeStruct((rows, model), BF16)
    return pl.pallas_call(
        functools.partial(retreat_kernel, depth, width, seqs),
        out_shape=(low,) * 5 + (wide, low, jax.ShapeDtypeStruct((2,) + bulk[1].shape[1:], BF16)),
        in_specs=[vmem] * (len(early) + len(tables)) + [anywhere] * (len(bulk) + len(late)),
        out_specs=(vmem,) * 6 + (anywhere,) * 2,
        scratch_shapes=[pltpu.VMEM(v.shape, v.dtype) for v in late]
        + [
            pltpu.VMEM((heads, seqs, dim, dim), BF16),
            pltpu.VMEM((rows, model), F32),
            pltpu.VMEM((rows, model), F32),
            pltpu.VMEM((rows, model), BF16),
            pltpu.VMEM((rows, model), F32),
            pltpu.VMEM((rows, model), F32),
        ]
        + state_scratch(heads, seqs, dim, width, depth)
        + [pltpu.SemaphoreType.DMA((len(late),)), pltpu.SemaphoreType.DMA((2, 12))],
        compiler_params=pltpu.CompilerParams(
            collective_id=3, has_side_effects=True, vmem_limit_bytes=60 * 1024 * 1024
        ),
        name="retreat",
    )(*early, *tables, *bulk, *late)


def on_device(
    tokens,
    w_query,
    w_key,
    w_value,
    w_ugate,
    w_output,
    w_left,
    w_right,
    w_down,
    decay_rate,
    cotangent,
):
    seq_count, group_len, model_width = tokens.shape
    head_count = decay_rate.shape[0]
    head_dim = model_width // head_count
    half_dim = head_dim // 2
    row_count = seq_count * group_len
    core = lax.axis_index("dp")

    shard = (w_left.T, w_right.T, w_down)
    grad_own = cotangent.reshape(row_count, model_width)

    position_block = lax.axis_index(("seq", "tensor"))
    places = (position_block * group_len + jnp.arange(group_len)).astype(F32)
    frequency = 10000.0 ** (-jnp.arange(half_dim, dtype=F32) / half_dim)
    angles = places[:, None] * frequency[None, :]
    cosine, sine_part = jnp.cos(angles), jnp.sin(angles)
    cosine = jnp.concatenate([cosine, cosine], axis=1)
    sine_part = jnp.concatenate([-sine_part, sine_part], axis=1)
    rows_in = tokens.reshape(row_count, model_width)
    depth = lax.axis_size("seq")
    width = lax.axis_size("tensor")
    rates = jnp.broadcast_to(decay_rate[:, None, None], (head_count, 1, group_len))
    blocks = jnp.arange(depth * width, dtype=F32)[:, None, None, None]
    powers = jnp.broadcast_to(
        jnp.exp(-decay_rate[None, :, None, None] * group_len * blocks),
        (depth * width, head_count, 1, head_dim),
    )
    (
        residual,
        rows_own,
        merged,
        gated_low,
        state_low,
        query_pre,
        key_pre,
        ugate,
        normed_low,
        query_low,
        key_low,
        value_low,
        query_dec,
        key_dec,
        weights_low,
        other,
        grad_nb,
    ) = attend(
        rows_in,
        (w_query, w_key, w_value, w_ugate, w_output),
        shard,
        grad_own,
        rates,
        powers,
        cosine,
        sine_part,
        seq_count,
        depth,
        width,
    )
    mixed, back, half_own, half_nb, back_in, first_y = hidden_part(
        rows_own, grad_own, grad_nb, shard, other
    )
    (
        grad_branch,
        grad_ugate_pre,
        grad_query_pre,
        grad_key_pre,
        grad_value_pre,
        grad_tokens,
        mixed_in,
        from_y,
    ) = retreat(
        (residual, back, back_in, grad_own),
        (rates, powers, cosine, sine_part),
        (mixed, half_nb),
        (
            w_output,
            merged,
            ugate,
            query_low,
            key_low,
            value_low,
            query_dec,
            weights_low,
            state_low,
            query_pre,
            w_query,
            w_ugate,
            key_dec,
            key_pre,
            w_key,
            w_value,
            rows_in,
        ),
        seq_count,
        depth,
        width,
    )

    hidden = w_down.shape[0]
    sums, hidden_sums, mixed_out = reduce_grads(
        (
            normed_low,
            gated_low,
            grad_query_pre,
            grad_key_pre,
            grad_value_pre,
            grad_ugate_pre,
            grad_branch,
        ),
        half_own,
        first_y,
        from_y,
        (residual, mixed, mixed_in),
        depth,
    )
    attention_grads = tuple(
        sums[i * model_width : (i + 1) * model_width].astype(F32) for i in range(5)
    )
    left_sum, right_sum, down_sum = (
        hidden_sums[i * hidden : (i + 1) * hidden].astype(F32) for i in range(3)
    )
    return (
        (mixed_out.reshape(tokens.shape), grad_tokens.reshape(tokens.shape))
        + attention_grads
        + (left_sum.T, right_sum.T, down_sum)
    )


def solution(mesh):
    rows = P("dp", ("seq", "tensor"), None)
    columns = P(None, "tensor")
    return jax.shard_map(
        on_device,
        mesh=mesh,
        in_specs=(rows, P(), P(), P(), P(), P(), columns, columns, P("tensor", None), P(), rows),
        out_specs=(rows, rows, P(), P(), P(), P(), P(), columns, columns, P("tensor", None)),
        check_vma=False,
    )
```

```python
import functools

import jax
import jax.numpy as jnp
from jax import lax
from jax.experimental import pallas as pl
from jax.experimental.pallas import tpu as pltpu
from jax.sharding import PartitionSpec as P


EPS = 1e-06
F32 = jnp.float32
BF16 = jnp.bfloat16


CHUNK = 256
LAG = 1


def added(first, second):
    return (first.astype(F32) + second.astype(F32)).astype(BF16)


RING = 8


def reduce_kernel(
    depth,
    factors,
    pair_own,
    pair_first,
    pair_rest,
    residual,
    mixed_own,
    mixed_nb,
    out,
    pair_out,
    mixed_out,
    pair_in,
    left_side,
    right_side,
    own,
    core_in,
    first_in,
    second_in,
    line_in,
    line_mid,
    pair_line,
    pair_mid,
    sems,
    pair_sems,
    load_sem,
    keep_sem,
    pair_keep_sem,
    base_part,
    mixed_part,
    pair_more,
    share_sem,
):
    core = lax.axis_index("dp")
    slot = lax.axis_index("tensor")
    place = lax.axis_index("seq")
    rows = out.shape[0]
    chunks = rows // CHUNK
    half, quarter, eighth = CHUNK // 2, CHUNK // 4, CHUNK // 8
    low_side = place < depth // 2
    outermost = (place == 0) | (place == depth - 1)
    middle = (place == depth // 2 - 1) | (place == depth // 2)
    inward = jnp.where(low_side, place + 1, place - 1)
    outward = jnp.where(low_side, place - 1, place + 1)

    barrier = pltpu.get_barrier_semaphore()

    def greet(peer):
        pl.semaphore_signal(
            barrier, inc=1, device_id=peer, device_id_type=pl.DeviceIdType.MESH
        )

    greet({"dp": 1 - core})
    greet({"tensor": slot ^ 1})
    greet({"tensor": slot ^ 2})

    @pl.when(place > 0)
    def _():
        greet({"seq": place - 1})

    @pl.when(place < depth - 1)
    def _():
        greet({"seq": place + 1})

    pl.semaphore_wait(barrier, jnp.where(outermost, 4, 5))

    def remote(source, target, sem, at, peer):
        return pltpu.make_async_remote_copy(
            src_ref=source,
            dst_ref=target,
            send_sem=sem.at[0, at],
            recv_sem=sem.at[1, at],
            device_id=peer,
            device_id_type=pl.DeviceIdType.MESH,
        )

    def span(start, size):
        return pl.ds(pl.multiple_of(start, size), size)

    def bits(q):
        first = jnp.where(q % 2 == 0, 1, 2)
        second = 3 - first
        return first, second, (slot & first) // first, (slot & second) // second

    def base(q):
        return pl.multiple_of(q * CHUNK, CHUNK)

    def to_core(q):
        return remote(
            own.at[q % RING, span((1 - core) * half, half)],
            core_in.at[q],
            sems.at[0],
            q,
            {"dp": 1 - core},
        )

    def to_first(q):
        first, _, f, _ = bits(q)
        return remote(
            core_in.at[q, span((1 - f) * quarter, quarter)],
            first_in.at[q],
            sems.at[1],
            q,
            {"tensor": slot ^ first},
        )

    def to_second(q):
        _, second, _, g = bits(q)
        return remote(
            first_in.at[q, span((1 - g) * eighth, eighth)],
            second_in.at[q],
            sems.at[2],
            q,
            {"tensor": slot ^ second},
        )

    def block(q):
        _, _, f, g = bits(q)
        return base(q) + core * half + f * quarter + g * eighth

    def keep(q):
        return pltpu.make_async_copy(
            line_mid.at[q], out.at[span(block(q), eighth)], keep_sem.at[q]
        )

    def back_second(q):
        _, second, _, _ = bits(q)
        at = span(block(q), eighth)
        return remote(line_mid.at[q], out.at[at], sems.at[3], q, {"tensor": slot ^ second})

    def back_first(q):
        first, _, f, _ = bits(q)
        at = span(base(q) + core * half + f * quarter, quarter)
        return remote(out.at[at], out.at[at], sems.at[4], q, {"tensor": slot ^ first})

    def back_core(q):
        at = span(base(q) + core * half, half)
        return remote(out.at[at], out.at[at], sems.at[5], q, {"dp": 1 - core})

    class Line:
        def __init__(self, mine, came, met, sem, offset):
            self.mine, self.came, self.met = mine, came, met
            self.sem, self.offset = sem, offset

        def inwards(self, q, source):
            return remote(
                source, self.came(q), self.sem.at[self.offset], q, {"seq": inward}
            )

        def across(self, q):
            return remote(
                self.came(q),
                self.met(q),
                self.sem.at[self.offset + 1],
                q,
                {"seq": depth - 1 - place},
            )

        def outwards(self, q):
            return remote(
                self.met(q), self.met(q), self.sem.at[self.offset + 2], q, {"seq": outward}
            )

        def step_in(self, q):
            @pl.when(outermost)
            def _():
                self.inwards(q, self.mine(q)).start()

        def step_middle(self, q):
            @pl.when(jnp.logical_not(outermost))
            def _():
                self.inwards(q, self.mine(q)).wait_recv()
                came = self.came(q)
                came[...] = added(self.mine(q)[...], came[...])

                @pl.when(middle)
                def _():
                    self.across(q).start()

                @pl.when(jnp.logical_not(middle))
                def _():
                    self.inwards(q, came).start()

        def step_out(self, q):
            @pl.when(middle)
            def _():
                self.across(q).wait_recv()
                met = self.met(q)
                met[...] = added(self.came(q)[...], met[...])

            @pl.when(jnp.logical_not(outermost))
            def _():
                @pl.when(jnp.logical_not(middle))
                def _():
                    self.outwards(q).wait_recv()

                self.outwards(q).start()

        def step_last(self, q):
            @pl.when(outermost)
            def _():
                self.outwards(q).wait_recv()

        def settle(self, q):
            @pl.when(outermost)
            def _():
                self.inwards(q, self.mine(q)).wait_send()

            @pl.when(jnp.logical_not(outermost))
            def _():
                @pl.when(middle)
                def _():
                    self.across(q).wait_send()

                @pl.when(jnp.logical_not(middle))
                def _():
                    self.inwards(q, self.came(q)).wait_send()

                self.outwards(q).wait_send()

    def second_mine(q):
        return second_in.at[q]

    line = Line(
        second_mine,
        lambda q: line_in.at[q],
        lambda q: line_mid.at[q],
        sems,
        6,
    )
    pair_chunks, pair_rows, pair_cols = pair_line.shape
    pair = Line(
        lambda q: pair_in.at[span(q * pair_rows, pair_rows)],
        lambda q: pair_line.at[q],
        lambda q: pair_mid.at[q],
        pair_sems,
        0,
    )

    def pair_block(q):
        return pair_out.at[span(q * pair_rows, pair_rows), span(core * pair_cols, pair_cols)]

    def pair_keep(q):
        return pltpu.make_async_copy(pair_mid.at[q], pair_block(q), pair_keep_sem.at[q])

    def pair_core(q):
        return remote(pair_mid.at[q], pair_block(q), pair_sems.at[3], q, {"dp": 1 - core})

    rights = len(factors) - 2
    loads = [
        pltpu.make_async_copy(g, t, load_sem.at[i])
        for i, (g, t) in enumerate(
            zip(
                factors,
                [left_side.at[0], left_side.at[1]] + [right_side.at[i] for i in range(rights)],
            )
        )
    ]
    tokens = residual.shape[0]
    parts = [
        pltpu.make_async_copy(a, b, load_sem.at[len(factors) + i])
        for i, (a, b) in enumerate(
            (
                (residual, base_part),
                (mixed_own.at[:tokens], mixed_part.at[0]),
                (mixed_nb, mixed_part.at[1]),
            )
        )
    ]
    hidden = pair_first.shape[0]
    thirds = [pl.ds(m * hidden, hidden) for m in range(3)]
    shares = [
        pltpu.make_async_copy(pair_own.at[m], pair_in.at[thirds[m]], share_sem.at[0, m])
        for m in range(3)
    ] + [
        pltpu.make_async_copy(
            pair_first if m == 0 else pair_rest.at[m - 1],
            pair_more.at[thirds[m]],
            share_sem.at[1, m],
        )
        for m in range(3)
    ]
    for load in [loads[0], loads[2]] + shares + [loads[1]] + loads[3:] + parts:
        load.start()
    per_matrix = chunks // rights

    def make(q):
        @pl.when(q >= RING)
        def _():
            to_core(q - RING).wait_send()

        m = q // per_matrix
        columns = pl.ds(pl.multiple_of((q % per_matrix) * CHUNK, CHUNK), CHUNK)
        own[q % RING] = times_rows(
            left_side[m // (rights - 1), :, columns], right_side[m]
        ).astype(BF16)

    def stage_a(q):
        to_core(q).wait_recv()
        came = core_in.at[q]
        came[...] = added(own[q % RING, span(core * half, half)], came[...])

    def stage_b(q):
        _, _, f, _ = bits(q)
        to_first(q).wait_recv()
        came = first_in.at[q]
        came[...] = added(core_in[q, span(f * quarter, quarter)], came[...])

    def stage_c(q):
        _, _, _, g = bits(q)
        to_second(q).wait_recv()
        came = second_in.at[q]
        came[...] = added(first_in[q, span(g * eighth, eighth)], came[...])

    pairs = chunks // 2

    def during(step, lag, count, action):
        i = step - lag

        @pl.when((i >= 0) & (i < count))
        def _():
            action(i)

    def both(action):
        def run(i):
            action(2 * i)
            action(2 * i + 1)

        return run

    def start(copy):
        return lambda q: copy(q).start()

    def arrived(copy, following):
        def run(q):
            copy(q).wait_recv()
            following(q).start()

        return run

    def last_then_second(q):
        line.step_last(q)
        keep(q).start()
        back_second(q).start()

    def second_arrived(q):
        back_second(q).wait_recv()
        keep(q).wait()
        back_first(q).start()

    def finish_pair(q):
        pair.step_last(q)
        pair_keep(q).start()
        pair_core(q).start()

    late = 2
    steps = max(pairs + 8 * LAG, pair_chunks + 3 * LAG + late) + 1

    @pl.loop(0, steps)
    def _(step):
        during(step, 8 * LAG, pairs, both(arrived(back_first, back_core)))
        during(step, 7 * LAG, pairs, both(second_arrived))
        during(step, 6 * LAG, pairs, both(last_then_second))
        during(step, 5 * LAG, pairs, both(line.step_out))
        during(step, 4 * LAG, pairs, both(line.step_middle))
        during(step, 3 * LAG, pairs, both(stage_c))
        during(step, 2 * LAG, pairs, both(stage_b))
        during(step, LAG, pairs, both(stage_a))
        during(step, 3 * LAG, pairs, both(line.step_in))
        during(step, 2 * LAG, pairs, both(start(to_second)))
        during(step, LAG, pairs, both(start(to_first)))
        for m in range(rights):

            @pl.when(step == m * per_matrix // 2)
            def _(m=m):
                loads[2 + m].wait()
                if m == 0:
                    loads[0].wait()
                if m == rights - 1:
                    loads[1].wait()

        during(step, 0, pairs, both(make))
        during(step, 0, pairs, both(start(to_core)))

        @pl.when(step == 1)
        def _():
            for share in shares:
                share.wait()
            for at in thirds:
                pair_in[at] = added(pair_in[at], pair_more[at])

        @pl.when(step == 3)
        def _():
            for part in parts:
                part.wait()
            mixed_out[...] = (
                base_part[...] + mixed_part[0].astype(F32) + mixed_part[1].astype(F32)
            ).astype(BF16)

        during(step, 3 * LAG + late, pair_chunks, finish_pair)
        during(step, 2 * LAG + late, pair_chunks, pair.step_out)
        during(step, LAG + late, pair_chunks, pair.step_middle)
        during(step, late, pair_chunks, pair.step_in)

    @pl.loop(0, chunks)
    def _(q):
        back_core(q).wait_recv()
        for copy in (to_first, to_second, back_second, back_first, back_core):
            copy(q).wait_send()

        @pl.when(q >= chunks - RING)
        def _():
            to_core(q).wait_send()

        line.settle(q)

    @pl.loop(0, pair_chunks)
    def _(q):
        pair_core(q).wait()
        pair_keep(q).wait()
        pair.settle(q)


def reduce_grads(factors, half_own, first_y, rest_y, mixed, depth):
    count, width = factors[0].shape
    rights = len(factors) - 2
    rows = width * rights
    chunks = rows // CHUNK
    pair_chunks = 12
    total_rows, pair_cols = 3 * half_own.shape[1], half_own.shape[2]
    pair_rows = total_rows // pair_chunks
    vmem = pl.BlockSpec(memory_space=pltpu.VMEM)
    anywhere = pl.BlockSpec(memory_space=pl.ANY)

    def body(*refs):
        reduce_kernel(depth, refs[: len(factors)], *refs[len(factors) :])

    return pl.pallas_call(
        body,
        out_shape=(
            jax.ShapeDtypeStruct((rows, width), BF16),
            jax.ShapeDtypeStruct((total_rows, 2 * pair_cols), BF16),
            jax.ShapeDtypeStruct((count, width), BF16),
        ),
        in_specs=[anywhere] * (len(factors) + 6),
        out_specs=(anywhere, anywhere, vmem),
        scratch_shapes=[
            pltpu.VMEM((total_rows, pair_cols), BF16),
            pltpu.VMEM((2, count, width), BF16),
            pltpu.VMEM((rights, count, width), BF16),
            pltpu.VMEM((RING, CHUNK, width), BF16),
            pltpu.VMEM((chunks, CHUNK // 2, width), BF16),
            pltpu.VMEM((chunks, CHUNK // 4, width), BF16),
            pltpu.VMEM((chunks, CHUNK // 8, width), BF16),
            pltpu.VMEM((chunks, CHUNK // 8, width), BF16),
            pltpu.VMEM((chunks, CHUNK // 8, width), BF16),
            pltpu.VMEM((pair_chunks, pair_rows, pair_cols), BF16),
            pltpu.VMEM((pair_chunks, pair_rows, pair_cols), BF16),
            pltpu.SemaphoreType.DMA((9, 2, chunks)),
            pltpu.SemaphoreType.DMA((4, 2, pair_chunks)),
            pltpu.SemaphoreType.DMA((len(factors) + 3,)),
            pltpu.SemaphoreType.DMA((chunks,)),
            pltpu.SemaphoreType.DMA((pair_chunks,)),
            pltpu.VMEM((count, width), F32),
            pltpu.VMEM((2, count, width), BF16),
            pltpu.VMEM((total_rows, pair_cols), BF16),
            pltpu.SemaphoreType.DMA((2, 3)),
        ],
        compiler_params=pltpu.CompilerParams(
            collective_id=1, has_side_effects=True, vmem_limit_bytes=60 * 1024 * 1024
        ),
        name="reduce_grads",
    )(*factors, half_own, first_y, rest_y, *mixed)


ROWS = 256


def times(x, w):
    return jnp.dot(x, w, preferred_element_type=F32)


def times_back(x, w):
    return lax.dot_general(x, w, (((1,), (1,)), ((), ())), preferred_element_type=F32)


def times_rows(x, y):
    return lax.dot_general(x, y, (((0,), (0,)), ((), ())), preferred_element_type=F32)


def hidden_kernel(
    rows_own,
    grads_own,
    grads_nb,
    late_left,
    late_right,
    late_down,
    late_other,
    mixed,
    back,
    half_own,
    half_nb,
    back_in,
    from_y,
    both,
    own,
    other,
    kept,
    theirs,
    moved,
    acc_mixed,
    acc_back,
    load_sem,
    sems,
):
    core = lax.axis_index("dp")
    slot = lax.axis_index("tensor")
    count, width = rows_own.shape
    half = width // 2
    blocks = count // ROWS
    pairs = (
        (late_left, own.at[0]),
        (late_right, own.at[1]),
        (late_down, own.at[2]),
        (late_other, other),
        (rows_own, both.at[0, :count]),
        (grads_own, both.at[1, :count]),
        (grads_nb, both.at[1, count:]),
    )
    loads = [pltpu.make_async_copy(a, b, load_sem.at[i]) for i, (a, b) in enumerate(pairs)]
    for i in (4, 5, 0, 1, 2, 3, 6):
        loads[i].start()

    def send(source, target, at, peer):
        return pltpu.make_async_remote_copy(
            src_ref=source,
            dst_ref=target,
            send_sem=sems.at[0, at],
            recv_sem=sems.at[1, at],
            device_id=peer,
            device_id_type=MESH,
        )

    def span(i):
        return pl.ds(pl.multiple_of(i * ROWS, ROWS), ROWS)

    def out_rows(i):
        return send(
            rows_own.at[span(i)], both.at[0, span(blocks + i)], i, {"tensor": slot ^ 1}
        )

    def return_rows(i):
        return send(
            back.at[span(blocks + i)], back_in.at[span(i)], blocks + i, {"tensor": slot ^ 1}
        )

    def to_core(which, m):
        return send(
            theirs.at[which, m], moved.at[which, m], 2 * blocks + 3 * which + m, {"dp": 1 - core}
        )

    hand = send(half_nb.at[0], from_y, 2 * blocks + 6, {"tensor": slot ^ 2})
    barrier = pltpu.get_barrier_semaphore()
    for peer in ({"tensor": slot ^ 1}, {"tensor": slot ^ 2}, {"dp": 1 - core}):
        pl.semaphore_signal(barrier, inc=1, device_id=peer, device_id_type=MESH)
    pl.semaphore_wait(barrier, 3)
    for i in range(blocks):
        out_rows(i).start()
    for i in (4, 5, 0, 1, 2):
        loads[i].wait()

    def unit(i, which, weights):
        rows, grads = both[0, span(i)], both[1, span(i)]
        e1, e2 = times_back(rows, weights[0]), times_back(rows, weights[1])
        dm = times_back(grads, weights[2])
        mid = (e1 * e2).astype(BF16)
        de1 = (dm * e2).astype(BF16)
        de2 = (dm * e1).astype(BF16)
        kept[which, 2, span(i)] = mid
        kept[which, 0, span(i)] = de1
        kept[which, 1, span(i)] = de2
        return times(mid, weights[2]), times(de1, weights[0]) + times(de2, weights[1])

    @pl.loop(0, 2 * blocks)
    def _(i):
        @pl.when(i >= blocks)
        def _():
            out_rows(i - blocks).wait_recv()

        @pl.when(i == blocks)
        def _():
            loads[6].wait()

        acc_mixed[...], acc_back[...] = unit(i, 0, own)

        @pl.when(i == 0)
        def _():
            loads[3].wait()

        more_mixed, more_back = unit(i, 1, other)
        mixed[span(i)] = (acc_mixed[...] + more_mixed).astype(BF16)
        back[span(i)] = (acc_back[...] + more_back).astype(BF16)

        @pl.when(i >= blocks)
        def _():
            return_rows(i - blocks).start()

    here = pl.ds(pl.multiple_of(core * half, half), half)
    there = pl.ds(pl.multiple_of((1 - core) * half, half), half)

    def products(which, out, m):
        theirs[which, m] = times_rows(kept[which, m], both[m // 2, :, there]).astype(BF16)
        to_core(which, m).start()
        out[m] = times_rows(kept[which, m], both[m // 2, :, here]).astype(BF16)

    def combine(which, out, m):
        to_core(which, m).wait_recv()
        out[m] = added(out[m], moved[which, m])

    products(1, half_nb, 0)
    combine(1, half_nb, 0)
    hand.start()

    @pl.loop(1, 3)
    def _(m):
        products(1, half_nb, m)

    @pl.loop(0, 3)
    def _(m):
        products(0, half_own, m)

    for m in range(1, 3):
        combine(1, half_nb, m)
    for m in range(3):
        combine(0, half_own, m)
    for i in range(blocks):
        out_rows(i).wait_send()
        return_rows(i).wait()
    for which in range(2):
        for m in range(3):
            to_core(which, m).wait_send()
    hand.wait()


def hidden_part(rows_own, grads_own, grads_nb, shard, other):
    count, width = rows_own.shape
    hidden = shard[0].shape[0]
    vmem = pl.BlockSpec(memory_space=pltpu.VMEM)
    anywhere = pl.BlockSpec(memory_space=pl.ANY)
    half = jax.ShapeDtypeStruct((3, hidden, width // 2), BF16)
    two = jax.ShapeDtypeStruct((2 * count, width), BF16)
    return pl.pallas_call(
        hidden_kernel,
        out_shape=(
            two,
            two,
            half,
            half,
            jax.ShapeDtypeStruct((count, width), BF16),
            jax.ShapeDtypeStruct((hidden, width // 2), BF16),
        ),
        in_specs=[anywhere] * 7,
        out_specs=(vmem,) * 4 + (anywhere,) * 2,
        scratch_shapes=[
            pltpu.VMEM((2, 2 * count, width), BF16),
            pltpu.VMEM((3, hidden, width), BF16),
            pltpu.VMEM((3, hidden, width), BF16),
            pltpu.VMEM((2, 3, 2 * count, hidden), BF16),
            pltpu.VMEM((2, 3, hidden, width // 2), BF16),
            pltpu.VMEM((2, 3, hidden, width // 2), BF16),
            pltpu.VMEM((ROWS, width), F32),
            pltpu.VMEM((ROWS, width), F32),
            pltpu.SemaphoreType.DMA((7,)),
            pltpu.SemaphoreType.DMA((2, 2 * (count // ROWS) + 7)),
        ],
        compiler_params=pltpu.CompilerParams(
            collective_id=4, has_side_effects=True, vmem_limit_bytes=54 * 1024 * 1024
        ),
        name="hidden_part",
    )(rows_own, grads_own, grads_nb, *shard, other)


MESH = pl.DeviceIdType.MESH


class States:
    def __init__(self, depth, width, backward, powers, local, came, total, far, outs, states, sems):
        self.depth, self.width, self.backward, self.powers = depth, width, backward, powers
        self.local, self.came, self.total, self.far = local, came, total, far
        self.outs, self.states, self.sems = outs, states, sems
        self.slot = lax.axis_index("tensor")
        self.place = lax.axis_index("seq")
        self.share = local.shape[0] // width

    def greet(self, more=()):
        barrier = pltpu.get_barrier_semaphore()
        for peer in more:
            pl.semaphore_signal(barrier, inc=1, device_id=peer, device_id_type=MESH)
        for b in range(1, self.width):
            pl.semaphore_signal(
                barrier, inc=1, device_id={"tensor": self.slot ^ b}, device_id_type=MESH
            )
        for j in range(1, self.depth):
            peer = lax.rem(self.place + j, self.depth)
            pl.semaphore_signal(barrier, inc=1, device_id={"seq": peer}, device_id_type=MESH)
        pl.semaphore_wait(barrier, self.width + self.depth - 2 + len(more))

    def copy(self, source, target, at, peer):
        return pltpu.make_async_remote_copy(
            src_ref=source,
            dst_ref=target,
            send_sem=self.sems.at[0, at],
            recv_sem=self.sems.at[1, at],
            device_id=peer,
            device_id_type=MESH,
        )

    def group(self, slot):
        return pl.ds(slot * self.share, self.share)

    def to_peer(self, b):
        peer = self.slot ^ b
        return self.copy(
            self.local.at[self.group(peer)], self.came.at[b - 1], b - 1, {"tensor": peer}
        )

    def to_far(self, j):
        peer = self.place - j if self.backward else self.place + j
        return self.copy(self.total, self.far.at[j - 1], self.width + j - 2, {"seq": peer})

    def has_far(self, j):
        return self.place >= j if self.backward else self.place + j < self.depth

    def from_far(self, j):
        return self.place + j < self.depth if self.backward else self.place >= j

    def to_owner(self, d):
        at = self.width + self.depth - 2 + d - 1
        return self.copy(
            self.outs.at[d - 1],
            self.states.at[self.group(self.slot)],
            at,
            {"tensor": self.slot ^ d},
        )

    def power(self, count, head):
        return self.powers[count, head]

    def piece(self, b, k, s):
        if b == 0:
            return self.local[self.slot * self.share + k, s].astype(F32)
        return self.came[b - 1, k, s].astype(F32)

    def gather(self):
        for b in range(1, self.width):
            self.to_peer(b).wait_recv()
        for k in range(self.share):
            head = self.slot * self.share + k
            for s in range(self.local.shape[1]):
                value = 0.0
                for b in range(self.width):
                    spot = self.slot ^ b
                    left = spot if self.backward else self.width - 1 - spot
                    value = value + self.power(left, head) * self.piece(b, k, s)
                self.total[k, s] = value.astype(BF16)
        for j in range(1, self.depth):

            @pl.when(self.has_far(j))
            def _(j=j):
                self.to_far(j).start()

    def send_back(self, entering, between):
        for j in range(1, self.depth):

            @pl.when(self.from_far(j))
            def _(j=j):
                self.to_far(j).wait_recv()

            @pl.when(jnp.logical_not(self.from_far(j)))
            def _(j=j):
                self.far[j - 1] = jnp.zeros(self.far.shape[1:], BF16)

        between()
        for k in range(self.share):
            head = self.slot * self.share + k
            for s in range(self.local.shape[1]):
                value = 0.0
                for j in range(1, self.depth):
                    value = value + self.power(self.width * (j - 1), head) * self.far[
                        j - 1, k, s
                    ].astype(F32)
                entering[k, s] = value
        for d in list(range(1, self.width)) + [0]:
            target = self.slot ^ d
            inner = self.width - 1 - target if self.backward else target
            for k in range(self.share):
                head = self.slot * self.share + k
                for s in range(self.local.shape[1]):
                    value = self.power(inner, head) * entering[k, s]
                    for b in range(self.width):
                        if b == d:
                            continue
                        source = self.slot ^ b
                        gap = source - target - 1 if self.backward else target - source - 1
                        coef = jnp.where(gap >= 0, self.power(jnp.maximum(gap, 0), head), 0.0)
                        value = value + coef * self.piece(b, k, s)
                    if d == 0:
                        self.states[head, s] = value.astype(BF16)
                    else:
                        self.outs[d - 1, k, s] = value.astype(BF16)
        for d in range(1, self.width):
            self.to_owner(d).start()

    def arrive(self):
        for d in range(1, self.width):
            at = self.width + self.depth - 2 + d - 1
            self.copy(
                self.outs.at[d - 1],
                self.states.at[self.group(self.slot ^ d)],
                at,
                {"tensor": self.slot ^ d},
            ).wait_recv()

    def settle(self):
        for b in range(1, self.width):
            self.to_peer(b).wait_send()
            self.to_owner(b).wait_send()
        for j in range(1, self.depth):

            @pl.when(self.has_far(j))
            def _(j=j):
                self.to_far(j).wait_send()


def state_scratch(heads, seqs, head_dim, width, depth):
    share = heads // width
    low = functools.partial(pltpu.VMEM, dtype=BF16)
    return [
        low((heads, seqs, head_dim, head_dim)),
        low((width - 1, share, seqs, head_dim, head_dim)),
        low((share, seqs, head_dim, head_dim)),
        low((depth - 1, share, seqs, head_dim, head_dim)),
        low((width - 1, share, seqs, head_dim, head_dim)),
        pltpu.VMEM((share, seqs, head_dim, head_dim), F32),
        pltpu.SemaphoreType.DMA((2, 2 * (width - 1) + depth - 1)),
    ]


def turn(values, cosine, sine_part):
    return values * cosine + pltpu.roll(values, values.shape[-1] // 2, 1) * sine_part


def square_mean(values):
    return jnp.mean(values * values, axis=-1, keepdims=True)


def decays(rates, head, length, dim):
    rate = rates[head]
    place = lax.broadcasted_iota(jnp.int32, (length, dim), 0).astype(F32)
    query = jnp.exp(-rate[:, :dim] * (place + 1.0))
    key = jnp.exp(-rate[:, :dim] * (length - 1.0 - place))
    return query, key


def lag_decay(rates, head, length):
    lag = (
        lax.broadcasted_iota(jnp.int32, (length, length), 0)
        - lax.broadcasted_iota(jnp.int32, (length, length), 1)
    ).astype(F32)
    return jnp.where(lag >= 0, jnp.exp(-rates[head] * jnp.maximum(lag, 0.0)), 0.0)


def attend_kernel(
    depth,
    width,
    seqs,
    first_x,
    first_key,
    first_value,
    late_query,
    late_gate,
    late_output,
    left,
    right,
    down,
    grads,
    rates,
    powers,
    cosine,
    sine_part,
    residual,
    normed_two,
    attended,
    gated,
    states,
    early_outs,
    other,
    grads_nb,
    early,
    x,
    w_key,
    w_value,
    w_query,
    w_gate,
    w_output,
    local,
    came,
    total,
    far,
    outs,
    entering,
    sems,
    load_sem,
    bulk_sems,
    store_sem,
):
    (
        query_pre,
        key_pre,
        gate,
        normed_one,
        query_low,
        key_low,
        value_low,
        query_dec,
        key_dec,
        scores_low,
    ) = early
    stores = [
        pltpu.make_async_copy(a, b, store_sem.at[i])
        for i, (a, b) in enumerate(zip(early, early_outs))
    ]
    rows, model = x.shape
    length = rows // seqs
    dim = cosine.shape[1]
    tile = model // width
    loads = [
        pltpu.make_async_copy(a, b, load_sem.at[i])
        for i, (a, b) in enumerate(
            (
                (late_query, w_query),
                (late_gate, w_gate),
                (late_output, w_output),
                (first_x, x),
                (first_key, w_key),
                (first_value, w_value),
            )
        )
    ]
    loads = loads[3:] + loads[:3]
    for load in loads:
        load.start()
    exchange = States(
        depth, width, False, powers, local, came, total, far, outs, states, sems
    )
    core = lax.axis_index("dp")
    parity = lax.rem(exchange.place, 2)
    shard = (left, right, down)
    part_rows, part_cols = left.shape[0] // 2, model // 2
    columns_here = pl.ds(pl.multiple_of(core * part_cols, part_cols), part_cols)

    def rows_of(which):
        return pl.ds(pl.multiple_of(which * part_rows, part_rows), part_rows)

    def send(source, target, at, peer):
        return pltpu.make_async_remote_copy(
            src_ref=source,
            dst_ref=target,
            send_sem=bulk_sems.at[0, at],
            recv_sem=bulk_sems.at[1, at],
            device_id=peer,
            device_id_type=MESH,
        )

    def fetch(m):
        at = (rows_of(parity), columns_here)
        return send(
            shard[m].at[at], other.at[(m,) + at], m, {"tensor": exchange.slot ^ 2}
        )

    def relay(m):
        at = other.at[m, rows_of(parity), columns_here]
        return send(at, at, 3 + m, {"seq": exchange.place + 1 - 2 * parity})

    def share(m, which):
        spot = parity if which == 0 else 1 - parity
        at = other.at[m, rows_of(spot), columns_here]
        return send(at, at, 6 + 2 * m + which, {"dp": 1 - core})

    def cross(s):
        at = pl.ds(s * length, length)
        return send(grads.at[at], grads_nb.at[at], 12 + s, {"tensor": exchange.slot ^ 1})

    def pass_on(m):
        fetch(m).wait_recv()
        relay(m).start()
        share(m, 0).start()

    def pass_last(m):
        relay(m).wait_recv()
        share(m, 1).start()

    exchange.greet((({"dp": 1 - core}),))
    fetch(0).start()
    cross(0).start()
    loads[0].wait()
    for s in range(seqs):
        at = pl.ds(s * length, length)
        value = x[at].astype(F32)
        normed_one[at] = (value * lax.rsqrt(square_mean(value) + EPS)).astype(BF16)

    per_tile = tile // dim
    loads[1].wait()
    loads[2].wait()

    @pl.loop(1, width + 1)
    def _(step):
        b = lax.rem(step, width)
        spot = exchange.slot ^ b
        columns = pl.ds(pl.multiple_of(spot * tile, tile), tile)
        key_pre[:, columns] = times(normed_one[...], w_key[:, columns])
        value_low[:, columns] = times(normed_one[...], w_value[:, columns]).astype(BF16)
        for k in range(per_tile):
            head = spot * per_tile + k
            own = pl.ds(pl.multiple_of(spot * tile + k * dim, dim), dim)
            _, key_weight = decays(rates, head, length, dim)
            for s in range(seqs):
                at = pl.ds(s * length, length)
                turned = turn(jax.nn.silu(key_pre[at, own]), cosine[...], sine_part[...])
                key_low[at, own] = turned.astype(BF16)
                dec = (turned * key_weight).astype(BF16)
                key_dec[at, own] = dec
                local[head, s] = times_rows(dec, value_low[at, own]).astype(BF16)

        for b_static in range(1, width):

            @pl.when(b == b_static)
            def _(b_static=b_static):
                exchange.to_peer(b_static).start()

    for s in range(1, seqs):
        cross(s).start()
    fetch(1).start()
    fetch(2).start()
    pass_on(0)
    loads[3].wait()
    loads[4].wait()

    def inner(spot):
        columns = pl.ds(pl.multiple_of(spot * tile, tile), tile)
        query_pre[:, columns] = times(normed_one[...], w_query[:, columns])
        gate[:, columns] = times(normed_one[...], w_gate[:, columns])
        for k in range(per_tile):
            head = spot * per_tile + k
            own = pl.ds(pl.multiple_of(spot * tile + k * dim, dim), dim)
            query_weight, _ = decays(rates, head, length, dim)
            mask = lag_decay(rates, head, length)
            for s in range(seqs):
                at = pl.ds(s * length, length)
                turned = turn(jax.nn.silu(query_pre[at, own]), cosine[...], sine_part[...])
                low_query = turned.astype(BF16)
                query_low[at, own] = low_query
                query_dec[at, own] = (turned * query_weight).astype(BF16)
                low_scores = (times_back(low_query, key_low[at, own]) * mask).astype(BF16)
                scores_low[head, s] = low_scores
                attended[at, own] = times(low_scores, value_low[at, own])

    half = width // 2

    @pl.loop(0, half)
    def _(spot):
        inner(spot)

    exchange.gather()

    @pl.loop(half, width)
    def _(spot):
        inner(spot)

    def relays():
        pass_on(1)
        pass_on(2)

    exchange.send_back(entering, relays)
    for store in stores:
        store.start()
    pass_last(0)
    loads[5].wait()
    exchange.arrive()
    pass_last(1)

    @pl.loop(0, width * per_tile)
    def _(head):
        own = pl.ds(pl.multiple_of(head * dim, dim), dim)
        for s in range(seqs):
            at = pl.ds(s * length, length)
            attended[at, own] += times(query_dec[at, own], states[head, s])

    for s in range(seqs):
        at = pl.ds(s * length, length)
        value = attended[at]
        gated[at] = (value * lax.rsqrt(square_mean(value) + EPS) * gate[at]).astype(BF16)

    @pl.loop(0, width)
    def _(spot):
        columns = pl.ds(pl.multiple_of(spot * tile, tile), tile)
        residual[:, columns] = x[:, columns].astype(F32) + times(
            gated[...], w_output[:, columns]
        )

    for s in range(seqs):
        at = pl.ds(s * length, length)
        value = residual[at]
        normed_two[at] = (value * lax.rsqrt(square_mean(value) + EPS)).astype(BF16)
    pass_last(2)
    for store in stores:
        store.wait()
    exchange.settle()
    for m in range(3):
        fetch(m).wait_send()
        relay(m).wait_send()
        share(m, 0).wait()
        share(m, 1).wait()
    for s in range(seqs):
        cross(s).wait()


def attend(x, weights, shard, grads, rates, powers, cosine, sine_part, seqs, depth, width):
    rows, model = x.shape
    heads = rates.shape[0]
    dim = model // heads
    length = rows // seqs
    vmem = pl.BlockSpec(memory_space=pltpu.VMEM)
    anywhere = pl.BlockSpec(memory_space=pl.ANY)
    wide = jax.ShapeDtypeStruct((rows, model), F32)
    low = jax.ShapeDtypeStruct((rows, model), BF16)
    w_query, w_key, w_value, w_gate, w_output = weights
    early = (wide,) * 3 + (low,) * 6 + (
        jax.ShapeDtypeStruct((heads, seqs, length, length), BF16),
    )

    def body(*refs):
        at = 14 + 5
        kept = at + len(early)
        scratch = kept + 2
        attend_kernel(
            depth,
            width,
            seqs,
            *refs[:at],
            refs[at:kept],
            *refs[kept:scratch],
            refs[scratch : scratch + len(early)],
            *refs[scratch + len(early) :],
        )

    return pl.pallas_call(
        body,
        out_shape=(
            wide,
            low,
            wide,
            low,
            jax.ShapeDtypeStruct((heads, seqs, dim, dim), BF16),
        )
        + early
        + (jax.ShapeDtypeStruct((3,) + shard[0].shape, BF16), low),
        in_specs=[anywhere] * 10 + [vmem] * 4,
        out_specs=(vmem,) * 5 + (anywhere,) * (len(early) + 2),
        scratch_shapes=[pltpu.VMEM(v.shape, v.dtype) for v in early]
        + [pltpu.VMEM((rows, model), BF16)]
        + [pltpu.VMEM((model, model), BF16)] * 5
        + state_scratch(heads, seqs, dim, width, depth)
        + [
            pltpu.SemaphoreType.DMA((6,)),
            pltpu.SemaphoreType.DMA((2, 12 + seqs)),
            pltpu.SemaphoreType.DMA((len(early),)),
        ],
        compiler_params=pltpu.CompilerParams(
            collective_id=2, has_side_effects=True, vmem_limit_bytes=56 * 1024 * 1024
        ),
        name="attend",
    )(
        x,
        w_key,
        w_value,
        w_query,
        w_gate,
        w_output,
        *shard,
        grads,
        rates,
        powers,
        cosine,
        sine_part,
    )


def retreat_kernel(
    depth,
    width,
    seqs,
    residual,
    back_own,
    back_in,
    grads,
    rates,
    powers,
    cosine,
    sine_part,
    mixed_nb,
    half_nb,
    *rest,
):
    late = rest[:17]
    (
        grad_mid_low,
        gate_low,
        query_out,
        key_out,
        value_out,
        grad_tokens,
        mixed_in,
        from_y,
    ) = rest[17:25]
    held = rest[25:42]
    (
        w_output,
        attended,
        gate,
        query_low,
        key_low,
        value_low,
        query_dec,
        scores_low,
        states_in,
        query_pre,
        w_query,
        w_gate,
        key_dec,
        key_pre,
        w_key,
        w_value,
        x,
    ) = held
    (
        states,
        grad_mid,
        work,
        grad_att,
        value_part,
        key_part,
        local,
        came,
        total,
        far,
        outs,
        entering,
        sems,
        load_sem,
        bulk_sems,
    ) = rest[42:]
    rows, model = residual.shape
    length = rows // seqs
    dim = cosine.shape[1]
    tile = model // width
    per_tile = tile // dim
    loads = [
        pltpu.make_async_copy(a, b, load_sem.at[i]) for i, (a, b) in enumerate(zip(late, held))
    ]
    for load in loads:
        load.start()
    exchange = States(
        depth, width, True, powers, local, came, total, far, outs, states, sems
    )

    def send(source, target, at, peer):
        return pltpu.make_async_remote_copy(
            src_ref=source,
            dst_ref=target,
            send_sem=bulk_sems.at[0, at],
            recv_sem=bulk_sems.at[1, at],
            device_id=peer,
            device_id_type=MESH,
        )

    crosses, hands = 4, 8
    cross_rows, hand_rows = rows // crosses, 2 * half_nb.shape[1] // hands

    def cross(k):
        at = pl.ds(k * cross_rows, cross_rows)
        source = mixed_nb.at[pl.ds(rows + k * cross_rows, cross_rows)]
        return send(source, mixed_in.at[at], k, {"tensor": exchange.slot ^ 1})

    def hand(k):
        m, at = k // (hands // 2), pl.ds(k % (hands // 2) * hand_rows, hand_rows)
        return send(
            half_nb.at[m + 1, at], from_y.at[m, at], crosses + k, {"tensor": exchange.slot ^ 2}
        )

    def start_bulk(some_crosses, some_hands):
        for k in some_crosses:
            cross(k).start()
        for k in some_hands:
            hand(k).start()

    exchange.greet()
    start_bulk(range(1), range(2))

    def spans():
        return [pl.ds(s * length, length) for s in range(seqs)]

    for at in spans():
        value = residual[at]
        scale = lax.rsqrt(square_mean(value) + EPS)
        normed = value * scale
        grad = back_own[at].astype(F32) + back_in[at].astype(F32)
        grad = grads[at].astype(F32) + scale * (
            grad - normed * jnp.mean(grad * normed, axis=-1, keepdims=True)
        )
        grad_mid[at] = grad
        grad_mid_low[at] = grad.astype(BF16)

    def columns_of(spot):
        return pl.ds(pl.multiple_of(spot * tile, tile), tile)

    for load in loads[:3]:
        load.wait()

    @pl.loop(0, width)
    def _(spot):
        work[:, columns_of(spot)] = times_back(grad_mid_low[...], w_output[columns_of(spot)])

    for at in spans():
        value = attended[at]
        scale = lax.rsqrt(square_mean(value) + EPS)
        normed = value * scale
        grad = work[at]
        gate_low[at] = (grad * normed).astype(BF16)
        grad = grad * gate[at]
        grad_att[at] = (
            scale * (grad - normed * jnp.mean(grad * normed, axis=-1, keepdims=True))
        ).astype(BF16)

    for load in loads[3:10]:
        load.wait()

    @pl.loop(1, width + 1)
    def _(step):
        b = lax.rem(step, width)
        spot = exchange.slot ^ b
        for k in range(per_tile):
            own = pl.ds(pl.multiple_of(spot * tile + k * dim, dim), dim)
            for s, at in enumerate(spans()):
                local[spot * per_tile + k, s] = times_rows(
                    query_dec[at, own], grad_att[at, own]
                ).astype(BF16)

        for b_static in range(1, width):

            @pl.when(b == b_static)
            def _(b_static=b_static):
                exchange.to_peer(b_static).start()

    start_bulk(range(1, 3), range(2, 5))

    def slope(values):
        sigmoid_v = jax.nn.sigmoid(values)
        return sigmoid_v * (1.0 + values * (1.0 - sigmoid_v))

    def inner(spot):
        for k in range(per_tile):
            head = spot * per_tile + k
            own = pl.ds(pl.multiple_of(spot * tile + k * dim, dim), dim)
            query_weight, _ = decays(rates, head, length, dim)
            mask = lag_decay(rates, head, length)
            for s, at in enumerate(spans()):
                grad = grad_att[at, own]
                value_part[at, own] = times_rows(scores_low[head, s], grad)
                score = (times_back(grad, value_low[at, own]) * mask).astype(BF16)
                key_part[at, own] = times_rows(score, query_low[at, own])
                turned = times(score, key_low[at, own]) + query_weight * times_back(
                    grad, states_in[head, s]
                )
                query_out[at, own] = (
                    turn(turned, cosine[...], -sine_part[...]) * slope(query_pre[at, own])
                ).astype(BF16)

    half = width // 2

    @pl.loop(0, half)
    def _(spot):
        inner(spot)

    exchange.gather()

    @pl.loop(half, width)
    def _(spot):
        inner(spot)

    exchange.send_back(entering, lambda: None)
    start_bulk(range(3, crosses), range(5, hands))
    for load in loads[10:]:
        load.wait()

    @pl.loop(0, width)
    def _(spot):
        at = columns_of(spot)
        work[:, at] = times_back(query_out[...], w_query[at]) + times_back(
            gate_low[...], w_gate[at]
        )

    exchange.arrive()

    @pl.loop(0, width * per_tile)
    def _(head):
        own = pl.ds(pl.multiple_of(head * dim, dim), dim)
        _, key_weight = decays(rates, head, length, dim)
        for s, at in enumerate(spans()):
            state = states[head, s]
            value_out[at, own] = (
                value_part[at, own] + times(key_dec[at, own], state)
            ).astype(BF16)
            turned = key_part[at, own] + key_weight * times_back(value_low[at, own], state)
            key_out[at, own] = (
                turn(turned, cosine[...], -sine_part[...]) * slope(key_pre[at, own])
            ).astype(BF16)

    @pl.loop(0, width)
    def _(spot):
        at = columns_of(spot)
        work[:, at] += times_back(key_out[...], w_key[at]) + times_back(
            value_out[...], w_value[at]
        )

    for at in spans():
        value = x[at].astype(F32)
        scale = lax.rsqrt(square_mean(value) + EPS)
        normed = value * scale
        grad = work[at]
        grad_tokens[at] = grad_mid[at] + scale * (
            grad - normed * jnp.mean(grad * normed, axis=-1, keepdims=True)
        )
    exchange.settle()
    for k in range(crosses):
        cross(k).wait()
    for k in range(hands):
        hand(k).wait()


def retreat(early, tables, bulk, late, seqs, depth, width):
    rows, model = early[0].shape
    heads = tables[0].shape[0]
    dim = model // heads
    vmem = pl.BlockSpec(memory_space=pltpu.VMEM)
    anywhere = pl.BlockSpec(memory_space=pl.ANY)
    wide = jax.ShapeDtypeStruct((rows, model), F32)
    low = jax.ShapeDtypeStruct((rows, model), BF16)
    return pl.pallas_call(
        functools.partial(retreat_kernel, depth, width, seqs),
        out_shape=(low,) * 5 + (wide, low, jax.ShapeDtypeStruct((2,) + bulk[1].shape[1:], BF16)),
        in_specs=[vmem] * (len(early) + len(tables)) + [anywhere] * (len(bulk) + len(late)),
        out_specs=(vmem,) * 6 + (anywhere,) * 2,
        scratch_shapes=[pltpu.VMEM(v.shape, v.dtype) for v in late]
        + [
            pltpu.VMEM((heads, seqs, dim, dim), BF16),
            pltpu.VMEM((rows, model), F32),
            pltpu.VMEM((rows, model), F32),
            pltpu.VMEM((rows, model), BF16),
            pltpu.VMEM((rows, model), F32),
            pltpu.VMEM((rows, model), F32),
        ]
        + state_scratch(heads, seqs, dim, width, depth)
        + [pltpu.SemaphoreType.DMA((len(late),)), pltpu.SemaphoreType.DMA((2, 12))],
        compiler_params=pltpu.CompilerParams(
            collective_id=3, has_side_effects=True, vmem_limit_bytes=60 * 1024 * 1024
        ),
        name="retreat",
    )(*early, *tables, *bulk, *late)


def on_device(
    tokens,
    w_query,
    w_key,
    w_value,
    w_ugate,
    w_output,
    w_left,
    w_right,
    w_down,
    decay_rate,
    cotangent,
):
    seq_count, group_len, model_width = tokens.shape
    head_count = decay_rate.shape[0]
    head_dim = model_width // head_count
    half_dim = head_dim // 2
    row_count = seq_count * group_len
    core = lax.axis_index("dp")

    shard = (w_left.T, w_right.T, w_down)
    grad_own = cotangent.reshape(row_count, model_width)

    position_block = lax.axis_index(("seq", "tensor"))
    places = (position_block * group_len + jnp.arange(group_len)).astype(F32)
    frequency = 10000.0 ** (-jnp.arange(half_dim, dtype=F32) / half_dim)
    angles = places[:, None] * frequency[None, :]
    cosine, sine_part = jnp.cos(angles), jnp.sin(angles)
    cosine = jnp.concatenate([cosine, cosine], axis=1)
    sine_part = jnp.concatenate([-sine_part, sine_part], axis=1)
    rows_in = tokens.reshape(row_count, model_width)
    depth = lax.axis_size("seq")
    width = lax.axis_size("tensor")
    rates = jnp.broadcast_to(decay_rate[:, None, None], (head_count, 1, group_len))
    blocks = jnp.arange(depth * width, dtype=F32)[:, None, None, None]
    powers = jnp.broadcast_to(
        jnp.exp(-decay_rate[None, :, None, None] * group_len * blocks),
        (depth * width, head_count, 1, head_dim),
    )
    (
        residual,
        rows_own,
        merged,
        gated_low,
        state_low,
        query_pre,
        key_pre,
        ugate,
        normed_low,
        query_low,
        key_low,
        value_low,
        query_dec,
        key_dec,
        weights_low,
        other,
        grad_nb,
    ) = attend(
        rows_in,
        (w_query, w_key, w_value, w_ugate, w_output),
        shard,
        grad_own,
        rates,
        powers,
        cosine,
        sine_part,
        seq_count,
        depth,
        width,
    )
    mixed, back, half_own, half_nb, back_in, first_y = hidden_part(
        rows_own, grad_own, grad_nb, shard, other
    )
    (
        grad_branch,
        grad_ugate_pre,
        grad_query_pre,
        grad_key_pre,
        grad_value_pre,
        grad_tokens,
        mixed_in,
        from_y,
    ) = retreat(
        (residual, back, back_in, grad_own),
        (rates, powers, cosine, sine_part),
        (mixed, half_nb),
        (
            w_output,
            merged,
            ugate,
            query_low,
            key_low,
            value_low,
            query_dec,
            weights_low,
            state_low,
            query_pre,
            w_query,
            w_ugate,
            key_dec,
            key_pre,
            w_key,
            w_value,
            rows_in,
        ),
        seq_count,
        depth,
        width,
    )

    hidden = w_down.shape[0]
    sums, hidden_sums, mixed_out = reduce_grads(
        (
            normed_low,
            gated_low,
            grad_query_pre,
            grad_key_pre,
            grad_value_pre,
            grad_ugate_pre,
            grad_branch,
        ),
        half_own,
        first_y,
        from_y,
        (residual, mixed, mixed_in),
        depth,
    )
    attention_grads = tuple(
        sums[i * model_width : (i + 1) * model_width].astype(F32) for i in range(5)
    )
    left_sum, right_sum, down_sum = (
        hidden_sums[i * hidden : (i + 1) * hidden].astype(F32) for i in range(3)
    )
    return (
        (mixed_out.reshape(tokens.shape), grad_tokens.reshape(tokens.shape))
        + attention_grads
        + (left_sum.T, right_sum.T, down_sum)
    )


def solution(mesh):
    rows = P("dp", ("seq", "tensor"), None)
    columns = P(None, "tensor")
    return jax.shard_map(
        on_device,
        mesh=mesh,
        in_specs=(rows, P(), P(), P(), P(), P(), columns, columns, P("tensor", None), P(), rows),
        out_specs=(rows, rows, P(), P(), P(), P(), P(), columns, columns, P("tensor", None)),
        check_vma=False,
    )
```

```python
import functools

import jax
import jax.numpy as jnp
from jax import lax
from jax.experimental import pallas as pl
from jax.experimental.pallas import tpu as pltpu
from jax.sharding import PartitionSpec as P


EPS = 1e-06
F32 = jnp.float32
BF16 = jnp.bfloat16


CHUNK = 256
LAG = 1


def added(first, second):
    return (first.astype(F32) + second.astype(F32)).astype(BF16)


RING = 8


def reduce_kernel(
    depth,
    factors,
    pair_own,
    pair_first,
    pair_rest,
    residual,
    mixed_own,
    mixed_nb,
    out,
    pair_out,
    mixed_out,
    pair_in,
    left_side,
    right_side,
    own,
    core_in,
    first_in,
    second_in,
    line_in,
    line_mid,
    pair_line,
    pair_mid,
    sems,
    pair_sems,
    load_sem,
    keep_sem,
    pair_keep_sem,
    base_part,
    mixed_part,
    pair_more,
    share_sem,
):
    core = lax.axis_index("dp")
    slot = lax.axis_index("tensor")
    place = lax.axis_index("seq")
    rows = out.shape[0]
    chunks = rows // CHUNK
    half, quarter, eighth = CHUNK // 2, CHUNK // 4, CHUNK // 8
    low_side = place < depth // 2
    outermost = (place == 0) | (place == depth - 1)
    middle = (place == depth // 2 - 1) | (place == depth // 2)
    inward = jnp.where(low_side, place + 1, place - 1)
    outward = jnp.where(outermost, inward, jnp.where(low_side, place - 1, place + 1))

    barrier = pltpu.get_barrier_semaphore()

    def greet(peer):
        pl.semaphore_signal(
            barrier, inc=1, device_id=peer, device_id_type=pl.DeviceIdType.MESH
        )

    greet({"dp": 1 - core})
    greet({"tensor": slot ^ 1})
    greet({"tensor": slot ^ 2})

    @pl.when(place > 0)
    def _():
        greet({"seq": place - 1})

    @pl.when(place < depth - 1)
    def _():
        greet({"seq": place + 1})

    pl.semaphore_wait(barrier, jnp.where(outermost, 4, 5))

    def remote(source, target, sem, at, peer):
        return pltpu.make_async_remote_copy(
            src_ref=source,
            dst_ref=target,
            send_sem=sem.at[0, at],
            recv_sem=sem.at[1, at],
            device_id=peer,
            device_id_type=pl.DeviceIdType.MESH,
        )

    def span(start, size):
        return pl.ds(pl.multiple_of(start, size), size)

    def bits(q):
        first = jnp.where(q % 2 == 0, 1, 2)
        second = 3 - first
        return first, second, (slot & first) // first, (slot & second) // second

    def base(q):
        return pl.multiple_of(q * CHUNK, CHUNK)

    def to_core(q):
        return remote(
            own.at[q % RING, span((1 - core) * half, half)],
            core_in.at[q],
            sems.at[0],
            q,
            {"dp": 1 - core},
        )

    def to_first(q):
        first, _, f, _ = bits(q)
        return remote(
            core_in.at[q, span((1 - f) * quarter, quarter)],
            first_in.at[q],
            sems.at[1],
            q,
            {"tensor": slot ^ first},
        )

    def to_second(q):
        _, second, _, g = bits(q)
        return remote(
            first_in.at[q, span((1 - g) * eighth, eighth)],
            second_in.at[q],
            sems.at[2],
            q,
            {"tensor": slot ^ second},
        )

    def block(q):
        _, _, f, g = bits(q)
        return base(q) + core * half + f * quarter + g * eighth

    def keep(q):
        return pltpu.make_async_copy(
            line_mid.at[q], out.at[span(block(q), eighth)], keep_sem.at[q]
        )

    def back_second(q):
        _, second, _, _ = bits(q)
        at = span(block(q), eighth)
        return remote(line_mid.at[q], out.at[at], sems.at[3], q, {"tensor": slot ^ second})

    def back_first(q):
        first, _, f, _ = bits(q)
        at = span(base(q) + core * half + f * quarter, quarter)
        return remote(out.at[at], out.at[at], sems.at[4], q, {"tensor": slot ^ first})

    def back_core(q):
        at = span(base(q) + core * half, half)
        return remote(out.at[at], out.at[at], sems.at[5], q, {"dp": 1 - core})

    class Line:
        def __init__(self, mine, came, met, sem, offset):
            self.mine, self.came, self.met = mine, came, met
            self.sem, self.offset = sem, offset

        def inwards(self, q, source):
            return remote(
                source, self.came(q), self.sem.at[self.offset], q, {"seq": inward}
            )

        def across(self, q):
            return remote(
                self.came(q),
                self.met(q),
                self.sem.at[self.offset + 1],
                q,
                {"seq": depth - 1 - place},
            )

        def outwards(self, q):
            return remote(
                self.met(q), self.met(q), self.sem.at[self.offset + 2], q, {"seq": outward}
            )

        def step_in(self, q):
            @pl.when(outermost)
            def _():
                self.inwards(q, self.mine(q)).start()

        def step_middle(self, q):
            @pl.when(jnp.logical_not(outermost))
            def _():
                self.inwards(q, self.mine(q)).wait_recv()
                came = self.came(q)
                came[...] = added(self.mine(q)[...], came[...])

                @pl.when(middle)
                def _():
                    self.across(q).start()

                @pl.when(jnp.logical_not(middle))
                def _():
                    self.inwards(q, came).start()

        def step_out(self, q):
            @pl.when(middle)
            def _():
                self.across(q).wait_recv()
                met = self.met(q)
                met[...] = added(self.came(q)[...], met[...])

            @pl.when(jnp.logical_not(outermost))
            def _():
                @pl.when(jnp.logical_not(middle))
                def _():
                    self.outwards(q).wait_recv()

                self.outwards(q).start()

        def step_last(self, q):
            @pl.when(outermost)
            def _():
                self.outwards(q).wait_recv()

        def settle(self, q):
            @pl.when(outermost)
            def _():
                self.inwards(q, self.mine(q)).wait_send()

            @pl.when(jnp.logical_not(outermost))
            def _():
                @pl.when(middle)
                def _():
                    self.across(q).wait_send()

                @pl.when(jnp.logical_not(middle))
                def _():
                    self.inwards(q, self.came(q)).wait_send()

                self.outwards(q).wait_send()

    def second_mine(q):
        return second_in.at[q]

    line = Line(
        second_mine,
        lambda q: line_in.at[q],
        lambda q: line_mid.at[q],
        sems,
        6,
    )
    pair_chunks, pair_rows, pair_cols = pair_line.shape
    pair = Line(
        lambda q: pair_in.at[span(q * pair_rows, pair_rows)],
        lambda q: pair_line.at[q],
        lambda q: pair_mid.at[q],
        pair_sems,
        0,
    )

    def pair_block(q):
        return pair_out.at[span(q * pair_rows, pair_rows), span(core * pair_cols, pair_cols)]

    def pair_keep(q):
        return pltpu.make_async_copy(pair_mid.at[q], pair_block(q), pair_keep_sem.at[q])

    def pair_core(q):
        return remote(pair_mid.at[q], pair_block(q), pair_sems.at[3], q, {"dp": 1 - core})

    rights = len(factors) - 2
    loads = [
        pltpu.make_async_copy(g, t, load_sem.at[i])
        for i, (g, t) in enumerate(
            zip(
                factors,
                [left_side.at[0], left_side.at[1]] + [right_side.at[i] for i in range(rights)],
            )
        )
    ]
    tokens = residual.shape[0]
    parts = [
        pltpu.make_async_copy(a, b, load_sem.at[len(factors) + i])
        for i, (a, b) in enumerate(
            (
                (residual, base_part),
                (mixed_own.at[:tokens], mixed_part.at[0]),
                (mixed_nb, mixed_part.at[1]),
            )
        )
    ]
    hidden = pair_first.shape[0]
    thirds = [pl.ds(m * hidden, hidden) for m in range(3)]
    shares = [
        pltpu.make_async_copy(pair_own.at[m], pair_in.at[thirds[m]], share_sem.at[0, m])
        for m in range(3)
    ] + [
        pltpu.make_async_copy(
            pair_first if m == 0 else pair_rest.at[m - 1],
            pair_more.at[thirds[m]],
            share_sem.at[1, m],
        )
        for m in range(3)
    ]
    for load in [loads[0], loads[2]] + shares + [loads[1]] + loads[3:] + parts:
        load.start()
    per_matrix = chunks // rights

    def make(q):
        @pl.when(q >= RING)
        def _():
            to_core(q - RING).wait_send()

        m = q // per_matrix
        columns = pl.ds(pl.multiple_of((q % per_matrix) * CHUNK, CHUNK), CHUNK)
        own[q % RING] = times_rows(
            left_side[m // (rights - 1), :, columns], right_side[m]
        ).astype(BF16)

    def stage_a(q):
        to_core(q).wait_recv()
        came = core_in.at[q]
        came[...] = added(own[q % RING, span(core * half, half)], came[...])

    def stage_b(q):
        _, _, f, _ = bits(q)
        to_first(q).wait_recv()
        came = first_in.at[q]
        came[...] = added(core_in[q, span(f * quarter, quarter)], came[...])

    def stage_c(q):
        _, _, _, g = bits(q)
        to_second(q).wait_recv()
        came = second_in.at[q]
        came[...] = added(first_in[q, span(g * eighth, eighth)], came[...])

    pairs = chunks // 2

    def during(step, lag, count, action):
        i = step - lag

        @pl.when((i >= 0) & (i < count))
        def _():
            action(i)

    def both(action):
        def run(i):
            action(2 * i)
            action(2 * i + 1)

        return run

    def start(copy):
        return lambda q: copy(q).start()

    def arrived(copy, following):
        def run(q):
            copy(q).wait_recv()
            following(q).start()

        return run

    def last_then_second(q):
        line.step_last(q)
        keep(q).start()
        back_second(q).start()

    def second_arrived(q):
        back_second(q).wait_recv()
        keep(q).wait()
        back_first(q).start()

    def finish_pair(q):
        pair.step_last(q)
        pair_keep(q).start()
        pair_core(q).start()

    late = 2
    steps = max(pairs + 8 * LAG, pair_chunks + 3 * LAG + late) + 1

    @pl.loop(0, steps)
    def _(step):
        during(step, 8 * LAG, pairs, both(arrived(back_first, back_core)))
        during(step, 7 * LAG, pairs, both(second_arrived))
        during(step, 6 * LAG, pairs, both(last_then_second))
        during(step, 5 * LAG, pairs, both(line.step_out))
        during(step, 4 * LAG, pairs, both(line.step_middle))
        during(step, 3 * LAG, pairs, both(stage_c))
        during(step, 2 * LAG, pairs, both(stage_b))
        during(step, LAG, pairs, both(stage_a))
        during(step, 3 * LAG, pairs, both(line.step_in))
        during(step, 2 * LAG, pairs, both(start(to_second)))
        during(step, LAG, pairs, both(start(to_first)))
        for m in range(rights):

            @pl.when(step == m * per_matrix // 2)
            def _(m=m):
                loads[2 + m].wait()
                if m == 0:
                    loads[0].wait()
                if m == rights - 1:
                    loads[1].wait()

        during(step, 0, pairs, both(make))
        during(step, 0, pairs, both(start(to_core)))

        @pl.when(step == 1)
        def _():
            for share in shares:
                share.wait()
            for at in thirds:
                pair_in[at] = added(pair_in[at], pair_more[at])

        @pl.when(step == 3)
        def _():
            for part in parts:
                part.wait()
            mixed_out[...] = (
                base_part[...] + mixed_part[0].astype(F32) + mixed_part[1].astype(F32)
            ).astype(BF16)

        during(step, 3 * LAG + late, pair_chunks, finish_pair)
        during(step, 2 * LAG + late, pair_chunks, pair.step_out)
        during(step, LAG + late, pair_chunks, pair.step_middle)
        during(step, late, pair_chunks, pair.step_in)

    @pl.loop(0, chunks)
    def _(q):
        back_core(q).wait_recv()
        for copy in (to_first, to_second, back_second, back_first, back_core):
            copy(q).wait_send()

        @pl.when(q >= chunks - RING)
        def _():
            to_core(q).wait_send()

        line.settle(q)

    @pl.loop(0, pair_chunks)
    def _(q):
        pair_core(q).wait()
        pair_keep(q).wait()
        pair.settle(q)


def reduce_grads(factors, half_own, first_y, rest_y, mixed, depth):
    count, width = factors[0].shape
    rights = len(factors) - 2
    rows = width * rights
    chunks = rows // CHUNK
    pair_chunks = 12
    total_rows, pair_cols = 3 * half_own.shape[1], half_own.shape[2]
    pair_rows = total_rows // pair_chunks
    vmem = pl.BlockSpec(memory_space=pltpu.VMEM)
    anywhere = pl.BlockSpec(memory_space=pl.ANY)

    def body(*refs):
        reduce_kernel(depth, refs[: len(factors)], *refs[len(factors) :])

    return pl.pallas_call(
        body,
        out_shape=(
            jax.ShapeDtypeStruct((rows, width), BF16),
            jax.ShapeDtypeStruct((total_rows, 2 * pair_cols), BF16),
            jax.ShapeDtypeStruct((count, width), BF16),
        ),
        in_specs=[anywhere] * (len(factors) + 6),
        out_specs=(anywhere, anywhere, vmem),
        scratch_shapes=[
            pltpu.VMEM((total_rows, pair_cols), BF16),
            pltpu.VMEM((2, count, width), BF16),
            pltpu.VMEM((rights, count, width), BF16),
            pltpu.VMEM((RING, CHUNK, width), BF16),
            pltpu.VMEM((chunks, CHUNK // 2, width), BF16),
            pltpu.VMEM((chunks, CHUNK // 4, width), BF16),
            pltpu.VMEM((chunks, CHUNK // 8, width), BF16),
            pltpu.VMEM((chunks, CHUNK // 8, width), BF16),
            pltpu.VMEM((chunks, CHUNK // 8, width), BF16),
            pltpu.VMEM((pair_chunks, pair_rows, pair_cols), BF16),
            pltpu.VMEM((pair_chunks, pair_rows, pair_cols), BF16),
            pltpu.SemaphoreType.DMA((9, 2, chunks)),
            pltpu.SemaphoreType.DMA((4, 2, pair_chunks)),
            pltpu.SemaphoreType.DMA((len(factors) + 3,)),
            pltpu.SemaphoreType.DMA((chunks,)),
            pltpu.SemaphoreType.DMA((pair_chunks,)),
            pltpu.VMEM((count, width), F32),
            pltpu.VMEM((2, count, width), BF16),
            pltpu.VMEM((total_rows, pair_cols), BF16),
            pltpu.SemaphoreType.DMA((2, 3)),
        ],
        compiler_params=pltpu.CompilerParams(
            collective_id=1, has_side_effects=True, vmem_limit_bytes=60 * 1024 * 1024
        ),
        name="reduce_grads",
    )(*factors, half_own, first_y, rest_y, *mixed)


ROWS = 256


def times(x, w):
    return jnp.dot(x, w, preferred_element_type=F32)


def times_back(x, w):
    return lax.dot_general(x, w, (((1,), (1,)), ((), ())), preferred_element_type=F32)


def times_rows(x, y):
    return lax.dot_general(x, y, (((0,), (0,)), ((), ())), preferred_element_type=F32)


def hidden_kernel(
    rows_own,
    grads_own,
    grads_nb,
    late_left,
    late_right,
    late_down,
    late_other,
    mixed,
    back,
    half_own,
    half_nb,
    back_in,
    from_y,
    both,
    own,
    other,
    kept,
    theirs,
    moved,
    acc_mixed,
    acc_back,
    load_sem,
    sems,
):
    core = lax.axis_index("dp")
    slot = lax.axis_index("tensor")
    count, width = rows_own.shape
    half = width // 2
    blocks = count // ROWS
    pairs = (
        (late_left, own.at[0]),
        (late_right, own.at[1]),
        (late_down, own.at[2]),
        (late_other, other),
        (rows_own, both.at[0, :count]),
        (grads_own, both.at[1, :count]),
        (grads_nb, both.at[1, count:]),
    )
    loads = [pltpu.make_async_copy(a, b, load_sem.at[i]) for i, (a, b) in enumerate(pairs)]
    for i in (4, 5, 0, 1, 2, 3, 6):
        loads[i].start()

    def send(source, target, at, peer):
        return pltpu.make_async_remote_copy(
            src_ref=source,
            dst_ref=target,
            send_sem=sems.at[0, at],
            recv_sem=sems.at[1, at],
            device_id=peer,
            device_id_type=MESH,
        )

    def span(i):
        return pl.ds(pl.multiple_of(i * ROWS, ROWS), ROWS)

    def out_rows(i):
        return send(
            rows_own.at[span(i)], both.at[0, span(blocks + i)], i, {"tensor": slot ^ 1}
        )

    def return_rows(i):
        return send(
            back.at[span(blocks + i)], back_in.at[span(i)], blocks + i, {"tensor": slot ^ 1}
        )

    def to_core(which, m):
        return send(
            theirs.at[which, m], moved.at[which, m], 2 * blocks + 3 * which + m, {"dp": 1 - core}
        )

    hand = send(half_nb.at[0], from_y, 2 * blocks + 6, {"tensor": slot ^ 2})
    barrier = pltpu.get_barrier_semaphore()
    for peer in ({"tensor": slot ^ 1}, {"tensor": slot ^ 2}, {"dp": 1 - core}):
        pl.semaphore_signal(barrier, inc=1, device_id=peer, device_id_type=MESH)
    pl.semaphore_wait(barrier, 3)
    for i in range(blocks):
        out_rows(i).start()
    for i in (4, 5, 0, 1, 2):
        loads[i].wait()

    def unit(i, which, weights):
        rows, grads = both[0, span(i)], both[1, span(i)]
        e1, e2 = times_back(rows, weights[0]), times_back(rows, weights[1])
        dm = times_back(grads, weights[2])
        mid = (e1 * e2).astype(BF16)
        de1 = (dm * e2).astype(BF16)
        de2 = (dm * e1).astype(BF16)
        kept[which, 2, span(i)] = mid
        kept[which, 0, span(i)] = de1
        kept[which, 1, span(i)] = de2
        return times(mid, weights[2]), times(de1, weights[0]) + times(de2, weights[1])

    @pl.loop(0, 2 * blocks)
    def _(i):
        @pl.when(i >= blocks)
        def _():
            out_rows(i - blocks).wait_recv()

        @pl.when(i == blocks)
        def _():
            loads[6].wait()

        acc_mixed[...], acc_back[...] = unit(i, 0, own)

        @pl.when(i == 0)
        def _():
            loads[3].wait()

        more_mixed, more_back = unit(i, 1, other)
        mixed[span(i)] = (acc_mixed[...] + more_mixed).astype(BF16)
        back[span(i)] = (acc_back[...] + more_back).astype(BF16)

        @pl.when(i >= blocks)
        def _():
            return_rows(i - blocks).start()

    here = pl.ds(pl.multiple_of(core * half, half), half)
    there = pl.ds(pl.multiple_of((1 - core) * half, half), half)

    def products(which, out, m):
        theirs[which, m] = times_rows(kept[which, m], both[m // 2, :, there]).astype(BF16)
        to_core(which, m).start()
        out[m] = times_rows(kept[which, m], both[m // 2, :, here]).astype(BF16)

    def combine(which, out, m):
        to_core(which, m).wait_recv()
        out[m] = added(out[m], moved[which, m])

    products(1, half_nb, 0)
    combine(1, half_nb, 0)
    hand.start()

    @pl.loop(1, 3)
    def _(m):
        products(1, half_nb, m)

    @pl.loop(0, 3)
    def _(m):
        products(0, half_own, m)

    for m in range(1, 3):
        combine(1, half_nb, m)
    for m in range(3):
        combine(0, half_own, m)
    for i in range(blocks):
        out_rows(i).wait_send()
        return_rows(i).wait()
    for which in range(2):
        for m in range(3):
            to_core(which, m).wait_send()
    hand.wait()


def hidden_part(rows_own, grads_own, grads_nb, shard, other):
    count, width = rows_own.shape
    hidden = shard[0].shape[0]
    vmem = pl.BlockSpec(memory_space=pltpu.VMEM)
    anywhere = pl.BlockSpec(memory_space=pl.ANY)
    half = jax.ShapeDtypeStruct((3, hidden, width // 2), BF16)
    two = jax.ShapeDtypeStruct((2 * count, width), BF16)
    return pl.pallas_call(
        hidden_kernel,
        out_shape=(
            two,
            two,
            half,
            half,
            jax.ShapeDtypeStruct((count, width), BF16),
            jax.ShapeDtypeStruct((hidden, width // 2), BF16),
        ),
        in_specs=[anywhere] * 7,
        out_specs=(vmem,) * 4 + (anywhere,) * 2,
        scratch_shapes=[
            pltpu.VMEM((2, 2 * count, width), BF16),
            pltpu.VMEM((3, hidden, width), BF16),
            pltpu.VMEM((3, hidden, width), BF16),
            pltpu.VMEM((2, 3, 2 * count, hidden), BF16),
            pltpu.VMEM((2, 3, hidden, width // 2), BF16),
            pltpu.VMEM((2, 3, hidden, width // 2), BF16),
            pltpu.VMEM((ROWS, width), F32),
            pltpu.VMEM((ROWS, width), F32),
            pltpu.SemaphoreType.DMA((7,)),
            pltpu.SemaphoreType.DMA((2, 2 * (count // ROWS) + 7)),
        ],
        compiler_params=pltpu.CompilerParams(
            collective_id=4, has_side_effects=True, vmem_limit_bytes=54 * 1024 * 1024
        ),
        name="hidden_part",
    )(rows_own, grads_own, grads_nb, *shard, other)


MESH = pl.DeviceIdType.MESH


class States:
    def __init__(self, depth, width, backward, powers, local, came, total, far, outs, states, sems):
        self.depth, self.width, self.backward, self.powers = depth, width, backward, powers
        self.local, self.came, self.total, self.far = local, came, total, far
        self.outs, self.states, self.sems = outs, states, sems
        self.slot = lax.axis_index("tensor")
        self.place = lax.axis_index("seq")
        self.share = local.shape[0] // width

    def greet(self, more=()):
        barrier = pltpu.get_barrier_semaphore()
        for peer in more:
            pl.semaphore_signal(barrier, inc=1, device_id=peer, device_id_type=MESH)
        for b in range(1, self.width):
            pl.semaphore_signal(
                barrier, inc=1, device_id={"tensor": self.slot ^ b}, device_id_type=MESH
            )
        for j in range(1, self.depth):
            peer = lax.rem(self.place + j, self.depth)
            pl.semaphore_signal(barrier, inc=1, device_id={"seq": peer}, device_id_type=MESH)
        pl.semaphore_wait(barrier, self.width + self.depth - 2 + len(more))

    def copy(self, source, target, at, peer):
        return pltpu.make_async_remote_copy(
            src_ref=source,
            dst_ref=target,
            send_sem=self.sems.at[0, at],
            recv_sem=self.sems.at[1, at],
            device_id=peer,
            device_id_type=MESH,
        )

    def group(self, slot):
        return pl.ds(slot * self.share, self.share)

    def to_peer(self, b):
        peer = self.slot ^ b
        return self.copy(
            self.local.at[self.group(peer)], self.came.at[b - 1], b - 1, {"tensor": peer}
        )

    def to_far(self, j):
        step = self.depth - j if self.backward else j
        peer = lax.rem(self.place + step, self.depth)
        return self.copy(self.total, self.far.at[j - 1], self.width + j - 2, {"seq": peer})

    def has_far(self, j):
        return self.place >= j if self.backward else self.place + j < self.depth

    def from_far(self, j):
        return self.place + j < self.depth if self.backward else self.place >= j

    def to_owner(self, d):
        at = self.width + self.depth - 2 + d - 1
        return self.copy(
            self.outs.at[d - 1],
            self.states.at[self.group(self.slot)],
            at,
            {"tensor": self.slot ^ d},
        )

    def power(self, count, head):
        return self.powers[count, head]

    def piece(self, b, k, s):
        if b == 0:
            return self.local[self.slot * self.share + k, s].astype(F32)
        return self.came[b - 1, k, s].astype(F32)

    def gather(self):
        for b in range(1, self.width):
            self.to_peer(b).wait_recv()
        for k in range(self.share):
            head = self.slot * self.share + k
            for s in range(self.local.shape[1]):
                value = 0.0
                for b in range(self.width):
                    spot = self.slot ^ b
                    left = spot if self.backward else self.width - 1 - spot
                    value = value + self.power(left, head) * self.piece(b, k, s)
                self.total[k, s] = value.astype(BF16)
        for j in range(1, self.depth):

            @pl.when(self.has_far(j))
            def _(j=j):
                self.to_far(j).start()

    def send_back(self, entering, between):
        for j in range(1, self.depth):

            @pl.when(self.from_far(j))
            def _(j=j):
                self.to_far(j).wait_recv()

            @pl.when(jnp.logical_not(self.from_far(j)))
            def _(j=j):
                self.far[j - 1] = jnp.zeros(self.far.shape[1:], BF16)

        between()
        for k in range(self.share):
            head = self.slot * self.share + k
            for s in range(self.local.shape[1]):
                value = 0.0
                for j in range(1, self.depth):
                    value = value + self.power(self.width * (j - 1), head) * self.far[
                        j - 1, k, s
                    ].astype(F32)
                entering[k, s] = value
        for d in list(range(1, self.width)) + [0]:
            target = self.slot ^ d
            inner = self.width - 1 - target if self.backward else target
            for k in range(self.share):
                head = self.slot * self.share + k
                for s in range(self.local.shape[1]):
                    value = self.power(inner, head) * entering[k, s]
                    for b in range(self.width):
                        if b == d:
                            continue
                        source = self.slot ^ b
                        gap = source - target - 1 if self.backward else target - source - 1
                        coef = jnp.where(gap >= 0, self.power(jnp.maximum(gap, 0), head), 0.0)
                        value = value + coef * self.piece(b, k, s)
                    if d == 0:
                        self.states[head, s] = value.astype(BF16)
                    else:
                        self.outs[d - 1, k, s] = value.astype(BF16)
        for d in range(1, self.width):
            self.to_owner(d).start()

    def arrive(self):
        for d in range(1, self.width):
            at = self.width + self.depth - 2 + d - 1
            self.copy(
                self.outs.at[d - 1],
                self.states.at[self.group(self.slot ^ d)],
                at,
                {"tensor": self.slot ^ d},
            ).wait_recv()

    def settle(self):
        for b in range(1, self.width):
            self.to_peer(b).wait_send()
            self.to_owner(b).wait_send()
        for j in range(1, self.depth):

            @pl.when(self.has_far(j))
            def _(j=j):
                self.to_far(j).wait_send()


def state_scratch(heads, seqs, head_dim, width, depth):
    share = heads // width
    low = functools.partial(pltpu.VMEM, dtype=BF16)
    return [
        low((heads, seqs, head_dim, head_dim)),
        low((width - 1, share, seqs, head_dim, head_dim)),
        low((share, seqs, head_dim, head_dim)),
        low((depth - 1, share, seqs, head_dim, head_dim)),
        low((width - 1, share, seqs, head_dim, head_dim)),
        pltpu.VMEM((share, seqs, head_dim, head_dim), F32),
        pltpu.SemaphoreType.DMA((2, 2 * (width - 1) + depth - 1)),
    ]


def turn(values, cosine, sine_part):
    return values * cosine + pltpu.roll(values, values.shape[-1] // 2, 1) * sine_part


def square_mean(values):
    return jnp.mean(values * values, axis=-1, keepdims=True)


def decays(rates, head, length, dim):
    rate = rates[head]
    place = lax.broadcasted_iota(jnp.int32, (length, dim), 0).astype(F32)
    query = jnp.exp(-rate[:, :dim] * (place + 1.0))
    key = jnp.exp(-rate[:, :dim] * (length - 1.0 - place))
    return query, key


def lag_decay(rates, head, length):
    lag = (
        lax.broadcasted_iota(jnp.int32, (length, length), 0)
        - lax.broadcasted_iota(jnp.int32, (length, length), 1)
    ).astype(F32)
    return jnp.where(lag >= 0, jnp.exp(-rates[head] * jnp.maximum(lag, 0.0)), 0.0)


def attend_kernel(
    depth,
    width,
    seqs,
    first_x,
    first_key,
    first_value,
    late_query,
    late_gate,
    late_output,
    left,
    right,
    down,
    grads,
    rates,
    powers,
    cosine,
    sine_part,
    residual,
    normed_two,
    attended,
    gated,
    states,
    early_outs,
    other,
    grads_nb,
    early,
    x,
    w_key,
    w_value,
    w_query,
    w_gate,
    w_output,
    local,
    came,
    total,
    far,
    outs,
    entering,
    sems,
    load_sem,
    bulk_sems,
    store_sem,
):
    (
        query_pre,
        key_pre,
        gate,
        normed_one,
        query_low,
        key_low,
        value_low,
        query_dec,
        key_dec,
        scores_low,
    ) = early
    stores = [
        pltpu.make_async_copy(a, b, store_sem.at[i])
        for i, (a, b) in enumerate(zip(early, early_outs))
    ]
    rows, model = x.shape
    length = rows // seqs
    dim = cosine.shape[1]
    tile = model // width
    loads = [
        pltpu.make_async_copy(a, b, load_sem.at[i])
        for i, (a, b) in enumerate(
            (
                (late_query, w_query),
                (late_gate, w_gate),
                (late_output, w_output),
                (first_x, x),
                (first_key, w_key),
                (first_value, w_value),
            )
        )
    ]
    loads = loads[3:] + loads[:3]
    for load in loads:
        load.start()
    exchange = States(
        depth, width, False, powers, local, came, total, far, outs, states, sems
    )
    core = lax.axis_index("dp")
    parity = lax.rem(exchange.place, 2)
    shard = (left, right, down)
    part_rows, part_cols = left.shape[0] // 2, model // 2
    columns_here = pl.ds(pl.multiple_of(core * part_cols, part_cols), part_cols)

    def rows_of(which):
        return pl.ds(pl.multiple_of(which * part_rows, part_rows), part_rows)

    def send(source, target, at, peer):
        return pltpu.make_async_remote_copy(
            src_ref=source,
            dst_ref=target,
            send_sem=bulk_sems.at[0, at],
            recv_sem=bulk_sems.at[1, at],
            device_id=peer,
            device_id_type=MESH,
        )

    def fetch(m):
        at = (rows_of(parity), columns_here)
        return send(
            shard[m].at[at], other.at[(m,) + at], m, {"tensor": exchange.slot ^ 2}
        )

    def relay(m):
        at = other.at[m, rows_of(parity), columns_here]
        return send(at, at, 3 + m, {"seq": exchange.place + 1 - 2 * parity})

    def share(m, which):
        spot = parity if which == 0 else 1 - parity
        at = other.at[m, rows_of(spot), columns_here]
        return send(at, at, 6 + 2 * m + which, {"dp": 1 - core})

    def cross(s):
        at = pl.ds(s * length, length)
        return send(grads.at[at], grads_nb.at[at], 12 + s, {"tensor": exchange.slot ^ 1})

    def pass_on(m):
        fetch(m).wait_recv()
        relay(m).start()
        share(m, 0).start()

    def pass_last(m):
        relay(m).wait_recv()
        share(m, 1).start()

    exchange.greet((({"dp": 1 - core}),))
    fetch(0).start()
    cross(0).start()
    loads[0].wait()
    for s in range(seqs):
        at = pl.ds(s * length, length)
        value = x[at].astype(F32)
        normed_one[at] = (value * lax.rsqrt(square_mean(value) + EPS)).astype(BF16)

    per_tile = tile // dim
    loads[1].wait()
    loads[2].wait()

    @pl.loop(1, width + 1)
    def _(step):
        b = lax.rem(step, width)
        spot = exchange.slot ^ b
        columns = pl.ds(pl.multiple_of(spot * tile, tile), tile)
        key_pre[:, columns] = times(normed_one[...], w_key[:, columns])
        value_low[:, columns] = times(normed_one[...], w_value[:, columns]).astype(BF16)
        for k in range(per_tile):
            head = spot * per_tile + k
            own = pl.ds(pl.multiple_of(spot * tile + k * dim, dim), dim)
            _, key_weight = decays(rates, head, length, dim)
            for s in range(seqs):
                at = pl.ds(s * length, length)
                turned = turn(jax.nn.silu(key_pre[at, own]), cosine[...], sine_part[...])
                key_low[at, own] = turned.astype(BF16)
                dec = (turned * key_weight).astype(BF16)
                key_dec[at, own] = dec
                local[head, s] = times_rows(dec, value_low[at, own]).astype(BF16)

        for b_static in range(1, width):

            @pl.when(b == b_static)
            def _(b_static=b_static):
                exchange.to_peer(b_static).start()

    for s in range(1, seqs):
        cross(s).start()
    fetch(1).start()
    fetch(2).start()
    pass_on(0)
    loads[3].wait()
    loads[4].wait()

    def inner(spot):
        columns = pl.ds(pl.multiple_of(spot * tile, tile), tile)
        query_pre[:, columns] = times(normed_one[...], w_query[:, columns])
        gate[:, columns] = times(normed_one[...], w_gate[:, columns])
        for k in range(per_tile):
            head = spot * per_tile + k
            own = pl.ds(pl.multiple_of(spot * tile + k * dim, dim), dim)
            query_weight, _ = decays(rates, head, length, dim)
            mask = lag_decay(rates, head, length)
            for s in range(seqs):
                at = pl.ds(s * length, length)
                turned = turn(jax.nn.silu(query_pre[at, own]), cosine[...], sine_part[...])
                low_query = turned.astype(BF16)
                query_low[at, own] = low_query
                query_dec[at, own] = (turned * query_weight).astype(BF16)
                low_scores = (times_back(low_query, key_low[at, own]) * mask).astype(BF16)
                scores_low[head, s] = low_scores
                attended[at, own] = times(low_scores, value_low[at, own])

    half = width // 2

    @pl.loop(0, half)
    def _(spot):
        inner(spot)

    exchange.gather()

    @pl.loop(half, width)
    def _(spot):
        inner(spot)

    def relays():
        pass_on(1)
        pass_on(2)

    exchange.send_back(entering, relays)
    for store in stores:
        store.start()
    pass_last(0)
    loads[5].wait()
    exchange.arrive()
    pass_last(1)

    @pl.loop(0, width * per_tile)
    def _(head):
        own = pl.ds(pl.multiple_of(head * dim, dim), dim)
        for s in range(seqs):
            at = pl.ds(s * length, length)
            attended[at, own] += times(query_dec[at, own], states[head, s])

    for s in range(seqs):
        at = pl.ds(s * length, length)
        value = attended[at]
        gated[at] = (value * lax.rsqrt(square_mean(value) + EPS) * gate[at]).astype(BF16)

    @pl.loop(0, width)
    def _(spot):
        columns = pl.ds(pl.multiple_of(spot * tile, tile), tile)
        residual[:, columns] = x[:, columns].astype(F32) + times(
            gated[...], w_output[:, columns]
        )

    for s in range(seqs):
        at = pl.ds(s * length, length)
        value = residual[at]
        normed_two[at] = (value * lax.rsqrt(square_mean(value) + EPS)).astype(BF16)
    pass_last(2)
    for store in stores:
        store.wait()
    exchange.settle()
    for m in range(3):
        fetch(m).wait_send()
        relay(m).wait_send()
        share(m, 0).wait()
        share(m, 1).wait()
    for s in range(seqs):
        cross(s).wait()


def attend(x, weights, shard, grads, rates, powers, cosine, sine_part, seqs, depth, width):
    rows, model = x.shape
    heads = rates.shape[0]
    dim = model // heads
    length = rows // seqs
    vmem = pl.BlockSpec(memory_space=pltpu.VMEM)
    anywhere = pl.BlockSpec(memory_space=pl.ANY)
    wide = jax.ShapeDtypeStruct((rows, model), F32)
    low = jax.ShapeDtypeStruct((rows, model), BF16)
    w_query, w_key, w_value, w_gate, w_output = weights
    early = (wide,) * 3 + (low,) * 6 + (
        jax.ShapeDtypeStruct((heads, seqs, length, length), BF16),
    )

    def body(*refs):
        at = 14 + 5
        kept = at + len(early)
        scratch = kept + 2
        attend_kernel(
            depth,
            width,
            seqs,
            *refs[:at],
            refs[at:kept],
            *refs[kept:scratch],
            refs[scratch : scratch + len(early)],
            *refs[scratch + len(early) :],
        )

    return pl.pallas_call(
        body,
        out_shape=(
            wide,
            low,
            wide,
            low,
            jax.ShapeDtypeStruct((heads, seqs, dim, dim), BF16),
        )
        + early
        + (jax.ShapeDtypeStruct((3,) + shard[0].shape, BF16), low),
        in_specs=[anywhere] * 10 + [vmem] * 4,
        out_specs=(vmem,) * 5 + (anywhere,) * (len(early) + 2),
        scratch_shapes=[pltpu.VMEM(v.shape, v.dtype) for v in early]
        + [pltpu.VMEM((rows, model), BF16)]
        + [pltpu.VMEM((model, model), BF16)] * 5
        + state_scratch(heads, seqs, dim, width, depth)
        + [
            pltpu.SemaphoreType.DMA((6,)),
            pltpu.SemaphoreType.DMA((2, 12 + seqs)),
            pltpu.SemaphoreType.DMA((len(early),)),
        ],
        compiler_params=pltpu.CompilerParams(
            collective_id=2, has_side_effects=True, vmem_limit_bytes=56 * 1024 * 1024
        ),
        name="attend",
    )(
        x,
        w_key,
        w_value,
        w_query,
        w_gate,
        w_output,
        *shard,
        grads,
        rates,
        powers,
        cosine,
        sine_part,
    )


def retreat_kernel(
    depth,
    width,
    seqs,
    residual,
    back_own,
    back_in,
    grads,
    rates,
    powers,
    cosine,
    sine_part,
    mixed_nb,
    half_nb,
    *rest,
):
    late = rest[:17]
    (
        grad_mid_low,
        gate_low,
        query_out,
        key_out,
        value_out,
        grad_tokens,
        mixed_in,
        from_y,
    ) = rest[17:25]
    held = rest[25:42]
    (
        w_output,
        attended,
        gate,
        query_low,
        key_low,
        value_low,
        query_dec,
        scores_low,
        states_in,
        query_pre,
        w_query,
        w_gate,
        key_dec,
        key_pre,
        w_key,
        w_value,
        x,
    ) = held
    (
        states,
        grad_mid,
        work,
        grad_att,
        value_part,
        key_part,
        local,
        came,
        total,
        far,
        outs,
        entering,
        sems,
        load_sem,
        bulk_sems,
    ) = rest[42:]
    rows, model = residual.shape
    length = rows // seqs
    dim = cosine.shape[1]
    tile = model // width
    per_tile = tile // dim
    loads = [
        pltpu.make_async_copy(a, b, load_sem.at[i]) for i, (a, b) in enumerate(zip(late, held))
    ]
    for load in loads:
        load.start()
    exchange = States(
        depth, width, True, powers, local, came, total, far, outs, states, sems
    )

    def send(source, target, at, peer):
        return pltpu.make_async_remote_copy(
            src_ref=source,
            dst_ref=target,
            send_sem=bulk_sems.at[0, at],
            recv_sem=bulk_sems.at[1, at],
            device_id=peer,
            device_id_type=MESH,
        )

    crosses, hands = 4, 8
    cross_rows, hand_rows = rows // crosses, 2 * half_nb.shape[1] // hands

    def cross(k):
        at = pl.ds(k * cross_rows, cross_rows)
        source = mixed_nb.at[pl.ds(rows + k * cross_rows, cross_rows)]
        return send(source, mixed_in.at[at], k, {"tensor": exchange.slot ^ 1})

    def hand(k):
        m, at = k // (hands // 2), pl.ds(k % (hands // 2) * hand_rows, hand_rows)
        return send(
            half_nb.at[m + 1, at], from_y.at[m, at], crosses + k, {"tensor": exchange.slot ^ 2}
        )

    def start_bulk(some_crosses, some_hands):
        for k in some_crosses:
            cross(k).start()
        for k in some_hands:
            hand(k).start()

    exchange.greet()
    start_bulk(range(1), range(2))

    def spans():
        return [pl.ds(s * length, length) for s in range(seqs)]

    for at in spans():
        value = residual[at]
        scale = lax.rsqrt(square_mean(value) + EPS)
        normed = value * scale
        grad = back_own[at].astype(F32) + back_in[at].astype(F32)
        grad = grads[at].astype(F32) + scale * (
            grad - normed * jnp.mean(grad * normed, axis=-1, keepdims=True)
        )
        grad_mid[at] = grad
        grad_mid_low[at] = grad.astype(BF16)

    def columns_of(spot):
        return pl.ds(pl.multiple_of(spot * tile, tile), tile)

    for load in loads[:3]:
        load.wait()

    @pl.loop(0, width)
    def _(spot):
        work[:, columns_of(spot)] = times_back(grad_mid_low[...], w_output[columns_of(spot)])

    for at in spans():
        value = attended[at]
        scale = lax.rsqrt(square_mean(value) + EPS)
        normed = value * scale
        grad = work[at]
        gate_low[at] = (grad * normed).astype(BF16)
        grad = grad * gate[at]
        grad_att[at] = (
            scale * (grad - normed * jnp.mean(grad * normed, axis=-1, keepdims=True))
        ).astype(BF16)

    for load in loads[3:10]:
        load.wait()

    @pl.loop(1, width + 1)
    def _(step):
        b = lax.rem(step, width)
        spot = exchange.slot ^ b
        for k in range(per_tile):
            own = pl.ds(pl.multiple_of(spot * tile + k * dim, dim), dim)
            for s, at in enumerate(spans()):
                local[spot * per_tile + k, s] = times_rows(
                    query_dec[at, own], grad_att[at, own]
                ).astype(BF16)

        for b_static in range(1, width):

            @pl.when(b == b_static)
            def _(b_static=b_static):
                exchange.to_peer(b_static).start()

    start_bulk(range(1, 3), range(2, 5))

    def slope(values):
        sigmoid_v = jax.nn.sigmoid(values)
        return sigmoid_v * (1.0 + values * (1.0 - sigmoid_v))

    def inner(spot):
        for k in range(per_tile):
            head = spot * per_tile + k
            own = pl.ds(pl.multiple_of(spot * tile + k * dim, dim), dim)
            query_weight, _ = decays(rates, head, length, dim)
            mask = lag_decay(rates, head, length)
            for s, at in enumerate(spans()):
                grad = grad_att[at, own]
                value_part[at, own] = times_rows(scores_low[head, s], grad)
                score = (times_back(grad, value_low[at, own]) * mask).astype(BF16)
                key_part[at, own] = times_rows(score, query_low[at, own])
                turned = times(score, key_low[at, own]) + query_weight * times_back(
                    grad, states_in[head, s]
                )
                query_out[at, own] = (
                    turn(turned, cosine[...], -sine_part[...]) * slope(query_pre[at, own])
                ).astype(BF16)

    half = width // 2

    @pl.loop(0, half)
    def _(spot):
        inner(spot)

    exchange.gather()

    @pl.loop(half, width)
    def _(spot):
        inner(spot)

    exchange.send_back(entering, lambda: None)
    start_bulk(range(3, crosses), range(5, hands))
    for load in loads[10:]:
        load.wait()

    @pl.loop(0, width)
    def _(spot):
        at = columns_of(spot)
        work[:, at] = times_back(query_out[...], w_query[at]) + times_back(
            gate_low[...], w_gate[at]
        )

    exchange.arrive()

    @pl.loop(0, width * per_tile)
    def _(head):
        own = pl.ds(pl.multiple_of(head * dim, dim), dim)
        _, key_weight = decays(rates, head, length, dim)
        for s, at in enumerate(spans()):
            state = states[head, s]
            value_out[at, own] = (
                value_part[at, own] + times(key_dec[at, own], state)
            ).astype(BF16)
            turned = key_part[at, own] + key_weight * times_back(value_low[at, own], state)
            key_out[at, own] = (
                turn(turned, cosine[...], -sine_part[...]) * slope(key_pre[at, own])
            ).astype(BF16)

    @pl.loop(0, width)
    def _(spot):
        at = columns_of(spot)
        work[:, at] += times_back(key_out[...], w_key[at]) + times_back(
            value_out[...], w_value[at]
        )

    for at in spans():
        value = x[at].astype(F32)
        scale = lax.rsqrt(square_mean(value) + EPS)
        normed = value * scale
        grad = work[at]
        grad_tokens[at] = grad_mid[at] + scale * (
            grad - normed * jnp.mean(grad * normed, axis=-1, keepdims=True)
        )
    exchange.settle()
    for k in range(crosses):
        cross(k).wait()
    for k in range(hands):
        hand(k).wait()


def retreat(early, tables, bulk, late, seqs, depth, width):
    rows, model = early[0].shape
    heads = tables[0].shape[0]
    dim = model // heads
    vmem = pl.BlockSpec(memory_space=pltpu.VMEM)
    anywhere = pl.BlockSpec(memory_space=pl.ANY)
    wide = jax.ShapeDtypeStruct((rows, model), F32)
    low = jax.ShapeDtypeStruct((rows, model), BF16)
    return pl.pallas_call(
        functools.partial(retreat_kernel, depth, width, seqs),
        out_shape=(low,) * 5 + (wide, low, jax.ShapeDtypeStruct((2,) + bulk[1].shape[1:], BF16)),
        in_specs=[vmem] * (len(early) + len(tables)) + [anywhere] * (len(bulk) + len(late)),
        out_specs=(vmem,) * 6 + (anywhere,) * 2,
        scratch_shapes=[pltpu.VMEM(v.shape, v.dtype) for v in late]
        + [
            pltpu.VMEM((heads, seqs, dim, dim), BF16),
            pltpu.VMEM((rows, model), F32),
            pltpu.VMEM((rows, model), F32),
            pltpu.VMEM((rows, model), BF16),
            pltpu.VMEM((rows, model), F32),
            pltpu.VMEM((rows, model), F32),
        ]
        + state_scratch(heads, seqs, dim, width, depth)
        + [pltpu.SemaphoreType.DMA((len(late),)), pltpu.SemaphoreType.DMA((2, 12))],
        compiler_params=pltpu.CompilerParams(
            collective_id=3, has_side_effects=True, vmem_limit_bytes=60 * 1024 * 1024
        ),
        name="retreat",
    )(*early, *tables, *bulk, *late)


def on_device(
    tokens,
    w_query,
    w_key,
    w_value,
    w_ugate,
    w_output,
    w_left,
    w_right,
    w_down,
    decay_rate,
    cotangent,
):
    seq_count, group_len, model_width = tokens.shape
    head_count = decay_rate.shape[0]
    head_dim = model_width // head_count
    half_dim = head_dim // 2
    row_count = seq_count * group_len
    core = lax.axis_index("dp")

    shard = (w_left.T, w_right.T, w_down)
    grad_own = cotangent.reshape(row_count, model_width)

    position_block = lax.axis_index(("seq", "tensor"))
    places = (position_block * group_len + jnp.arange(group_len)).astype(F32)
    frequency = 10000.0 ** (-jnp.arange(half_dim, dtype=F32) / half_dim)
    angles = places[:, None] * frequency[None, :]
    cosine, sine_part = jnp.cos(angles), jnp.sin(angles)
    cosine = jnp.concatenate([cosine, cosine], axis=1)
    sine_part = jnp.concatenate([-sine_part, sine_part], axis=1)
    rows_in = tokens.reshape(row_count, model_width)
    depth = lax.axis_size("seq")
    width = lax.axis_size("tensor")
    rates = jnp.broadcast_to(decay_rate[:, None, None], (head_count, 1, group_len))
    blocks = jnp.arange(depth * width, dtype=F32)[:, None, None, None]
    powers = jnp.broadcast_to(
        jnp.exp(-decay_rate[None, :, None, None] * group_len * blocks),
        (depth * width, head_count, 1, head_dim),
    )
    (
        residual,
        rows_own,
        merged,
        gated_low,
        state_low,
        query_pre,
        key_pre,
        ugate,
        normed_low,
        query_low,
        key_low,
        value_low,
        query_dec,
        key_dec,
        weights_low,
        other,
        grad_nb,
    ) = attend(
        rows_in,
        (w_query, w_key, w_value, w_ugate, w_output),
        shard,
        grad_own,
        rates,
        powers,
        cosine,
        sine_part,
        seq_count,
        depth,
        width,
    )
    mixed, back, half_own, half_nb, back_in, first_y = hidden_part(
        rows_own, grad_own, grad_nb, shard, other
    )
    (
        grad_branch,
        grad_ugate_pre,
        grad_query_pre,
        grad_key_pre,
        grad_value_pre,
        grad_tokens,
        mixed_in,
        from_y,
    ) = retreat(
        (residual, back, back_in, grad_own),
        (rates, powers, cosine, sine_part),
        (mixed, half_nb),
        (
            w_output,
            merged,
            ugate,
            query_low,
            key_low,
            value_low,
            query_dec,
            weights_low,
            state_low,
            query_pre,
            w_query,
            w_ugate,
            key_dec,
            key_pre,
            w_key,
            w_value,
            rows_in,
        ),
        seq_count,
        depth,
        width,
    )

    hidden = w_down.shape[0]
    sums, hidden_sums, mixed_out = reduce_grads(
        (
            normed_low,
            gated_low,
            grad_query_pre,
            grad_key_pre,
            grad_value_pre,
            grad_ugate_pre,
            grad_branch,
        ),
        half_own,
        first_y,
        from_y,
        (residual, mixed, mixed_in),
        depth,
    )
    attention_grads = tuple(
        sums[i * model_width : (i + 1) * model_width].astype(F32) for i in range(5)
    )
    left_sum, right_sum, down_sum = (
        hidden_sums[i * hidden : (i + 1) * hidden].astype(F32) for i in range(3)
    )
    return (
        (mixed_out.reshape(tokens.shape), grad_tokens.reshape(tokens.shape))
        + attention_grads
        + (left_sum.T, right_sum.T, down_sum)
    )


def solution(mesh):
    rows = P("dp", ("seq", "tensor"), None)
    columns = P(None, "tensor")
    return jax.shard_map(
        on_device,
        mesh=mesh,
        in_specs=(rows, P(), P(), P(), P(), P(), columns, columns, P("tensor", None), P(), rows),
        out_specs=(rows, rows, P(), P(), P(), P(), P(), columns, columns, P("tensor", None)),
        check_vma=False,
    )
```
